32 devices in a mesh: ctx: 4 (over y, x), head: 8 (over z, core).
Axes of the slice: x: 2, y: 2, z: 4, core: 2. Of those that a mesh axis runs over, the one named last changes fastest.
Arguments:
- state: bfloat16 [4096, 2048], P('ctx'), may hold values from -6 to 6
- norm_gain: bfloat16 [2048], replicated, may hold values from 0.5 to 1.5
- w_qkv: bfloat16 [3, 2048, 2048], P(None, None, 'head'), may hold values from -2 to 2
- w_out: bfloat16 [2048, 2048], P('head'), may hold values from -0.125 to 0.125
- probe: bfloat16 [4096, 2048], P('ctx'), may hold values from -6 to 6
- noise: bfloat16 [4096, 2048], P(('ctx', 'head')), may hold values from -6 to 6
- segment_ids: int32 [4096], P('ctx'), may hold values from 0 to 2, never falling along the last dimension, each value on 1 to 3072 neighbouring positions
Outputs:
- new_state: float32 [4096, 2048], P(('ctx', 'head'))
The draws below stay inside these ranges and needn't reach their ends.
Inputs may be any that keep to these rules, and one draw needn't show every extreme that they name: `segment_ids`: segment numbers never fall along the sequence; a segment holds at most 3072 positions.
All inputs are finite; a program needn't handle non-finite values.
Results may differ from the reference program's by a relative error of at most 0.011.
Values may be sent and summed in bfloat16 or wider, within the bound.
A program may use at most 128 MiB of HBM per device.

```python
import math
import jax
import jax.numpy as jnp
import numpy as np
from jax import lax

D = 2048
HEADS = 16
HEAD_DIM = 128
SEQ = 4096
SEG_MOST = 3072


def state_values(key):
    noise_key = jax.random.fold_in(key, 0)
    drawn_draw = jnp.clip(jax.random.normal(noise_key, (SEQ, D), jnp.float32), -6.0, 6.0)
    result = drawn_draw
    return result


def draw_state(key, part):
    return state_values(key).astype(jnp.bfloat16)


def draw_probe(key, part):
    shared = state_values(key)
    fresh = jnp.clip(jax.random.normal(jax.random.fold_in(key, 4242), (SEQ, D), jnp.float32), -6.0, 6.0)
    return jnp.clip(0.8 * shared + 0.6 * fresh, -6.0, 6.0).astype(jnp.bfloat16)


def draw_w_qkv(key, part):
    base_key, scale_key = jax.random.split(key, 2)
    spread = D ** (-0.5)
    base_draw = jnp.clip(jax.random.normal(base_key, (3, D, D), jnp.float32), -6.0, 6.0) * spread
    head_scale = jnp.exp(jax.random.uniform(scale_key, (HEADS,), jnp.float32, jnp.log(1.2), jnp.log(1.9)))
    column_scale = jnp.repeat(head_scale, HEAD_DIM)[None, :]
    query_part = base_draw[0] * column_scale
    key_part = base_draw[1] * column_scale
    value_part = base_draw[2]
    mixed_draw = jnp.stack([query_part, key_part, value_part])
    return jnp.clip(mixed_draw, -2.0, 2.0).astype(jnp.bfloat16)


def levels(key, extent, pieces, low, top_value):
    def one(axis_at, blocks):
        heights = jax.random.uniform(jax.random.fold_in(jax.random.fold_in(key, 6), axis_at), (blocks,), jnp.float32, low / len(pieces), top_value / len(pieces))
        return jnp.repeat(jnp.exp(heights), extent[axis_at] // blocks).reshape((-1,) + (1,) * (len(extent) - axis_at - 1))

    level = one(*pieces[0])
    for cut in pieces[1:]:
        level = level * one(*cut)
    return level


def length_profile(amount, total, bound, slope):
    portions = [(1 << 20) // math.isqrt(standing ** slope) + 1 for standing in range(2, amount + 1)]
    rest, counts = total - bound - (amount - 1), [1] * (amount - 1)
    while rest > 0:
        movable = [i for i in range(amount - 1) if counts[i] < bound]
        pool, budget = sum([portions[i] for i in movable]), rest
        for i in movable:
            addition = min(bound - counts[i], max(1, budget * portions[i] // pool), rest)
            counts[i] = counts[i] + addition
            rest = rest - addition
    return np.array([bound] + counts)


def ragged_sizes(stream_key, amount, total, limit, skew):
    if amount == 2:
        one = jax.random.randint(stream_key, (), max(1, total - limit), min(limit, total - 1) + 1)
        return jnp.stack([one, total - one])
    sizes = jnp.asarray(length_profile(amount, total, limit, skew), jnp.int32)
    couples = (amount - 1) // 2
    donor, taker = sizes[1:1 + 2 * couples:2], sizes[2:2 + 2 * couples:2]
    room = jnp.minimum(donor - 1, limit - taker)
    moved = jax.random.randint(jax.random.fold_in(stream_key, 1), (couples,), 0, 1 << 20) % (room + 1)
    sizes = sizes.at[1:1 + 2 * couples:2].set(donor - moved).at[2:2 + 2 * couples:2].set(taker + moved)
    return sizes[jax.random.permutation(jax.random.fold_in(stream_key, 2), amount)]


def bell_draw(key, shape, scale, reach, pieces=(), kind=jnp.bfloat16):
    gain = levels(key, shape, pieces, -0.22, 0.18) if pieces else 1.0
    values = jax.random.normal(key, shape, jnp.float32) * scale * gain
    return jnp.minimum(jnp.maximum(values, -reach), reach).astype(kind)


def setup_inputs(seed: int = 0) -> dict:
    key_list = jax.random.split(jax.random.key(seed), 8)
    state = draw_state(jax.random.fold_in(key_list[7], 71), 0)
    norm_gain = jnp.clip(1.0 + 0.1 * jax.random.normal(key_list[1], (D,), jnp.float32), 0.5, 1.5).astype(jnp.bfloat16)
    w_qkv = draw_w_qkv(jax.random.fold_in(key_list[7], 71), 0)
    w_out = bell_draw(key_list[3], (D, D), D ** -0.5, 0.125, ((0, 8),))
    probe = draw_probe(jax.random.fold_in(key_list[7], 71), 0)
    noise = bell_draw(key_list[5], (SEQ, D), 1.0, 6.0, ((0, 32),))
    segment_ids = jnp.searchsorted(jnp.cumsum(ragged_sizes(key_list[6], 3, SEQ, SEG_MOST, 0)), jnp.arange(SEQ), side="right").astype(jnp.int32)
    return {"state": state, "norm_gain": norm_gain, "w_qkv": w_qkv, "w_out": w_out, "probe": probe, "noise": noise, "segment_ids": segment_ids}


EPSILON = 1e-05
STEP_SIZE = 0.25
NEGATIVE = -1e+30

def row_scale(matrix):
    return lax.rsqrt(lax.optimization_barrier(jnp.mean(matrix * matrix, axis=-1, keepdims=True)) + EPSILON)

def readout_grad(layer_out, probe_full):
    scale_y = row_scale(layer_out)
    return scale_y * probe_full - layer_out * scale_y ** 3 * lax.optimization_barrier(jnp.mean(probe_full * layer_out, axis=-1, keepdims=True))

def reference(state, norm_gain, w_qkv, w_out, probe, noise, segment_ids):
    state_f = state.astype(jnp.float32)
    gain_full = norm_gain.astype(jnp.float32)
    inverse = row_scale(state_f)
    normed = (state_f * inverse * gain_full).astype(jnp.bfloat16)
    score_scale = HEAD_DIM ** (-0.5)
    positions = jnp.arange(SEQ, dtype=jnp.int32)
    allowed = (positions[None, :] <= positions[:, None]) & (segment_ids[None, :] == segment_ids[:, None])
    head_proj = w_qkv.reshape(3, D, HEADS, HEAD_DIM).transpose(2, 0, 1, 3)
    head_out = w_out.reshape(HEADS, HEAD_DIM, D)

    def forward_head(weights):
        queries = jnp.dot(normed, weights[0], preferred_element_type=jnp.float32).astype(jnp.bfloat16)
        key_heads = jnp.dot(normed, weights[1], preferred_element_type=jnp.float32).astype(jnp.bfloat16)
        values = jnp.dot(normed, weights[2], preferred_element_type=jnp.float32).astype(jnp.bfloat16)
        scores = jnp.dot(queries, key_heads.T, preferred_element_type=jnp.float32) * score_scale
        scores = jnp.where(allowed, scores, NEGATIVE)
        row_max = lax.optimization_barrier(jnp.max(scores, axis=1))
        exp_scores = jnp.where(allowed, jnp.exp(scores - row_max[:, None]), 0.0)
        totals = lax.optimization_barrier(jnp.sum(exp_scores, axis=1))
        outputs = (jnp.dot(exp_scores.astype(jnp.bfloat16), values, preferred_element_type=jnp.float32) / totals[:, None]).astype(jnp.bfloat16)
        return (queries, key_heads, values, outputs, row_max + jnp.log(totals))
    queries, key_heads, values, outputs, log_totals = lax.map(forward_head, head_proj)
    joined = outputs.transpose(1, 0, 2).reshape(SEQ, D)
    layer_out = state_f + jnp.dot(joined, w_out, preferred_element_type=jnp.float32)
    readout = readout_grad(layer_out, probe.astype(jnp.float32))
    readout_half = readout.astype(jnp.bfloat16)

    def backward_head(running, head_item):
        weights, out_weight, query_h, key_h, value_h, output_h, log_h = head_item
        grads_out = jnp.dot(readout_half, out_weight.T, preferred_element_type=jnp.float32).astype(jnp.bfloat16)
        deltas = lax.optimization_barrier(jnp.sum(grads_out.astype(jnp.float32) * output_h.astype(jnp.float32), axis=1))
        scores = jnp.dot(query_h, key_h.T, preferred_element_type=jnp.float32) * score_scale
        probabilities = jnp.where(allowed, jnp.exp(scores - log_h[:, None]), 0.0)
        dprobs = jnp.dot(grads_out, value_h.T, preferred_element_type=jnp.float32)
        dscores = probabilities * (dprobs - deltas[:, None])
        prob_half = probabilities.astype(jnp.bfloat16)
        dscore_half = dscores.astype(jnp.bfloat16)
        value_grad = jnp.dot(prob_half.T, grads_out, preferred_element_type=jnp.float32).astype(jnp.bfloat16)
        key_grad = (jnp.dot(dscore_half.T, query_h, preferred_element_type=jnp.float32) * score_scale).astype(jnp.bfloat16)
        query_grad = (jnp.dot(dscore_half, key_h, preferred_element_type=jnp.float32) * score_scale).astype(jnp.bfloat16)
        running = running + jnp.dot(query_grad, weights[0].T, preferred_element_type=jnp.float32)
        running = running + jnp.dot(key_grad, weights[1].T, preferred_element_type=jnp.float32)
        running = running + jnp.dot(value_grad, weights[2].T, preferred_element_type=jnp.float32)
        return (running, None)
    normed_grad, _ = lax.scan(backward_head, jnp.zeros((SEQ, D), jnp.float32), (head_proj, head_out, queries, key_heads, values, outputs, log_totals))
    gain_grad = normed_grad * gain_full
    gradient = readout + inverse * gain_grad - state_f * inverse ** 3 * lax.optimization_barrier(jnp.mean(gain_grad * state_f, axis=-1, keepdims=True))
    return state_f - STEP_SIZE * gradient + jnp.sqrt(2.0 * STEP_SIZE) * noise.astype(jnp.float32)
```

```python
import functools

import jax
import jax.numpy as jnp
from jax import lax
from jax.experimental import pallas as pl
from jax.experimental.pallas import tpu as pltpu
from jax.sharding import PartitionSpec as P

HEAD_DIM = 128
EPSILON = 1e-05
STEP_SIZE = 0.25
NOISE_SCALE = (2.0 * STEP_SIZE) ** 0.5
NEGATIVE = -1e30
LOG2E = 1.4426950408889634
MESH = pl.DeviceIdType.MESH
VMEM = pl.BlockSpec(memory_space=pltpu.VMEM)
ANY = pl.BlockSpec(memory_space=pl.ANY)
NT = (((1,), (1,)), ((), ()))
TN = (((0,), (0,)), ((), ()))
FORWARD_BLOCKS = (512, 512)
BACKWARD_BLOCKS = (512, 512)


def row_scale(matrix):
    return lax.rsqrt(jnp.mean(matrix * matrix, axis=-1, keepdims=True) + EPSILON)


def dot32(left, right, dims):
    return lax.dot_general(left, right, dims, preferred_element_type=jnp.float32)


def greet(axis, number, me):
    barrier = pltpu.get_barrier_semaphore()
    for step in range(1, number):
        pl.semaphore_signal(
            barrier, inc=1, device_id={axis: lax.rem(me + step, number)}, device_id_type=MESH
        )
    pl.semaphore_wait(barrier, number - 1)


def gather_kernel(
    number, key_ref, value_ref, seg_ref, normed_ref, w_ref, keys, values, segs, query_out, send_sem,
    recv_sem, own_sem,
):
    me = lax.axis_index("ctx")
    rows = key_ref.shape[0]
    greet("ctx", number, me)

    def place(index):
        return pl.ds(pl.multiple_of(index * rows, rows), rows)

    def send(slot, source, target, peer):
        copy = pltpu.make_async_remote_copy(
            src_ref=source,
            dst_ref=target,
            send_sem=send_sem.at[slot],
            recv_sem=recv_sem.at[slot],
            device_id={"ctx": peer},
            device_id_type=MESH,
        )
        copy.start()
        return copy

    mine = place(me)
    copies = []
    for step in range(1, number):
        copies.append(send(step, seg_ref, segs.at[me], lax.rem(me + step, number)))
    relay = number == 4
    if relay:
        low, high = lax.rem(me, 2), me // 2
        across, along = high * 2 + 1 - low, (1 - high) * 2 + low
        key_first = send(number, key_ref, keys.at[mine], across)
        value_first = send(number + 1, value_ref, values.at[mine], along)
        copies.append(send(number + 2, value_ref, values.at[mine], across))
        copies.append(send(number + 3, key_ref, keys.at[mine], along))
    else:
        for step in range(1, number):
            peer = lax.rem(me + step, number)
            copies.append(send(number + 2 * step, key_ref, keys.at[mine], peer))
            copies.append(send(number + 2 * step + 1, value_ref, values.at[mine], peer))
    pairs = ((key_ref, keys.at[mine]), (value_ref, values.at[mine]), (seg_ref, segs.at[me]))
    for index, (source, target) in enumerate(pairs):
        copy = pltpu.make_async_copy(source, target, own_sem.at[index])
        copy.start()
        copies.append(copy)
    tile = min(256, rows)

    def project(piece, _):
        at = pl.ds(pl.multiple_of(piece * tile, tile), tile)
        query_out[at, :] = jnp.dot(
            normed_ref[at, :], w_ref[...], preferred_element_type=jnp.float32
        ).astype(jnp.bfloat16)
        return 0

    lax.fori_loop(0, rows // tile, project, 0)
    if relay:
        key_first.wait()
        copies.append(send(number + 4, keys.at[place(across)], keys.at[place(across)], along))
        value_first.wait()
        copies.append(send(number + 5, values.at[place(along)], values.at[place(along)], across))
    for copy in copies:
        copy.wait()


def gather_keys(number, key_rows, value_rows, segment_ids, normed, w_query):
    rows, width = key_rows.shape
    seg = segment_ids.reshape(-1, 128)
    full = jax.ShapeDtypeStruct((number * rows, width), key_rows.dtype)
    keys, values, segs, queries = pl.pallas_call(
        functools.partial(gather_kernel, number),
        out_shape=(
            full,
            full,
            jax.ShapeDtypeStruct((number,) + seg.shape, seg.dtype),
            jax.ShapeDtypeStruct((rows, width), key_rows.dtype),
        ),
        in_specs=[VMEM] * 5,
        out_specs=(ANY, ANY, ANY, VMEM),
        scratch_shapes=[
            pltpu.SemaphoreType.DMA((3 * number + 6,)),
            pltpu.SemaphoreType.DMA((3 * number + 6,)),
            pltpu.SemaphoreType.DMA((3,)),
        ],
        compiler_params=pltpu.CompilerParams(collective_id=0, has_side_effects=True),
    )(key_rows, value_rows, seg, normed, w_query)
    return keys, values, segs.reshape(-1), queries


def block_ranges(table, index):
    return [table[index, column] for column in range(4)]


def forward_kernel(
    heads, bq, bk, table, query_ref, key_ref, value_ref, start_ref, pos_ref, out_ref, log_ref
):
    factor = HEAD_DIM ** (-0.5) * LOG2E
    blocks = query_ref.shape[0] // bq

    def one_block(index, _):
        low, inner_low, inner_high, high = block_ranges(table, index)
        rows = pl.ds(pl.multiple_of(index * bq, bq), bq)
        start, pos = start_ref[index], pos_ref[index]

        def step(masked, piece, carry):
            keys_at = pl.ds(pl.multiple_of(piece * bk, bk), bk)
            if masked:
                key_pos = piece * bk + lax.broadcasted_iota(jnp.int32, (bk, bq), 0)
                allowed = (key_pos >= start) & (key_pos <= pos)
            result = []
            for head in range(heads):
                top, total, acc = carry[head]
                cols = pl.ds(head * HEAD_DIM, HEAD_DIM)
                scores = dot32(key_ref[keys_at, cols], query_ref[rows, cols], NT)
                if masked:
                    scores = jnp.where(allowed, scores, NEGATIVE)
                new_top = jnp.maximum(top, jnp.max(scores, axis=0, keepdims=True) * factor)
                weights = jnp.exp2(scores * factor - new_top)
                scale = jnp.exp2(top - new_top)
                total = total * scale + jnp.sum(weights, axis=0, keepdims=True)
                acc = acc * scale + dot32(
                    value_ref[keys_at, cols], weights.astype(jnp.bfloat16), TN
                )
                result.append((new_top, total, acc))
            return tuple(result)

        carry = tuple(
            (
                jnp.full((1, bq), NEGATIVE, jnp.float32),
                jnp.zeros((1, bq), jnp.float32),
                jnp.zeros((HEAD_DIM, bq), jnp.float32),
            )
            for _ in range(heads)
        )
        carry = lax.fori_loop(low, inner_low, functools.partial(step, True), carry)
        carry = lax.fori_loop(inner_low, inner_high, functools.partial(step, False), carry)
        carry = lax.fori_loop(inner_high, high, functools.partial(step, True), carry)
        for head in range(heads):
            top, total, acc = carry[head]
            out_ref[rows, pl.ds(head * HEAD_DIM, HEAD_DIM)] = (acc / total).T.astype(jnp.bfloat16)
            log_ref[index, pl.ds(head, 1), :] = top + jnp.log2(total)
        return 0

    lax.fori_loop(0, blocks, one_block, 0)


def backward_kernel(
    heads, bq, bk, table, query_ref, key_ref, value_ref, grad_ref, out_ref, log_ref, start_ref,
    pos_ref, query_out, pair_out, pair_acc,
):
    score_scale = HEAD_DIM ** (-0.5)
    factor = score_scale * LOG2E
    blocks = query_ref.shape[0] // bq
    width = heads * HEAD_DIM
    pair_rows = pair_acc.shape[0]

    def clear(piece, _):
        at = pl.ds(pl.multiple_of(piece * bk, bk), bk)
        pair_acc[at, :] = jnp.zeros((bk, 2 * width), jnp.float32)
        return 0

    lax.fori_loop(0, pair_rows // bk, clear, 0)

    def one_block(index, _):
        low, inner_low, inner_high, high = block_ranges(table, index)
        rows = pl.ds(pl.multiple_of(index * bq, bq), bq)
        start, pos = start_ref[index], pos_ref[index]
        deltas, logs = [], []
        for head in range(heads):
            cols = pl.ds(head * HEAD_DIM, HEAD_DIM)
            product = grad_ref[rows, cols].astype(jnp.float32) * out_ref[rows, cols].astype(
                jnp.float32
            )
            deltas.append(jnp.sum(product.T, axis=0, keepdims=True))
            logs.append(log_ref[index, pl.ds(head, 1), :])

        def step(masked, piece, carry):
            keys_at = pl.ds(pl.multiple_of(piece * bk, bk), bk)
            if masked:
                key_pos = piece * bk + lax.broadcasted_iota(jnp.int32, (bk, bq), 0)
                allowed = (key_pos >= start) & (key_pos <= pos)
            result = []
            for head in range(heads):
                cols = pl.ds(head * HEAD_DIM, HEAD_DIM)
                value_cols = pl.ds(width + head * HEAD_DIM, HEAD_DIM)
                key_block, query_block = key_ref[keys_at, cols], query_ref[rows, cols]
                grad_block = grad_ref[rows, cols]
                scores = dot32(key_block, query_block, NT)
                probabilities = jnp.exp2(scores * factor - logs[head])
                if masked:
                    probabilities = jnp.where(allowed, probabilities, 0.0)
                dprobs = dot32(value_ref[keys_at, cols], grad_block, NT)
                dscores = (probabilities * (dprobs - deltas[head])).astype(jnp.bfloat16)
                pair_acc[keys_at, value_cols] += jnp.dot(
                    probabilities.astype(jnp.bfloat16),
                    grad_block,
                    preferred_element_type=jnp.float32,
                )
                pair_acc[keys_at, cols] += jnp.dot(
                    dscores, query_block, preferred_element_type=jnp.float32
                )
                result.append(carry[head] + dot32(key_block, dscores, TN))
            return tuple(result)

        carry = tuple(jnp.zeros((HEAD_DIM, bq), jnp.float32) for _ in range(heads))
        carry = lax.fori_loop(low, inner_low, functools.partial(step, True), carry)
        carry = lax.fori_loop(inner_low, inner_high, functools.partial(step, False), carry)
        carry = lax.fori_loop(inner_high, high, functools.partial(step, True), carry)
        for head in range(heads):
            query_out[rows, pl.ds(head * HEAD_DIM, HEAD_DIM)] = (
                carry[head].T * score_scale
            ).astype(jnp.bfloat16)
        return 0

    lax.fori_loop(0, blocks, one_block, 0)

    def flush(piece, _):
        at = pl.ds(pl.multiple_of(piece * bk, bk), bk)
        pair_out[at, :width] = (pair_acc[at, :width] * score_scale).astype(jnp.bfloat16)
        pair_out[at, width:] = pair_acc[at, width:].astype(jnp.bfloat16)
        return 0

    lax.fori_loop(0, pair_rows // bk, flush, 0)


def make_table(start, pos, bq, bk):
    starts, places = start.reshape(-1, bq), pos.reshape(-1, bq)
    low = starts[:, 0] // bk
    inner_low = (starts[:, -1] + bk - 1) // bk
    inner_high = jnp.maximum(inner_low, (places[:, 0] + 1) // bk)
    high = places[:, -1] // bk + 1
    return jnp.stack([low, inner_low, inner_high, high], axis=1).astype(jnp.int32)


def middle_kernel(
    number, part_ref, w_any, state_ref, probe_ref, grad_out, readout_out, w_ref, joined, half,
    sending, landing, send_sem, recv_sem, back_send, back_recv, w_sem,
):
    me = lax.axis_index("head")
    width = part_ref.shape[1]
    own = state_ref.shape[0]
    model = state_ref.shape[1]
    w_copy = pltpu.make_async_copy(w_any, w_ref, w_sem)
    w_copy.start()
    greet("head", number, me)
    my_cols = pl.ds(pl.multiple_of(me * width, width), width)
    my_rows = pl.ds(pl.multiple_of(me * own, own), own)
    copies = []
    for step in range(1, number):
        peer = lax.rem(me + step, number)
        copy = pltpu.make_async_remote_copy(
            src_ref=part_ref.at[pl.ds(pl.multiple_of(peer * own, own), own)],
            dst_ref=joined.at[:, my_cols],
            send_sem=send_sem.at[step],
            recv_sem=recv_sem.at[step],
            device_id={"head": peer},
            device_id_type=MESH,
        )
        copy.start()
        copies.append(copy)
    joined[:, my_cols] = part_ref[my_rows, :]
    w_copy.wait()
    for copy in copies:
        copy.wait()

    tile = min(256, model)

    def project(piece, carry):
        squares, products = carry
        cols = pl.ds(pl.multiple_of(piece * tile, tile), tile)
        layer = state_ref[:, cols].astype(jnp.float32) + jnp.dot(
            joined[...], w_ref[:, cols], preferred_element_type=jnp.float32
        )
        readout_out[:, cols] = layer
        squares = squares + jnp.sum(layer * layer, axis=1, keepdims=True)
        products = products + jnp.sum(
            layer * probe_ref[:, cols].astype(jnp.float32), axis=1, keepdims=True
        )
        return squares, products

    zero = jnp.zeros((own, 1), jnp.float32)
    squares, products = lax.fori_loop(0, model // tile, project, (zero, zero))
    scale = lax.rsqrt(squares / model + EPSILON)
    bend = scale**3 * (products / model)

    def finish(piece, _):
        cols = pl.ds(pl.multiple_of(piece * tile, tile), tile)
        readout = scale * probe_ref[:, cols].astype(jnp.float32) - readout_out[:, cols] * bend
        readout_out[:, cols] = readout
        half[:, cols] = readout.astype(jnp.bfloat16)
        return 0

    lax.fori_loop(0, model // tile, finish, 0)
    copies = []
    for step in range(1, number):
        peer = lax.rem(me + step, number)
        sending[step] = dot32(
            half[...], w_ref[pl.ds(pl.multiple_of(peer * width, width), width), :], NT
        ).astype(jnp.bfloat16)
        copy = pltpu.make_async_remote_copy(
            src_ref=sending.at[step],
            dst_ref=landing.at[my_rows],
            send_sem=back_send.at[step],
            recv_sem=back_recv.at[step],
            device_id={"head": peer},
            device_id_type=MESH,
        )
        copy.start()
        copies.append(copy)
    landing[my_rows, :] = dot32(half[...], w_ref[my_cols, :], NT).astype(jnp.bfloat16)
    for copy in copies:
        copy.wait()
    grad_out[...] = landing[...]


def middle(number, part, w_full, state_own, probe_own):
    rows, width = part.shape
    own, model = state_own.shape
    return pl.pallas_call(
        functools.partial(middle_kernel, number),
        out_shape=(
            jax.ShapeDtypeStruct((rows, width), jnp.bfloat16),
            jax.ShapeDtypeStruct((own, model), jnp.float32),
        ),
        in_specs=[VMEM, ANY, VMEM, VMEM],
        out_specs=(VMEM, VMEM),
        scratch_shapes=[
            pltpu.VMEM(w_full.shape, jnp.bfloat16),
            pltpu.VMEM((own, number * width), jnp.bfloat16),
            pltpu.VMEM((own, model), jnp.bfloat16),
            pltpu.VMEM((number, own, width), jnp.bfloat16),
            pltpu.VMEM((rows, width), jnp.bfloat16),
            pltpu.SemaphoreType.DMA((number,)),
            pltpu.SemaphoreType.DMA((number,)),
            pltpu.SemaphoreType.DMA((number,)),
            pltpu.SemaphoreType.DMA((number,)),
            pltpu.SemaphoreType.DMA,
        ],
        compiler_params=pltpu.CompilerParams(
            collective_id=1, has_side_effects=True, vmem_limit_bytes=60 * 2**20
        ),
    )(part, w_full, state_own, probe_own)


def tail_kernel(
    ctx_count, number, pair_any, query_ref, w_ref, sum_out, own_pair, arriving, gathered, terms,
    from_partner, reduced, landing, ctx_send, ctx_recv, p_send, p_recv, z_send, z_recv, own_sem,
):
    ctx, me = lax.axis_index("ctx"), lax.axis_index("head")
    groups = number // 2
    group, core = me // 2, lax.rem(me, 2)
    partner = group * 2 + 1 - core
    rows, width = query_ref.shape
    own, model = sum_out.shape
    chunk = 2 * own
    own_copy = pltpu.make_async_copy(
        pair_any.at[pl.ds(pl.multiple_of(ctx * rows, rows), rows)], own_pair, own_sem
    )
    own_copy.start()
    barrier = pltpu.get_barrier_semaphore()
    peers = [{"ctx": lax.rem(ctx + step, ctx_count)} for step in range(1, ctx_count)]
    peers.append({"head": partner})
    for step in range(1, groups):
        peers.append({"head": lax.rem(group + step, groups) * 2 + core})
    for peer in peers:
        pl.semaphore_signal(barrier, inc=1, device_id=peer, device_id_type=MESH)
    pl.semaphore_wait(barrier, len(peers))

    def chunk_start(order):
        dest = lax.rem(group + order + 1, groups)
        return dest, pl.multiple_of(dest * chunk, chunk)

    def ctx_copy(order, step):
        target = lax.rem(ctx - step + ctx_count, ctx_count)
        _, first = chunk_start(order)
        return pltpu.make_async_remote_copy(
            src_ref=pair_any.at[pl.ds(pl.multiple_of(target * rows + first, chunk), chunk)],
            dst_ref=arriving.at[order, step - 1],
            send_sem=ctx_send.at[order, step],
            recv_sem=ctx_recv.at[order, step],
            device_id={"ctx": target},
            device_id_type=MESH,
        )

    for order in range(groups):
        for step in range(1, ctx_count):

            @pl.when(step <= ctx)
            def _():
                ctx_copy(order, step).start()

    own_copy.wait()
    tile = min(512, model)
    mine = pl.ds(pl.multiple_of(core * own, own), own)
    theirs = pl.ds(pl.multiple_of((1 - core) * own, own), own)
    waiting = []
    for order in range(groups):
        dest, first = chunk_start(order)
        at = pl.ds(first, chunk)
        gathered[...] = own_pair[at, :].astype(jnp.float32)
        for step in range(1, ctx_count):

            @pl.when(ctx + step < ctx_count)
            def _():
                ctx_copy(order, step).wait_recv()
                gathered[...] += arriving[order, step - 1].astype(jnp.float32)

        def multiply(piece, _):
            cols = pl.ds(pl.multiple_of(piece * tile, tile), tile)
            term = dot32(query_ref[at, :], w_ref[0, cols, :], NT)
            term += dot32(gathered[:, :width].astype(jnp.bfloat16), w_ref[1, cols, :], NT)
            term += dot32(gathered[:, width:].astype(jnp.bfloat16), w_ref[2, cols, :], NT)
            terms[order, :, cols] = term.astype(jnp.bfloat16)
            return 0

        lax.fori_loop(0, model // tile, multiply, 0)
        copy = pltpu.make_async_remote_copy(
            src_ref=terms.at[order, theirs],
            dst_ref=from_partner.at[order],
            send_sem=p_send.at[order],
            recv_sem=p_recv.at[order],
            device_id={"head": partner},
            device_id_type=MESH,
        )
        copy.start()
        copy.wait()
        both = terms[order, mine, :].astype(jnp.float32) + from_partner[order].astype(jnp.float32)
        if order < groups - 1:
            reduced[order] = both.astype(jnp.bfloat16)
            copy = pltpu.make_async_remote_copy(
                src_ref=reduced.at[order],
                dst_ref=landing.at[order],
                send_sem=z_send.at[order],
                recv_sem=z_recv.at[order],
                device_id={"head": dest * 2 + core},
                device_id_type=MESH,
            )
            copy.start()
            waiting.append(copy)
        else:
            sum_out[...] = both
    for order, copy in enumerate(waiting):
        copy.wait()
        sum_out[...] += landing[order].astype(jnp.float32)
    for order in range(groups):
        for step in range(1, ctx_count):

            @pl.when(step <= ctx)
            def _():
                ctx_copy(order, step).wait_send()


def tail(ctx_count, number, pair, query_grad, w_qkv):
    rows, width = query_grad.shape
    model = w_qkv.shape[1]
    own, groups = rows // number, number // 2
    half, full = jnp.bfloat16, jnp.float32
    dma = pltpu.SemaphoreType.DMA
    return pl.pallas_call(
        functools.partial(tail_kernel, ctx_count, number),
        out_shape=jax.ShapeDtypeStruct((own, model), full),
        in_specs=[ANY, VMEM, VMEM],
        out_specs=VMEM,
        scratch_shapes=[
            pltpu.VMEM((rows, 2 * width), half),
            pltpu.VMEM((groups, ctx_count - 1, 2 * own, 2 * width), half),
            pltpu.VMEM((2 * own, 2 * width), full),
            pltpu.VMEM((groups, 2 * own, model), half),
            pltpu.VMEM((groups, own, model), half),
            pltpu.VMEM((groups, own, model), half),
            pltpu.VMEM((groups, own, model), half),
            dma((groups, ctx_count)),
            dma((groups, ctx_count)),
            dma((groups,)),
            dma((groups,)),
            dma((groups,)),
            dma((groups,)),
            dma,
        ],
        compiler_params=pltpu.CompilerParams(
            collective_id=2, has_side_effects=True, vmem_limit_bytes=60 * 2**20
        ),
    )(pair, query_grad, w_qkv)


def body(state, norm_gain, w_qkv, w_out, probe, noise, segment_ids):
    local_rows, model_width = state.shape
    width = w_qkv.shape[2]
    local_heads = width // HEAD_DIM
    head_count = lax.axis_size("head")
    ctx_count = lax.axis_size("ctx")
    ctx_index = lax.axis_index("ctx")
    own_rows = local_rows // head_count
    row_start = lax.axis_index("head") * own_rows
    w_full = lax.all_gather(w_out, "head", axis=0, tiled=True)
    state_f = state.astype(jnp.float32)
    gain_full = norm_gain.astype(jnp.float32)
    inverse = row_scale(state_f)
    normed = (state_f * inverse * gain_full).astype(jnp.bfloat16)

    def project(index):
        return jnp.dot(normed, w_qkv[index], preferred_element_type=jnp.float32).astype(
            jnp.bfloat16
        )

    key_rows, value_rows = project(1), project(2)
    keys, values, segs, query_rows = gather_keys(
        ctx_count, key_rows, value_rows, segment_ids, normed, w_qkv[0]
    )
    total_rows = keys.shape[0]
    pos = ctx_index * local_rows + jnp.arange(local_rows, dtype=jnp.int32)
    start = jnp.sum((segs[None, :] < segment_ids[:, None]).astype(jnp.int32), axis=1)
    fq, fk = (min(local_rows, size) for size in FORWARD_BLOCKS)
    gq, gk = (min(local_rows, size) for size in BACKWARD_BLOCKS)
    smem = pl.BlockSpec(memory_space=pltpu.SMEM)
    params = pltpu.CompilerParams(vmem_limit_bytes=60 * 2**20)
    outputs, logs = pl.pallas_call(
        functools.partial(forward_kernel, local_heads, fq, fk),
        out_shape=(
            jax.ShapeDtypeStruct((local_rows, width), jnp.bfloat16),
            jax.ShapeDtypeStruct((local_rows // fq, local_heads, fq), jnp.float32),
        ),
        in_specs=[smem] + [VMEM] * 5,
        out_specs=(VMEM, VMEM),
        compiler_params=params,
        cost_estimate=pl.CostEstimate(
            flops=4 * local_rows * total_rows * width, bytes_accessed=0, transcendentals=0
        ),
    )(
        make_table(start, pos, fq, fk),
        query_rows,
        keys,
        values,
        start.reshape(-1, 1, fq),
        pos.reshape(-1, 1, fq),
    )
    state_half = lax.dynamic_slice_in_dim(state, row_start, own_rows, 0)
    probe_own = lax.dynamic_slice_in_dim(probe, row_start, own_rows, 0)
    state_own = state_half.astype(jnp.float32)
    inverse_own = row_scale(state_own)
    grads_out, readout_own = middle(head_count, outputs, w_full, state_half, probe_own)
    query_grad, pair = pl.pallas_call(
        functools.partial(backward_kernel, local_heads, gq, gk),
        out_shape=(
            jax.ShapeDtypeStruct((local_rows, width), jnp.bfloat16),
            jax.ShapeDtypeStruct((total_rows, 2 * width), jnp.bfloat16),
        ),
        in_specs=[smem] + [VMEM] * 8,
        out_specs=(VMEM, VMEM),
        scratch_shapes=[pltpu.VMEM((total_rows, 2 * width), jnp.float32)],
        compiler_params=params,
        cost_estimate=pl.CostEstimate(
            flops=10 * local_rows * total_rows * width, bytes_accessed=0, transcendentals=0
        ),
    )(
        make_table(start, pos, gq, gk),
        query_rows,
        keys,
        values,
        grads_out,
        outputs,
        logs.reshape(local_rows // fq, local_heads, fq),
        start.reshape(-1, 1, gq),
        pos.reshape(-1, 1, gq),
    )
    normed_grad = tail(ctx_count, head_count, pair, query_grad, w_qkv)
    gain_grad = normed_grad * gain_full
    gradient = (
        readout_own
        + inverse_own * gain_grad
        - state_own * inverse_own**3 * jnp.mean(gain_grad * state_own, axis=-1, keepdims=True)
    )
    return state_own - STEP_SIZE * gradient + jnp.sqrt(2.0 * STEP_SIZE) * noise.astype(jnp.float32)


def remote(source, target, send_sem, recv_sem, ctx, head):
    return pltpu.make_async_remote_copy(
        src_ref=source,
        dst_ref=target,
        send_sem=send_sem,
        recv_sem=recv_sem,
        device_id={"ctx": ctx, "head": head},
        device_id_type=MESH,
    )


def place():
    ctx, me = lax.axis_index("ctx"), lax.axis_index("head")
    return ctx, me, me // 2, lax.rem(me, 2)


def meet(peers):
    barrier = pltpu.get_barrier_semaphore()
    for ctx, head in peers:
        pl.semaphore_signal(
            barrier, inc=1, device_id={"ctx": ctx, "head": head}, device_id_type=MESH
        )
    pl.semaphore_wait(barrier, len(peers))


def far_first(groups, group, step):
    result = 0
    for index in range(groups):
        order = sorted(range(groups), key=lambda other: (-abs(other - index), -other))
        result = jnp.where(group == index, order[step], result)
    return result


def project_kernel(
    ctx_count, head_count, state_any, w_any, gain_ref, seg_ref, query_out, kv_out, segs_out,
    state_v, w_v, query_buf, kv_buf, state_sem, w_sem, q_send, q_recv, kv_send, kv_recv, pass_send,
    seg_send, seg_recv, own_q, own_kv, own_seg,
):
    ctx, me, group, core = place()
    rows, model = state_any.shape
    own, groups = rows // head_count, head_count // 2
    slots = w_any.shape[2] // HEAD_DIM
    chunk = 2 * own
    partner = group * 2 + 1 - core

    def at(piece):
        return pl.ds(pl.multiple_of(piece * chunk, chunk), chunk)

    def load_state(piece):
        return pltpu.make_async_copy(
            state_any.at[at(piece)], state_v.at[at(piece)], state_sem.at[piece]
        )

    load_state(0).start()
    w_loads = [pltpu.make_async_copy(w_any.at[t], w_v.at[t], w_sem.at[t]) for t in range(3)]
    for copy in w_loads:
        copy.start()
    for piece in range(1, groups):
        load_state(piece).start()
    peers = [(lax.rem(ctx + step, ctx_count), me) for step in range(1, ctx_count)]
    peers += [(lax.rem(ctx + step, ctx_count), partner) for step in range(ctx_count)]
    meet(peers)
    segs = []
    for step in range(1, ctx_count):
        copy = remote(
            seg_ref, segs_out.at[ctx], seg_send.at[step], seg_recv.at[step],
            lax.rem(ctx + step, ctx_count), me,
        )
        copy.start()
        segs.append(copy)
    copy = pltpu.make_async_copy(seg_ref, segs_out.at[ctx], own_seg)
    copy.start()
    segs.append(copy)
    for copy in w_loads:
        copy.wait()
    gain = gain_ref[...].astype(jnp.float32)

    def away(slot, kind, piece, dest):
        head = group * 2 + kind
        return (
            remote(
                query_buf.at[slot, piece, kind], query_out.at[ctx, piece],
                q_send.at[slot, kind, piece], q_recv.at[ctx, piece], dest, head,
            ),
            remote(
                kv_buf.at[slot, kind, piece], kv_out.at[kind, ctx, piece],
                kv_send.at[slot, kind, piece], kv_recv.at[kind, ctx, piece], dest, head,
            ),
        )

    def local(slot, piece):
        result = [
            pltpu.make_async_copy(
                query_buf.at[slot, piece, core], query_out.at[ctx, piece], own_q.at[piece]
            )
        ]
        for kind in range(2):
            result.append(
                pltpu.make_async_copy(
                    kv_buf.at[slot, kind, piece], kv_out.at[kind, ctx, piece],
                    own_kv.at[kind, piece],
                )
            )
        return result

    def beside(slot, piece):
        result = [
            remote(
                query_buf.at[slot, piece, 1 - core], query_out.at[ctx, piece],
                q_send.at[slot, 1 - core, piece], q_recv.at[ctx, piece], ctx, partner,
            )
        ]
        for kind in range(2):
            result.append(
                remote(
                    kv_buf.at[slot, kind, piece], kv_out.at[kind, ctx, piece],
                    kv_send.at[slot, kind, piece], kv_recv.at[kind, ctx, piece], ctx, partner,
                )
            )
        return result

    def project(piece, _):
        load_state(piece).wait()
        block = state_v[at(piece), :].astype(jnp.float32)
        normed = (block * row_scale(block) * gain).astype(jnp.bfloat16)
        for t in range(3):
            result = jnp.dot(normed, w_v[t], preferred_element_type=jnp.float32).astype(
                jnp.bfloat16
            )
            for slot in range(slots):
                part = result[:, slot * HEAD_DIM : (slot + 1) * HEAD_DIM]
                if t == 0:
                    query_buf[slot, piece, 0] = part[:own]
                    query_buf[slot, piece, 1] = part[own:]
                else:
                    kv_buf[slot, t - 1, piece] = part
        for slot in range(slots):
            dest = core * slots + slot

            @pl.when(dest != ctx)
            def _():
                for kind in range(2):
                    for copy in away(slot, kind, piece, dest):
                        copy.start()

            @pl.when(dest == ctx)
            def _():
                for copy in local(slot, piece) + beside(slot, piece):
                    copy.start()

        return 0

    lax.fori_loop(0, groups, project, 0)

    def hand_over(piece, step):
        source = lax.rem(ctx + step, ctx_count)
        return remote(
            kv_out.at[core, source, piece], kv_out.at[core, source, piece],
            pass_send.at[step, piece], kv_recv.at[core, source, piece], ctx, partner,
        )

    def forward(piece, _):
        for step in range(1, ctx_count):
            copy = hand_over(piece, step)
            copy.wait_recv()
            copy.start()
        return 0

    lax.fori_loop(0, groups, forward, 0)

    def got_query(source, piece):
        remote(
            query_out.at[source, piece], query_out.at[source, piece], q_send.at[0, 0, piece],
            q_recv.at[source, piece], ctx, partner,
        ).wait_recv()

    def got_kv(kind, source, piece):
        remote(
            kv_out.at[kind, source, piece], kv_out.at[kind, source, piece],
            kv_send.at[0, 0, piece], kv_recv.at[kind, source, piece], ctx, partner,
        ).wait_recv()

    mine = ctx // slots == core

    def finish(piece, _):
        for step in range(1, ctx_count):
            source = lax.rem(ctx + step, ctx_count)
            got_query(source, piece)
            got_kv(1 - core, source, piece)
            hand_over(piece, step).wait_send()
        for slot in range(slots):
            dest = core * slots + slot

            @pl.when(dest != ctx)
            def _():
                for kind in range(2):
                    for copy in away(slot, kind, piece, dest):
                        copy.wait_send()

            @pl.when(dest == ctx)
            def _():
                for copy in local(slot, piece):
                    copy.wait()
                for copy in beside(slot, piece):
                    copy.wait_send()

        @pl.when(jnp.logical_not(mine))
        def _():
            got_query(ctx, piece)
            for kind in range(2):
                got_kv(kind, ctx, piece)

        return 0

    lax.fori_loop(0, groups, finish, 0)
    for copy in segs:
        copy.wait()


def project_heads(ctx_count, head_count, state, w_qkv, gain, segment_ids):
    rows, model = state.shape
    width = w_qkv.shape[2]
    own, groups, slots = rows // head_count, head_count // 2, width // HEAD_DIM
    seg = segment_ids.reshape(-1, 128)
    half, dma = jnp.bfloat16, pltpu.SemaphoreType.DMA
    return pl.pallas_call(
        functools.partial(project_kernel, ctx_count, head_count),
        out_shape=(
            jax.ShapeDtypeStruct((ctx_count, groups, own, HEAD_DIM), half),
            jax.ShapeDtypeStruct((2, ctx_count, groups, 2 * own, HEAD_DIM), half),
            jax.ShapeDtypeStruct((ctx_count,) + seg.shape, seg.dtype),
        ),
        in_specs=[ANY, ANY, VMEM, VMEM],
        out_specs=(ANY, ANY, ANY),
        scratch_shapes=[
            pltpu.VMEM((rows, model), half),
            pltpu.VMEM(w_qkv.shape, half),
            pltpu.VMEM((slots, groups, 2, own, HEAD_DIM), half),
            pltpu.VMEM((slots, 2, groups, 2 * own, HEAD_DIM), half),
            dma((groups,)),
            dma((3,)),
            dma((slots, 2, groups)),
            dma((ctx_count, groups)),
            dma((slots, 2, groups)),
            dma((2, ctx_count, groups)),
            dma((ctx_count, groups)),
            dma((ctx_count,)),
            dma((ctx_count,)),
            dma((groups,)),
            dma((2, groups)),
            dma,
        ],
        compiler_params=pltpu.CompilerParams(
            collective_id=0, has_side_effects=True, vmem_limit_bytes=60 * 2**20
        ),
    )(state, w_qkv, gain, seg)


def segment_bounds(segs_ref):
    segs = segs_ref[...]

    def below(value):
        return jnp.sum(jnp.where(segs < value, 1.0, 0.0)).astype(jnp.int32)

    return below(1), below(2)


def tile_plan(bounds, rows, own, parts, sub, bk, tile, core):
    first_bound, second_bound = bounds

    def start_of(pos):
        return jnp.where(pos >= second_bound, second_bound, jnp.where(pos >= first_bound, first_bound, 0))

    blocks = sub // own
    base = tile * rows + core * own
    places = []
    for part in range(parts):
        lane = lax.broadcasted_iota(jnp.int32, (1, sub), 1)
        pos = base + (lane // own + part * blocks) * (2 * own) + lane % own
        places.append((start_of(pos), pos))
    first, last = base, base + (parts * blocks - 1) * 2 * own + own - 1
    low = start_of(first) // bk
    inner_low = (start_of(last) + bk - 1) // bk
    inner_high = jnp.maximum(inner_low, (first + 1) // bk)
    high = last // bk + 1
    return places, low, inner_low, inner_high, high


def head_forward_kernel(
    rows, own, parts, sub, bk, segs_ref, query_ref, kv_ref, out_ref, log_ref
):
    factor = HEAD_DIM ** (-0.5) * LOG2E
    core = lax.rem(lax.axis_index("head"), 2)
    bounds = segment_bounds(segs_ref)
    tiles = query_ref.shape[0] // (parts * sub)

    def one_tile(tile, _):
        places, low, inner_low, inner_high, high = tile_plan(
            bounds, rows, own, parts, sub, bk, tile, core
        )

        def at(part):
            return pl.ds(pl.multiple_of((tile * parts + part) * sub, sub), sub)

        def step(masked, piece, carry):
            keys_at = pl.ds(pl.multiple_of(piece * bk, bk), bk)
            if masked:
                key_pos = piece * bk + lax.broadcasted_iota(jnp.int32, (bk, sub), 0)
            result = []
            for part in range(parts):
                top, total, acc = carry[part]
                scores = dot32(kv_ref[0, keys_at, :], query_ref[at(part), :], NT)
                if masked:
                    start, pos = places[part]
                    scores = jnp.where((key_pos >= start) & (key_pos <= pos), scores, NEGATIVE)
                new_top = jnp.maximum(top, jnp.max(scores, axis=0, keepdims=True) * factor)
                weights = jnp.exp2(scores * factor - new_top)
                scale = jnp.exp2(top - new_top)
                total = total * scale + jnp.sum(weights, axis=0, keepdims=True)
                acc = acc * scale + dot32(kv_ref[1, keys_at, :], weights.astype(jnp.bfloat16), TN)
                result.append((new_top, total, acc))
            return tuple(result)

        carry = tuple(
            (
                jnp.full((1, sub), NEGATIVE, jnp.float32),
                jnp.zeros((1, sub), jnp.float32),
                jnp.zeros((HEAD_DIM, sub), jnp.float32),
            )
            for _ in range(parts)
        )
        carry = lax.fori_loop(low, inner_low, functools.partial(step, True), carry)
        carry = lax.fori_loop(inner_low, inner_high, functools.partial(step, False), carry)
        carry = lax.fori_loop(inner_high, high, functools.partial(step, True), carry)
        for part in range(parts):
            top, total, acc = carry[part]
            out_ref[at(part), :] = (acc / total).T.astype(jnp.bfloat16)
            log_ref[tile, pl.ds(part, 1), :] = top + jnp.log2(total)
        return 0

    lax.fori_loop(0, tiles, one_tile, 0)


def head_backward_kernel(
    rows, own, parts, sub, bk, segs_ref, query_ref, kv_ref, grad_ref, out_ref, log_ref, query_out,
    pair_out, pair_acc,
):
    score_scale = HEAD_DIM ** (-0.5)
    factor = score_scale * LOG2E
    core = lax.rem(lax.axis_index("head"), 2)
    bounds = segment_bounds(segs_ref)
    tiles = query_ref.shape[0] // (parts * sub)
    pair_rows = pair_acc.shape[0]

    def clear(piece, _):
        at = pl.ds(pl.multiple_of(piece * bk, bk), bk)
        pair_acc[at, :] = jnp.zeros((bk, 2 * HEAD_DIM), jnp.float32)
        return 0

    lax.fori_loop(0, pair_rows // bk, clear, 0)

    def one_tile(tile, _):
        places, low, inner_low, inner_high, high = tile_plan(
            bounds, rows, own, parts, sub, bk, tile, core
        )

        def at(part):
            return pl.ds(pl.multiple_of((tile * parts + part) * sub, sub), sub)

        deltas, logs = [], []
        for part in range(parts):
            product = grad_ref[at(part), :].astype(jnp.float32) * out_ref[at(part), :].astype(
                jnp.float32
            )
            deltas.append(jnp.sum(product.T, axis=0, keepdims=True))
            logs.append(log_ref[tile, pl.ds(part, 1), :])

        def step(masked, piece, carry):
            keys_at = pl.ds(pl.multiple_of(piece * bk, bk), bk)
            if masked:
                key_pos = piece * bk + lax.broadcasted_iota(jnp.int32, (bk, sub), 0)
            result = []
            key_block, value_block = kv_ref[0, keys_at, :], kv_ref[1, keys_at, :]
            for part in range(parts):
                query_block, grad_block = query_ref[at(part), :], grad_ref[at(part), :]
                scores = dot32(key_block, query_block, NT)
                probabilities = jnp.exp2(scores * factor - logs[part])
                if masked:
                    start, pos = places[part]
                    probabilities = jnp.where(
                        (key_pos >= start) & (key_pos <= pos), probabilities, 0.0
                    )
                dprobs = dot32(value_block, grad_block, NT)
                dscores = (probabilities * (dprobs - deltas[part])).astype(jnp.bfloat16)
                pair_acc[keys_at, HEAD_DIM:] += jnp.dot(
                    probabilities.astype(jnp.bfloat16),
                    grad_block,
                    preferred_element_type=jnp.float32,
                )
                pair_acc[keys_at, :HEAD_DIM] += jnp.dot(
                    dscores, query_block, preferred_element_type=jnp.float32
                )
                result.append(carry[part] + dot32(key_block, dscores, TN))
            return tuple(result)

        carry = tuple(jnp.zeros((HEAD_DIM, sub), jnp.float32) for _ in range(parts))
        carry = lax.fori_loop(low, inner_low, functools.partial(step, True), carry)
        carry = lax.fori_loop(inner_low, inner_high, functools.partial(step, False), carry)
        carry = lax.fori_loop(inner_high, high, functools.partial(step, True), carry)
        for part in range(parts):
            query_out[at(part), :] = (carry[part].T * score_scale).astype(jnp.bfloat16)
        return 0

    lax.fori_loop(0, tiles, one_tile, 0)

    def flush(piece, _):
        at = pl.ds(pl.multiple_of(piece * bk, bk), bk)
        pair_out[at, :HEAD_DIM] = (pair_acc[at, :HEAD_DIM] * score_scale).astype(jnp.bfloat16)
        pair_out[at, HEAD_DIM:] = pair_acc[at, HEAD_DIM:].astype(jnp.bfloat16)
        return 0

    lax.fori_loop(0, pair_rows // bk, flush, 0)


def readout_kernel(
    ctx_count, head_count, part_ref, w_any, state_any, probe_any, grad_out, readout_out, w_ref,
    joined, half, sending, state_own, probe_own, out_send, out_recv, back_send, back_recv, own_sem,
    w_sem, row_sem,
):
    ctx, me, group, core = place()
    groups = head_count // 2
    own, model = readout_out.shape
    my_rows = pl.ds(pl.multiple_of(me * own, own), own)
    row_loads = [
        pltpu.make_async_copy(state_any.at[my_rows], state_own, row_sem.at[0]),
        pltpu.make_async_copy(probe_any.at[my_rows], probe_own, row_sem.at[1]),
    ]
    for copy in row_loads:
        copy.start()
    quarter = w_any.shape[2]

    def load_w(index):
        piece, head = index // head_count, lax.rem(index, head_count)
        first = pl.multiple_of((head * ctx_count + piece) * quarter, quarter)
        return pltpu.make_async_copy(
            w_any.at[piece, head], w_ref.at[pl.ds(first, quarter)], w_sem.at[index]
        )

    def start_w(index, _):
        load_w(index).start()
        return 0

    def wait_w(index, _):
        load_w(index).wait()
        return 0

    lax.fori_loop(0, ctx_count * head_count, start_w, 0)
    peers = []
    for far in range(groups):
        for step in range(ctx_count):
            if far or step:
                peers.append(
                    (lax.rem(ctx + step, ctx_count), lax.rem(group + far, groups) * 2 + core)
                )
    meet(peers)

    def cols_of(group_at, ctx_at):
        head = group_at * ctx_count + ctx_at
        return pl.ds(pl.multiple_of(head * HEAD_DIM, HEAD_DIM), HEAD_DIM)

    copies = []
    for order in range(groups):
        other = far_first(groups, group, order)
        for step in range(ctx_count):
            peer = lax.rem(ctx + step, ctx_count)
            if order == groups - 1 and step == 0:
                continue
            copy = remote(
                part_ref.at[peer, other], joined.at[:, cols_of(group, ctx)],
                out_send.at[order, step], out_recv.at[group, ctx], peer, other * 2 + core,
            )
            copy.start()
            copies.append(copy)
    joined[:, cols_of(group, ctx)] = part_ref[ctx, group]
    for copy in row_loads:
        copy.wait()
    lax.fori_loop(0, ctx_count * head_count, wait_w, 0)
    sources = []
    for far in range(groups):
        for step in range(ctx_count):
            if far or step:
                sources.append((lax.rem(group + far, groups), lax.rem(ctx + step, ctx_count)))
    for other, peer in sources:
        remote(
            part_ref.at[peer, other], joined.at[:, cols_of(other, peer)], out_send.at[0, 0],
            out_recv.at[other, peer], peer, other * 2 + core,
        ).wait_recv()
    for copy in copies:
        copy.wait_send()
    tile = min(256, model)

    def project(piece, carry):
        squares, products = carry
        cols = pl.ds(pl.multiple_of(piece * tile, tile), tile)
        layer = state_own[:, cols].astype(jnp.float32) + jnp.dot(
            joined[...], w_ref[:, cols], preferred_element_type=jnp.float32
        )
        readout_out[:, cols] = layer
        squares = squares + jnp.sum(layer * layer, axis=1, keepdims=True)
        products = products + jnp.sum(
            layer * probe_own[:, cols].astype(jnp.float32), axis=1, keepdims=True
        )
        return squares, products

    zero = jnp.zeros((own, 1), jnp.float32)
    squares, products = lax.fori_loop(0, model // tile, project, (zero, zero))
    scale = lax.rsqrt(squares / model + EPSILON)
    bend = scale**3 * (products / model)

    def finish(piece, _):
        cols = pl.ds(pl.multiple_of(piece * tile, tile), tile)
        readout = scale * probe_own[:, cols].astype(jnp.float32) - readout_out[:, cols] * bend
        readout_out[:, cols] = readout
        half[:, cols] = readout.astype(jnp.bfloat16)
        return 0

    lax.fori_loop(0, model // tile, finish, 0)
    wide = ctx_count * HEAD_DIM
    copies = []
    for order in range(groups):
        other = far_first(groups, group, order)
        result = dot32(
            half[...], w_ref[pl.ds(pl.multiple_of(other * wide, wide), wide), :], NT
        ).astype(jnp.bfloat16)
        for index in range(ctx_count):
            sending[order, index] = result[:, index * HEAD_DIM : (index + 1) * HEAD_DIM]
        for step in range(ctx_count):
            peer = lax.rem(ctx + step, ctx_count)
            if order == groups - 1 and step == 0:
                continue
            copy = remote(
                sending.at[order, peer], grad_out.at[ctx, group], back_send.at[order, step],
                back_recv.at[ctx, group], peer, other * 2 + core,
            )
            copy.start()
            copies.append(copy)
    copy = pltpu.make_async_copy(sending.at[groups - 1, ctx], grad_out.at[ctx, group], own_sem)
    copy.start()
    for other, peer in sources:
        remote(
            sending.at[0, 0], grad_out.at[peer, other], back_send.at[0, 0],
            back_recv.at[peer, other], peer, other * 2 + core,
        ).wait_recv()
    for remote_copy in copies:
        remote_copy.wait_send()
    copy.wait()


def readout_step(ctx_count, head_count, part, w_full, state, probe):
    rows, model = state.shape
    own, groups = rows // head_count, head_count // 2
    half, full, dma = jnp.bfloat16, jnp.float32, pltpu.SemaphoreType.DMA
    return pl.pallas_call(
        functools.partial(readout_kernel, ctx_count, head_count),
        out_shape=(
            jax.ShapeDtypeStruct(part.shape, half),
            jax.ShapeDtypeStruct((own, model), full),
        ),
        in_specs=[VMEM, ANY, ANY, ANY],
        out_specs=(ANY, VMEM),
        scratch_shapes=[
            pltpu.VMEM((model, model), half),
            pltpu.VMEM((own, model), half),
            pltpu.VMEM((own, model), half),
            pltpu.VMEM((groups, ctx_count, own, HEAD_DIM), half),
            pltpu.VMEM((own, model), half),
            pltpu.VMEM((own, model), half),
            dma((groups, ctx_count)),
            dma((groups, ctx_count)),
            dma((groups, ctx_count)),
            dma((ctx_count, groups)),
            dma,
            dma((ctx_count * head_count,)),
            dma((2,)),
        ],
        compiler_params=pltpu.CompilerParams(
            collective_id=1, has_side_effects=True, vmem_limit_bytes=60 * 2**20
        ),
    )(part, w_full, state, probe)


def finish_kernel(
    ctx_count, head_count, query_ref, pair_ref, w_any, state_any, noise_ref, readout_ref, gain_ref,
    new_out, w_both, beside, away, terms_in, partial, sending, total, state_own, b_send, b_recv,
    w_send, w_recv, a_send, a_recv, z_send, z_recv, own_sem,
):
    ctx, me, group, core = place()
    groups = head_count // 2
    own, model = new_out.shape
    slots = ctx_count // 2
    partner = group * 2 + 1 - core
    my_rows = pl.ds(pl.multiple_of(me * own, own), own)
    loads = [
        pltpu.make_async_copy(w_any, w_both.at[core], own_sem.at[0]),
        pltpu.make_async_copy(state_any.at[my_rows], state_own, own_sem.at[1]),
    ]
    for copy in loads:
        copy.start()
    peers = [(ctx, partner)]
    peers += [(lax.rem(ctx + step, ctx_count), me) for step in range(1, ctx_count)]
    peers += [(ctx, lax.rem(group + far, groups) * 2 + core) for far in range(1, groups)]
    meet(peers)
    dests = [far_first(groups, group, order) for order in range(groups)]
    copies = []
    for order, dest in enumerate(dests):
        copy = remote(
            pair_ref.at[:, dest, 1 - core], beside.at[order], b_send.at[order], b_recv.at[order],
            ctx, partner,
        )
        copy.start()
        copies.append(copy)
    w_copy = remote(w_any, w_both.at[core], w_send, w_recv, ctx, partner)
    w_copy.start()

    def stripe(source):
        slot = lax.rem(source, slots)
        return pl.ds(pl.multiple_of(slot * HEAD_DIM, HEAD_DIM), HEAD_DIM)

    def exchange(order, dest, step):
        peer = lax.rem(ctx + step, ctx_count)
        return remote(
            away.at[order, step], terms_in.at[dest, ctx // slots, :, :, stripe(ctx)],
            a_send.at[order, step], a_recv.at[dest, ctx], peer, me,
        )

    def arrived(dest, step):
        source = lax.rem(ctx + step, ctx_count)
        remote(
            away.at[0, 0], terms_in.at[dest, source // slots, :, :, stripe(source)],
            a_send.at[0, 0], a_recv.at[dest, source], source, me,
        ).wait_recv()

    for order, dest in enumerate(dests):
        copies[order].wait_recv()
        for step in range(1, ctx_count):
            peer = lax.rem(ctx + step, ctx_count)
            pair = pair_ref[peer, dest, core].astype(jnp.float32) + beside[order, peer].astype(
                jnp.float32
            )
            pair = pair.astype(jnp.bfloat16)
            away[order, step, 0] = query_ref[peer, dest]
            away[order, step, 1] = pair[:, :HEAD_DIM]
            away[order, step, 2] = pair[:, HEAD_DIM:]
            exchange(order, dest, step).start()
        pair = pair_ref[ctx, dest, core].astype(jnp.float32) + beside[order, ctx].astype(
            jnp.float32
        )
        pair = pair.astype(jnp.bfloat16)
        at = stripe(ctx)
        terms_in[dest, ctx // slots, 0, :, at] = query_ref[ctx, dest]
        terms_in[dest, ctx // slots, 1, :, at] = pair[:, :HEAD_DIM]
        terms_in[dest, ctx // slots, 2, :, at] = pair[:, HEAD_DIM:]
    for copy in loads:
        copy.wait()
    w_copy.wait()
    pieces = partial.shape[2]
    tile = model // pieces

    def chain(order, dest, piece):
        up = dest > group
        line = jnp.where(up, 0, 1)
        peer = jnp.where(up, group + 1, group - 1)
        return remote(
            sending.at[order, piece], partial.at[line, dest, piece], z_send.at[order, piece],
            z_recv.at[line, dest, piece], ctx, peer * 2 + core,
        )

    def came(line, dest, piece):
        remote(
            sending.at[0, piece], partial.at[line, dest, piece], z_send.at[0, piece],
            z_recv.at[line, dest, piece], ctx, partner,
        ).wait_recv()

    def term(dest, piece):
        cols = pl.ds(pl.multiple_of(piece * tile, tile), tile)
        result = None
        for half in range(2):
            for kind in range(3):
                part = dot32(terms_in[dest, half, kind], w_both[half, kind, cols, :], NT)
                result = part if result is None else result + part
        return result

    for order, dest in enumerate(dests[:-1]):
        for step in range(1, ctx_count):
            arrived(dest, step)
        line = jnp.where(dest > group, 0, 1)
        inner = (group > 0) & (group < groups - 1)

        def one_piece(piece, _):
            total[...] = term(dest, piece)

            @pl.when(inner)
            def _():
                came(line, dest, piece)
                total[...] += partial[line, dest, piece].astype(jnp.float32)

            sending[order, piece] = total[...].astype(jnp.bfloat16)
            chain(order, dest, piece).start()
            return 0

        lax.fori_loop(0, pieces, one_piece, 0)

    for step in range(1, ctx_count):
        arrived(group, step)

    state = state_own[...].astype(jnp.float32)
    inverse = row_scale(state)

    def last_piece(piece, slope):
        cols = pl.ds(pl.multiple_of(piece * tile, tile), tile)
        total[...] = term(group, piece)

        @pl.when(group > 0)
        def _():
            came(0, group, piece)
            total[...] += partial[0, group, piece].astype(jnp.float32)

        @pl.when(group < groups - 1)
        def _():
            came(1, group, piece)
            total[...] += partial[1, group, piece].astype(jnp.float32)

        gained = total[...] * gain_ref[:, cols].astype(jnp.float32)
        new_out[:, cols] = gained
        return slope + jnp.sum(
            gained * state_own[:, cols].astype(jnp.float32), axis=1, keepdims=True
        )

    slope = lax.fori_loop(0, pieces, last_piece, jnp.zeros((own, 1), jnp.float32))
    bend = inverse**3 * (slope / model)

    def update(piece, _):
        cols = pl.ds(pl.multiple_of(piece * tile, tile), tile)
        here = state_own[:, cols].astype(jnp.float32)
        gradient = readout_ref[:, cols] + inverse * new_out[:, cols] - here * bend
        new_out[:, cols] = (
            here - STEP_SIZE * gradient + NOISE_SCALE * noise_ref[:, cols].astype(jnp.float32)
        )
        return 0

    lax.fori_loop(0, pieces, update, 0)
    for order, dest in enumerate(dests):
        copies[order].wait_send()
        for step in range(1, ctx_count):
            exchange(order, dest, step).wait_send()
        if order < groups - 1:
            for piece in range(pieces):
                chain(order, dest, piece).wait_send()


def finish_step(ctx_count, head_count, query_grad, pair, w_qkv, state, noise, readout, gain):
    own, model = readout.shape
    width = w_qkv.shape[2]
    groups, pieces = head_count // 2, 4
    half, full, dma = jnp.bfloat16, jnp.float32, pltpu.SemaphoreType.DMA
    tile = model // pieces
    return pl.pallas_call(
        functools.partial(finish_kernel, ctx_count, head_count),
        out_shape=jax.ShapeDtypeStruct((own, model), full),
        in_specs=[VMEM, VMEM, ANY, ANY, VMEM, VMEM, VMEM],
        out_specs=VMEM,
        scratch_shapes=[
            pltpu.VMEM((2,) + w_qkv.shape, half),
            pltpu.VMEM((groups, ctx_count, own, 2 * HEAD_DIM), half),
            pltpu.VMEM((groups, ctx_count, 3, own, HEAD_DIM), half),
            pltpu.VMEM((groups, 2, 3, own, width), half),
            pltpu.VMEM((2, groups, pieces, own, tile), half),
            pltpu.VMEM((groups, pieces, own, tile), half),
            pltpu.VMEM((own, tile), full),
            pltpu.VMEM((own, model), half),
            dma((groups,)),
            dma((groups,)),
            dma,
            dma,
            dma((groups, ctx_count)),
            dma((groups, ctx_count)),
            dma((groups, pieces)),
            dma((2, groups, pieces)),
            dma((2,)),
        ],
        compiler_params=pltpu.CompilerParams(
            collective_id=2, has_side_effects=True, vmem_limit_bytes=60 * 2**20
        ),
    )(query_grad, pair, w_qkv, state, noise, readout, gain)


def heads_body(state, norm_gain, w_qkv, w_out, probe, noise, segment_ids):
    rows, model = state.shape
    head_count, ctx_count = lax.axis_size("head"), lax.axis_size("ctx")
    own, groups = rows // head_count, head_count // 2
    quarter = w_out.shape[0] // ctx_count
    w_part = lax.dynamic_slice_in_dim(w_out, lax.axis_index("ctx") * quarter, quarter, 0)
    w_full = lax.all_gather(lax.all_gather(w_part, "head", axis=0), "ctx", axis=0)
    gain = norm_gain.reshape(1, model)
    queries, kv, segs = project_heads(ctx_count, head_count, state, w_qkv, gain, segment_ids)
    mine, total = ctx_count * groups * own, ctx_count * rows
    queries, kv = queries.reshape(mine, HEAD_DIM), kv.reshape(2, total, HEAD_DIM)
    parts, sub = 2, groups * own // 2
    tiles, bk = ctx_count, min(rows, 512)
    params = pltpu.CompilerParams(vmem_limit_bytes=60 * 2**20)
    outputs, logs = pl.pallas_call(
        functools.partial(head_forward_kernel, rows, own, parts, sub, bk),
        out_shape=(
            jax.ShapeDtypeStruct((mine, HEAD_DIM), jnp.bfloat16),
            jax.ShapeDtypeStruct((tiles, parts, sub), jnp.float32),
        ),
        in_specs=[VMEM] * 3,
        out_specs=(VMEM, VMEM),
        compiler_params=params,
        cost_estimate=pl.CostEstimate(
            flops=4 * mine * total * HEAD_DIM, bytes_accessed=0, transcendentals=0
        ),
    )(segs, queries, kv)
    shape = (ctx_count, groups, own, HEAD_DIM)
    grads_out, readout = readout_step(
        ctx_count, head_count, outputs.reshape(shape), w_full, state, probe
    )
    query_grad, pair = pl.pallas_call(
        functools.partial(head_backward_kernel, rows, own, parts, sub, bk),
        out_shape=(
            jax.ShapeDtypeStruct((mine, HEAD_DIM), jnp.bfloat16),
            jax.ShapeDtypeStruct((total, 2 * HEAD_DIM), jnp.bfloat16),
        ),
        in_specs=[VMEM] * 6,
        out_specs=(VMEM, VMEM),
        scratch_shapes=[pltpu.VMEM((total, 2 * HEAD_DIM), jnp.float32)],
        compiler_params=params,
        cost_estimate=pl.CostEstimate(
            flops=10 * mine * total * HEAD_DIM, bytes_accessed=0, transcendentals=0
        ),
    )(segs, queries, kv, grads_out.reshape(mine, HEAD_DIM), outputs, logs)
    return finish_step(
        ctx_count, head_count, query_grad.reshape(shape),
        pair.reshape(ctx_count, groups, 2, own, 2 * HEAD_DIM), w_qkv, state, noise, readout, gain,
    )


def solution(mesh):
    placed = (
        P("ctx", None),
        P(),
        P(None, None, "head"),
        P("head", None),
        P("ctx", None),
        P(("ctx", "head"), None),
        P("ctx"),
    )

    def step(*args):
        heads = args[2].shape[2] // HEAD_DIM
        return (heads_body if 2 * heads == lax.axis_size("ctx") else body)(*args)

    return jax.shard_map(
        step, mesh=mesh, in_specs=placed, out_specs=P(("ctx", "head"), None), check_vma=False
    )
```

```python
import functools

import jax
import jax.numpy as jnp
from jax import lax
from jax.experimental import pallas as pl
from jax.experimental.pallas import tpu as pltpu
from jax.sharding import PartitionSpec as P

HEAD_DIM = 128
EPSILON = 1e-05
STEP_SIZE = 0.25
NOISE_SCALE = (2.0 * STEP_SIZE) ** 0.5
NEGATIVE = -1e30
LOG2E = 1.4426950408889634
MESH = pl.DeviceIdType.MESH
VMEM = pl.BlockSpec(memory_space=pltpu.VMEM)
ANY = pl.BlockSpec(memory_space=pl.ANY)
NT = (((1,), (1,)), ((), ()))
TN = (((0,), (0,)), ((), ()))
FORWARD_BLOCKS = (512, 512)
BACKWARD_BLOCKS = (512, 512)


def row_scale(matrix):
    return lax.rsqrt(jnp.mean(matrix * matrix, axis=-1, keepdims=True) + EPSILON)


def dot32(left, right, dims):
    return lax.dot_general(left, right, dims, preferred_element_type=jnp.float32)


def greet(axis, number, me):
    barrier = pltpu.get_barrier_semaphore()
    for step in range(1, number):
        pl.semaphore_signal(
            barrier, inc=1, device_id={axis: lax.rem(me + step, number)}, device_id_type=MESH
        )
    pl.semaphore_wait(barrier, number - 1)


def gather_kernel(
    number, key_ref, value_ref, seg_ref, normed_ref, w_ref, keys, values, segs, query_out, send_sem,
    recv_sem, own_sem,
):
    me = lax.axis_index("ctx")
    rows = key_ref.shape[0]
    greet("ctx", number, me)

    def place(index):
        return pl.ds(pl.multiple_of(index * rows, rows), rows)

    def send(slot, source, target, peer):
        copy = pltpu.make_async_remote_copy(
            src_ref=source,
            dst_ref=target,
            send_sem=send_sem.at[slot],
            recv_sem=recv_sem.at[slot],
            device_id={"ctx": peer},
            device_id_type=MESH,
        )
        copy.start()
        return copy

    mine = place(me)
    copies = []
    for step in range(1, number):
        copies.append(send(step, seg_ref, segs.at[me], lax.rem(me + step, number)))
    relay = number == 4
    if relay:
        low, high = lax.rem(me, 2), me // 2
        across, along = high * 2 + 1 - low, (1 - high) * 2 + low
        key_first = send(number, key_ref, keys.at[mine], across)
        value_first = send(number + 1, value_ref, values.at[mine], along)
        copies.append(send(number + 2, value_ref, values.at[mine], across))
        copies.append(send(number + 3, key_ref, keys.at[mine], along))
    else:
        for step in range(1, number):
            peer = lax.rem(me + step, number)
            copies.append(send(number + 2 * step, key_ref, keys.at[mine], peer))
            copies.append(send(number + 2 * step + 1, value_ref, values.at[mine], peer))
    pairs = ((key_ref, keys.at[mine]), (value_ref, values.at[mine]), (seg_ref, segs.at[me]))
    for index, (source, target) in enumerate(pairs):
        copy = pltpu.make_async_copy(source, target, own_sem.at[index])
        copy.start()
        copies.append(copy)
    tile = min(256, rows)

    def project(piece, _):
        at = pl.ds(pl.multiple_of(piece * tile, tile), tile)
        query_out[at, :] = jnp.dot(
            normed_ref[at, :], w_ref[...], preferred_element_type=jnp.float32
        ).astype(jnp.bfloat16)
        return 0

    lax.fori_loop(0, rows // tile, project, 0)
    if relay:
        key_first.wait()
        copies.append(send(number + 4, keys.at[place(across)], keys.at[place(across)], along))
        value_first.wait()
        copies.append(send(number + 5, values.at[place(along)], values.at[place(along)], across))
    for copy in copies:
        copy.wait()


def gather_keys(number, key_rows, value_rows, segment_ids, normed, w_query):
    rows, width = key_rows.shape
    seg = segment_ids.reshape(-1, 128)
    full = jax.ShapeDtypeStruct((number * rows, width), key_rows.dtype)
    keys, values, segs, queries = pl.pallas_call(
        functools.partial(gather_kernel, number),
        out_shape=(
            full,
            full,
            jax.ShapeDtypeStruct((number,) + seg.shape, seg.dtype),
            jax.ShapeDtypeStruct((rows, width), key_rows.dtype),
        ),
        in_specs=[VMEM] * 5,
        out_specs=(ANY, ANY, ANY, VMEM),
        scratch_shapes=[
            pltpu.SemaphoreType.DMA((3 * number + 6,)),
            pltpu.SemaphoreType.DMA((3 * number + 6,)),
            pltpu.SemaphoreType.DMA((3,)),
        ],
        compiler_params=pltpu.CompilerParams(collective_id=0, has_side_effects=True),
    )(key_rows, value_rows, seg, normed, w_query)
    return keys, values, segs.reshape(-1), queries


def block_ranges(table, index):
    return [table[index, column] for column in range(4)]


def forward_kernel(
    heads, bq, bk, table, query_ref, key_ref, value_ref, start_ref, pos_ref, out_ref, log_ref
):
    factor = HEAD_DIM ** (-0.5) * LOG2E
    blocks = query_ref.shape[0] // bq

    def one_block(index, _):
        low, inner_low, inner_high, high = block_ranges(table, index)
        rows = pl.ds(pl.multiple_of(index * bq, bq), bq)
        start, pos = start_ref[index], pos_ref[index]

        def step(masked, piece, carry):
            keys_at = pl.ds(pl.multiple_of(piece * bk, bk), bk)
            if masked:
                key_pos = piece * bk + lax.broadcasted_iota(jnp.int32, (bk, bq), 0)
                allowed = (key_pos >= start) & (key_pos <= pos)
            result = []
            for head in range(heads):
                top, total, acc = carry[head]
                cols = pl.ds(head * HEAD_DIM, HEAD_DIM)
                scores = dot32(key_ref[keys_at, cols], query_ref[rows, cols], NT)
                if masked:
                    scores = jnp.where(allowed, scores, NEGATIVE)
                new_top = jnp.maximum(top, jnp.max(scores, axis=0, keepdims=True) * factor)
                weights = jnp.exp2(scores * factor - new_top)
                scale = jnp.exp2(top - new_top)
                total = total * scale + jnp.sum(weights, axis=0, keepdims=True)
                acc = acc * scale + dot32(
                    value_ref[keys_at, cols], weights.astype(jnp.bfloat16), TN
                )
                result.append((new_top, total, acc))
            return tuple(result)

        carry = tuple(
            (
                jnp.full((1, bq), NEGATIVE, jnp.float32),
                jnp.zeros((1, bq), jnp.float32),
                jnp.zeros((HEAD_DIM, bq), jnp.float32),
            )
            for _ in range(heads)
        )
        carry = lax.fori_loop(low, inner_low, functools.partial(step, True), carry)
        carry = lax.fori_loop(inner_low, inner_high, functools.partial(step, False), carry)
        carry = lax.fori_loop(inner_high, high, functools.partial(step, True), carry)
        for head in range(heads):
            top, total, acc = carry[head]
            out_ref[rows, pl.ds(head * HEAD_DIM, HEAD_DIM)] = (acc / total).T.astype(jnp.bfloat16)
            log_ref[index, pl.ds(head, 1), :] = top + jnp.log2(total)
        return 0

    lax.fori_loop(0, blocks, one_block, 0)


def backward_kernel(
    heads, bq, bk, table, query_ref, key_ref, value_ref, grad_ref, out_ref, log_ref, start_ref,
    pos_ref, query_out, pair_out, pair_acc,
):
    score_scale = HEAD_DIM ** (-0.5)
    factor = score_scale * LOG2E
    blocks = query_ref.shape[0] // bq
    width = heads * HEAD_DIM
    pair_rows = pair_acc.shape[0]

    def clear(piece, _):
        at = pl.ds(pl.multiple_of(piece * bk, bk), bk)
        pair_acc[at, :] = jnp.zeros((bk, 2 * width), jnp.float32)
        return 0

    lax.fori_loop(0, pair_rows // bk, clear, 0)

    def one_block(index, _):
        low, inner_low, inner_high, high = block_ranges(table, index)
        rows = pl.ds(pl.multiple_of(index * bq, bq), bq)
        start, pos = start_ref[index], pos_ref[index]
        deltas, logs = [], []
        for head in range(heads):
            cols = pl.ds(head * HEAD_DIM, HEAD_DIM)
            product = grad_ref[rows, cols].astype(jnp.float32) * out_ref[rows, cols].astype(
                jnp.float32
            )
            deltas.append(jnp.sum(product.T, axis=0, keepdims=True))
            logs.append(log_ref[index, pl.ds(head, 1), :])

        def step(masked, piece, carry):
            keys_at = pl.ds(pl.multiple_of(piece * bk, bk), bk)
            if masked:
                key_pos = piece * bk + lax.broadcasted_iota(jnp.int32, (bk, bq), 0)
                allowed = (key_pos >= start) & (key_pos <= pos)
            result = []
            for head in range(heads):
                cols = pl.ds(head * HEAD_DIM, HEAD_DIM)
                value_cols = pl.ds(width + head * HEAD_DIM, HEAD_DIM)
                key_block, query_block = key_ref[keys_at, cols], query_ref[rows, cols]
                grad_block = grad_ref[rows, cols]
                scores = dot32(key_block, query_block, NT)
                probabilities = jnp.exp2(scores * factor - logs[head])
                if masked:
                    probabilities = jnp.where(allowed, probabilities, 0.0)
                dprobs = dot32(value_ref[keys_at, cols], grad_block, NT)
                dscores = (probabilities * (dprobs - deltas[head])).astype(jnp.bfloat16)
                pair_acc[keys_at, value_cols] += jnp.dot(
                    probabilities.astype(jnp.bfloat16),
                    grad_block,
                    preferred_element_type=jnp.float32,
                )
                pair_acc[keys_at, cols] += jnp.dot(
                    dscores, query_block, preferred_element_type=jnp.float32
                )
                result.append(carry[head] + dot32(key_block, dscores, TN))
            return tuple(result)

        carry = tuple(jnp.zeros((HEAD_DIM, bq), jnp.float32) for _ in range(heads))
        carry = lax.fori_loop(low, inner_low, functools.partial(step, True), carry)
        carry = lax.fori_loop(inner_low, inner_high, functools.partial(step, False), carry)
        carry = lax.fori_loop(inner_high, high, functools.partial(step, True), carry)
        for head in range(heads):
            query_out[rows, pl.ds(head * HEAD_DIM, HEAD_DIM)] = (
                carry[head].T * score_scale
            ).astype(jnp.bfloat16)
        return 0

    lax.fori_loop(0, blocks, one_block, 0)

    def flush(piece, _):
        at = pl.ds(pl.multiple_of(piece * bk, bk), bk)
        pair_out[at, :width] = (pair_acc[at, :width] * score_scale).astype(jnp.bfloat16)
        pair_out[at, width:] = pair_acc[at, width:].astype(jnp.bfloat16)
        return 0

    lax.fori_loop(0, pair_rows // bk, flush, 0)


def make_table(start, pos, bq, bk):
    starts, places = start.reshape(-1, bq), pos.reshape(-1, bq)
    low = starts[:, 0] // bk
    inner_low = (starts[:, -1] + bk - 1) // bk
    inner_high = jnp.maximum(inner_low, (places[:, 0] + 1) // bk)
    high = places[:, -1] // bk + 1
    return jnp.stack([low, inner_low, inner_high, high], axis=1).astype(jnp.int32)


def middle_kernel(
    number, part_ref, w_any, state_ref, probe_ref, grad_out, readout_out, w_ref, joined, half,
    sending, landing, send_sem, recv_sem, back_send, back_recv, w_sem,
):
    me = lax.axis_index("head")
    width = part_ref.shape[1]
    own = state_ref.shape[0]
    model = state_ref.shape[1]
    w_copy = pltpu.make_async_copy(w_any, w_ref, w_sem)
    w_copy.start()
    greet("head", number, me)
    my_cols = pl.ds(pl.multiple_of(me * width, width), width)
    my_rows = pl.ds(pl.multiple_of(me * own, own), own)
    copies = []
    for step in range(1, number):
        peer = lax.rem(me + step, number)
        copy = pltpu.make_async_remote_copy(
            src_ref=part_ref.at[pl.ds(pl.multiple_of(peer * own, own), own)],
            dst_ref=joined.at[:, my_cols],
            send_sem=send_sem.at[step],
            recv_sem=recv_sem.at[step],
            device_id={"head": peer},
            device_id_type=MESH,
        )
        copy.start()
        copies.append(copy)
    joined[:, my_cols] = part_ref[my_rows, :]
    w_copy.wait()
    for copy in copies:
        copy.wait()

    tile = min(256, model)

    def project(piece, carry):
        squares, products = carry
        cols = pl.ds(pl.multiple_of(piece * tile, tile), tile)
        layer = state_ref[:, cols].astype(jnp.float32) + jnp.dot(
            joined[...], w_ref[:, cols], preferred_element_type=jnp.float32
        )
        readout_out[:, cols] = layer
        squares = squares + jnp.sum(layer * layer, axis=1, keepdims=True)
        products = products + jnp.sum(
            layer * probe_ref[:, cols].astype(jnp.float32), axis=1, keepdims=True
        )
        return squares, products

    zero = jnp.zeros((own, 1), jnp.float32)
    squares, products = lax.fori_loop(0, model // tile, project, (zero, zero))
    scale = lax.rsqrt(squares / model + EPSILON)
    bend = scale**3 * (products / model)

    def finish(piece, _):
        cols = pl.ds(pl.multiple_of(piece * tile, tile), tile)
        readout = scale * probe_ref[:, cols].astype(jnp.float32) - readout_out[:, cols] * bend
        readout_out[:, cols] = readout
        half[:, cols] = readout.astype(jnp.bfloat16)
        return 0

    lax.fori_loop(0, model // tile, finish, 0)
    copies = []
    for step in range(1, number):
        peer = lax.rem(me + step, number)
        sending[step] = dot32(
            half[...], w_ref[pl.ds(pl.multiple_of(peer * width, width), width), :], NT
        ).astype(jnp.bfloat16)
        copy = pltpu.make_async_remote_copy(
            src_ref=sending.at[step],
            dst_ref=landing.at[my_rows],
            send_sem=back_send.at[step],
            recv_sem=back_recv.at[step],
            device_id={"head": peer},
            device_id_type=MESH,
        )
        copy.start()
        copies.append(copy)
    landing[my_rows, :] = dot32(half[...], w_ref[my_cols, :], NT).astype(jnp.bfloat16)
    for copy in copies:
        copy.wait()
    grad_out[...] = landing[...]


def middle(number, part, w_full, state_own, probe_own):
    rows, width = part.shape
    own, model = state_own.shape
    return pl.pallas_call(
        functools.partial(middle_kernel, number),
        out_shape=(
            jax.ShapeDtypeStruct((rows, width), jnp.bfloat16),
            jax.ShapeDtypeStruct((own, model), jnp.float32),
        ),
        in_specs=[VMEM, ANY, VMEM, VMEM],
        out_specs=(VMEM, VMEM),
        scratch_shapes=[
            pltpu.VMEM(w_full.shape, jnp.bfloat16),
            pltpu.VMEM((own, number * width), jnp.bfloat16),
            pltpu.VMEM((own, model), jnp.bfloat16),
            pltpu.VMEM((number, own, width), jnp.bfloat16),
            pltpu.VMEM((rows, width), jnp.bfloat16),
            pltpu.SemaphoreType.DMA((number,)),
            pltpu.SemaphoreType.DMA((number,)),
            pltpu.SemaphoreType.DMA((number,)),
            pltpu.SemaphoreType.DMA((number,)),
            pltpu.SemaphoreType.DMA,
        ],
        compiler_params=pltpu.CompilerParams(
            collective_id=1, has_side_effects=True, vmem_limit_bytes=60 * 2**20
        ),
    )(part, w_full, state_own, probe_own)


def tail_kernel(
    ctx_count, number, pair_any, query_ref, w_ref, sum_out, own_pair, arriving, gathered, terms,
    from_partner, reduced, landing, ctx_send, ctx_recv, p_send, p_recv, z_send, z_recv, own_sem,
):
    ctx, me = lax.axis_index("ctx"), lax.axis_index("head")
    groups = number // 2
    group, core = me // 2, lax.rem(me, 2)
    partner = group * 2 + 1 - core
    rows, width = query_ref.shape
    own, model = sum_out.shape
    chunk = 2 * own
    own_copy = pltpu.make_async_copy(
        pair_any.at[pl.ds(pl.multiple_of(ctx * rows, rows), rows)], own_pair, own_sem
    )
    own_copy.start()
    barrier = pltpu.get_barrier_semaphore()
    peers = [{"ctx": lax.rem(ctx + step, ctx_count)} for step in range(1, ctx_count)]
    peers.append({"head": partner})
    for step in range(1, groups):
        peers.append({"head": lax.rem(group + step, groups) * 2 + core})
    for peer in peers:
        pl.semaphore_signal(barrier, inc=1, device_id=peer, device_id_type=MESH)
    pl.semaphore_wait(barrier, len(peers))

    def chunk_start(order):
        dest = lax.rem(group + order + 1, groups)
        return dest, pl.multiple_of(dest * chunk, chunk)

    def ctx_copy(order, step):
        target = lax.rem(ctx - step + ctx_count, ctx_count)
        _, first = chunk_start(order)
        return pltpu.make_async_remote_copy(
            src_ref=pair_any.at[pl.ds(pl.multiple_of(target * rows + first, chunk), chunk)],
            dst_ref=arriving.at[order, step - 1],
            send_sem=ctx_send.at[order, step],
            recv_sem=ctx_recv.at[order, step],
            device_id={"ctx": target},
            device_id_type=MESH,
        )

    for order in range(groups):
        for step in range(1, ctx_count):

            @pl.when(step <= ctx)
            def _():
                ctx_copy(order, step).start()

    own_copy.wait()
    tile = min(512, model)
    mine = pl.ds(pl.multiple_of(core * own, own), own)
    theirs = pl.ds(pl.multiple_of((1 - core) * own, own), own)
    waiting = []
    for order in range(groups):
        dest, first = chunk_start(order)
        at = pl.ds(first, chunk)
        gathered[...] = own_pair[at, :].astype(jnp.float32)
        for step in range(1, ctx_count):

            @pl.when(ctx + step < ctx_count)
            def _():
                ctx_copy(order, step).wait_recv()
                gathered[...] += arriving[order, step - 1].astype(jnp.float32)

        def multiply(piece, _):
            cols = pl.ds(pl.multiple_of(piece * tile, tile), tile)
            term = dot32(query_ref[at, :], w_ref[0, cols, :], NT)
            term += dot32(gathered[:, :width].astype(jnp.bfloat16), w_ref[1, cols, :], NT)
            term += dot32(gathered[:, width:].astype(jnp.bfloat16), w_ref[2, cols, :], NT)
            terms[order, :, cols] = term.astype(jnp.bfloat16)
            return 0

        lax.fori_loop(0, model // tile, multiply, 0)
        copy = pltpu.make_async_remote_copy(
            src_ref=terms.at[order, theirs],
            dst_ref=from_partner.at[order],
            send_sem=p_send.at[order],
            recv_sem=p_recv.at[order],
            device_id={"head": partner},
            device_id_type=MESH,
        )
        copy.start()
        copy.wait()
        both = terms[order, mine, :].astype(jnp.float32) + from_partner[order].astype(jnp.float32)
        if order < groups - 1:
            reduced[order] = both.astype(jnp.bfloat16)
            copy = pltpu.make_async_remote_copy(
                src_ref=reduced.at[order],
                dst_ref=landing.at[order],
                send_sem=z_send.at[order],
                recv_sem=z_recv.at[order],
                device_id={"head": dest * 2 + core},
                device_id_type=MESH,
            )
            copy.start()
            waiting.append(copy)
        else:
            sum_out[...] = both
    for order, copy in enumerate(waiting):
        copy.wait()
        sum_out[...] += landing[order].astype(jnp.float32)
    for order in range(groups):
        for step in range(1, ctx_count):

            @pl.when(step <= ctx)
            def _():
                ctx_copy(order, step).wait_send()


def tail(ctx_count, number, pair, query_grad, w_qkv):
    rows, width = query_grad.shape
    model = w_qkv.shape[1]
    own, groups = rows // number, number // 2
    half, full = jnp.bfloat16, jnp.float32
    dma = pltpu.SemaphoreType.DMA
    return pl.pallas_call(
        functools.partial(tail_kernel, ctx_count, number),
        out_shape=jax.ShapeDtypeStruct((own, model), full),
        in_specs=[ANY, VMEM, VMEM],
        out_specs=VMEM,
        scratch_shapes=[
            pltpu.VMEM((rows, 2 * width), half),
            pltpu.VMEM((groups, ctx_count - 1, 2 * own, 2 * width), half),
            pltpu.VMEM((2 * own, 2 * width), full),
            pltpu.VMEM((groups, 2 * own, model), half),
            pltpu.VMEM((groups, own, model), half),
            pltpu.VMEM((groups, own, model), half),
            pltpu.VMEM((groups, own, model), half),
            dma((groups, ctx_count)),
            dma((groups, ctx_count)),
            dma((groups,)),
            dma((groups,)),
            dma((groups,)),
            dma((groups,)),
            dma,
        ],
        compiler_params=pltpu.CompilerParams(
            collective_id=2, has_side_effects=True, vmem_limit_bytes=60 * 2**20
        ),
    )(pair, query_grad, w_qkv)


def body(state, norm_gain, w_qkv, w_out, probe, noise, segment_ids):
    local_rows, model_width = state.shape
    width = w_qkv.shape[2]
    local_heads = width // HEAD_DIM
    head_count = lax.axis_size("head")
    ctx_count = lax.axis_size("ctx")
    ctx_index = lax.axis_index("ctx")
    own_rows = local_rows // head_count
    row_start = lax.axis_index("head") * own_rows
    w_full = lax.all_gather(w_out, "head", axis=0, tiled=True)
    state_f = state.astype(jnp.float32)
    gain_full = norm_gain.astype(jnp.float32)
    inverse = row_scale(state_f)
    normed = (state_f * inverse * gain_full).astype(jnp.bfloat16)

    def project(index):
        return jnp.dot(normed, w_qkv[index], preferred_element_type=jnp.float32).astype(
            jnp.bfloat16
        )

    key_rows, value_rows = project(1), project(2)
    keys, values, segs, query_rows = gather_keys(
        ctx_count, key_rows, value_rows, segment_ids, normed, w_qkv[0]
    )
    total_rows = keys.shape[0]
    pos = ctx_index * local_rows + jnp.arange(local_rows, dtype=jnp.int32)
    start = jnp.sum((segs[None, :] < segment_ids[:, None]).astype(jnp.int32), axis=1)
    fq, fk = (min(local_rows, size) for size in FORWARD_BLOCKS)
    gq, gk = (min(local_rows, size) for size in BACKWARD_BLOCKS)
    smem = pl.BlockSpec(memory_space=pltpu.SMEM)
    params = pltpu.CompilerParams(vmem_limit_bytes=60 * 2**20)
    outputs, logs = pl.pallas_call(
        functools.partial(forward_kernel, local_heads, fq, fk),
        out_shape=(
            jax.ShapeDtypeStruct((local_rows, width), jnp.bfloat16),
            jax.ShapeDtypeStruct((local_rows // fq, local_heads, fq), jnp.float32),
        ),
        in_specs=[smem] + [VMEM] * 5,
        out_specs=(VMEM, VMEM),
        compiler_params=params,
        cost_estimate=pl.CostEstimate(
            flops=4 * local_rows * total_rows * width, bytes_accessed=0, transcendentals=0
        ),
    )(
        make_table(start, pos, fq, fk),
        query_rows,
        keys,
        values,
        start.reshape(-1, 1, fq),
        pos.reshape(-1, 1, fq),
    )
    state_half = lax.dynamic_slice_in_dim(state, row_start, own_rows, 0)
    probe_own = lax.dynamic_slice_in_dim(probe, row_start, own_rows, 0)
    state_own = state_half.astype(jnp.float32)
    inverse_own = row_scale(state_own)
    grads_out, readout_own = middle(head_count, outputs, w_full, state_half, probe_own)
    query_grad, pair = pl.pallas_call(
        functools.partial(backward_kernel, local_heads, gq, gk),
        out_shape=(
            jax.ShapeDtypeStruct((local_rows, width), jnp.bfloat16),
            jax.ShapeDtypeStruct((total_rows, 2 * width), jnp.bfloat16),
        ),
        in_specs=[smem] + [VMEM] * 8,
        out_specs=(VMEM, VMEM),
        scratch_shapes=[pltpu.VMEM((total_rows, 2 * width), jnp.float32)],
        compiler_params=params,
        cost_estimate=pl.CostEstimate(
            flops=10 * local_rows * total_rows * width, bytes_accessed=0, transcendentals=0
        ),
    )(
        make_table(start, pos, gq, gk),
        query_rows,
        keys,
        values,
        grads_out,
        outputs,
        logs.reshape(local_rows // fq, local_heads, fq),
        start.reshape(-1, 1, gq),
        pos.reshape(-1, 1, gq),
    )
    normed_grad = tail(ctx_count, head_count, pair, query_grad, w_qkv)
    gain_grad = normed_grad * gain_full
    gradient = (
        readout_own
        + inverse_own * gain_grad
        - state_own * inverse_own**3 * jnp.mean(gain_grad * state_own, axis=-1, keepdims=True)
    )
    return state_own - STEP_SIZE * gradient + jnp.sqrt(2.0 * STEP_SIZE) * noise.astype(jnp.float32)


def remote(source, target, send_sem, recv_sem, ctx, head):
    return pltpu.make_async_remote_copy(
        src_ref=source,
        dst_ref=target,
        send_sem=send_sem,
        recv_sem=recv_sem,
        device_id={"ctx": ctx, "head": head},
        device_id_type=MESH,
    )


def place():
    ctx, me = lax.axis_index("ctx"), lax.axis_index("head")
    return ctx, me, me // 2, lax.rem(me, 2)


def meet(peers):
    barrier = pltpu.get_barrier_semaphore()
    for ctx, head in peers:
        pl.semaphore_signal(
            barrier, inc=1, device_id={"ctx": ctx, "head": head}, device_id_type=MESH
        )
    pl.semaphore_wait(barrier, len(peers))


def far_first(groups, group, step):
    result = 0
    for index in range(groups):
        order = sorted(range(groups), key=lambda other: (-abs(other - index), -other))
        result = jnp.where(group == index, order[step], result)
    return result


def front_kernel(
    ctx_count, head_count, state_any, w_any, gain_ref, seg_ref, w_out_any, probe_any, query_out,
    kv_out, segs_out, part_out, log_out, grad_out, readout_out, state_v, w_v, query_buf, kv_buf,
    w_ref, joined, half, sending, state_own, probe_own, load_sem, w_sem, q_send, q_recv, kv_send,
    kv_recv, pass_send, seg_send, seg_recv, own_q, own_kv, line_send, line_recv, plane_send,
    plane_recv, beside_send, beside_recv, shard_send, shard_recv, shard_sem, out_send, out_recv,
    back_send, back_recv, own_sem, row_sem,
):
    ctx, me, group, core = place()
    rows, model = state_any.shape
    own, groups = rows // head_count, head_count // 2
    slots = w_any.shape[2] // HEAD_DIM
    chunk = 2 * own
    partner = group * 2 + 1 - core

    def at(piece):
        return pl.ds(pl.multiple_of(piece * chunk, chunk), chunk)

    def own_at(piece):
        return pl.ds(pl.multiple_of(piece * own, own), own)

    def load_state(piece):
        return pltpu.make_async_copy(
            state_any.at[at(piece)], state_v.at[at(piece)], load_sem.at[piece]
        )

    load_state(0).start()
    w_loads = [pltpu.make_async_copy(w_any.at[t], w_v.at[t], w_sem.at[t]) for t in range(3)]
    for copy in w_loads:
        copy.start()
    for piece in range(1, groups):
        load_state(piece).start()
    my_rows = own_at(me)
    shard = w_out_any.shape[0]
    part, quarter = shard // 2, shard // ctx_count
    later_loads = [
        pltpu.make_async_copy(state_any.at[my_rows], state_own, row_sem.at[0]),
        pltpu.make_async_copy(probe_any.at[my_rows], probe_own, row_sem.at[1]),
        pltpu.make_async_copy(
            w_out_any, w_ref.at[pl.ds(pl.multiple_of(me * shard, shard), shard)], shard_sem
        ),
    ]
    for copy in later_loads:
        copy.start()
    peers = [(lax.rem(ctx + step, ctx_count), partner) for step in range(ctx_count)]
    for far in range(groups):
        for step in range(ctx_count):
            if far or step:
                peers.append(
                    (lax.rem(ctx + step, ctx_count), lax.rem(group + far, groups) * 2 + core)
                )
    meet(peers)

    low, high = lax.rem(ctx, 2), ctx // 2
    which = lax.rem(low + high, 2)
    across, along = high * 2 + 1 - low, (1 - high) * 2 + low

    def shard_rows(origin, first, size):
        return pl.ds(pl.multiple_of((origin * 2 + core) * shard + first, size), size)

    def line_copy(way, origin, mine):
        here = shard_rows(origin, which * part, part)
        source = (
            w_out_any.at[pl.ds(pl.multiple_of(which * part, part), part)]
            if mine
            else w_ref.at[here]
        )
        other = group + 1 if way == 0 else group - 1
        return remote(
            source, w_ref.at[here], line_send.at[way, origin], line_recv.at[origin], ctx,
            other * 2 + core,
        )

    def plane_copy(axis, origin, kept):
        here = shard_rows(origin, kept * part + axis * quarter, quarter)
        return remote(
            w_ref.at[here], w_ref.at[here], plane_send.at[axis, origin],
            plane_recv.at[axis, origin], along if axis else across, me,
        )

    def beside_copy(kind, origin):
        here = shard_rows(origin, jnp.where(kind == 0, which, 1 - which) * part, part)
        return remote(
            w_ref.at[here], w_ref.at[here], beside_send.at[kind, origin],
            beside_recv.at[kind, origin], ctx, partner,
        )

    def shard_copy():
        return remote(
            w_out_any, w_ref.at[pl.ds(pl.multiple_of(me * shard, shard), shard)], shard_send,
            shard_recv, ctx, partner,
        )

    has_up, has_down = group < groups - 1, group > 0

    @pl.when(has_up)
    def _():
        line_copy(0, group, True).start()

    @pl.when(has_down)
    def _():
        line_copy(1, group, True).start()

    shard_copy().start()

    def each_origin(distance, work):
        for way in range(2):
            origin = group - distance if way == 0 else group + distance

            @pl.when(origin >= 0 if way == 0 else origin < groups)
            def _():
                work(way, origin)

    def line_arrived(distance):
        def work(way, origin):
            line_copy(way, origin, False).wait_recv()

            @pl.when(has_up if way == 0 else has_down)
            def _():
                line_copy(way, origin, False).start()

            for axis in range(2):
                plane_copy(axis, origin, which).start()
            beside_copy(0, origin).start()

        each_origin(distance, work)

    def plane_arrived(distance):
        def work(way, origin):
            for axis in range(2):
                plane_copy(axis, origin, 1 - which).wait_recv()
            beside_copy(1, origin).start()

        each_origin(distance, work)

    def weights_sent(distance):
        def work(way, origin):
            @pl.when(has_up if way == 0 else has_down)
            def _():
                line_copy(way, origin, False).wait_send()

            for axis in range(2):
                plane_copy(axis, origin, which).wait_send()
            for kind in range(2):
                beside_copy(kind, origin).wait_send()

        each_origin(distance, work)

    def beside_arrived(distance):
        def work(way, origin):
            for kind in range(2):
                beside_copy(kind, origin).wait_recv()

        each_origin(distance, work)

    segs = []
    for step in range(1, ctx_count):
        copy = remote(
            seg_ref, segs_out.at[ctx], seg_send.at[step], seg_recv.at[step],
            lax.rem(ctx + step, ctx_count), me,
        )
        copy.start()
        segs.append(copy)
    segs_out[ctx] = seg_ref[...]
    for copy in w_loads:
        copy.wait()
    gain = gain_ref[...].astype(jnp.float32)

    def away(slot, kind, piece, dest):
        head = group * 2 + kind
        return (
            remote(
                query_buf.at[slot, piece, kind], query_out.at[ctx, own_at(piece)],
                q_send.at[slot, kind, piece], q_recv.at[ctx, piece], dest, head,
            ),
            remote(
                kv_buf.at[slot, kind, piece], kv_out.at[kind, ctx, at(piece)],
                kv_send.at[slot, kind, piece], kv_recv.at[kind, ctx, piece], dest, head,
            ),
        )

    def beside(slot, piece):
        result = [
            remote(
                query_buf.at[slot, piece, 1 - core], query_out.at[ctx, own_at(piece)],
                q_send.at[slot, 1 - core, piece], q_recv.at[ctx, piece], ctx, partner,
            )
        ]
        for kind in range(2):
            result.append(
                remote(
                    kv_buf.at[slot, kind, piece], kv_out.at[kind, ctx, at(piece)],
                    kv_send.at[slot, kind, piece], kv_recv.at[kind, ctx, piece], ctx, partner,
                )
            )
        return result

    def project(piece, _):
        load_state(piece).wait()
        block = state_v[at(piece), :].astype(jnp.float32)
        normed = (block * row_scale(block) * gain).astype(jnp.bfloat16)
        for t in range(3):
            result = jnp.dot(normed, w_v[t], preferred_element_type=jnp.float32).astype(
                jnp.bfloat16
            )
            for slot in range(slots):
                cut = result[:, slot * HEAD_DIM : (slot + 1) * HEAD_DIM]
                if t == 0:
                    query_buf[slot, piece, 0] = cut[:own]
                    query_buf[slot, piece, 1] = cut[own:]
                else:
                    kv_buf[slot, t - 1, piece] = cut
        for slot in range(slots):
            dest = core * slots + slot

            @pl.when(dest != ctx)
            def _():
                for kind in range(2):
                    for copy in away(slot, kind, piece, dest):
                        copy.start()

            @pl.when(dest == ctx)
            def _():
                for copy in beside(slot, piece):
                    copy.start()
                query_out[ctx, own_at(piece), :] = query_buf[slot, piece, core]
                for kind in range(2):
                    kv_out[kind, ctx, at(piece), :] = kv_buf[slot, kind, piece]

        return 0

    lax.fori_loop(0, groups, project, 0)
    line_arrived(1)

    def hand_over(piece, step):
        source = lax.rem(ctx + step, ctx_count)
        return remote(
            kv_out.at[core, source, at(piece)], kv_out.at[core, source, at(piece)],
            pass_send.at[step, piece], kv_recv.at[core, source, piece], ctx, partner,
        )

    def forward(piece, _):
        for step in range(1, ctx_count):
            copy = hand_over(piece, step)
            copy.wait_recv()
            copy.start()
        return 0

    lax.fori_loop(0, groups, forward, 0)
    line_arrived(2)
    plane_arrived(1)

    def got_query(source, piece):
        remote(
            query_out.at[source, own_at(piece)], query_out.at[source, own_at(piece)],
            q_send.at[0, 0, piece], q_recv.at[source, piece], ctx, partner,
        ).wait_recv()

    def got_kv(kind, source, piece):
        remote(
            kv_out.at[kind, source, at(piece)], kv_out.at[kind, source, at(piece)],
            kv_send.at[0, 0, piece], kv_recv.at[kind, source, piece], ctx, partner,
        ).wait_recv()

    def gather(piece, _):
        for step in range(1, ctx_count):
            source = lax.rem(ctx + step, ctx_count)
            got_query(source, piece)
            got_kv(1 - core, source, piece)
            hand_over(piece, step).wait_send()

        @pl.when(ctx // slots != core)
        def _():
            got_query(ctx, piece)
            for kind in range(2):
                got_kv(kind, ctx, piece)

        return 0

    lax.fori_loop(0, groups, gather, 0)
    for copy in segs:
        copy.wait()

    def cols_of(group_at, ctx_at):
        head = group_at * ctx_count + ctx_at
        return pl.ds(pl.multiple_of(head * HEAD_DIM, HEAD_DIM), HEAD_DIM)

    factor = HEAD_DIM ** (-0.5) * LOG2E
    sub = groups * own
    seg_all = segs_out[...]

    def below(value):
        count = jnp.where(seg_all < value, 1.0, 0.0)
        for axis in (0, 1, 2):
            count = jnp.sum(count, axis=axis, keepdims=True)
        return count[0]

    first_bound, second_bound = below(1), below(2)
    lane = lax.broadcasted_iota(jnp.int32, (1, sub), 1)
    inside = (lane // own) * (2 * own) + core * own + lane % own
    key_row = lax.broadcasted_iota(jnp.int32, (rows, sub), 0)

    def out_copy(tile, order, other):
        return remote(
            part_out.at[tile, own_at(other)], joined.at[:, cols_of(group, ctx)],
            out_send.at[tile, order], out_recv.at[group, ctx], tile, other * 2 + core,
        )

    def one_tile(tile, _):
        query = query_out[tile]
        pos = (tile * rows + inside).astype(jnp.float32)
        start = jnp.where(
            pos >= second_bound, second_bound, jnp.where(pos >= first_bound, first_bound, 0.0)
        ).astype(jnp.int32)

        def step(diagonal, piece, carry):
            top, total, acc = carry
            scores = dot32(kv_out[0, piece], query, NT)
            allowed = key_row >= start - piece * rows
            if diagonal:
                allowed = allowed & (key_row <= inside)
            scores = jnp.where(allowed, scores, NEGATIVE)
            new_top = jnp.maximum(top, jnp.max(scores, axis=0, keepdims=True) * factor)
            weights = jnp.exp2(scores * factor - new_top)
            scale = jnp.exp2(top - new_top)
            total = total * scale + jnp.sum(weights, axis=0, keepdims=True)
            acc = acc * scale + dot32(kv_out[1, piece], weights.astype(jnp.bfloat16), TN)
            return new_top, total, acc

        carry = (
            jnp.full((1, sub), NEGATIVE, jnp.float32),
            jnp.zeros((1, sub), jnp.float32),
            jnp.zeros((HEAD_DIM, sub), jnp.float32),
        )
        carry = lax.fori_loop(0, tile, functools.partial(step, False), carry)
        top, total, acc = step(True, tile, carry)
        part_out[tile] = (acc / total).T.astype(jnp.bfloat16)
        log_out[tile] = top + jnp.log2(total)
        for order in range(groups):
            other = far_first(groups, group, order)
            if order == groups - 1:

                @pl.when(tile != ctx)
                def _():
                    out_copy(tile, order, other).start()

                @pl.when(tile == ctx)
                def _():
                    joined[:, cols_of(group, ctx)] = part_out[tile, own_at(group), :]

            else:
                out_copy(tile, order, other).start()

        for distance in range(3, groups):

            @pl.when(tile == distance - 1)
            def _():
                line_arrived(distance)
                plane_arrived(distance - 1)

        return 0

    lax.fori_loop(0, ctx_count, one_tile, 0)
    for distance in range(max(2, groups - 1), groups):
        plane_arrived(distance)
    for copy in later_loads:
        copy.wait()
    sources = []
    for far in range(groups):
        for step in range(ctx_count):
            if far or step:
                sources.append((lax.rem(group + far, groups), lax.rem(ctx + step, ctx_count)))
    for other, peer in sources:
        remote(
            part_out.at[0, own_at(0)], joined.at[:, cols_of(other, peer)], out_send.at[0, 0],
            out_recv.at[other, peer], peer, other * 2 + core,
        ).wait_recv()
    shard_copy().wait_recv()
    for distance in range(1, groups):
        beside_arrived(distance)
    tile = min(256, model)

    def layer(piece, carry):
        squares, products = carry
        cols = pl.ds(pl.multiple_of(piece * tile, tile), tile)
        layer = state_own[:, cols].astype(jnp.float32) + jnp.dot(
            joined[...], w_ref[:, cols], preferred_element_type=jnp.float32
        )
        readout_out[:, cols] = layer
        squares = squares + jnp.sum(layer * layer, axis=1, keepdims=True)
        products = products + jnp.sum(
            layer * probe_own[:, cols].astype(jnp.float32), axis=1, keepdims=True
        )
        return squares, products

    zero = jnp.zeros((own, 1), jnp.float32)
    squares, products = lax.fori_loop(0, model // tile, layer, (zero, zero))
    scale = lax.rsqrt(squares / model + EPSILON)
    bend = scale**3 * (products / model)

    def finish(piece, _):
        cols = pl.ds(pl.multiple_of(piece * tile, tile), tile)
        readout = scale * probe_own[:, cols].astype(jnp.float32) - readout_out[:, cols] * bend
        readout_out[:, cols] = readout
        half[:, cols] = readout.astype(jnp.bfloat16)
        return 0

    lax.fori_loop(0, model // tile, finish, 0)
    wide = ctx_count * HEAD_DIM
    copies = []
    for order in range(groups):
        other = far_first(groups, group, order)
        result = dot32(
            half[...], w_ref[pl.ds(pl.multiple_of(other * wide, wide), wide), :], NT
        ).astype(jnp.bfloat16)
        for index in range(ctx_count):
            sending[order, index] = result[:, index * HEAD_DIM : (index + 1) * HEAD_DIM]
        for step in range(ctx_count):
            peer = lax.rem(ctx + step, ctx_count)
            if order == groups - 1 and step == 0:
                continue
            copy = remote(
                sending.at[order, peer], grad_out.at[ctx, group], back_send.at[order, step],
                back_recv.at[ctx, group], peer, other * 2 + core,
            )
            copy.start()
            copies.append(copy)
    last = pltpu.make_async_copy(sending.at[groups - 1, ctx], grad_out.at[ctx, group], own_sem)
    last.start()

    def sent(piece, _):
        for slot in range(slots):
            dest = core * slots + slot

            @pl.when(dest != ctx)
            def _():
                for kind in range(2):
                    for copy in away(slot, kind, piece, dest):
                        copy.wait_send()

            @pl.when(dest == ctx)
            def _():
                for copy in beside(slot, piece):
                    copy.wait_send()

        return 0

    lax.fori_loop(0, groups, sent, 0)

    @pl.when(has_up)
    def _():
        line_copy(0, group, True).wait_send()

    @pl.when(has_down)
    def _():
        line_copy(1, group, True).wait_send()

    shard_copy().wait_send()
    for distance in range(1, groups):
        weights_sent(distance)

    def parts_sent(tile, _):
        for order in range(groups):
            other = far_first(groups, group, order)
            if order == groups - 1:

                @pl.when(tile != ctx)
                def _():
                    out_copy(tile, order, other).wait_send()

            else:
                out_copy(tile, order, other).wait_send()
        return 0

    lax.fori_loop(0, ctx_count, parts_sent, 0)
    for other, peer in sources:
        remote(
            sending.at[0, 0], grad_out.at[peer, other], back_send.at[0, 0],
            back_recv.at[peer, other], peer, other * 2 + core,
        ).wait_recv()
    for copy in copies:
        copy.wait_send()
    last.wait()


def front(ctx_count, head_count, state, w_qkv, gain, segment_ids, w_out, probe):
    rows, model = state.shape
    width = w_qkv.shape[2]
    own, groups, slots = rows // head_count, head_count // 2, width // HEAD_DIM
    seg = segment_ids.reshape(-1, 128)
    half, full, dma = jnp.bfloat16, jnp.float32, pltpu.SemaphoreType.DMA
    shape = jax.ShapeDtypeStruct
    return pl.pallas_call(
        functools.partial(front_kernel, ctx_count, head_count),
        out_shape=(
            shape((ctx_count, groups * own, HEAD_DIM), half),
            shape((2, ctx_count, rows, HEAD_DIM), half),
            shape((ctx_count,) + seg.shape, seg.dtype),
            shape((ctx_count, groups * own, HEAD_DIM), half),
            shape((ctx_count, 1, groups * own), full),
            shape((ctx_count, groups, own, HEAD_DIM), half),
            shape((own, model), full),
        ),
        in_specs=[ANY, ANY, VMEM, VMEM, ANY, ANY],
        out_specs=(VMEM, VMEM, VMEM, VMEM, VMEM, ANY, VMEM),
        scratch_shapes=[
            pltpu.VMEM((rows, model), half),
            pltpu.VMEM(w_qkv.shape, half),
            pltpu.VMEM((slots, groups, 2, own, HEAD_DIM), half),
            pltpu.VMEM((slots, 2, groups, 2 * own, HEAD_DIM), half),
            pltpu.VMEM((model, model), half),
            pltpu.VMEM((own, model), half),
            pltpu.VMEM((own, model), half),
            pltpu.VMEM((groups, ctx_count, own, HEAD_DIM), half),
            pltpu.VMEM((own, model), half),
            pltpu.VMEM((own, model), half),
            dma((groups,)),
            dma((3,)),
            dma((slots, 2, groups)),
            dma((ctx_count, groups)),
            dma((slots, 2, groups)),
            dma((2, ctx_count, groups)),
            dma((ctx_count, groups)),
            dma((ctx_count,)),
            dma((ctx_count,)),
            dma((groups,)),
            dma((2, groups)),
            dma((2, groups)),
            dma((groups,)),
            dma((2, groups)),
            dma((2, groups)),
            dma((2, groups)),
            dma((2, groups)),
            dma,
            dma,
            dma,
            dma((ctx_count, groups)),
            dma((groups, ctx_count)),
            dma((groups, ctx_count)),
            dma((ctx_count, groups)),
            dma,
            dma((2,)),
        ],
        compiler_params=pltpu.CompilerParams(
            collective_id=0, has_side_effects=True, vmem_limit_bytes=62 * 2**20
        ),
    )(state, w_qkv, gain, seg, w_out, probe)


def segment_bounds(segs_ref):
    segs = segs_ref[...]

    def below(value):
        return jnp.sum(jnp.where(segs < value, 1.0, 0.0)).astype(jnp.int32)

    return below(1), below(2)


def tile_plan(bounds, rows, own, parts, sub, bk, tile, core):
    first_bound, second_bound = bounds

    def start_of(pos):
        return jnp.where(pos >= second_bound, second_bound, jnp.where(pos >= first_bound, first_bound, 0))

    blocks = sub // own
    base = tile * rows + core * own
    places = []
    for part in range(parts):
        lane = lax.broadcasted_iota(jnp.int32, (1, sub), 1)
        pos = base + (lane // own + part * blocks) * (2 * own) + lane % own
        places.append((start_of(pos), pos))
    first, last = base, base + (parts * blocks - 1) * 2 * own + own - 1
    low = start_of(first) // bk
    inner_low = (start_of(last) + bk - 1) // bk
    inner_high = jnp.maximum(inner_low, (first + 1) // bk)
    high = last // bk + 1
    return places, low, inner_low, inner_high, high


def head_backward_kernel(
    rows, own, parts, sub, bk, segs_ref, query_ref, kv_ref, grad_ref, out_ref, log_ref, query_out,
    pair_out, pair_acc,
):
    score_scale = HEAD_DIM ** (-0.5)
    factor = score_scale * LOG2E
    core = lax.rem(lax.axis_index("head"), 2)
    bounds = segment_bounds(segs_ref)
    tiles = query_ref.shape[0] // (parts * sub)
    pair_rows = pair_acc.shape[0]

    def clear(piece, _):
        at = pl.ds(pl.multiple_of(piece * bk, bk), bk)
        pair_acc[at, :] = jnp.zeros((bk, 2 * HEAD_DIM), jnp.float32)
        return 0

    lax.fori_loop(0, pair_rows // bk, clear, 0)

    def one_tile(tile, _):
        places, low, inner_low, inner_high, high = tile_plan(
            bounds, rows, own, parts, sub, bk, tile, core
        )

        def at(part):
            return pl.ds(pl.multiple_of((tile * parts + part) * sub, sub), sub)

        deltas, logs = [], []
        for part in range(parts):
            product = grad_ref[at(part), :].astype(jnp.float32) * out_ref[at(part), :].astype(
                jnp.float32
            )
            deltas.append(jnp.sum(product.T, axis=0, keepdims=True))
            logs.append(log_ref[tile, pl.ds(part, 1), :])

        def step(masked, piece, carry):
            keys_at = pl.ds(pl.multiple_of(piece * bk, bk), bk)
            if masked:
                key_pos = piece * bk + lax.broadcasted_iota(jnp.int32, (bk, sub), 0)
            result = []
            key_block, value_block = kv_ref[0, keys_at, :], kv_ref[1, keys_at, :]
            for part in range(parts):
                query_block, grad_block = query_ref[at(part), :], grad_ref[at(part), :]
                scores = dot32(key_block, query_block, NT)
                probabilities = jnp.exp2(scores * factor - logs[part])
                if masked:
                    start, pos = places[part]
                    probabilities = jnp.where(
                        (key_pos >= start) & (key_pos <= pos), probabilities, 0.0
                    )
                dprobs = dot32(value_block, grad_block, NT)
                dscores = (probabilities * (dprobs - deltas[part])).astype(jnp.bfloat16)
                pair_acc[keys_at, HEAD_DIM:] += jnp.dot(
                    probabilities.astype(jnp.bfloat16),
                    grad_block,
                    preferred_element_type=jnp.float32,
                )
                pair_acc[keys_at, :HEAD_DIM] += jnp.dot(
                    dscores, query_block, preferred_element_type=jnp.float32
                )
                result.append(carry[part] + dot32(key_block, dscores, TN))
            return tuple(result)

        carry = tuple(jnp.zeros((HEAD_DIM, sub), jnp.float32) for _ in range(parts))
        carry = lax.fori_loop(low, inner_low, functools.partial(step, True), carry)
        carry = lax.fori_loop(inner_low, inner_high, functools.partial(step, False), carry)
        carry = lax.fori_loop(inner_high, high, functools.partial(step, True), carry)
        for part in range(parts):
            query_out[at(part), :] = (carry[part].T * score_scale).astype(jnp.bfloat16)
        return 0

    lax.fori_loop(0, tiles, one_tile, 0)

    def flush(piece, _):
        at = pl.ds(pl.multiple_of(piece * bk, bk), bk)
        pair_out[at, :HEAD_DIM] = (pair_acc[at, :HEAD_DIM] * score_scale).astype(jnp.bfloat16)
        pair_out[at, HEAD_DIM:] = pair_acc[at, HEAD_DIM:].astype(jnp.bfloat16)
        return 0

    lax.fori_loop(0, pair_rows // bk, flush, 0)


def finish_kernel(
    ctx_count, head_count, query_ref, pair_ref, w_any, state_any, noise_ref, readout_ref, gain_ref,
    new_out, w_both, beside, away, terms_in, partial, sending, total, state_own, b_send, b_recv,
    w_send, w_recv, a_send, a_recv, z_send, z_recv, own_sem,
):
    ctx, me, group, core = place()
    groups = head_count // 2
    own, model = new_out.shape
    slots = ctx_count // 2
    partner = group * 2 + 1 - core
    my_rows = pl.ds(pl.multiple_of(me * own, own), own)
    loads = [
        pltpu.make_async_copy(w_any, w_both.at[core], own_sem.at[0]),
        pltpu.make_async_copy(state_any.at[my_rows], state_own, own_sem.at[1]),
    ]
    for copy in loads:
        copy.start()
    peers = [(ctx, partner)]
    peers += [(lax.rem(ctx + step, ctx_count), me) for step in range(1, ctx_count)]
    peers += [(ctx, lax.rem(group + far, groups) * 2 + core) for far in range(1, groups)]
    meet(peers)
    dests = [far_first(groups, group, order) for order in range(groups)]
    copies = []
    for order, dest in enumerate(dests):
        copy = remote(
            pair_ref.at[:, dest, 1 - core], beside.at[order], b_send.at[order], b_recv.at[order],
            ctx, partner,
        )
        copy.start()
        copies.append(copy)
    w_copy = remote(w_any, w_both.at[core], w_send, w_recv, ctx, partner)
    w_copy.start()

    def stripe(source):
        slot = lax.rem(source, slots)
        return pl.ds(pl.multiple_of(slot * HEAD_DIM, HEAD_DIM), HEAD_DIM)

    def exchange(order, dest, step):
        peer = lax.rem(ctx + step, ctx_count)
        return remote(
            away.at[order, step], terms_in.at[dest, ctx // slots, :, :, stripe(ctx)],
            a_send.at[order, step], a_recv.at[dest, ctx], peer, me,
        )

    def arrived(dest, step):
        source = lax.rem(ctx + step, ctx_count)
        remote(
            away.at[0, 0], terms_in.at[dest, source // slots, :, :, stripe(source)],
            a_send.at[0, 0], a_recv.at[dest, source], source, me,
        ).wait_recv()

    for order, dest in enumerate(dests):
        copies[order].wait_recv()
        for step in range(1, ctx_count):
            peer = lax.rem(ctx + step, ctx_count)
            pair = pair_ref[peer, dest, core].astype(jnp.float32) + beside[order, peer].astype(
                jnp.float32
            )
            pair = pair.astype(jnp.bfloat16)
            away[order, step, 0] = query_ref[peer, dest]
            away[order, step, 1] = pair[:, :HEAD_DIM]
            away[order, step, 2] = pair[:, HEAD_DIM:]
            exchange(order, dest, step).start()
        pair = pair_ref[ctx, dest, core].astype(jnp.float32) + beside[order, ctx].astype(
            jnp.float32
        )
        pair = pair.astype(jnp.bfloat16)
        at = stripe(ctx)
        terms_in[dest, ctx // slots, 0, :, at] = query_ref[ctx, dest]
        terms_in[dest, ctx // slots, 1, :, at] = pair[:, :HEAD_DIM]
        terms_in[dest, ctx // slots, 2, :, at] = pair[:, HEAD_DIM:]
    for copy in loads:
        copy.wait()
    w_copy.wait()
    pieces = partial.shape[2]
    tile = model // pieces

    def chain(order, dest, piece):
        up = dest > group
        line = jnp.where(up, 0, 1)
        peer = jnp.where(up, group + 1, group - 1)
        return remote(
            sending.at[order, piece], partial.at[line, dest, piece], z_send.at[order, piece],
            z_recv.at[line, dest, piece], ctx, peer * 2 + core,
        )

    def came(line, dest, piece):
        remote(
            sending.at[0, piece], partial.at[line, dest, piece], z_send.at[0, piece],
            z_recv.at[line, dest, piece], ctx, partner,
        ).wait_recv()

    def term(dest, piece):
        cols = pl.ds(pl.multiple_of(piece * tile, tile), tile)
        result = None
        for half in range(2):
            for kind in range(3):
                part = dot32(terms_in[dest, half, kind], w_both[half, kind, cols, :], NT)
                result = part if result is None else result + part
        return result

    for order, dest in enumerate(dests[:-1]):
        for step in range(1, ctx_count):
            arrived(dest, step)
        line = jnp.where(dest > group, 0, 1)
        inner = (group > 0) & (group < groups - 1)

        def one_piece(piece, _):
            total[...] = term(dest, piece)

            @pl.when(inner)
            def _():
                came(line, dest, piece)
                total[...] += partial[line, dest, piece].astype(jnp.float32)

            sending[order, piece] = total[...].astype(jnp.bfloat16)
            chain(order, dest, piece).start()
            return 0

        lax.fori_loop(0, pieces, one_piece, 0)

    for step in range(1, ctx_count):
        arrived(group, step)

    state = state_own[...].astype(jnp.float32)
    inverse = row_scale(state)

    def last_piece(piece, slope):
        cols = pl.ds(pl.multiple_of(piece * tile, tile), tile)
        total[...] = term(group, piece)

        @pl.when(group > 0)
        def _():
            came(0, group, piece)
            total[...] += partial[0, group, piece].astype(jnp.float32)

        @pl.when(group < groups - 1)
        def _():
            came(1, group, piece)
            total[...] += partial[1, group, piece].astype(jnp.float32)

        gained = total[...] * gain_ref[:, cols].astype(jnp.float32)
        new_out[:, cols] = gained
        return slope + jnp.sum(
            gained * state_own[:, cols].astype(jnp.float32), axis=1, keepdims=True
        )

    slope = lax.fori_loop(0, pieces, last_piece, jnp.zeros((own, 1), jnp.float32))
    bend = inverse**3 * (slope / model)

    def update(piece, _):
        cols = pl.ds(pl.multiple_of(piece * tile, tile), tile)
        here = state_own[:, cols].astype(jnp.float32)
        gradient = readout_ref[:, cols] + inverse * new_out[:, cols] - here * bend
        new_out[:, cols] = (
            here - STEP_SIZE * gradient + NOISE_SCALE * noise_ref[:, cols].astype(jnp.float32)
        )
        return 0

    lax.fori_loop(0, pieces, update, 0)
    for order, dest in enumerate(dests):
        copies[order].wait_send()
        for step in range(1, ctx_count):
            exchange(order, dest, step).wait_send()
        if order < groups - 1:
            for piece in range(pieces):
                chain(order, dest, piece).wait_send()


def finish_step(ctx_count, head_count, query_grad, pair, w_qkv, state, noise, readout, gain):
    own, model = readout.shape
    width = w_qkv.shape[2]
    groups, pieces = head_count // 2, 4
    half, full, dma = jnp.bfloat16, jnp.float32, pltpu.SemaphoreType.DMA
    tile = model // pieces
    return pl.pallas_call(
        functools.partial(finish_kernel, ctx_count, head_count),
        out_shape=jax.ShapeDtypeStruct((own, model), full),
        in_specs=[VMEM, VMEM, ANY, ANY, VMEM, VMEM, VMEM],
        out_specs=VMEM,
        scratch_shapes=[
            pltpu.VMEM((2,) + w_qkv.shape, half),
            pltpu.VMEM((groups, ctx_count, own, 2 * HEAD_DIM), half),
            pltpu.VMEM((groups, ctx_count, 3, own, HEAD_DIM), half),
            pltpu.VMEM((groups, 2, 3, own, width), half),
            pltpu.VMEM((2, groups, pieces, own, tile), half),
            pltpu.VMEM((groups, pieces, own, tile), half),
            pltpu.VMEM((own, tile), full),
            pltpu.VMEM((own, model), half),
            dma((groups,)),
            dma((groups,)),
            dma,
            dma,
            dma((groups, ctx_count)),
            dma((groups, ctx_count)),
            dma((groups, pieces)),
            dma((2, groups, pieces)),
            dma((2,)),
        ],
        compiler_params=pltpu.CompilerParams(
            collective_id=2, has_side_effects=True, vmem_limit_bytes=60 * 2**20
        ),
    )(query_grad, pair, w_qkv, state, noise, readout, gain)


def heads_body(state, norm_gain, w_qkv, w_out, probe, noise, segment_ids):
    rows, model = state.shape
    head_count, ctx_count = lax.axis_size("head"), lax.axis_size("ctx")
    own, groups = rows // head_count, head_count // 2
    gain = norm_gain.reshape(1, model)
    queries, kv, segs, outputs, logs, grads_out, readout = front(
        ctx_count, head_count, state, w_qkv, gain, segment_ids, w_out, probe
    )
    mine, total = ctx_count * groups * own, ctx_count * rows
    parts, sub, bk = 1, groups * own, min(rows, 512)
    query_grad, pair = pl.pallas_call(
        functools.partial(head_backward_kernel, rows, own, parts, sub, bk),
        out_shape=(
            jax.ShapeDtypeStruct((mine, HEAD_DIM), jnp.bfloat16),
            jax.ShapeDtypeStruct((total, 2 * HEAD_DIM), jnp.bfloat16),
        ),
        in_specs=[VMEM] * 6,
        out_specs=(VMEM, VMEM),
        scratch_shapes=[pltpu.VMEM((total, 2 * HEAD_DIM), jnp.float32)],
        compiler_params=pltpu.CompilerParams(vmem_limit_bytes=60 * 2**20),
        cost_estimate=pl.CostEstimate(
            flops=10 * mine * total * HEAD_DIM, bytes_accessed=0, transcendentals=0
        ),
    )(
        segs, queries.reshape(mine, HEAD_DIM), kv.reshape(2, total, HEAD_DIM),
        grads_out.reshape(mine, HEAD_DIM), outputs.reshape(mine, HEAD_DIM), logs,
    )
    return finish_step(
        ctx_count, head_count, query_grad.reshape(ctx_count, groups, own, HEAD_DIM),
        pair.reshape(ctx_count, groups, 2, own, 2 * HEAD_DIM), w_qkv, state, noise, readout, gain,
    )


def solution(mesh):
    placed = (
        P("ctx", None),
        P(),
        P(None, None, "head"),
        P("head", None),
        P("ctx", None),
        P(("ctx", "head"), None),
        P("ctx"),
    )

    def step(*args):
        heads = args[2].shape[2] // HEAD_DIM
        return (heads_body if lax.axis_size("ctx") == 2 * heads == 4 else body)(*args)

    return jax.shard_map(
        step, mesh=mesh, in_specs=placed, out_specs=P(("ctx", "head"), None), check_vma=False
    )
```

```python
import functools

import jax
import jax.numpy as jnp
from jax import lax
from jax.experimental import pallas as pl
from jax.experimental.pallas import tpu as pltpu
from jax.sharding import PartitionSpec as P

HEAD_DIM = 128
EPSILON = 1e-05
STEP_SIZE = 0.25
NOISE_SCALE = (2.0 * STEP_SIZE) ** 0.5
NEGATIVE = -1e30
LOG2E = 1.4426950408889634
MESH = pl.DeviceIdType.MESH
VMEM = pl.BlockSpec(memory_space=pltpu.VMEM)
ANY = pl.BlockSpec(memory_space=pl.ANY)
NT = (((1,), (1,)), ((), ()))
TN = (((0,), (0,)), ((), ()))
FORWARD_BLOCKS = (512, 512)
BACKWARD_BLOCKS = (512, 512)


def row_scale(matrix):
    return lax.rsqrt(jnp.mean(matrix * matrix, axis=-1, keepdims=True) + EPSILON)


def dot32(left, right, dims):
    return lax.dot_general(left, right, dims, preferred_element_type=jnp.float32)


def greet(axis, number, me):
    barrier = pltpu.get_barrier_semaphore()
    for step in range(1, number):
        pl.semaphore_signal(
            barrier, inc=1, device_id={axis: lax.rem(me + step, number)}, device_id_type=MESH
        )
    pl.semaphore_wait(barrier, number - 1)


def gather_kernel(
    number, key_ref, value_ref, seg_ref, normed_ref, w_ref, keys, values, segs, query_out, send_sem,
    recv_sem, own_sem,
):
    me = lax.axis_index("ctx")
    rows = key_ref.shape[0]
    greet("ctx", number, me)

    def place(index):
        return pl.ds(pl.multiple_of(index * rows, rows), rows)

    def send(slot, source, target, peer):
        copy = pltpu.make_async_remote_copy(
            src_ref=source,
            dst_ref=target,
            send_sem=send_sem.at[slot],
            recv_sem=recv_sem.at[slot],
            device_id={"ctx": peer},
            device_id_type=MESH,
        )
        copy.start()
        return copy

    mine = place(me)
    copies = []
    for step in range(1, number):
        copies.append(send(step, seg_ref, segs.at[me], lax.rem(me + step, number)))
    relay = number == 4
    if relay:
        low, high = lax.rem(me, 2), me // 2
        across, along = high * 2 + 1 - low, (1 - high) * 2 + low
        key_first = send(number, key_ref, keys.at[mine], across)
        value_first = send(number + 1, value_ref, values.at[mine], along)
        copies.append(send(number + 2, value_ref, values.at[mine], across))
        copies.append(send(number + 3, key_ref, keys.at[mine], along))
    else:
        for step in range(1, number):
            peer = lax.rem(me + step, number)
            copies.append(send(number + 2 * step, key_ref, keys.at[mine], peer))
            copies.append(send(number + 2 * step + 1, value_ref, values.at[mine], peer))
    pairs = ((key_ref, keys.at[mine]), (value_ref, values.at[mine]), (seg_ref, segs.at[me]))
    for index, (source, target) in enumerate(pairs):
        copy = pltpu.make_async_copy(source, target, own_sem.at[index])
        copy.start()
        copies.append(copy)
    tile = min(256, rows)

    def project(piece, _):
        at = pl.ds(pl.multiple_of(piece * tile, tile), tile)
        query_out[at, :] = jnp.dot(
            normed_ref[at, :], w_ref[...], preferred_element_type=jnp.float32
        ).astype(jnp.bfloat16)
        return 0

    lax.fori_loop(0, rows // tile, project, 0)
    if relay:
        key_first.wait()
        copies.append(send(number + 4, keys.at[place(across)], keys.at[place(across)], along))
        value_first.wait()
        copies.append(send(number + 5, values.at[place(along)], values.at[place(along)], across))
    for copy in copies:
        copy.wait()


def gather_keys(number, key_rows, value_rows, segment_ids, normed, w_query):
    rows, width = key_rows.shape
    seg = segment_ids.reshape(-1, 128)
    full = jax.ShapeDtypeStruct((number * rows, width), key_rows.dtype)
    keys, values, segs, queries = pl.pallas_call(
        functools.partial(gather_kernel, number),
        out_shape=(
            full,
            full,
            jax.ShapeDtypeStruct((number,) + seg.shape, seg.dtype),
            jax.ShapeDtypeStruct((rows, width), key_rows.dtype),
        ),
        in_specs=[VMEM] * 5,
        out_specs=(ANY, ANY, ANY, VMEM),
        scratch_shapes=[
            pltpu.SemaphoreType.DMA((3 * number + 6,)),
            pltpu.SemaphoreType.DMA((3 * number + 6,)),
            pltpu.SemaphoreType.DMA((3,)),
        ],
        compiler_params=pltpu.CompilerParams(collective_id=0, has_side_effects=True),
    )(key_rows, value_rows, seg, normed, w_query)
    return keys, values, segs.reshape(-1), queries


def block_ranges(table, index):
    return [table[index, column] for column in range(4)]


def forward_kernel(
    heads, bq, bk, table, query_ref, key_ref, value_ref, start_ref, pos_ref, out_ref, log_ref
):
    factor = HEAD_DIM ** (-0.5) * LOG2E
    blocks = query_ref.shape[0] // bq

    def one_block(index, _):
        low, inner_low, inner_high, high = block_ranges(table, index)
        rows = pl.ds(pl.multiple_of(index * bq, bq), bq)
        start, pos = start_ref[index], pos_ref[index]

        def step(masked, piece, carry):
            keys_at = pl.ds(pl.multiple_of(piece * bk, bk), bk)
            if masked:
                key_pos = piece * bk + lax.broadcasted_iota(jnp.int32, (bk, bq), 0)
                allowed = (key_pos >= start) & (key_pos <= pos)
            result = []
            for head in range(heads):
                top, total, acc = carry[head]
                cols = pl.ds(head * HEAD_DIM, HEAD_DIM)
                scores = dot32(key_ref[keys_at, cols], query_ref[rows, cols], NT)
                if masked:
                    scores = jnp.where(allowed, scores, NEGATIVE)
                new_top = jnp.maximum(top, jnp.max(scores, axis=0, keepdims=True) * factor)
                weights = jnp.exp2(scores * factor - new_top)
                scale = jnp.exp2(top - new_top)
                total = total * scale + jnp.sum(weights, axis=0, keepdims=True)
                acc = acc * scale + dot32(
                    value_ref[keys_at, cols], weights.astype(jnp.bfloat16), TN
                )
                result.append((new_top, total, acc))
            return tuple(result)

        carry = tuple(
            (
                jnp.full((1, bq), NEGATIVE, jnp.float32),
                jnp.zeros((1, bq), jnp.float32),
                jnp.zeros((HEAD_DIM, bq), jnp.float32),
            )
            for _ in range(heads)
        )
        carry = lax.fori_loop(low, inner_low, functools.partial(step, True), carry)
        carry = lax.fori_loop(inner_low, inner_high, functools.partial(step, False), carry)
        carry = lax.fori_loop(inner_high, high, functools.partial(step, True), carry)
        for head in range(heads):
            top, total, acc = carry[head]
            out_ref[rows, pl.ds(head * HEAD_DIM, HEAD_DIM)] = (acc / total).T.astype(jnp.bfloat16)
            log_ref[index, pl.ds(head, 1), :] = top + jnp.log2(total)
        return 0

    lax.fori_loop(0, blocks, one_block, 0)


def backward_kernel(
    heads, bq, bk, table, query_ref, key_ref, value_ref, grad_ref, out_ref, log_ref, start_ref,
    pos_ref, query_out, pair_out, pair_acc,
):
    score_scale = HEAD_DIM ** (-0.5)
    factor = score_scale * LOG2E
    blocks = query_ref.shape[0] // bq
    width = heads * HEAD_DIM
    pair_rows = pair_acc.shape[0]

    def clear(piece, _):
        at = pl.ds(pl.multiple_of(piece * bk, bk), bk)
        pair_acc[at, :] = jnp.zeros((bk, 2 * width), jnp.float32)
        return 0

    lax.fori_loop(0, pair_rows // bk, clear, 0)

    def one_block(index, _):
        low, inner_low, inner_high, high = block_ranges(table, index)
        rows = pl.ds(pl.multiple_of(index * bq, bq), bq)
        start, pos = start_ref[index], pos_ref[index]
        deltas, logs = [], []
        for head in range(heads):
            cols = pl.ds(head * HEAD_DIM, HEAD_DIM)
            product = grad_ref[rows, cols].astype(jnp.float32) * out_ref[rows, cols].astype(
                jnp.float32
            )
            deltas.append(jnp.sum(product.T, axis=0, keepdims=True))
            logs.append(log_ref[index, pl.ds(head, 1), :])

        def step(masked, piece, carry):
            keys_at = pl.ds(pl.multiple_of(piece * bk, bk), bk)
            if masked:
                key_pos = piece * bk + lax.broadcasted_iota(jnp.int32, (bk, bq), 0)
                allowed = (key_pos >= start) & (key_pos <= pos)
            result = []
            for head in range(heads):
                cols = pl.ds(head * HEAD_DIM, HEAD_DIM)
                value_cols = pl.ds(width + head * HEAD_DIM, HEAD_DIM)
                key_block, query_block = key_ref[keys_at, cols], query_ref[rows, cols]
                grad_block = grad_ref[rows, cols]
                scores = dot32(key_block, query_block, NT)
                probabilities = jnp.exp2(scores * factor - logs[head])
                if masked:
                    probabilities = jnp.where(allowed, probabilities, 0.0)
                dprobs = dot32(value_ref[keys_at, cols], grad_block, NT)
                dscores = (probabilities * (dprobs - deltas[head])).astype(jnp.bfloat16)
                pair_acc[keys_at, value_cols] += jnp.dot(
                    probabilities.astype(jnp.bfloat16),
                    grad_block,
                    preferred_element_type=jnp.float32,
                )
                pair_acc[keys_at, cols] += jnp.dot(
                    dscores, query_block, preferred_element_type=jnp.float32
                )
                result.append(carry[head] + dot32(key_block, dscores, TN))
            return tuple(result)

        carry = tuple(jnp.zeros((HEAD_DIM, bq), jnp.float32) for _ in range(heads))
        carry = lax.fori_loop(low, inner_low, functools.partial(step, True), carry)
        carry = lax.fori_loop(inner_low, inner_high, functools.partial(step, False), carry)
        carry = lax.fori_loop(inner_high, high, functools.partial(step, True), carry)
        for head in range(heads):
            query_out[rows, pl.ds(head * HEAD_DIM, HEAD_DIM)] = (
                carry[head].T * score_scale
            ).astype(jnp.bfloat16)
        return 0

    lax.fori_loop(0, blocks, one_block, 0)

    def flush(piece, _):
        at = pl.ds(pl.multiple_of(piece * bk, bk), bk)
        pair_out[at, :width] = (pair_acc[at, :width] * score_scale).astype(jnp.bfloat16)
        pair_out[at, width:] = pair_acc[at, width:].astype(jnp.bfloat16)
        return 0

    lax.fori_loop(0, pair_rows // bk, flush, 0)


def make_table(start, pos, bq, bk):
    starts, places = start.reshape(-1, bq), pos.reshape(-1, bq)
    low = starts[:, 0] // bk
    inner_low = (starts[:, -1] + bk - 1) // bk
    inner_high = jnp.maximum(inner_low, (places[:, 0] + 1) // bk)
    high = places[:, -1] // bk + 1
    return jnp.stack([low, inner_low, inner_high, high], axis=1).astype(jnp.int32)


def middle_kernel(
    number, part_ref, w_any, state_ref, probe_ref, grad_out, readout_out, w_ref, joined, half,
    sending, landing, send_sem, recv_sem, back_send, back_recv, w_sem,
):
    me = lax.axis_index("head")
    width = part_ref.shape[1]
    own = state_ref.shape[0]
    model = state_ref.shape[1]
    w_copy = pltpu.make_async_copy(w_any, w_ref, w_sem)
    w_copy.start()
    greet("head", number, me)
    my_cols = pl.ds(pl.multiple_of(me * width, width), width)
    my_rows = pl.ds(pl.multiple_of(me * own, own), own)
    copies = []
    for step in range(1, number):
        peer = lax.rem(me + step, number)
        copy = pltpu.make_async_remote_copy(
            src_ref=part_ref.at[pl.ds(pl.multiple_of(peer * own, own), own)],
            dst_ref=joined.at[:, my_cols],
            send_sem=send_sem.at[step],
            recv_sem=recv_sem.at[step],
            device_id={"head": peer},
            device_id_type=MESH,
        )
        copy.start()
        copies.append(copy)
    joined[:, my_cols] = part_ref[my_rows, :]
    w_copy.wait()
    for copy in copies:
        copy.wait()

    tile = min(256, model)

    def project(piece, carry):
        squares, products = carry
        cols = pl.ds(pl.multiple_of(piece * tile, tile), tile)
        layer = state_ref[:, cols].astype(jnp.float32) + jnp.dot(
            joined[...], w_ref[:, cols], preferred_element_type=jnp.float32
        )
        readout_out[:, cols] = layer
        squares = squares + jnp.sum(layer * layer, axis=1, keepdims=True)
        products = products + jnp.sum(
            layer * probe_ref[:, cols].astype(jnp.float32), axis=1, keepdims=True
        )
        return squares, products

    zero = jnp.zeros((own, 1), jnp.float32)
    squares, products = lax.fori_loop(0, model // tile, project, (zero, zero))
    scale = lax.rsqrt(squares / model + EPSILON)
    bend = scale**3 * (products / model)

    def finish(piece, _):
        cols = pl.ds(pl.multiple_of(piece * tile, tile), tile)
        readout = scale * probe_ref[:, cols].astype(jnp.float32) - readout_out[:, cols] * bend
        readout_out[:, cols] = readout
        half[:, cols] = readout.astype(jnp.bfloat16)
        return 0

    lax.fori_loop(0, model // tile, finish, 0)
    copies = []
    for step in range(1, number):
        peer = lax.rem(me + step, number)
        sending[step] = dot32(
            half[...], w_ref[pl.ds(pl.multiple_of(peer * width, width), width), :], NT
        ).astype(jnp.bfloat16)
        copy = pltpu.make_async_remote_copy(
            src_ref=sending.at[step],
            dst_ref=landing.at[my_rows],
            send_sem=back_send.at[step],
            recv_sem=back_recv.at[step],
            device_id={"head": peer},
            device_id_type=MESH,
        )
        copy.start()
        copies.append(copy)
    landing[my_rows, :] = dot32(half[...], w_ref[my_cols, :], NT).astype(jnp.bfloat16)
    for copy in copies:
        copy.wait()
    grad_out[...] = landing[...]


def middle(number, part, w_full, state_own, probe_own):
    rows, width = part.shape
    own, model = state_own.shape
    return pl.pallas_call(
        functools.partial(middle_kernel, number),
        out_shape=(
            jax.ShapeDtypeStruct((rows, width), jnp.bfloat16),
            jax.ShapeDtypeStruct((own, model), jnp.float32),
        ),
        in_specs=[VMEM, ANY, VMEM, VMEM],
        out_specs=(VMEM, VMEM),
        scratch_shapes=[
            pltpu.VMEM(w_full.shape, jnp.bfloat16),
            pltpu.VMEM((own, number * width), jnp.bfloat16),
            pltpu.VMEM((own, model), jnp.bfloat16),
            pltpu.VMEM((number, own, width), jnp.bfloat16),
            pltpu.VMEM((rows, width), jnp.bfloat16),
            pltpu.SemaphoreType.DMA((number,)),
            pltpu.SemaphoreType.DMA((number,)),
            pltpu.SemaphoreType.DMA((number,)),
            pltpu.SemaphoreType.DMA((number,)),
            pltpu.SemaphoreType.DMA,
        ],
        compiler_params=pltpu.CompilerParams(
            collective_id=1, has_side_effects=True, vmem_limit_bytes=60 * 2**20
        ),
    )(part, w_full, state_own, probe_own)


def tail_kernel(
    ctx_count, number, pair_any, query_ref, w_ref, sum_out, own_pair, arriving, gathered, terms,
    from_partner, reduced, landing, ctx_send, ctx_recv, p_send, p_recv, z_send, z_recv, own_sem,
):
    ctx, me = lax.axis_index("ctx"), lax.axis_index("head")
    groups = number // 2
    group, core = me // 2, lax.rem(me, 2)
    partner = group * 2 + 1 - core
    rows, width = query_ref.shape
    own, model = sum_out.shape
    chunk = 2 * own
    own_copy = pltpu.make_async_copy(
        pair_any.at[pl.ds(pl.multiple_of(ctx * rows, rows), rows)], own_pair, own_sem
    )
    own_copy.start()
    barrier = pltpu.get_barrier_semaphore()
    peers = [{"ctx": lax.rem(ctx + step, ctx_count)} for step in range(1, ctx_count)]
    peers.append({"head": partner})
    for step in range(1, groups):
        peers.append({"head": lax.rem(group + step, groups) * 2 + core})
    for peer in peers:
        pl.semaphore_signal(barrier, inc=1, device_id=peer, device_id_type=MESH)
    pl.semaphore_wait(barrier, len(peers))

    def chunk_start(order):
        dest = lax.rem(group + order + 1, groups)
        return dest, pl.multiple_of(dest * chunk, chunk)

    def ctx_copy(order, step):
        target = lax.rem(ctx - step + ctx_count, ctx_count)
        _, first = chunk_start(order)
        return pltpu.make_async_remote_copy(
            src_ref=pair_any.at[pl.ds(pl.multiple_of(target * rows + first, chunk), chunk)],
            dst_ref=arriving.at[order, step - 1],
            send_sem=ctx_send.at[order, step],
            recv_sem=ctx_recv.at[order, step],
            device_id={"ctx": target},
            device_id_type=MESH,
        )

    for order in range(groups):
        for step in range(1, ctx_count):

            @pl.when(step <= ctx)
            def _():
                ctx_copy(order, step).start()

    own_copy.wait()
    tile = min(512, model)
    mine = pl.ds(pl.multiple_of(core * own, own), own)
    theirs = pl.ds(pl.multiple_of((1 - core) * own, own), own)
    waiting = []
    for order in range(groups):
        dest, first = chunk_start(order)
        at = pl.ds(first, chunk)
        gathered[...] = own_pair[at, :].astype(jnp.float32)
        for step in range(1, ctx_count):

            @pl.when(ctx + step < ctx_count)
            def _():
                ctx_copy(order, step).wait_recv()
                gathered[...] += arriving[order, step - 1].astype(jnp.float32)

        def multiply(piece, _):
            cols = pl.ds(pl.multiple_of(piece * tile, tile), tile)
            term = dot32(query_ref[at, :], w_ref[0, cols, :], NT)
            term += dot32(gathered[:, :width].astype(jnp.bfloat16), w_ref[1, cols, :], NT)
            term += dot32(gathered[:, width:].astype(jnp.bfloat16), w_ref[2, cols, :], NT)
            terms[order, :, cols] = term.astype(jnp.bfloat16)
            return 0

        lax.fori_loop(0, model // tile, multiply, 0)
        copy = pltpu.make_async_remote_copy(
            src_ref=terms.at[order, theirs],
            dst_ref=from_partner.at[order],
            send_sem=p_send.at[order],
            recv_sem=p_recv.at[order],
            device_id={"head": partner},
            device_id_type=MESH,
        )
        copy.start()
        copy.wait()
        both = terms[order, mine, :].astype(jnp.float32) + from_partner[order].astype(jnp.float32)
        if order < groups - 1:
            reduced[order] = both.astype(jnp.bfloat16)
            copy = pltpu.make_async_remote_copy(
                src_ref=reduced.at[order],
                dst_ref=landing.at[order],
                send_sem=z_send.at[order],
                recv_sem=z_recv.at[order],
                device_id={"head": dest * 2 + core},
                device_id_type=MESH,
            )
            copy.start()
            waiting.append(copy)
        else:
            sum_out[...] = both
    for order, copy in enumerate(waiting):
        copy.wait()
        sum_out[...] += landing[order].astype(jnp.float32)
    for order in range(groups):
        for step in range(1, ctx_count):

            @pl.when(step <= ctx)
            def _():
                ctx_copy(order, step).wait_send()


def tail(ctx_count, number, pair, query_grad, w_qkv):
    rows, width = query_grad.shape
    model = w_qkv.shape[1]
    own, groups = rows // number, number // 2
    half, full = jnp.bfloat16, jnp.float32
    dma = pltpu.SemaphoreType.DMA
    return pl.pallas_call(
        functools.partial(tail_kernel, ctx_count, number),
        out_shape=jax.ShapeDtypeStruct((own, model), full),
        in_specs=[ANY, VMEM, VMEM],
        out_specs=VMEM,
        scratch_shapes=[
            pltpu.VMEM((rows, 2 * width), half),
            pltpu.VMEM((groups, ctx_count - 1, 2 * own, 2 * width), half),
            pltpu.VMEM((2 * own, 2 * width), full),
            pltpu.VMEM((groups, 2 * own, model), half),
            pltpu.VMEM((groups, own, model), half),
            pltpu.VMEM((groups, own, model), half),
            pltpu.VMEM((groups, own, model), half),
            dma((groups, ctx_count)),
            dma((groups, ctx_count)),
            dma((groups,)),
            dma((groups,)),
            dma((groups,)),
            dma((groups,)),
            dma,
        ],
        compiler_params=pltpu.CompilerParams(
            collective_id=2, has_side_effects=True, vmem_limit_bytes=60 * 2**20
        ),
    )(pair, query_grad, w_qkv)


def body(state, norm_gain, w_qkv, w_out, probe, noise, segment_ids):
    local_rows, model_width = state.shape
    width = w_qkv.shape[2]
    local_heads = width // HEAD_DIM
    head_count = lax.axis_size("head")
    ctx_count = lax.axis_size("ctx")
    ctx_index = lax.axis_index("ctx")
    own_rows = local_rows // head_count
    row_start = lax.axis_index("head") * own_rows
    w_full = lax.all_gather(w_out, "head", axis=0, tiled=True)
    state_f = state.astype(jnp.float32)
    gain_full = norm_gain.astype(jnp.float32)
    inverse = row_scale(state_f)
    normed = (state_f * inverse * gain_full).astype(jnp.bfloat16)

    def project(index):
        return jnp.dot(normed, w_qkv[index], preferred_element_type=jnp.float32).astype(
            jnp.bfloat16
        )

    key_rows, value_rows = project(1), project(2)
    keys, values, segs, query_rows = gather_keys(
        ctx_count, key_rows, value_rows, segment_ids, normed, w_qkv[0]
    )
    total_rows = keys.shape[0]
    pos = ctx_index * local_rows + jnp.arange(local_rows, dtype=jnp.int32)
    start = jnp.sum((segs[None, :] < segment_ids[:, None]).astype(jnp.int32), axis=1)
    fq, fk = (min(local_rows, size) for size in FORWARD_BLOCKS)
    gq, gk = (min(local_rows, size) for size in BACKWARD_BLOCKS)
    smem = pl.BlockSpec(memory_space=pltpu.SMEM)
    params = pltpu.CompilerParams(vmem_limit_bytes=60 * 2**20)
    outputs, logs = pl.pallas_call(
        functools.partial(forward_kernel, local_heads, fq, fk),
        out_shape=(
            jax.ShapeDtypeStruct((local_rows, width), jnp.bfloat16),
            jax.ShapeDtypeStruct((local_rows // fq, local_heads, fq), jnp.float32),
        ),
        in_specs=[smem] + [VMEM] * 5,
        out_specs=(VMEM, VMEM),
        compiler_params=params,
        cost_estimate=pl.CostEstimate(
            flops=4 * local_rows * total_rows * width, bytes_accessed=0, transcendentals=0
        ),
    )(
        make_table(start, pos, fq, fk),
        query_rows,
        keys,
        values,
        start.reshape(-1, 1, fq),
        pos.reshape(-1, 1, fq),
    )
    state_half = lax.dynamic_slice_in_dim(state, row_start, own_rows, 0)
    probe_own = lax.dynamic_slice_in_dim(probe, row_start, own_rows, 0)
    state_own = state_half.astype(jnp.float32)
    inverse_own = row_scale(state_own)
    grads_out, readout_own = middle(head_count, outputs, w_full, state_half, probe_own)
    query_grad, pair = pl.pallas_call(
        functools.partial(backward_kernel, local_heads, gq, gk),
        out_shape=(
            jax.ShapeDtypeStruct((local_rows, width), jnp.bfloat16),
            jax.ShapeDtypeStruct((total_rows, 2 * width), jnp.bfloat16),
        ),
        in_specs=[smem] + [VMEM] * 8,
        out_specs=(VMEM, VMEM),
        scratch_shapes=[pltpu.VMEM((total_rows, 2 * width), jnp.float32)],
        compiler_params=params,
        cost_estimate=pl.CostEstimate(
            flops=10 * local_rows * total_rows * width, bytes_accessed=0, transcendentals=0
        ),
    )(
        make_table(start, pos, gq, gk),
        query_rows,
        keys,
        values,
        grads_out,
        outputs,
        logs.reshape(local_rows // fq, local_heads, fq),
        start.reshape(-1, 1, gq),
        pos.reshape(-1, 1, gq),
    )
    normed_grad = tail(ctx_count, head_count, pair, query_grad, w_qkv)
    gain_grad = normed_grad * gain_full
    gradient = (
        readout_own
        + inverse_own * gain_grad
        - state_own * inverse_own**3 * jnp.mean(gain_grad * state_own, axis=-1, keepdims=True)
    )
    return state_own - STEP_SIZE * gradient + jnp.sqrt(2.0 * STEP_SIZE) * noise.astype(jnp.float32)


def remote(source, target, send_sem, recv_sem, ctx, head):
    return pltpu.make_async_remote_copy(
        src_ref=source,
        dst_ref=target,
        send_sem=send_sem,
        recv_sem=recv_sem,
        device_id={"ctx": ctx, "head": head},
        device_id_type=MESH,
    )


def place():
    ctx, me = lax.axis_index("ctx"), lax.axis_index("head")
    return ctx, me, me // 2, lax.rem(me, 2)


def announce(peers):
    barrier = pltpu.get_barrier_semaphore()
    for ctx, head in peers:
        pl.semaphore_signal(
            barrier, inc=1, device_id={"ctx": ctx, "head": head}, device_id_type=MESH
        )


def await_all(peers):
    pl.semaphore_wait(pltpu.get_barrier_semaphore(), len(peers))


def meet(peers):
    announce(peers)
    await_all(peers)


def far_first(groups, group, step):
    result = 0
    for index in range(groups):
        order = sorted(range(groups), key=lambda other: (-abs(other - index), -other))
        result = jnp.where(group == index, order[step], result)
    return result


def front_kernel(
    ctx_count, head_count, state_any, w_any, gain_ref, seg_ref, w_out_any, probe_any, query_any,
    kv_any, segs_out, part_any, log_out, grad_out, readout_any, w_pair, state_v, w_v, query_buf,
    kv_buf, w_ref, joined, half, sending, state_own, probe_own, query_out, kv_out, part_out,
    readout_out, load_sem, w_sem, q_send, q_recv, kv_send, kv_recv, pass_send, seg_send, seg_recv,
    line_send, line_recv, plane_send, plane_recv, beside_send, beside_recv, shard_send, shard_recv,
    shard_sem, out_send, out_recv, back_send, back_recv, own_sem, row_sem, pair_send, pair_recv,
    leave_sem,
):
    ctx, me, group, core = place()
    rows, model = state_any.shape
    own, groups = rows // head_count, head_count // 2
    slots = w_any.shape[2] // HEAD_DIM
    chunk = 2 * own
    partner = group * 2 + 1 - core

    def at(piece):
        return pl.ds(pl.multiple_of(piece * chunk, chunk), chunk)

    def own_at(piece):
        return pl.ds(pl.multiple_of(piece * own, own), own)

    def load_state(piece):
        return pltpu.make_async_copy(
            state_any.at[at(piece)], state_v.at[at(piece)], load_sem.at[piece]
        )

    load_state(0).start()
    w_loads = [pltpu.make_async_copy(w_any.at[t], w_v.at[t], w_sem.at[t]) for t in range(3)]
    for copy in w_loads:
        copy.start()
    for piece in range(1, groups):
        load_state(piece).start()
    my_rows = own_at(me)
    shard = w_out_any.shape[0]
    part, quarter = shard // 2, shard // ctx_count
    later_loads = [
        pltpu.make_async_copy(state_any.at[my_rows], state_own, row_sem.at[0]),
        pltpu.make_async_copy(probe_any.at[my_rows], probe_own, row_sem.at[1]),
        pltpu.make_async_copy(
            w_out_any, w_ref.at[pl.ds(pl.multiple_of(me * shard, shard), shard)], shard_sem
        ),
    ]
    for copy in later_loads:
        copy.start()
    peers = [(lax.rem(ctx + step, ctx_count), partner) for step in range(ctx_count)]
    for far in range(groups):
        for step in range(ctx_count):
            if far or step:
                peers.append(
                    (lax.rem(ctx + step, ctx_count), lax.rem(group + far, groups) * 2 + core)
                )
    announce(peers)

    low, high = lax.rem(ctx, 2), ctx // 2
    which = lax.rem(low + high, 2)
    across, along = high * 2 + 1 - low, (1 - high) * 2 + low

    def shard_rows(origin, first, size):
        return pl.ds(pl.multiple_of((origin * 2 + core) * shard + first, size), size)

    def line_copy(way, origin, axis, mine):
        first = which * part + axis * quarter
        here = shard_rows(origin, first, quarter)
        source = (
            w_out_any.at[pl.ds(pl.multiple_of(first, quarter), quarter)] if mine else w_ref.at[here]
        )
        other = group + 1 if way == 0 else group - 1
        return remote(
            source, w_ref.at[here], line_send.at[way, axis, origin], line_recv.at[axis, origin],
            ctx, other * 2 + core,
        )

    def plane_copy(axis, origin, kept):
        here = shard_rows(origin, kept * part + axis * quarter, quarter)
        return remote(
            w_ref.at[here], w_ref.at[here], plane_send.at[axis, origin],
            plane_recv.at[axis, origin], along if axis else across, me,
        )

    def beside_copy(kind, origin):
        kept = which if kind < 2 else 1 - which
        here = shard_rows(origin, kept * part + (kind % 2) * quarter, quarter)
        return remote(
            w_ref.at[here], w_ref.at[here], beside_send.at[kind, origin],
            beside_recv.at[kind, origin], ctx, partner,
        )

    def shard_copy():
        return remote(
            w_out_any, w_ref.at[pl.ds(pl.multiple_of(me * shard, shard), shard)], shard_send,
            shard_recv, ctx, partner,
        )

    has_up, has_down = group < groups - 1, group > 0

    def each_origin(distance, work):
        for way in range(2):
            origin = group - distance if way == 0 else group + distance

            @pl.when(origin >= 0 if way == 0 else origin < groups)
            def _():
                work(way, origin)

    def line_arrived(distance, axis):
        def work(way, origin):
            line_copy(way, origin, axis, False).wait_recv()

            @pl.when(has_up if way == 0 else has_down)
            def _():
                line_copy(way, origin, axis, False).start()

            plane_copy(axis, origin, which).start()
            beside_copy(axis, origin).start()

        each_origin(distance, work)

    def plane_arrived(distance, axis):
        def work(way, origin):
            plane_copy(axis, origin, 1 - which).wait_recv()
            beside_copy(2 + axis, origin).start()

        each_origin(distance, work)

    def weights_sent(distance):
        def work(way, origin):
            for axis in range(2):

                @pl.when(has_up if way == 0 else has_down)
                def _():
                    line_copy(way, origin, axis, False).wait_send()

                plane_copy(axis, origin, which).wait_send()
            for kind in range(4):
                beside_copy(kind, origin).wait_send()

        each_origin(distance, work)

    def own_lines(work):
        for axis in range(2):

            @pl.when(has_up)
            def _():
                work(line_copy(0, group, axis, True))

            @pl.when(has_down)
            def _():
                work(line_copy(1, group, axis, True))

    for copy in w_loads:
        copy.wait()
    gain = gain_ref[...].astype(jnp.float32).reshape(1, model)

    def away(slot, kind, piece, dest):
        head = group * 2 + kind
        return (
            remote(
                query_buf.at[slot, piece, kind], query_out.at[ctx, own_at(piece)],
                q_send.at[slot, kind, piece], q_recv.at[ctx, piece], dest, head,
            ),
            remote(
                kv_buf.at[slot, kind, piece], kv_out.at[kind, ctx, at(piece)],
                kv_send.at[slot, kind, piece], kv_recv.at[kind, ctx, piece], dest, head,
            ),
        )

    def beside(slot, piece):
        result = [
            remote(
                query_buf.at[slot, piece, 1 - core], query_out.at[ctx, own_at(piece)],
                q_send.at[slot, 1 - core, piece], q_recv.at[ctx, piece], ctx, partner,
            )
        ]
        for kind in range(2):
            result.append(
                remote(
                    kv_buf.at[slot, kind, piece], kv_out.at[kind, ctx, at(piece)],
                    kv_send.at[slot, kind, piece], kv_recv.at[kind, ctx, piece], ctx, partner,
                )
            )
        return result

    def project(piece):
        load_state(piece).wait()
        block = state_v[at(piece), :].astype(jnp.float32)
        normed = (block * row_scale(block) * gain).astype(jnp.bfloat16)
        for t in range(3):
            result = jnp.dot(normed, w_v[t], preferred_element_type=jnp.float32).astype(
                jnp.bfloat16
            )
            for slot in range(slots):
                cut = result[:, slot * HEAD_DIM : (slot + 1) * HEAD_DIM]
                if t == 0:
                    query_buf[slot, piece, 0] = cut[:own]
                    query_buf[slot, piece, 1] = cut[own:]
                else:
                    kv_buf[slot, t - 1, piece] = cut

    def send_heads(piece):
        for slot in range(slots):
            dest = core * slots + slot

            @pl.when(dest != ctx)
            def _():
                for kind in range(2):
                    for copy in away(slot, kind, piece, dest):
                        copy.start()

            @pl.when(dest == ctx)
            def _():
                query_out[ctx, own_at(piece), :] = query_buf[slot, piece, core]
                for kind in range(2):
                    kv_out[kind, ctx, at(piece), :] = kv_buf[slot, kind, piece]
                for copy in beside(slot, piece):
                    copy.start()

    project(0)
    await_all(peers)
    own_lines(lambda copy: copy.start())
    send_heads(0)
    shard_copy().start()
    segs = []
    for step in range(1, ctx_count):
        copy = remote(
            seg_ref, segs_out.at[ctx], seg_send.at[step], seg_recv.at[step],
            lax.rem(ctx + step, ctx_count), me,
        )
        copy.start()
        segs.append(copy)
    segs_out[ctx] = seg_ref[...]

    def project_and_send(piece, _):
        project(piece)
        send_heads(piece)
        return 0

    lax.fori_loop(1, groups, project_and_send, 0)

    def hand_over(piece, step):
        source = lax.rem(ctx + step, ctx_count)
        return remote(
            kv_out.at[core, source, at(piece)], kv_out.at[core, source, at(piece)],
            pass_send.at[step, piece], kv_recv.at[core, source, piece], ctx, partner,
        )

    for piece in range(groups):
        for step in range(1, ctx_count):
            copy = hand_over(piece, step)
            copy.wait_recv()
            copy.start()
        if piece == 0:
            line_arrived(1, 0)
        if piece == min(2, groups - 1):
            line_arrived(1, 1)
    line_arrived(2, 0)

    def got_query(source, piece):
        remote(
            query_out.at[source, own_at(piece)], query_out.at[source, own_at(piece)],
            q_send.at[0, 0, piece], q_recv.at[source, piece], ctx, partner,
        ).wait_recv()

    def got_kv(kind, source, piece):
        remote(
            kv_out.at[kind, source, at(piece)], kv_out.at[kind, source, at(piece)],
            kv_send.at[0, 0, piece], kv_recv.at[kind, source, piece], ctx, partner,
        ).wait_recv()

    def gather(piece, _):
        for step in range(1, ctx_count):
            source = lax.rem(ctx + step, ctx_count)
            got_query(source, piece)
            got_kv(1 - core, source, piece)
            hand_over(piece, step).wait_send()

        @pl.when(ctx // slots != core)
        def _():
            got_query(ctx, piece)
            for kind in range(2):
                got_kv(kind, ctx, piece)

        return 0

    lax.fori_loop(0, groups, gather, 0)
    for copy in segs:
        copy.wait()
    leaving = [
        pltpu.make_async_copy(query_out, query_any, leave_sem.at[0]),
        pltpu.make_async_copy(kv_out, kv_any, leave_sem.at[1]),
    ]
    for copy in leaving:
        copy.start()
    pair_copy = remote(w_any, w_pair, pair_send, pair_recv, ctx, partner)
    pair_copy.start()
    for axis in range(2):
        plane_arrived(1, axis)

    def cols_of(group_at, ctx_at):
        head = group_at * ctx_count + ctx_at
        return pl.ds(pl.multiple_of(head * HEAD_DIM, HEAD_DIM), HEAD_DIM)

    factor = HEAD_DIM ** (-0.5) * LOG2E
    sub = groups * own
    seg_all = segs_out[...]

    def below(value):
        count = jnp.where(seg_all < value, 1.0, 0.0)
        for axis in (0, 1, 2):
            count = jnp.sum(count, axis=axis, keepdims=True)
        return count[0]

    first_bound, second_bound = below(1), below(2)
    lane = lax.broadcasted_iota(jnp.int32, (1, sub), 1)
    inside = (lane // own) * (2 * own) + core * own + lane % own
    key_row = lax.broadcasted_iota(jnp.int32, (rows, sub), 0)

    def out_copy(tile, order, other):
        return remote(
            part_out.at[tile, own_at(other)], joined.at[:, cols_of(group, ctx)],
            out_send.at[tile, order], out_recv.at[group, ctx], tile, other * 2 + core,
        )

    def one_tile(tile, _):
        query = query_out[tile]
        pos = (tile * rows + inside).astype(jnp.float32)
        start = jnp.where(
            pos >= second_bound, second_bound, jnp.where(pos >= first_bound, first_bound, 0.0)
        ).astype(jnp.int32)

        def step(diagonal, piece, carry):
            top, total, acc = carry
            scores = dot32(kv_out[0, piece], query, NT)
            allowed = key_row >= start - piece * rows
            if diagonal:
                allowed = allowed & (key_row <= inside)
            scores = jnp.where(allowed, scores, NEGATIVE)
            new_top = jnp.maximum(top, jnp.max(scores, axis=0, keepdims=True) * factor)
            weights = jnp.exp2(scores * factor - new_top)
            scale = jnp.exp2(top - new_top)
            total = total * scale + jnp.sum(weights, axis=0, keepdims=True)
            acc = acc * scale + dot32(kv_out[1, piece], weights.astype(jnp.bfloat16), TN)
            return new_top, total, acc

        carry = (
            jnp.full((1, sub), NEGATIVE, jnp.float32),
            jnp.zeros((1, sub), jnp.float32),
            jnp.zeros((HEAD_DIM, sub), jnp.float32),
        )
        carry = lax.fori_loop(0, tile, functools.partial(step, False), carry)
        top, total, acc = step(True, tile, carry)
        part_out[tile] = (acc / total).T.astype(jnp.bfloat16)
        log_out[tile] = top + jnp.log2(total)
        for order in range(groups):
            other = far_first(groups, group, order)
            if order == groups - 1:

                @pl.when(tile != ctx)
                def _():
                    out_copy(tile, order, other).start()

                @pl.when(tile == ctx)
                def _():
                    joined[:, cols_of(group, ctx)] = part_out[tile, own_at(group), :]

            else:
                out_copy(tile, order, other).start()

        @pl.when(tile == 1)
        def _():
            line_arrived(2, 1)

        @pl.when(tile == 2)
        def _():
            for axis in range(2):
                plane_arrived(2, axis)

        return 0

    lax.fori_loop(0, ctx_count, one_tile, 0)
    leaving.append(pltpu.make_async_copy(part_out, part_any, leave_sem.at[2]))
    leaving[-1].start()
    for copy in later_loads:
        copy.wait()
    sources = []
    for far in range(groups):
        for step in range(ctx_count):
            if far or step:
                sources.append((lax.rem(group + far, groups), lax.rem(ctx + step, ctx_count)))
    tile = min(256, model)
    wide = ctx_count * HEAD_DIM
    zero = jnp.zeros((own, 1), jnp.float32)
    squares = products = zero
    for order in range(groups - 1, -1, -1):
        other = far_first(groups, group, order)
        if order == groups - 1:
            shard_copy().wait_recv()
        else:
            if order == max(groups - 3, 0):
                for distance in range(3, groups):
                    for axis in range(2):
                        line_arrived(distance, axis)
            if order == 0:
                for distance in range(3, groups):
                    for axis in range(2):
                        plane_arrived(distance, axis)
            for kind in range(4):
                beside_copy(kind, other).wait_recv()
        for step in range(ctx_count):
            if order == groups - 1 and step == 0:
                continue
            peer = lax.rem(ctx + step, ctx_count)
            remote(
                part_out.at[0, own_at(0)], joined.at[:, cols_of(other, peer)], out_send.at[0, 0],
                out_recv.at[other, peer], peer, other * 2 + core,
            ).wait_recv()
        heads = pl.ds(pl.multiple_of(other * wide, wide), wide)

        def layer(piece, carry):
            cols = pl.ds(pl.multiple_of(piece * tile, tile), tile)
            result = jnp.dot(
                joined[:, heads], w_ref[heads, cols], preferred_element_type=jnp.float32
            )
            if order == groups - 1:
                result = result + state_own[:, cols].astype(jnp.float32)
            else:
                result = result + readout_out[:, cols]
            readout_out[:, cols] = result
            if order:
                return carry
            squares, products = carry
            squares = squares + jnp.sum(result * result, axis=1, keepdims=True)
            products = products + jnp.sum(
                result * probe_own[:, cols].astype(jnp.float32), axis=1, keepdims=True
            )
            return squares, products

        squares, products = lax.fori_loop(0, model // tile, layer, (squares, products))
    scale = lax.rsqrt(squares / model + EPSILON)
    bend = scale**3 * (products / model)

    def finish(piece, _):
        cols = pl.ds(pl.multiple_of(piece * tile, tile), tile)
        readout = scale * probe_own[:, cols].astype(jnp.float32) - readout_out[:, cols] * bend
        readout_out[:, cols] = readout
        half[:, cols] = readout.astype(jnp.bfloat16)
        return 0

    lax.fori_loop(0, model // tile, finish, 0)
    leaving.append(pltpu.make_async_copy(readout_out, readout_any, leave_sem.at[3]))
    leaving[-1].start()
    copies = []
    for order in range(groups):
        other = far_first(groups, group, order)
        result = dot32(
            half[...], w_ref[pl.ds(pl.multiple_of(other * wide, wide), wide), :], NT
        ).astype(jnp.bfloat16)
        for index in range(ctx_count):
            sending[order, index] = result[:, index * HEAD_DIM : (index + 1) * HEAD_DIM]
        for step in range(ctx_count):
            peer = lax.rem(ctx + step, ctx_count)
            if order == groups - 1 and step == 0:
                continue
            copy = remote(
                sending.at[order, peer], grad_out.at[ctx, group], back_send.at[order, step],
                back_recv.at[ctx, group], peer, other * 2 + core,
            )
            copy.start()
            copies.append(copy)
    last = pltpu.make_async_copy(sending.at[groups - 1, ctx], grad_out.at[ctx, group], own_sem)
    last.start()

    def sent(piece, _):
        for slot in range(slots):
            dest = core * slots + slot

            @pl.when(dest != ctx)
            def _():
                for kind in range(2):
                    for copy in away(slot, kind, piece, dest):
                        copy.wait_send()

            @pl.when(dest == ctx)
            def _():
                for copy in beside(slot, piece):
                    copy.wait_send()

        return 0

    lax.fori_loop(0, groups, sent, 0)

    own_lines(lambda copy: copy.wait_send())
    shard_copy().wait_send()
    for distance in range(1, groups):
        weights_sent(distance)

    def parts_sent(tile, _):
        for order in range(groups):
            other = far_first(groups, group, order)
            if order == groups - 1:

                @pl.when(tile != ctx)
                def _():
                    out_copy(tile, order, other).wait_send()

            else:
                out_copy(tile, order, other).wait_send()
        return 0

    lax.fori_loop(0, ctx_count, parts_sent, 0)
    for other, peer in sources:
        remote(
            sending.at[0, 0], grad_out.at[peer, other], back_send.at[0, 0],
            back_recv.at[peer, other], peer, other * 2 + core,
        ).wait_recv()
    for copy in copies:
        copy.wait_send()
    last.wait()
    for copy in leaving:
        copy.wait()
    pair_copy.wait()


def front(ctx_count, head_count, state, w_qkv, gain, segment_ids, w_out, probe):
    rows, model = state.shape
    width = w_qkv.shape[2]
    own, groups, slots = rows // head_count, head_count // 2, width // HEAD_DIM
    seg = segment_ids.reshape(-1, 128)
    half, full, dma = jnp.bfloat16, jnp.float32, pltpu.SemaphoreType.DMA
    shape = jax.ShapeDtypeStruct
    return pl.pallas_call(
        functools.partial(front_kernel, ctx_count, head_count),
        out_shape=(
            shape((ctx_count, groups * own, HEAD_DIM), half),
            shape((2, ctx_count, rows, HEAD_DIM), half),
            shape((ctx_count,) + seg.shape, seg.dtype),
            shape((ctx_count, groups * own, HEAD_DIM), half),
            shape((ctx_count, 1, groups * own), full),
            shape((ctx_count, groups, own, HEAD_DIM), half),
            shape((own, model), full),
            shape(w_qkv.shape, half),
        ),
        in_specs=[ANY, ANY, VMEM, VMEM, ANY, ANY],
        out_specs=(ANY, ANY, VMEM, ANY, VMEM, ANY, ANY, ANY),
        scratch_shapes=[
            pltpu.VMEM((rows, model), half),
            pltpu.VMEM(w_qkv.shape, half),
            pltpu.VMEM((slots, groups, 2, own, HEAD_DIM), half),
            pltpu.VMEM((slots, 2, groups, 2 * own, HEAD_DIM), half),
            pltpu.VMEM((model, model), half),
            pltpu.VMEM((own, model), half),
            pltpu.VMEM((own, model), half),
            pltpu.VMEM((groups, ctx_count, own, HEAD_DIM), half),
            pltpu.VMEM((own, model), half),
            pltpu.VMEM((own, model), half),
            pltpu.VMEM((ctx_count, groups * own, HEAD_DIM), half),
            pltpu.VMEM((2, ctx_count, rows, HEAD_DIM), half),
            pltpu.VMEM((ctx_count, groups * own, HEAD_DIM), half),
            pltpu.VMEM((own, model), full),
            dma((groups,)),
            dma((3,)),
            dma((slots, 2, groups)),
            dma((ctx_count, groups)),
            dma((slots, 2, groups)),
            dma((2, ctx_count, groups)),
            dma((ctx_count, groups)),
            dma((ctx_count,)),
            dma((ctx_count,)),
            dma((2, 2, groups)),
            dma((2, groups)),
            dma((2, groups)),
            dma((2, groups)),
            dma((4, groups)),
            dma((4, groups)),
            dma,
            dma,
            dma,
            dma((ctx_count, groups)),
            dma((groups, ctx_count)),
            dma((groups, ctx_count)),
            dma((ctx_count, groups)),
            dma,
            dma((2,)),
            dma,
            dma,
            dma((4,)),
        ],
        compiler_params=pltpu.CompilerParams(
            collective_id=0, has_side_effects=True, vmem_limit_bytes=62 * 2**20
        ),
    )(state, w_qkv, gain, seg, w_out, probe)


def segment_bounds(segs_ref):
    segs = segs_ref[...]

    def below(value):
        return jnp.sum(jnp.where(segs < value, 1.0, 0.0)).astype(jnp.int32)

    return below(1), below(2)


def tile_plan(bounds, rows, own, parts, sub, bk, tile, core):
    first_bound, second_bound = bounds

    def start_of(pos):
        return jnp.where(pos >= second_bound, second_bound, jnp.where(pos >= first_bound, first_bound, 0))

    blocks = sub // own
    base = tile * rows + core * own
    places = []
    for part in range(parts):
        lane = lax.broadcasted_iota(jnp.int32, (1, sub), 1)
        pos = base + (lane // own + part * blocks) * (2 * own) + lane % own
        places.append((start_of(pos), pos))
    first, last = base, base + (parts * blocks - 1) * 2 * own + own - 1
    low = start_of(first) // bk
    inner_low = (start_of(last) + bk - 1) // bk
    inner_high = jnp.maximum(inner_low, (first + 1) // bk)
    high = last // bk + 1
    return places, low, inner_low, inner_high, high


def head_backward_kernel(
    rows, own, parts, sub, bk, segs_ref, query_ref, kv_ref, grad_ref, out_ref, log_ref, query_out,
    pair_out, pair_acc,
):
    score_scale = HEAD_DIM ** (-0.5)
    factor = score_scale * LOG2E
    core = lax.rem(lax.axis_index("head"), 2)
    bounds = segment_bounds(segs_ref)
    tiles = query_ref.shape[0] // (parts * sub)
    pair_rows = pair_acc.shape[0]

    def clear(piece, _):
        at = pl.ds(pl.multiple_of(piece * bk, bk), bk)
        pair_acc[at, :] = jnp.zeros((bk, 2 * HEAD_DIM), jnp.float32)
        return 0

    lax.fori_loop(0, pair_rows // bk, clear, 0)

    def one_tile(tile, _):
        places, low, inner_low, inner_high, high = tile_plan(
            bounds, rows, own, parts, sub, bk, tile, core
        )

        def at(part):
            return pl.ds(pl.multiple_of((tile * parts + part) * sub, sub), sub)

        deltas, logs = [], []
        for part in range(parts):
            product = grad_ref[at(part), :].astype(jnp.float32) * out_ref[at(part), :].astype(
                jnp.float32
            )
            deltas.append(jnp.sum(product.T, axis=0, keepdims=True))
            logs.append(log_ref[tile, pl.ds(part, 1), :])

        def step(masked, piece, carry):
            keys_at = pl.ds(pl.multiple_of(piece * bk, bk), bk)
            if masked:
                key_pos = piece * bk + lax.broadcasted_iota(jnp.int32, (bk, sub), 0)
            result = []
            key_block, value_block = kv_ref[0, keys_at, :], kv_ref[1, keys_at, :]
            for part in range(parts):
                query_block, grad_block = query_ref[at(part), :], grad_ref[at(part), :]
                scores = dot32(key_block, query_block, NT)
                probabilities = jnp.exp2(scores * factor - logs[part])
                if masked:
                    start, pos = places[part]
                    probabilities = jnp.where(
                        (key_pos >= start) & (key_pos <= pos), probabilities, 0.0
                    )
                dprobs = dot32(value_block, grad_block, NT)
                dscores = (probabilities * (dprobs - deltas[part])).astype(jnp.bfloat16)
                pair_acc[keys_at, HEAD_DIM:] += jnp.dot(
                    probabilities.astype(jnp.bfloat16),
                    grad_block,
                    preferred_element_type=jnp.float32,
                )
                pair_acc[keys_at, :HEAD_DIM] += jnp.dot(
                    dscores, query_block, preferred_element_type=jnp.float32
                )
                result.append(carry[part] + dot32(key_block, dscores, TN))
            return tuple(result)

        carry = tuple(jnp.zeros((HEAD_DIM, sub), jnp.float32) for _ in range(parts))
        carry = lax.fori_loop(low, inner_low, functools.partial(step, True), carry)
        carry = lax.fori_loop(inner_low, inner_high, functools.partial(step, False), carry)
        carry = lax.fori_loop(inner_high, high, functools.partial(step, True), carry)
        for part in range(parts):
            query_out[at(part), :] = (carry[part].T * score_scale).astype(jnp.bfloat16)
        return 0

    lax.fori_loop(0, tiles, one_tile, 0)

    def flush(piece, _):
        at = pl.ds(pl.multiple_of(piece * bk, bk), bk)
        pair_out[at, :HEAD_DIM] = (pair_acc[at, :HEAD_DIM] * score_scale).astype(jnp.bfloat16)
        pair_out[at, HEAD_DIM:] = pair_acc[at, HEAD_DIM:].astype(jnp.bfloat16)
        return 0

    lax.fori_loop(0, pair_rows // bk, flush, 0)


def finish_kernel(
    ctx_count, head_count, query_ref, pair_ref, w_any, w_pair, state_any, noise_ref, readout_ref,
    gain_ref, new_out, w_both, beside, away, terms_in, partial, sending, total, state_own, b_send,
    b_recv, a_send, a_recv, z_send, z_recv, own_sem,
):
    ctx, me, group, core = place()
    groups = head_count // 2
    own, model = new_out.shape
    slots = ctx_count // 2
    partner = group * 2 + 1 - core
    my_rows = pl.ds(pl.multiple_of(me * own, own), own)
    loads = [
        pltpu.make_async_copy(w_any, w_both.at[core], own_sem.at[0]),
        pltpu.make_async_copy(w_pair, w_both.at[1 - core], own_sem.at[1]),
        pltpu.make_async_copy(state_any.at[my_rows], state_own, own_sem.at[2]),
    ]
    for copy in loads:
        copy.start()
    peers = [(ctx, partner)]
    peers += [(lax.rem(ctx + step, ctx_count), me) for step in range(1, ctx_count)]
    peers += [(ctx, lax.rem(group + far, groups) * 2 + core) for far in range(1, groups)]
    meet(peers)
    dests = [far_first(groups, group, order) for order in range(groups)]
    copies = []
    for order, dest in enumerate(dests):
        copy = remote(
            pair_ref.at[:, dest, 1 - core], beside.at[order], b_send.at[order], b_recv.at[order],
            ctx, partner,
        )
        copy.start()
        copies.append(copy)

    def stripe(source):
        slot = lax.rem(source, slots)
        return pl.ds(pl.multiple_of(slot * HEAD_DIM, HEAD_DIM), HEAD_DIM)

    def exchange(order, dest, step):
        peer = lax.rem(ctx + step, ctx_count)
        return remote(
            away.at[order, step], terms_in.at[dest, ctx // slots, :, :, stripe(ctx)],
            a_send.at[order, step], a_recv.at[dest, ctx], peer, me,
        )

    def arrived(dest, step):
        source = lax.rem(ctx + step, ctx_count)
        remote(
            away.at[0, 0], terms_in.at[dest, source // slots, :, :, stripe(source)],
            a_send.at[0, 0], a_recv.at[dest, source], source, me,
        ).wait_recv()

    for order, dest in enumerate(dests):
        copies[order].wait_recv()
        for step in range(1, ctx_count):
            peer = lax.rem(ctx + step, ctx_count)
            pair = pair_ref[peer, dest, core].astype(jnp.float32) + beside[order, peer].astype(
                jnp.float32
            )
            pair = pair.astype(jnp.bfloat16)
            away[order, step, 0] = query_ref[peer, dest]
            away[order, step, 1] = pair[:, :HEAD_DIM]
            away[order, step, 2] = pair[:, HEAD_DIM:]
            exchange(order, dest, step).start()
        pair = pair_ref[ctx, dest, core].astype(jnp.float32) + beside[order, ctx].astype(
            jnp.float32
        )
        pair = pair.astype(jnp.bfloat16)
        at = stripe(ctx)
        terms_in[dest, ctx // slots, 0, :, at] = query_ref[ctx, dest]
        terms_in[dest, ctx // slots, 1, :, at] = pair[:, :HEAD_DIM]
        terms_in[dest, ctx // slots, 2, :, at] = pair[:, HEAD_DIM:]
    for copy in loads:
        copy.wait()
    pieces = partial.shape[2]
    tile = model // pieces

    def chain(order, dest, piece):
        up = dest > group
        line = jnp.where(up, 0, 1)
        peer = jnp.where(up, group + 1, group - 1)
        return remote(
            sending.at[order, piece], partial.at[line, dest, piece], z_send.at[order, piece],
            z_recv.at[line, dest, piece], ctx, peer * 2 + core,
        )

    def came(line, dest, piece):
        remote(
            sending.at[0, piece], partial.at[line, dest, piece], z_send.at[0, piece],
            z_recv.at[line, dest, piece], ctx, partner,
        ).wait_recv()

    def term(dest, piece):
        cols = pl.ds(pl.multiple_of(piece * tile, tile), tile)
        result = None
        for half in range(2):
            for kind in range(3):
                part = dot32(terms_in[dest, half, kind], w_both[half, kind, cols, :], NT)
                result = part if result is None else result + part
        return result

    for order, dest in enumerate(dests[:-1]):
        for step in range(1, ctx_count):
            arrived(dest, step)
        line = jnp.where(dest > group, 0, 1)
        inner = (group > 0) & (group < groups - 1)

        def one_piece(piece, _):
            total[...] = term(dest, piece)

            @pl.when(inner)
            def _():
                came(line, dest, piece)
                total[...] += partial[line, dest, piece].astype(jnp.float32)

            sending[order, piece] = total[...].astype(jnp.bfloat16)
            chain(order, dest, piece).start()
            return 0

        lax.fori_loop(0, pieces, one_piece, 0)

    for step in range(1, ctx_count):
        arrived(group, step)

    state = state_own[...].astype(jnp.float32)
    inverse = row_scale(state)

    def last_piece(piece, slope):
        cols = pl.ds(pl.multiple_of(piece * tile, tile), tile)
        total[...] = term(group, piece)

        @pl.when(group > 0)
        def _():
            came(0, group, piece)
            total[...] += partial[0, group, piece].astype(jnp.float32)

        @pl.when(group < groups - 1)
        def _():
            came(1, group, piece)
            total[...] += partial[1, group, piece].astype(jnp.float32)

        gained = total[...] * gain_ref[cols].astype(jnp.float32).reshape(1, tile)
        new_out[:, cols] = gained
        return slope + jnp.sum(
            gained * state_own[:, cols].astype(jnp.float32), axis=1, keepdims=True
        )

    slope = lax.fori_loop(0, pieces, last_piece, jnp.zeros((own, 1), jnp.float32))
    bend = inverse**3 * (slope / model)

    def update(piece, _):
        cols = pl.ds(pl.multiple_of(piece * tile, tile), tile)
        here = state_own[:, cols].astype(jnp.float32)
        gradient = readout_ref[:, cols] + inverse * new_out[:, cols] - here * bend
        new_out[:, cols] = (
            here - STEP_SIZE * gradient + NOISE_SCALE * noise_ref[:, cols].astype(jnp.float32)
        )
        return 0

    lax.fori_loop(0, pieces, update, 0)
    for order, dest in enumerate(dests):
        copies[order].wait_send()
        for step in range(1, ctx_count):
            exchange(order, dest, step).wait_send()
        if order < groups - 1:
            for piece in range(pieces):
                chain(order, dest, piece).wait_send()


def finish_step(
    ctx_count, head_count, query_grad, pair, w_qkv, w_pair, state, noise, readout, gain
):
    own, model = readout.shape
    width = w_qkv.shape[2]
    groups, pieces = head_count // 2, 4
    half, full, dma = jnp.bfloat16, jnp.float32, pltpu.SemaphoreType.DMA
    tile = model // pieces
    return pl.pallas_call(
        functools.partial(finish_kernel, ctx_count, head_count),
        out_shape=jax.ShapeDtypeStruct((own, model), full),
        in_specs=[VMEM, VMEM, ANY, ANY, ANY, VMEM, VMEM, VMEM],
        out_specs=VMEM,
        scratch_shapes=[
            pltpu.VMEM((2,) + w_qkv.shape, half),
            pltpu.VMEM((groups, ctx_count, own, 2 * HEAD_DIM), half),
            pltpu.VMEM((groups, ctx_count, 3, own, HEAD_DIM), half),
            pltpu.VMEM((groups, 2, 3, own, width), half),
            pltpu.VMEM((2, groups, pieces, own, tile), half),
            pltpu.VMEM((groups, pieces, own, tile), half),
            pltpu.VMEM((own, tile), full),
            pltpu.VMEM((own, model), half),
            dma((groups,)),
            dma((groups,)),
            dma((groups, ctx_count)),
            dma((groups, ctx_count)),
            dma((groups, pieces)),
            dma((2, groups, pieces)),
            dma((3,)),
        ],
        compiler_params=pltpu.CompilerParams(
            collective_id=2, has_side_effects=True, vmem_limit_bytes=60 * 2**20
        ),
    )(query_grad, pair, w_qkv, w_pair, state, noise, readout, gain)


def heads_body(state, norm_gain, w_qkv, w_out, probe, noise, segment_ids):
    rows, model = state.shape
    head_count, ctx_count = lax.axis_size("head"), lax.axis_size("ctx")
    own, groups = rows // head_count, head_count // 2
    queries, kv, segs, outputs, logs, grads_out, readout, w_pair = front(
        ctx_count, head_count, state, w_qkv, norm_gain, segment_ids, w_out, probe
    )
    mine, total = ctx_count * groups * own, ctx_count * rows
    parts, sub, bk = 1, groups * own, min(rows, 512)
    query_grad, pair = pl.pallas_call(
        functools.partial(head_backward_kernel, rows, own, parts, sub, bk),
        out_shape=(
            jax.ShapeDtypeStruct((mine, HEAD_DIM), jnp.bfloat16),
            jax.ShapeDtypeStruct((total, 2 * HEAD_DIM), jnp.bfloat16),
        ),
        in_specs=[VMEM] * 6,
        out_specs=(VMEM, VMEM),
        scratch_shapes=[pltpu.VMEM((total, 2 * HEAD_DIM), jnp.float32)],
        compiler_params=pltpu.CompilerParams(vmem_limit_bytes=60 * 2**20),
        cost_estimate=pl.CostEstimate(
            flops=10 * mine * total * HEAD_DIM, bytes_accessed=0, transcendentals=0
        ),
    )(
        segs, queries.reshape(mine, HEAD_DIM), kv.reshape(2, total, HEAD_DIM),
        grads_out.reshape(mine, HEAD_DIM), outputs.reshape(mine, HEAD_DIM), logs,
    )
    return finish_step(
        ctx_count, head_count, query_grad.reshape(ctx_count, groups, own, HEAD_DIM),
        pair.reshape(ctx_count, groups, 2, own, 2 * HEAD_DIM), w_qkv, w_pair, state, noise, readout,
        norm_gain,
    )


def solution(mesh):
    placed = (
        P("ctx", None),
        P(),
        P(None, None, "head"),
        P("head", None),
        P("ctx", None),
        P(("ctx", "head"), None),
        P("ctx"),
    )

    def step(*args):
        heads = args[2].shape[2] // HEAD_DIM
        return (heads_body if lax.axis_size("ctx") == 2 * heads == 4 else body)(*args)

    return jax.shard_map(
        step, mesh=mesh, in_specs=placed, out_specs=P(("ctx", "head"), None), check_vma=False
    )
```

```python
import functools

import jax
import jax.numpy as jnp
from jax import lax
from jax.experimental import pallas as pl
from jax.experimental.pallas import tpu as pltpu
from jax.sharding import PartitionSpec as P

HEAD_DIM = 128
EPSILON = 1e-05
STEP_SIZE = 0.25
NOISE_SCALE = (2.0 * STEP_SIZE) ** 0.5
NEGATIVE = -1e30
LOG2E = 1.4426950408889634
MESH = pl.DeviceIdType.MESH
VMEM = pl.BlockSpec(memory_space=pltpu.VMEM)
ANY = pl.BlockSpec(memory_space=pl.ANY)
NT = (((1,), (1,)), ((), ()))
TN = (((0,), (0,)), ((), ()))
FORWARD_BLOCKS = (512, 512)
BACKWARD_BLOCKS = (512, 512)


def row_scale(matrix):
    return lax.rsqrt(jnp.mean(matrix * matrix, axis=-1, keepdims=True) + EPSILON)


def dot32(left, right, dims):
    return lax.dot_general(left, right, dims, preferred_element_type=jnp.float32)


def greet(axis, number, me):
    barrier = pltpu.get_barrier_semaphore()
    for step in range(1, number):
        pl.semaphore_signal(
            barrier, inc=1, device_id={axis: lax.rem(me + step, number)}, device_id_type=MESH
        )
    pl.semaphore_wait(barrier, number - 1)


def gather_kernel(
    number, key_ref, value_ref, seg_ref, normed_ref, w_ref, keys, values, segs, query_out, send_sem,
    recv_sem, own_sem,
):
    me = lax.axis_index("ctx")
    rows = key_ref.shape[0]
    greet("ctx", number, me)

    def place(index):
        return pl.ds(pl.multiple_of(index * rows, rows), rows)

    def send(slot, source, target, peer):
        copy = pltpu.make_async_remote_copy(
            src_ref=source,
            dst_ref=target,
            send_sem=send_sem.at[slot],
            recv_sem=recv_sem.at[slot],
            device_id={"ctx": peer},
            device_id_type=MESH,
        )
        copy.start()
        return copy

    mine = place(me)
    copies = []
    for step in range(1, number):
        copies.append(send(step, seg_ref, segs.at[me], lax.rem(me + step, number)))
    relay = number == 4
    if relay:
        low, high = lax.rem(me, 2), me // 2
        across, along = high * 2 + 1 - low, (1 - high) * 2 + low
        key_first = send(number, key_ref, keys.at[mine], across)
        value_first = send(number + 1, value_ref, values.at[mine], along)
        copies.append(send(number + 2, value_ref, values.at[mine], across))
        copies.append(send(number + 3, key_ref, keys.at[mine], along))
    else:
        for step in range(1, number):
            peer = lax.rem(me + step, number)
            copies.append(send(number + 2 * step, key_ref, keys.at[mine], peer))
            copies.append(send(number + 2 * step + 1, value_ref, values.at[mine], peer))
    pairs = ((key_ref, keys.at[mine]), (value_ref, values.at[mine]), (seg_ref, segs.at[me]))
    for index, (source, target) in enumerate(pairs):
        copy = pltpu.make_async_copy(source, target, own_sem.at[index])
        copy.start()
        copies.append(copy)
    tile = min(256, rows)

    def project(piece, _):
        at = pl.ds(pl.multiple_of(piece * tile, tile), tile)
        query_out[at, :] = jnp.dot(
            normed_ref[at, :], w_ref[...], preferred_element_type=jnp.float32
        ).astype(jnp.bfloat16)
        return 0

    lax.fori_loop(0, rows // tile, project, 0)
    if relay:
        key_first.wait()
        copies.append(send(number + 4, keys.at[place(across)], keys.at[place(across)], along))
        value_first.wait()
        copies.append(send(number + 5, values.at[place(along)], values.at[place(along)], across))
    for copy in copies:
        copy.wait()


def gather_keys(number, key_rows, value_rows, segment_ids, normed, w_query):
    rows, width = key_rows.shape
    seg = segment_ids.reshape(-1, 128)
    full = jax.ShapeDtypeStruct((number * rows, width), key_rows.dtype)
    keys, values, segs, queries = pl.pallas_call(
        functools.partial(gather_kernel, number),
        out_shape=(
            full,
            full,
            jax.ShapeDtypeStruct((number,) + seg.shape, seg.dtype),
            jax.ShapeDtypeStruct((rows, width), key_rows.dtype),
        ),
        in_specs=[VMEM] * 5,
        out_specs=(ANY, ANY, ANY, VMEM),
        scratch_shapes=[
            pltpu.SemaphoreType.DMA((3 * number + 6,)),
            pltpu.SemaphoreType.DMA((3 * number + 6,)),
            pltpu.SemaphoreType.DMA((3,)),
        ],
        compiler_params=pltpu.CompilerParams(collective_id=0, has_side_effects=True),
    )(key_rows, value_rows, seg, normed, w_query)
    return keys, values, segs.reshape(-1), queries


def block_ranges(table, index):
    return [table[index, column] for column in range(4)]


def forward_kernel(
    heads, bq, bk, table, query_ref, key_ref, value_ref, start_ref, pos_ref, out_ref, log_ref
):
    factor = HEAD_DIM ** (-0.5) * LOG2E
    blocks = query_ref.shape[0] // bq

    def one_block(index, _):
        low, inner_low, inner_high, high = block_ranges(table, index)
        rows = pl.ds(pl.multiple_of(index * bq, bq), bq)
        start, pos = start_ref[index], pos_ref[index]

        def step(masked, piece, carry):
            keys_at = pl.ds(pl.multiple_of(piece * bk, bk), bk)
            if masked:
                key_pos = piece * bk + lax.broadcasted_iota(jnp.int32, (bk, bq), 0)
                allowed = (key_pos >= start) & (key_pos <= pos)
            result = []
            for head in range(heads):
                top, total, acc = carry[head]
                cols = pl.ds(head * HEAD_DIM, HEAD_DIM)
                scores = dot32(key_ref[keys_at, cols], query_ref[rows, cols], NT)
                if masked:
                    scores = jnp.where(allowed, scores, NEGATIVE)
                new_top = jnp.maximum(top, jnp.max(scores, axis=0, keepdims=True) * factor)
                weights = jnp.exp2(scores * factor - new_top)
                scale = jnp.exp2(top - new_top)
                total = total * scale + jnp.sum(weights, axis=0, keepdims=True)
                acc = acc * scale + dot32(
                    value_ref[keys_at, cols], weights.astype(jnp.bfloat16), TN
                )
                result.append((new_top, total, acc))
            return tuple(result)

        carry = tuple(
            (
                jnp.full((1, bq), NEGATIVE, jnp.float32),
                jnp.zeros((1, bq), jnp.float32),
                jnp.zeros((HEAD_DIM, bq), jnp.float32),
            )
            for _ in range(heads)
        )
        carry = lax.fori_loop(low, inner_low, functools.partial(step, True), carry)
        carry = lax.fori_loop(inner_low, inner_high, functools.partial(step, False), carry)
        carry = lax.fori_loop(inner_high, high, functools.partial(step, True), carry)
        for head in range(heads):
            top, total, acc = carry[head]
            out_ref[rows, pl.ds(head * HEAD_DIM, HEAD_DIM)] = (acc / total).T.astype(jnp.bfloat16)
            log_ref[index, pl.ds(head, 1), :] = top + jnp.log2(total)
        return 0

    lax.fori_loop(0, blocks, one_block, 0)


def backward_kernel(
    heads, bq, bk, table, query_ref, key_ref, value_ref, grad_ref, out_ref, log_ref, start_ref,
    pos_ref, query_out, pair_out, pair_acc,
):
    score_scale = HEAD_DIM ** (-0.5)
    factor = score_scale * LOG2E
    blocks = query_ref.shape[0] // bq
    width = heads * HEAD_DIM
    pair_rows = pair_acc.shape[0]

    def clear(piece, _):
        at = pl.ds(pl.multiple_of(piece * bk, bk), bk)
        pair_acc[at, :] = jnp.zeros((bk, 2 * width), jnp.float32)
        return 0

    lax.fori_loop(0, pair_rows // bk, clear, 0)

    def one_block(index, _):
        low, inner_low, inner_high, high = block_ranges(table, index)
        rows = pl.ds(pl.multiple_of(index * bq, bq), bq)
        start, pos = start_ref[index], pos_ref[index]
        deltas, logs = [], []
        for head in range(heads):
            cols = pl.ds(head * HEAD_DIM, HEAD_DIM)
            product = grad_ref[rows, cols].astype(jnp.float32) * out_ref[rows, cols].astype(
                jnp.float32
            )
            deltas.append(jnp.sum(product.T, axis=0, keepdims=True))
            logs.append(log_ref[index, pl.ds(head, 1), :])

        def step(masked, piece, carry):
            keys_at = pl.ds(pl.multiple_of(piece * bk, bk), bk)
            if masked:
                key_pos = piece * bk + lax.broadcasted_iota(jnp.int32, (bk, bq), 0)
                allowed = (key_pos >= start) & (key_pos <= pos)
            result = []
            for head in range(heads):
                cols = pl.ds(head * HEAD_DIM, HEAD_DIM)
                value_cols = pl.ds(width + head * HEAD_DIM, HEAD_DIM)
                key_block, query_block = key_ref[keys_at, cols], query_ref[rows, cols]
                grad_block = grad_ref[rows, cols]
                scores = dot32(key_block, query_block, NT)
                probabilities = jnp.exp2(scores * factor - logs[head])
                if masked:
                    probabilities = jnp.where(allowed, probabilities, 0.0)
                dprobs = dot32(value_ref[keys_at, cols], grad_block, NT)
                dscores = (probabilities * (dprobs - deltas[head])).astype(jnp.bfloat16)
                pair_acc[keys_at, value_cols] += jnp.dot(
                    probabilities.astype(jnp.bfloat16),
                    grad_block,
                    preferred_element_type=jnp.float32,
                )
                pair_acc[keys_at, cols] += jnp.dot(
                    dscores, query_block, preferred_element_type=jnp.float32
                )
                result.append(carry[head] + dot32(key_block, dscores, TN))
            return tuple(result)

        carry = tuple(jnp.zeros((HEAD_DIM, bq), jnp.float32) for _ in range(heads))
        carry = lax.fori_loop(low, inner_low, functools.partial(step, True), carry)
        carry = lax.fori_loop(inner_low, inner_high, functools.partial(step, False), carry)
        carry = lax.fori_loop(inner_high, high, functools.partial(step, True), carry)
        for head in range(heads):
            query_out[rows, pl.ds(head * HEAD_DIM, HEAD_DIM)] = (
                carry[head].T * score_scale
            ).astype(jnp.bfloat16)
        return 0

    lax.fori_loop(0, blocks, one_block, 0)

    def flush(piece, _):
        at = pl.ds(pl.multiple_of(piece * bk, bk), bk)
        pair_out[at, :width] = (pair_acc[at, :width] * score_scale).astype(jnp.bfloat16)
        pair_out[at, width:] = pair_acc[at, width:].astype(jnp.bfloat16)
        return 0

    lax.fori_loop(0, pair_rows // bk, flush, 0)


def make_table(start, pos, bq, bk):
    starts, places = start.reshape(-1, bq), pos.reshape(-1, bq)
    low = starts[:, 0] // bk
    inner_low = (starts[:, -1] + bk - 1) // bk
    inner_high = jnp.maximum(inner_low, (places[:, 0] + 1) // bk)
    high = places[:, -1] // bk + 1
    return jnp.stack([low, inner_low, inner_high, high], axis=1).astype(jnp.int32)


def middle_kernel(
    number, part_ref, w_any, state_ref, probe_ref, grad_out, readout_out, w_ref, joined, half,
    sending, landing, send_sem, recv_sem, back_send, back_recv, w_sem,
):
    me = lax.axis_index("head")
    width = part_ref.shape[1]
    own = state_ref.shape[0]
    model = state_ref.shape[1]
    w_copy = pltpu.make_async_copy(w_any, w_ref, w_sem)
    w_copy.start()
    greet("head", number, me)
    my_cols = pl.ds(pl.multiple_of(me * width, width), width)
    my_rows = pl.ds(pl.multiple_of(me * own, own), own)
    copies = []
    for step in range(1, number):
        peer = lax.rem(me + step, number)
        copy = pltpu.make_async_remote_copy(
            src_ref=part_ref.at[pl.ds(pl.multiple_of(peer * own, own), own)],
            dst_ref=joined.at[:, my_cols],
            send_sem=send_sem.at[step],
            recv_sem=recv_sem.at[step],
            device_id={"head": peer},
            device_id_type=MESH,
        )
        copy.start()
        copies.append(copy)
    joined[:, my_cols] = part_ref[my_rows, :]
    w_copy.wait()
    for copy in copies:
        copy.wait()

    tile = min(256, model)

    def project(piece, carry):
        squares, products = carry
        cols = pl.ds(pl.multiple_of(piece * tile, tile), tile)
        layer = state_ref[:, cols].astype(jnp.float32) + jnp.dot(
            joined[...], w_ref[:, cols], preferred_element_type=jnp.float32
        )
        readout_out[:, cols] = layer
        squares = squares + jnp.sum(layer * layer, axis=1, keepdims=True)
        products = products + jnp.sum(
            layer * probe_ref[:, cols].astype(jnp.float32), axis=1, keepdims=True
        )
        return squares, products

    zero = jnp.zeros((own, 1), jnp.float32)
    squares, products = lax.fori_loop(0, model // tile, project, (zero, zero))
    scale = lax.rsqrt(squares / model + EPSILON)
    bend = scale**3 * (products / model)

    def finish(piece, _):
        cols = pl.ds(pl.multiple_of(piece * tile, tile), tile)
        readout = scale * probe_ref[:, cols].astype(jnp.float32) - readout_out[:, cols] * bend
        readout_out[:, cols] = readout
        half[:, cols] = readout.astype(jnp.bfloat16)
        return 0

    lax.fori_loop(0, model // tile, finish, 0)
    copies = []
    for step in range(1, number):
        peer = lax.rem(me + step, number)
        sending[step] = dot32(
            half[...], w_ref[pl.ds(pl.multiple_of(peer * width, width), width), :], NT
        ).astype(jnp.bfloat16)
        copy = pltpu.make_async_remote_copy(
            src_ref=sending.at[step],
            dst_ref=landing.at[my_rows],
            send_sem=back_send.at[step],
            recv_sem=back_recv.at[step],
            device_id={"head": peer},
            device_id_type=MESH,
        )
        copy.start()
        copies.append(copy)
    landing[my_rows, :] = dot32(half[...], w_ref[my_cols, :], NT).astype(jnp.bfloat16)
    for copy in copies:
        copy.wait()
    grad_out[...] = landing[...]


def middle(number, part, w_full, state_own, probe_own):
    rows, width = part.shape
    own, model = state_own.shape
    return pl.pallas_call(
        functools.partial(middle_kernel, number),
        out_shape=(
            jax.ShapeDtypeStruct((rows, width), jnp.bfloat16),
            jax.ShapeDtypeStruct((own, model), jnp.float32),
        ),
        in_specs=[VMEM, ANY, VMEM, VMEM],
        out_specs=(VMEM, VMEM),
        scratch_shapes=[
            pltpu.VMEM(w_full.shape, jnp.bfloat16),
            pltpu.VMEM((own, number * width), jnp.bfloat16),
            pltpu.VMEM((own, model), jnp.bfloat16),
            pltpu.VMEM((number, own, width), jnp.bfloat16),
            pltpu.VMEM((rows, width), jnp.bfloat16),
            pltpu.SemaphoreType.DMA((number,)),
            pltpu.SemaphoreType.DMA((number,)),
            pltpu.SemaphoreType.DMA((number,)),
            pltpu.SemaphoreType.DMA((number,)),
            pltpu.SemaphoreType.DMA,
        ],
        compiler_params=pltpu.CompilerParams(
            collective_id=1, has_side_effects=True, vmem_limit_bytes=60 * 2**20
        ),
    )(part, w_full, state_own, probe_own)


def tail_kernel(
    ctx_count, number, pair_any, query_ref, w_ref, sum_out, own_pair, arriving, gathered, terms,
    from_partner, reduced, landing, ctx_send, ctx_recv, p_send, p_recv, z_send, z_recv, own_sem,
):
    ctx, me = lax.axis_index("ctx"), lax.axis_index("head")
    groups = number // 2
    group, core = me // 2, lax.rem(me, 2)
    partner = group * 2 + 1 - core
    rows, width = query_ref.shape
    own, model = sum_out.shape
    chunk = 2 * own
    own_copy = pltpu.make_async_copy(
        pair_any.at[pl.ds(pl.multiple_of(ctx * rows, rows), rows)], own_pair, own_sem
    )
    own_copy.start()
    barrier = pltpu.get_barrier_semaphore()
    peers = [{"ctx": lax.rem(ctx + step, ctx_count)} for step in range(1, ctx_count)]
    peers.append({"head": partner})
    for step in range(1, groups):
        peers.append({"head": lax.rem(group + step, groups) * 2 + core})
    for peer in peers:
        pl.semaphore_signal(barrier, inc=1, device_id=peer, device_id_type=MESH)
    pl.semaphore_wait(barrier, len(peers))

    def chunk_start(order):
        dest = lax.rem(group + order + 1, groups)
        return dest, pl.multiple_of(dest * chunk, chunk)

    def ctx_copy(order, step):
        target = lax.rem(ctx - step + ctx_count, ctx_count)
        _, first = chunk_start(order)
        return pltpu.make_async_remote_copy(
            src_ref=pair_any.at[pl.ds(pl.multiple_of(target * rows + first, chunk), chunk)],
            dst_ref=arriving.at[order, step - 1],
            send_sem=ctx_send.at[order, step],
            recv_sem=ctx_recv.at[order, step],
            device_id={"ctx": target},
            device_id_type=MESH,
        )

    for order in range(groups):
        for step in range(1, ctx_count):

            @pl.when(step <= ctx)
            def _():
                ctx_copy(order, step).start()

    own_copy.wait()
    tile = min(512, model)
    mine = pl.ds(pl.multiple_of(core * own, own), own)
    theirs = pl.ds(pl.multiple_of((1 - core) * own, own), own)
    waiting = []
    for order in range(groups):
        dest, first = chunk_start(order)
        at = pl.ds(first, chunk)
        gathered[...] = own_pair[at, :].astype(jnp.float32)
        for step in range(1, ctx_count):

            @pl.when(ctx + step < ctx_count)
            def _():
                ctx_copy(order, step).wait_recv()
                gathered[...] += arriving[order, step - 1].astype(jnp.float32)

        def multiply(piece, _):
            cols = pl.ds(pl.multiple_of(piece * tile, tile), tile)
            term = dot32(query_ref[at, :], w_ref[0, cols, :], NT)
            term += dot32(gathered[:, :width].astype(jnp.bfloat16), w_ref[1, cols, :], NT)
            term += dot32(gathered[:, width:].astype(jnp.bfloat16), w_ref[2, cols, :], NT)
            terms[order, :, cols] = term.astype(jnp.bfloat16)
            return 0

        lax.fori_loop(0, model // tile, multiply, 0)
        copy = pltpu.make_async_remote_copy(
            src_ref=terms.at[order, theirs],
            dst_ref=from_partner.at[order],
            send_sem=p_send.at[order],
            recv_sem=p_recv.at[order],
            device_id={"head": partner},
            device_id_type=MESH,
        )
        copy.start()
        copy.wait()
        both = terms[order, mine, :].astype(jnp.float32) + from_partner[order].astype(jnp.float32)
        if order < groups - 1:
            reduced[order] = both.astype(jnp.bfloat16)
            copy = pltpu.make_async_remote_copy(
                src_ref=reduced.at[order],
                dst_ref=landing.at[order],
                send_sem=z_send.at[order],
                recv_sem=z_recv.at[order],
                device_id={"head": dest * 2 + core},
                device_id_type=MESH,
            )
            copy.start()
            waiting.append(copy)
        else:
            sum_out[...] = both
    for order, copy in enumerate(waiting):
        copy.wait()
        sum_out[...] += landing[order].astype(jnp.float32)
    for order in range(groups):
        for step in range(1, ctx_count):

            @pl.when(step <= ctx)
            def _():
                ctx_copy(order, step).wait_send()


def tail(ctx_count, number, pair, query_grad, w_qkv):
    rows, width = query_grad.shape
    model = w_qkv.shape[1]
    own, groups = rows // number, number // 2
    half, full = jnp.bfloat16, jnp.float32
    dma = pltpu.SemaphoreType.DMA
    return pl.pallas_call(
        functools.partial(tail_kernel, ctx_count, number),
        out_shape=jax.ShapeDtypeStruct((own, model), full),
        in_specs=[ANY, VMEM, VMEM],
        out_specs=VMEM,
        scratch_shapes=[
            pltpu.VMEM((rows, 2 * width), half),
            pltpu.VMEM((groups, ctx_count - 1, 2 * own, 2 * width), half),
            pltpu.VMEM((2 * own, 2 * width), full),
            pltpu.VMEM((groups, 2 * own, model), half),
            pltpu.VMEM((groups, own, model), half),
            pltpu.VMEM((groups, own, model), half),
            pltpu.VMEM((groups, own, model), half),
            dma((groups, ctx_count)),
            dma((groups, ctx_count)),
            dma((groups,)),
            dma((groups,)),
            dma((groups,)),
            dma((groups,)),
            dma,
        ],
        compiler_params=pltpu.CompilerParams(
            collective_id=2, has_side_effects=True, vmem_limit_bytes=60 * 2**20
        ),
    )(pair, query_grad, w_qkv)


def body(state, norm_gain, w_qkv, w_out, probe, noise, segment_ids):
    local_rows, model_width = state.shape
    width = w_qkv.shape[2]
    local_heads = width // HEAD_DIM
    head_count = lax.axis_size("head")
    ctx_count = lax.axis_size("ctx")
    ctx_index = lax.axis_index("ctx")
    own_rows = local_rows // head_count
    row_start = lax.axis_index("head") * own_rows
    w_full = lax.all_gather(w_out, "head", axis=0, tiled=True)
    state_f = state.astype(jnp.float32)
    gain_full = norm_gain.astype(jnp.float32)
    inverse = row_scale(state_f)
    normed = (state_f * inverse * gain_full).astype(jnp.bfloat16)

    def project(index):
        return jnp.dot(normed, w_qkv[index], preferred_element_type=jnp.float32).astype(
            jnp.bfloat16
        )

    key_rows, value_rows = project(1), project(2)
    keys, values, segs, query_rows = gather_keys(
        ctx_count, key_rows, value_rows, segment_ids, normed, w_qkv[0]
    )
    total_rows = keys.shape[0]
    pos = ctx_index * local_rows + jnp.arange(local_rows, dtype=jnp.int32)
    start = jnp.sum((segs[None, :] < segment_ids[:, None]).astype(jnp.int32), axis=1)
    fq, fk = (min(local_rows, size) for size in FORWARD_BLOCKS)
    gq, gk = (min(local_rows, size) for size in BACKWARD_BLOCKS)
    smem = pl.BlockSpec(memory_space=pltpu.SMEM)
    params = pltpu.CompilerParams(vmem_limit_bytes=60 * 2**20)
    outputs, logs = pl.pallas_call(
        functools.partial(forward_kernel, local_heads, fq, fk),
        out_shape=(
            jax.ShapeDtypeStruct((local_rows, width), jnp.bfloat16),
            jax.ShapeDtypeStruct((local_rows // fq, local_heads, fq), jnp.float32),
        ),
        in_specs=[smem] + [VMEM] * 5,
        out_specs=(VMEM, VMEM),
        compiler_params=params,
        cost_estimate=pl.CostEstimate(
            flops=4 * local_rows * total_rows * width, bytes_accessed=0, transcendentals=0
        ),
    )(
        make_table(start, pos, fq, fk),
        query_rows,
        keys,
        values,
        start.reshape(-1, 1, fq),
        pos.reshape(-1, 1, fq),
    )
    state_half = lax.dynamic_slice_in_dim(state, row_start, own_rows, 0)
    probe_own = lax.dynamic_slice_in_dim(probe, row_start, own_rows, 0)
    state_own = state_half.astype(jnp.float32)
    inverse_own = row_scale(state_own)
    grads_out, readout_own = middle(head_count, outputs, w_full, state_half, probe_own)
    query_grad, pair = pl.pallas_call(
        functools.partial(backward_kernel, local_heads, gq, gk),
        out_shape=(
            jax.ShapeDtypeStruct((local_rows, width), jnp.bfloat16),
            jax.ShapeDtypeStruct((total_rows, 2 * width), jnp.bfloat16),
        ),
        in_specs=[smem] + [VMEM] * 8,
        out_specs=(VMEM, VMEM),
        scratch_shapes=[pltpu.VMEM((total_rows, 2 * width), jnp.float32)],
        compiler_params=params,
        cost_estimate=pl.CostEstimate(
            flops=10 * local_rows * total_rows * width, bytes_accessed=0, transcendentals=0
        ),
    )(
        make_table(start, pos, gq, gk),
        query_rows,
        keys,
        values,
        grads_out,
        outputs,
        logs.reshape(local_rows // fq, local_heads, fq),
        start.reshape(-1, 1, gq),
        pos.reshape(-1, 1, gq),
    )
    normed_grad = tail(ctx_count, head_count, pair, query_grad, w_qkv)
    gain_grad = normed_grad * gain_full
    gradient = (
        readout_own
        + inverse_own * gain_grad
        - state_own * inverse_own**3 * jnp.mean(gain_grad * state_own, axis=-1, keepdims=True)
    )
    return state_own - STEP_SIZE * gradient + jnp.sqrt(2.0 * STEP_SIZE) * noise.astype(jnp.float32)


def remote(source, target, send_sem, recv_sem, ctx, head):
    return pltpu.make_async_remote_copy(
        src_ref=source,
        dst_ref=target,
        send_sem=send_sem,
        recv_sem=recv_sem,
        device_id={"ctx": ctx, "head": head},
        device_id_type=MESH,
    )


def place():
    ctx, me = lax.axis_index("ctx"), lax.axis_index("head")
    return ctx, me, me // 2, lax.rem(me, 2)


def announce(peers):
    barrier = pltpu.get_barrier_semaphore()
    for ctx, head in peers:
        pl.semaphore_signal(
            barrier, inc=1, device_id={"ctx": ctx, "head": head}, device_id_type=MESH
        )


def await_all(peers):
    pl.semaphore_wait(pltpu.get_barrier_semaphore(), len(peers))


def meet(peers):
    announce(peers)
    await_all(peers)


def far_first(groups, group, step):
    result = 0
    for index in range(groups):
        order = sorted(range(groups), key=lambda other: (-abs(other - index), -other))
        result = jnp.where(group == index, order[step], result)
    return result


def front_kernel(
    ctx_count, head_count, state_any, w_any, gain_ref, seg_ref, w_out_any, probe_any, query_any,
    kv_any, segs_out, part_any, log_out, grad_out, readout_any, w_pair, state_v, w_v, query_buf,
    kv_buf, w_ref, joined, half, sending, state_own, probe_own, query_out, kv_out, part_out,
    readout_out, load_sem, w_sem, q_send, q_recv, kv_send, kv_recv, pass_send, seg_send, seg_recv,
    line_send, line_recv, plane_send, plane_recv, beside_send, beside_recv, shard_send, shard_recv,
    shard_sem, out_send, out_recv, back_send, back_recv, own_sem, row_sem, pair_send, pair_recv,
    leave_sem,
):
    ctx, me, group, core = place()
    rows, model = state_any.shape
    own, groups = rows // head_count, head_count // 2
    slots = w_any.shape[2] // HEAD_DIM
    chunk = 2 * own
    partner = group * 2 + 1 - core

    def at(piece):
        return pl.ds(pl.multiple_of(piece * chunk, chunk), chunk)

    def own_at(piece):
        return pl.ds(pl.multiple_of(piece * own, own), own)

    def load_state(piece):
        return pltpu.make_async_copy(
            state_any.at[at(piece)], state_v.at[at(piece)], load_sem.at[piece]
        )

    load_state(0).start()
    w_loads = [pltpu.make_async_copy(w_any.at[t], w_v.at[t], w_sem.at[t]) for t in range(3)]
    for copy in w_loads:
        copy.start()
    for piece in range(1, groups):
        load_state(piece).start()
    my_rows = own_at(me)
    shard = w_out_any.shape[0]
    part, quarter = shard // 2, shard // ctx_count
    later_loads = [
        pltpu.make_async_copy(state_any.at[my_rows], state_own, row_sem.at[0]),
        pltpu.make_async_copy(probe_any.at[my_rows], probe_own, row_sem.at[1]),
        pltpu.make_async_copy(
            w_out_any, w_ref.at[pl.ds(pl.multiple_of(me * shard, shard), shard)], shard_sem
        ),
    ]
    for copy in later_loads:
        copy.start()
    peers = [(lax.rem(ctx + step, ctx_count), partner) for step in range(ctx_count)]
    for far in range(groups):
        for step in range(ctx_count):
            if far or step:
                peers.append(
                    (lax.rem(ctx + step, ctx_count), lax.rem(group + far, groups) * 2 + core)
                )
    announce(peers)

    low, high = lax.rem(ctx, 2), ctx // 2
    which = lax.rem(low + high, 2)
    across, along = high * 2 + 1 - low, (1 - high) * 2 + low

    def shard_rows(origin, first, size):
        return pl.ds(pl.multiple_of((origin * 2 + core) * shard + first, size), size)

    def line_copy(way, origin, axis, mine):
        first = which * part + axis * quarter
        here = shard_rows(origin, first, quarter)
        source = (
            w_out_any.at[pl.ds(pl.multiple_of(first, quarter), quarter)] if mine else w_ref.at[here]
        )
        other = group + 1 if way == 0 else group - 1
        return remote(
            source, w_ref.at[here], line_send.at[way, axis, origin], line_recv.at[axis, origin],
            ctx, other * 2 + core,
        )

    def plane_copy(axis, origin, kept):
        here = shard_rows(origin, kept * part + axis * quarter, quarter)
        return remote(
            w_ref.at[here], w_ref.at[here], plane_send.at[axis, origin],
            plane_recv.at[axis, origin], along if axis else across, me,
        )

    def beside_copy(kind, origin):
        kept = which if kind < 2 else 1 - which
        here = shard_rows(origin, kept * part + (kind % 2) * quarter, quarter)
        return remote(
            w_ref.at[here], w_ref.at[here], beside_send.at[kind, origin],
            beside_recv.at[kind, origin], ctx, partner,
        )

    def shard_copy():
        return remote(
            w_out_any, w_ref.at[pl.ds(pl.multiple_of(me * shard, shard), shard)], shard_send,
            shard_recv, ctx, partner,
        )

    has_up, has_down = group < groups - 1, group > 0

    def each_origin(distance, work):
        for way in range(2):
            origin = group - distance if way == 0 else group + distance

            @pl.when(origin >= 0 if way == 0 else origin < groups)
            def _():
                work(way, origin)

    def line_arrived(distance, axis):
        def work(way, origin):
            line_copy(way, origin, axis, False).wait_recv()

            @pl.when(has_up if way == 0 else has_down)
            def _():
                line_copy(way, origin, axis, False).start()

            plane_copy(axis, origin, which).start()
            beside_copy(axis, origin).start()

        each_origin(distance, work)

    def plane_arrived(distance, axis):
        def work(way, origin):
            plane_copy(axis, origin, 1 - which).wait_recv()
            beside_copy(2 + axis, origin).start()

        each_origin(distance, work)

    def weights_sent(distance):
        def work(way, origin):
            for axis in range(2):

                @pl.when(has_up if way == 0 else has_down)
                def _():
                    line_copy(way, origin, axis, False).wait_send()

                plane_copy(axis, origin, which).wait_send()
            for kind in range(4):
                beside_copy(kind, origin).wait_send()

        each_origin(distance, work)

    def own_lines(work):
        for axis in range(2):

            @pl.when(has_up)
            def _():
                work(line_copy(0, group, axis, True))

            @pl.when(has_down)
            def _():
                work(line_copy(1, group, axis, True))

    for copy in w_loads:
        copy.wait()
    gain = gain_ref[...].astype(jnp.float32).reshape(1, model)

    def away(slot, kind, piece, dest):
        head = group * 2 + kind
        return (
            remote(
                query_buf.at[slot, piece, kind], query_out.at[ctx, own_at(piece)],
                q_send.at[slot, kind, piece], q_recv.at[ctx, piece], dest, head,
            ),
            remote(
                kv_buf.at[slot, kind, piece], kv_out.at[kind, ctx, at(piece)],
                kv_send.at[slot, kind, piece], kv_recv.at[kind, ctx, piece], dest, head,
            ),
        )

    def beside(slot, piece):
        result = [
            remote(
                query_buf.at[slot, piece, 1 - core], query_out.at[ctx, own_at(piece)],
                q_send.at[slot, 1 - core, piece], q_recv.at[ctx, piece], ctx, partner,
            )
        ]
        for kind in range(2):
            result.append(
                remote(
                    kv_buf.at[slot, kind, piece], kv_out.at[kind, ctx, at(piece)],
                    kv_send.at[slot, kind, piece], kv_recv.at[kind, ctx, piece], ctx, partner,
                )
            )
        return result

    def project(piece):
        load_state(piece).wait()
        block = state_v[at(piece), :].astype(jnp.float32)
        normed = (block * row_scale(block) * gain).astype(jnp.bfloat16)
        for t in range(3):
            result = jnp.dot(normed, w_v[t], preferred_element_type=jnp.float32).astype(
                jnp.bfloat16
            )
            for slot in range(slots):
                cut = result[:, slot * HEAD_DIM : (slot + 1) * HEAD_DIM]
                if t == 0:
                    query_buf[slot, piece, 0] = cut[:own]
                    query_buf[slot, piece, 1] = cut[own:]
                else:
                    kv_buf[slot, t - 1, piece] = cut

    def send_heads(piece):
        for slot in range(slots):
            dest = core * slots + slot

            @pl.when(dest != ctx)
            def _():
                for kind in range(2):
                    for copy in away(slot, kind, piece, dest):
                        copy.start()

            @pl.when(dest == ctx)
            def _():
                query_out[ctx, own_at(piece), :] = query_buf[slot, piece, core]
                for kind in range(2):
                    kv_out[kind, ctx, at(piece), :] = kv_buf[slot, kind, piece]
                for copy in beside(slot, piece):
                    copy.start()

    project(0)
    await_all(peers)
    own_lines(lambda copy: copy.start())
    send_heads(0)
    shard_copy().start()
    segs = []
    for step in range(1, ctx_count):
        copy = remote(
            seg_ref, segs_out.at[ctx], seg_send.at[step], seg_recv.at[step],
            lax.rem(ctx + step, ctx_count), me,
        )
        copy.start()
        segs.append(copy)
    segs_out[ctx] = seg_ref[...]

    def project_and_send(piece, _):
        project(piece)
        send_heads(piece)
        return 0

    lax.fori_loop(1, groups, project_and_send, 0)

    def hand_over(piece, step):
        source = lax.rem(ctx + step, ctx_count)
        return remote(
            kv_out.at[core, source, at(piece)], kv_out.at[core, source, at(piece)],
            pass_send.at[step, piece], kv_recv.at[core, source, piece], ctx, partner,
        )

    for piece in range(groups):
        for step in range(1, ctx_count):
            copy = hand_over(piece, step)
            copy.wait_recv()
            copy.start()
        if piece == 0:
            line_arrived(1, 0)
        if piece == min(2, groups - 1):
            line_arrived(1, 1)
    line_arrived(2, 0)

    def got_query(source, piece):
        remote(
            query_out.at[source, own_at(piece)], query_out.at[source, own_at(piece)],
            q_send.at[0, 0, piece], q_recv.at[source, piece], ctx, partner,
        ).wait_recv()

    def got_kv(kind, source, piece):
        remote(
            kv_out.at[kind, source, at(piece)], kv_out.at[kind, source, at(piece)],
            kv_send.at[0, 0, piece], kv_recv.at[kind, source, piece], ctx, partner,
        ).wait_recv()

    def gather(piece, _):
        for step in range(1, ctx_count):
            source = lax.rem(ctx + step, ctx_count)
            got_query(source, piece)
            got_kv(1 - core, source, piece)
            hand_over(piece, step).wait_send()

        @pl.when(ctx // slots != core)
        def _():
            got_query(ctx, piece)
            for kind in range(2):
                got_kv(kind, ctx, piece)

        return 0

    lax.fori_loop(0, groups, gather, 0)
    for copy in segs:
        copy.wait()
    leaving = [
        pltpu.make_async_copy(query_out, query_any, leave_sem.at[0]),
        pltpu.make_async_copy(kv_out, kv_any, leave_sem.at[1]),
    ]
    for copy in leaving:
        copy.start()
    pair_copy = remote(w_any, w_pair, pair_send, pair_recv, ctx, partner)
    pair_copy.start()

    def cols_of(group_at, ctx_at):
        head = group_at * ctx_count + ctx_at
        return pl.ds(pl.multiple_of(head * HEAD_DIM, HEAD_DIM), HEAD_DIM)

    factor = HEAD_DIM ** (-0.5) * LOG2E
    sub = groups * own
    seg_all = segs_out[...]

    def below(value):
        count = jnp.where(seg_all < value, 1.0, 0.0)
        for axis in (0, 1, 2):
            count = jnp.sum(count, axis=axis, keepdims=True)
        return count[0]

    first_bound, second_bound = below(1), below(2)
    lane = lax.broadcasted_iota(jnp.int32, (1, sub), 1)
    inside = (lane // own) * (2 * own) + core * own + lane % own
    key_row = lax.broadcasted_iota(jnp.int32, (rows, sub), 0)

    def out_copy(tile, order, other):
        return remote(
            part_out.at[tile, own_at(other)], joined.at[:, cols_of(group, ctx)],
            out_send.at[tile, order], out_recv.at[group, ctx], tile, other * 2 + core,
        )

    def one_tile(tile, _):
        query = query_out[tile]
        pos = (tile * rows + inside).astype(jnp.float32)
        start = jnp.where(
            pos >= second_bound, second_bound, jnp.where(pos >= first_bound, first_bound, 0.0)
        ).astype(jnp.int32)

        def step(diagonal, piece, carry):
            top, total, acc = carry
            scores = dot32(kv_out[0, piece], query, NT)
            allowed = key_row >= start - piece * rows
            if diagonal:
                allowed = allowed & (key_row <= inside)
            scores = jnp.where(allowed, scores, NEGATIVE)
            new_top = jnp.maximum(top, jnp.max(scores, axis=0, keepdims=True) * factor)
            weights = jnp.exp2(scores * factor - new_top)
            scale = jnp.exp2(top - new_top)
            total = total * scale + jnp.sum(weights, axis=0, keepdims=True)
            acc = acc * scale + dot32(kv_out[1, piece], weights.astype(jnp.bfloat16), TN)
            return new_top, total, acc

        carry = (
            jnp.full((1, sub), NEGATIVE, jnp.float32),
            jnp.zeros((1, sub), jnp.float32),
            jnp.zeros((HEAD_DIM, sub), jnp.float32),
        )
        carry = lax.fori_loop(0, tile, functools.partial(step, False), carry)
        top, total, acc = step(True, tile, carry)
        part_out[tile] = (acc / total).T.astype(jnp.bfloat16)
        log_out[tile] = top + jnp.log2(total)
        for order in range(groups):
            other = far_first(groups, group, order)
            if order == groups - 1:

                @pl.when(tile != ctx)
                def _():
                    out_copy(tile, order, other).start()

                @pl.when(tile == ctx)
                def _():
                    joined[:, cols_of(group, ctx)] = part_out[tile, own_at(group), :]

            else:
                out_copy(tile, order, other).start()

        @pl.when(tile == 1)
        def _():
            line_arrived(2, 1)

        return 0

    lax.fori_loop(0, ctx_count, one_tile, 0)
    leaving.append(pltpu.make_async_copy(part_out, part_any, leave_sem.at[2]))
    leaving[-1].start()
    for copy in later_loads:
        copy.wait()
    sources = []
    for far in range(groups):
        for step in range(ctx_count):
            if far or step:
                sources.append((lax.rem(group + far, groups), lax.rem(ctx + step, ctx_count)))
    tile = min(256, model)
    wide = ctx_count * HEAD_DIM
    zero = jnp.zeros((own, 1), jnp.float32)
    for axis in range(2):
        plane_arrived(1, axis)
    for distance in range(3, groups):
        line_arrived(distance, 0)
    for axis in range(2):
        plane_arrived(2, axis)
    for distance in range(3, groups):
        line_arrived(distance, 1)
    shard_copy().wait_recv()

    def heads_arrived(order):
        other = far_first(groups, group, order)
        if order < groups - 1:
            for kind in range(4):
                beside_copy(kind, other).wait_recv()
        for step in range(ctx_count):
            if order < groups - 1 or step:
                peer = lax.rem(ctx + step, ctx_count)
                remote(
                    part_out.at[0, own_at(0)], joined.at[:, cols_of(other, peer)],
                    out_send.at[0, 0], out_recv.at[other, peer], peer, other * 2 + core,
                ).wait_recv()

    for order in range(groups - 1, 0, -1):
        heads_arrived(order)
    farthest = far_first(groups, group, 0)
    near = pl.ds(pl.multiple_of(jnp.where(farthest == 0, wide, 0), wide), model - wide)
    far = pl.ds(pl.multiple_of(farthest * wide, wide), wide)

    def near_layer(piece, _):
        cols = pl.ds(pl.multiple_of(piece * tile, tile), tile)
        readout_out[:, cols] = state_own[:, cols].astype(jnp.float32) + jnp.dot(
            joined[:, near], w_ref[near, cols], preferred_element_type=jnp.float32
        )
        return 0

    lax.fori_loop(0, model // tile, near_layer, 0)
    for distance in range(3, groups):
        for axis in range(2):
            plane_arrived(distance, axis)
    heads_arrived(0)

    def layer(piece, carry):
        squares, products = carry
        cols = pl.ds(pl.multiple_of(piece * tile, tile), tile)
        result = readout_out[:, cols] + jnp.dot(
            joined[:, far], w_ref[far, cols], preferred_element_type=jnp.float32
        )
        readout_out[:, cols] = result
        squares = squares + jnp.sum(result * result, axis=1, keepdims=True)
        products = products + jnp.sum(
            result * probe_own[:, cols].astype(jnp.float32), axis=1, keepdims=True
        )
        return squares, products

    squares, products = lax.fori_loop(0, model // tile, layer, (zero, zero))
    scale = lax.rsqrt(squares / model + EPSILON)
    bend = scale**3 * (products / model)

    def finish(piece, _):
        cols = pl.ds(pl.multiple_of(piece * tile, tile), tile)
        readout = scale * probe_own[:, cols].astype(jnp.float32) - readout_out[:, cols] * bend
        readout_out[:, cols] = readout
        half[:, cols] = readout.astype(jnp.bfloat16)
        return 0

    lax.fori_loop(0, model // tile, finish, 0)
    leaving.append(pltpu.make_async_copy(readout_out, readout_any, leave_sem.at[3]))
    leaving[-1].start()
    copies = []
    for order in range(groups):
        other = far_first(groups, group, order)
        result = dot32(
            half[...], w_ref[pl.ds(pl.multiple_of(other * wide, wide), wide), :], NT
        ).astype(jnp.bfloat16)
        for index in range(ctx_count):
            sending[order, index] = result[:, index * HEAD_DIM : (index + 1) * HEAD_DIM]
        for step in range(ctx_count):
            peer = lax.rem(ctx + step, ctx_count)
            if order == groups - 1 and step == 0:
                continue
            copy = remote(
                sending.at[order, peer], grad_out.at[ctx, group], back_send.at[order, step],
                back_recv.at[ctx, group], peer, other * 2 + core,
            )
            copy.start()
            copies.append(copy)
    last = pltpu.make_async_copy(sending.at[groups - 1, ctx], grad_out.at[ctx, group], own_sem)
    last.start()

    def sent(piece, _):
        for slot in range(slots):
            dest = core * slots + slot

            @pl.when(dest != ctx)
            def _():
                for kind in range(2):
                    for copy in away(slot, kind, piece, dest):
                        copy.wait_send()

            @pl.when(dest == ctx)
            def _():
                for copy in beside(slot, piece):
                    copy.wait_send()

        return 0

    lax.fori_loop(0, groups, sent, 0)

    own_lines(lambda copy: copy.wait_send())
    shard_copy().wait_send()
    for distance in range(1, groups):
        weights_sent(distance)

    def parts_sent(tile, _):
        for order in range(groups):
            other = far_first(groups, group, order)
            if order == groups - 1:

                @pl.when(tile != ctx)
                def _():
                    out_copy(tile, order, other).wait_send()

            else:
                out_copy(tile, order, other).wait_send()
        return 0

    lax.fori_loop(0, ctx_count, parts_sent, 0)
    for other, peer in sources:
        remote(
            sending.at[0, 0], grad_out.at[peer, other], back_send.at[0, 0],
            back_recv.at[peer, other], peer, other * 2 + core,
        ).wait_recv()
    for copy in copies:
        copy.wait_send()
    last.wait()
    for copy in leaving:
        copy.wait()
    pair_copy.wait()


def front(ctx_count, head_count, state, w_qkv, gain, segment_ids, w_out, probe):
    rows, model = state.shape
    width = w_qkv.shape[2]
    own, groups, slots = rows // head_count, head_count // 2, width // HEAD_DIM
    seg = segment_ids.reshape(-1, 128)
    half, full, dma = jnp.bfloat16, jnp.float32, pltpu.SemaphoreType.DMA
    shape = jax.ShapeDtypeStruct
    return pl.pallas_call(
        functools.partial(front_kernel, ctx_count, head_count),
        out_shape=(
            shape((ctx_count, groups * own, HEAD_DIM), half),
            shape((2, ctx_count, rows, HEAD_DIM), half),
            shape((ctx_count,) + seg.shape, seg.dtype),
            shape((ctx_count, groups * own, HEAD_DIM), half),
            shape((ctx_count, 1, groups * own), full),
            shape((ctx_count, groups, own, HEAD_DIM), half),
            shape((own, model), full),
            shape(w_qkv.shape, half),
        ),
        in_specs=[ANY, ANY, VMEM, VMEM, ANY, ANY],
        out_specs=(ANY, ANY, VMEM, ANY, VMEM, ANY, ANY, ANY),
        scratch_shapes=[
            pltpu.VMEM((rows, model), half),
            pltpu.VMEM(w_qkv.shape, half),
            pltpu.VMEM((slots, groups, 2, own, HEAD_DIM), half),
            pltpu.VMEM((slots, 2, groups, 2 * own, HEAD_DIM), half),
            pltpu.VMEM((model, model), half),
            pltpu.VMEM((own, model), half),
            pltpu.VMEM((own, model), half),
            pltpu.VMEM((groups, ctx_count, own, HEAD_DIM), half),
            pltpu.VMEM((own, model), half),
            pltpu.VMEM((own, model), half),
            pltpu.VMEM((ctx_count, groups * own, HEAD_DIM), half),
            pltpu.VMEM((2, ctx_count, rows, HEAD_DIM), half),
            pltpu.VMEM((ctx_count, groups * own, HEAD_DIM), half),
            pltpu.VMEM((own, model), full),
            dma((groups,)),
            dma((3,)),
            dma((slots, 2, groups)),
            dma((ctx_count, groups)),
            dma((slots, 2, groups)),
            dma((2, ctx_count, groups)),
            dma((ctx_count, groups)),
            dma((ctx_count,)),
            dma((ctx_count,)),
            dma((2, 2, groups)),
            dma((2, groups)),
            dma((2, groups)),
            dma((2, groups)),
            dma((4, groups)),
            dma((4, groups)),
            dma,
            dma,
            dma,
            dma((ctx_count, groups)),
            dma((groups, ctx_count)),
            dma((groups, ctx_count)),
            dma((ctx_count, groups)),
            dma,
            dma((2,)),
            dma,
            dma,
            dma((4,)),
        ],
        compiler_params=pltpu.CompilerParams(
            collective_id=0, has_side_effects=True, vmem_limit_bytes=62 * 2**20
        ),
    )(state, w_qkv, gain, seg, w_out, probe)


def segment_bounds(segs_ref):
    segs = segs_ref[...]

    def below(value):
        return jnp.sum(jnp.where(segs < value, 1.0, 0.0)).astype(jnp.int32)

    return below(1), below(2)


def tile_plan(bounds, rows, own, parts, sub, bk, tile, core):
    first_bound, second_bound = bounds

    def start_of(pos):
        return jnp.where(pos >= second_bound, second_bound, jnp.where(pos >= first_bound, first_bound, 0))

    blocks = sub // own
    base = tile * rows + core * own
    places = []
    for part in range(parts):
        lane = lax.broadcasted_iota(jnp.int32, (1, sub), 1)
        pos = base + (lane // own + part * blocks) * (2 * own) + lane % own
        places.append((start_of(pos), pos))
    first, last = base, base + (parts * blocks - 1) * 2 * own + own - 1
    low = start_of(first) // bk
    inner_low = (start_of(last) + bk - 1) // bk
    inner_high = jnp.maximum(inner_low, (first + 1) // bk)
    high = last // bk + 1
    return places, low, inner_low, inner_high, high


def head_backward_kernel(
    rows, own, parts, sub, bk, segs_ref, query_ref, kv_ref, grad_ref, out_ref, log_ref, query_out,
    pair_out, pair_acc,
):
    score_scale = HEAD_DIM ** (-0.5)
    factor = score_scale * LOG2E
    core = lax.rem(lax.axis_index("head"), 2)
    bounds = segment_bounds(segs_ref)
    tiles = query_ref.shape[0] // (parts * sub)
    pair_rows = pair_acc.shape[0]

    def clear(piece, _):
        at = pl.ds(pl.multiple_of(piece * bk, bk), bk)
        pair_acc[at, :] = jnp.zeros((bk, 2 * HEAD_DIM), jnp.float32)
        return 0

    lax.fori_loop(0, pair_rows // bk, clear, 0)

    def one_tile(tile, _):
        places, low, inner_low, inner_high, high = tile_plan(
            bounds, rows, own, parts, sub, bk, tile, core
        )

        def at(part):
            return pl.ds(pl.multiple_of((tile * parts + part) * sub, sub), sub)

        deltas, logs = [], []
        for part in range(parts):
            product = grad_ref[at(part), :].astype(jnp.float32) * out_ref[at(part), :].astype(
                jnp.float32
            )
            deltas.append(jnp.sum(product.T, axis=0, keepdims=True))
            logs.append(log_ref[tile, pl.ds(part, 1), :])

        def step(masked, piece, carry):
            keys_at = pl.ds(pl.multiple_of(piece * bk, bk), bk)
            if masked:
                key_pos = piece * bk + lax.broadcasted_iota(jnp.int32, (bk, sub), 0)
            result = []
            key_block, value_block = kv_ref[0, keys_at, :], kv_ref[1, keys_at, :]
            for part in range(parts):
                query_block, grad_block = query_ref[at(part), :], grad_ref[at(part), :]
                scores = dot32(key_block, query_block, NT)
                probabilities = jnp.exp2(scores * factor - logs[part])
                if masked:
                    start, pos = places[part]
                    probabilities = jnp.where(
                        (key_pos >= start) & (key_pos <= pos), probabilities, 0.0
                    )
                dprobs = dot32(value_block, grad_block, NT)
                dscores = (probabilities * (dprobs - deltas[part])).astype(jnp.bfloat16)
                pair_acc[keys_at, HEAD_DIM:] += jnp.dot(
                    probabilities.astype(jnp.bfloat16),
                    grad_block,
                    preferred_element_type=jnp.float32,
                )
                pair_acc[keys_at, :HEAD_DIM] += jnp.dot(
                    dscores, query_block, preferred_element_type=jnp.float32
                )
                result.append(carry[part] + dot32(key_block, dscores, TN))
            return tuple(result)

        carry = tuple(jnp.zeros((HEAD_DIM, sub), jnp.float32) for _ in range(parts))
        carry = lax.fori_loop(low, inner_low, functools.partial(step, True), carry)
        carry = lax.fori_loop(inner_low, inner_high, functools.partial(step, False), carry)
        carry = lax.fori_loop(inner_high, high, functools.partial(step, True), carry)
        for part in range(parts):
            query_out[at(part), :] = (carry[part].T * score_scale).astype(jnp.bfloat16)
        return 0

    lax.fori_loop(0, tiles, one_tile, 0)

    def flush(piece, _):
        at = pl.ds(pl.multiple_of(piece * bk, bk), bk)
        pair_out[at, :HEAD_DIM] = (pair_acc[at, :HEAD_DIM] * score_scale).astype(jnp.bfloat16)
        pair_out[at, HEAD_DIM:] = pair_acc[at, HEAD_DIM:].astype(jnp.bfloat16)
        return 0

    lax.fori_loop(0, pair_rows // bk, flush, 0)


def finish_kernel(
    ctx_count, head_count, query_ref, pair_ref, w_any, w_pair, state_any, noise_ref, readout_ref,
    gain_ref, new_out, w_both, beside, away, terms_in, partial, sending, total, state_own, b_send,
    b_recv, a_send, a_recv, z_send, z_recv, own_sem,
):
    ctx, me, group, core = place()
    groups = head_count // 2
    own, model = new_out.shape
    slots = ctx_count // 2
    partner = group * 2 + 1 - core
    my_rows = pl.ds(pl.multiple_of(me * own, own), own)
    loads = [
        pltpu.make_async_copy(w_any, w_both.at[core], own_sem.at[0]),
        pltpu.make_async_copy(w_pair, w_both.at[1 - core], own_sem.at[1]),
        pltpu.make_async_copy(state_any.at[my_rows], state_own, own_sem.at[2]),
    ]
    for copy in loads:
        copy.start()
    peers = [(ctx, partner)]
    peers += [(lax.rem(ctx + step, ctx_count), me) for step in range(1, ctx_count)]
    peers += [(ctx, lax.rem(group + far, groups) * 2 + core) for far in range(1, groups)]
    meet(peers)
    dests = [far_first(groups, group, order) for order in range(groups)]
    copies = []
    for order, dest in enumerate(dests):
        copy = remote(
            pair_ref.at[:, dest, 1 - core], beside.at[order], b_send.at[order], b_recv.at[order],
            ctx, partner,
        )
        copy.start()
        copies.append(copy)

    def stripe(source):
        slot = lax.rem(source, slots)
        return pl.ds(pl.multiple_of(slot * HEAD_DIM, HEAD_DIM), HEAD_DIM)

    def exchange(order, dest, step):
        peer = lax.rem(ctx + step, ctx_count)
        return remote(
            away.at[order, step], terms_in.at[dest, ctx // slots, :, :, stripe(ctx)],
            a_send.at[order, step], a_recv.at[dest, ctx], peer, me,
        )

    def arrived(dest, step):
        source = lax.rem(ctx + step, ctx_count)
        remote(
            away.at[0, 0], terms_in.at[dest, source // slots, :, :, stripe(source)],
            a_send.at[0, 0], a_recv.at[dest, source], source, me,
        ).wait_recv()

    for order, dest in enumerate(dests):
        copies[order].wait_recv()
        for step in range(1, ctx_count):
            peer = lax.rem(ctx + step, ctx_count)
            pair = pair_ref[peer, dest, core].astype(jnp.float32) + beside[order, peer].astype(
                jnp.float32
            )
            pair = pair.astype(jnp.bfloat16)
            away[order, step, 0] = query_ref[peer, dest]
            away[order, step, 1] = pair[:, :HEAD_DIM]
            away[order, step, 2] = pair[:, HEAD_DIM:]
            exchange(order, dest, step).start()
        pair = pair_ref[ctx, dest, core].astype(jnp.float32) + beside[order, ctx].astype(
            jnp.float32
        )
        pair = pair.astype(jnp.bfloat16)
        at = stripe(ctx)
        terms_in[dest, ctx // slots, 0, :, at] = query_ref[ctx, dest]
        terms_in[dest, ctx // slots, 1, :, at] = pair[:, :HEAD_DIM]
        terms_in[dest, ctx // slots, 2, :, at] = pair[:, HEAD_DIM:]
    for copy in loads:
        copy.wait()
    pieces = partial.shape[2]
    tile = model // pieces

    def chain(order, dest, piece):
        up = dest > group
        line = jnp.where(up, 0, 1)
        peer = jnp.where(up, group + 1, group - 1)
        return remote(
            sending.at[order, piece], partial.at[line, dest, piece], z_send.at[order, piece],
            z_recv.at[line, dest, piece], ctx, peer * 2 + core,
        )

    def came(line, dest, piece):
        remote(
            sending.at[0, piece], partial.at[line, dest, piece], z_send.at[0, piece],
            z_recv.at[line, dest, piece], ctx, partner,
        ).wait_recv()

    def term(dest, piece):
        cols = pl.ds(pl.multiple_of(piece * tile, tile), tile)
        result = None
        for half in range(2):
            for kind in range(3):
                part = dot32(terms_in[dest, half, kind], w_both[half, kind, cols, :], NT)
                result = part if result is None else result + part
        return result

    for order, dest in enumerate(dests[:-1]):
        for step in range(1, ctx_count):
            arrived(dest, step)
        line = jnp.where(dest > group, 0, 1)
        inner = (group > 0) & (group < groups - 1)

        def one_piece(piece, _):
            total[...] = term(dest, piece)

            @pl.when(inner)
            def _():
                came(line, dest, piece)
                total[...] += partial[line, dest, piece].astype(jnp.float32)

            sending[order, piece] = total[...].astype(jnp.bfloat16)
            chain(order, dest, piece).start()
            return 0

        lax.fori_loop(0, pieces, one_piece, 0)

    for step in range(1, ctx_count):
        arrived(group, step)

    state = state_own[...].astype(jnp.float32)
    inverse = row_scale(state)

    def last_piece(piece, slope):
        cols = pl.ds(pl.multiple_of(piece * tile, tile), tile)
        total[...] = term(group, piece)

        @pl.when(group > 0)
        def _():
            came(0, group, piece)
            total[...] += partial[0, group, piece].astype(jnp.float32)

        @pl.when(group < groups - 1)
        def _():
            came(1, group, piece)
            total[...] += partial[1, group, piece].astype(jnp.float32)

        gained = total[...] * gain_ref[cols].astype(jnp.float32).reshape(1, tile)
        new_out[:, cols] = gained
        return slope + jnp.sum(
            gained * state_own[:, cols].astype(jnp.float32), axis=1, keepdims=True
        )

    slope = lax.fori_loop(0, pieces, last_piece, jnp.zeros((own, 1), jnp.float32))
    bend = inverse**3 * (slope / model)

    def update(piece, _):
        cols = pl.ds(pl.multiple_of(piece * tile, tile), tile)
        here = state_own[:, cols].astype(jnp.float32)
        gradient = readout_ref[:, cols] + inverse * new_out[:, cols] - here * bend
        new_out[:, cols] = (
            here - STEP_SIZE * gradient + NOISE_SCALE * noise_ref[:, cols].astype(jnp.float32)
        )
        return 0

    lax.fori_loop(0, pieces, update, 0)
    for order, dest in enumerate(dests):
        copies[order].wait_send()
        for step in range(1, ctx_count):
            exchange(order, dest, step).wait_send()
        if order < groups - 1:
            for piece in range(pieces):
                chain(order, dest, piece).wait_send()


def finish_step(
    ctx_count, head_count, query_grad, pair, w_qkv, w_pair, state, noise, readout, gain
):
    own, model = readout.shape
    width = w_qkv.shape[2]
    groups, pieces = head_count // 2, 4
    half, full, dma = jnp.bfloat16, jnp.float32, pltpu.SemaphoreType.DMA
    tile = model // pieces
    return pl.pallas_call(
        functools.partial(finish_kernel, ctx_count, head_count),
        out_shape=jax.ShapeDtypeStruct((own, model), full),
        in_specs=[VMEM, VMEM, ANY, ANY, ANY, VMEM, VMEM, VMEM],
        out_specs=VMEM,
        scratch_shapes=[
            pltpu.VMEM((2,) + w_qkv.shape, half),
            pltpu.VMEM((groups, ctx_count, own, 2 * HEAD_DIM), half),
            pltpu.VMEM((groups, ctx_count, 3, own, HEAD_DIM), half),
            pltpu.VMEM((groups, 2, 3, own, width), half),
            pltpu.VMEM((2, groups, pieces, own, tile), half),
            pltpu.VMEM((groups, pieces, own, tile), half),
            pltpu.VMEM((own, tile), full),
            pltpu.VMEM((own, model), half),
            dma((groups,)),
            dma((groups,)),
            dma((groups, ctx_count)),
            dma((groups, ctx_count)),
            dma((groups, pieces)),
            dma((2, groups, pieces)),
            dma((3,)),
        ],
        compiler_params=pltpu.CompilerParams(
            collective_id=2, has_side_effects=True, vmem_limit_bytes=60 * 2**20
        ),
    )(query_grad, pair, w_qkv, w_pair, state, noise, readout, gain)


def heads_body(state, norm_gain, w_qkv, w_out, probe, noise, segment_ids):
    rows, model = state.shape
    head_count, ctx_count = lax.axis_size("head"), lax.axis_size("ctx")
    own, groups = rows // head_count, head_count // 2
    queries, kv, segs, outputs, logs, grads_out, readout, w_pair = front(
        ctx_count, head_count, state, w_qkv, norm_gain, segment_ids, w_out, probe
    )
    mine, total = ctx_count * groups * own, ctx_count * rows
    parts, sub, bk = 1, groups * own, min(rows, 512)
    query_grad, pair = pl.pallas_call(
        functools.partial(head_backward_kernel, rows, own, parts, sub, bk),
        out_shape=(
            jax.ShapeDtypeStruct((mine, HEAD_DIM), jnp.bfloat16),
            jax.ShapeDtypeStruct((total, 2 * HEAD_DIM), jnp.bfloat16),
        ),
        in_specs=[VMEM] * 6,
        out_specs=(VMEM, VMEM),
        scratch_shapes=[pltpu.VMEM((total, 2 * HEAD_DIM), jnp.float32)],
        compiler_params=pltpu.CompilerParams(vmem_limit_bytes=60 * 2**20),
        cost_estimate=pl.CostEstimate(
            flops=10 * mine * total * HEAD_DIM, bytes_accessed=0, transcendentals=0
        ),
    )(
        segs, queries.reshape(mine, HEAD_DIM), kv.reshape(2, total, HEAD_DIM),
        grads_out.reshape(mine, HEAD_DIM), outputs.reshape(mine, HEAD_DIM), logs,
    )
    return finish_step(
        ctx_count, head_count, query_grad.reshape(ctx_count, groups, own, HEAD_DIM),
        pair.reshape(ctx_count, groups, 2, own, 2 * HEAD_DIM), w_qkv, w_pair, state, noise, readout,
        norm_gain,
    )


def solution(mesh):
    placed = (
        P("ctx", None),
        P(),
        P(None, None, "head"),
        P("head", None),
        P("ctx", None),
        P(("ctx", "head"), None),
        P("ctx"),
    )

    def step(*args):
        heads = args[2].shape[2] // HEAD_DIM
        return (heads_body if lax.axis_size("ctx") == 2 * heads == 4 else body)(*args)

    return jax.shard_map(
        step, mesh=mesh, in_specs=placed, out_specs=P(("ctx", "head"), None), check_vma=False
    )
```

```python
import functools

import jax
import jax.numpy as jnp
from jax import lax
from jax.experimental import pallas as pl
from jax.experimental.pallas import tpu as pltpu
from jax.sharding import PartitionSpec as P

HEAD_DIM = 128
EPSILON = 1e-05
STEP_SIZE = 0.25
NOISE_SCALE = (2.0 * STEP_SIZE) ** 0.5
NEGATIVE = -1e30
LOG2E = 1.4426950408889634
MESH = pl.DeviceIdType.MESH
VMEM = pl.BlockSpec(memory_space=pltpu.VMEM)
ANY = pl.BlockSpec(memory_space=pl.ANY)
NT = (((1,), (1,)), ((), ()))
TN = (((0,), (0,)), ((), ()))
FORWARD_BLOCKS = (512, 512)
BACKWARD_BLOCKS = (512, 512)


def row_scale(matrix):
    return lax.rsqrt(jnp.mean(matrix * matrix, axis=-1, keepdims=True) + EPSILON)


def dot32(left, right, dims):
    return lax.dot_general(left, right, dims, preferred_element_type=jnp.float32)


def greet(axis, number, me):
    barrier = pltpu.get_barrier_semaphore()
    for step in range(1, number):
        pl.semaphore_signal(
            barrier, inc=1, device_id={axis: lax.rem(me + step, number)}, device_id_type=MESH
        )
    pl.semaphore_wait(barrier, number - 1)


def gather_kernel(
    number, key_ref, value_ref, seg_ref, normed_ref, w_ref, keys, values, segs, query_out, send_sem,
    recv_sem, own_sem,
):
    me = lax.axis_index("ctx")
    rows = key_ref.shape[0]
    greet("ctx", number, me)

    def place(index):
        return pl.ds(pl.multiple_of(index * rows, rows), rows)

    def send(slot, source, target, peer):
        copy = pltpu.make_async_remote_copy(
            src_ref=source,
            dst_ref=target,
            send_sem=send_sem.at[slot],
            recv_sem=recv_sem.at[slot],
            device_id={"ctx": peer},
            device_id_type=MESH,
        )
        copy.start()
        return copy

    mine = place(me)
    copies = []
    for step in range(1, number):
        copies.append(send(step, seg_ref, segs.at[me], lax.rem(me + step, number)))
    relay = number == 4
    if relay:
        low, high = lax.rem(me, 2), me // 2
        across, along = high * 2 + 1 - low, (1 - high) * 2 + low
        key_first = send(number, key_ref, keys.at[mine], across)
        value_first = send(number + 1, value_ref, values.at[mine], along)
        copies.append(send(number + 2, value_ref, values.at[mine], across))
        copies.append(send(number + 3, key_ref, keys.at[mine], along))
    else:
        for step in range(1, number):
            peer = lax.rem(me + step, number)
            copies.append(send(number + 2 * step, key_ref, keys.at[mine], peer))
            copies.append(send(number + 2 * step + 1, value_ref, values.at[mine], peer))
    pairs = ((key_ref, keys.at[mine]), (value_ref, values.at[mine]), (seg_ref, segs.at[me]))
    for index, (source, target) in enumerate(pairs):
        copy = pltpu.make_async_copy(source, target, own_sem.at[index])
        copy.start()
        copies.append(copy)
    tile = min(256, rows)

    def project(piece, _):
        at = pl.ds(pl.multiple_of(piece * tile, tile), tile)
        query_out[at, :] = jnp.dot(
            normed_ref[at, :], w_ref[...], preferred_element_type=jnp.float32
        ).astype(jnp.bfloat16)
        return 0

    lax.fori_loop(0, rows // tile, project, 0)
    if relay:
        key_first.wait()
        copies.append(send(number + 4, keys.at[place(across)], keys.at[place(across)], along))
        value_first.wait()
        copies.append(send(number + 5, values.at[place(along)], values.at[place(along)], across))
    for copy in copies:
        copy.wait()


def gather_keys(number, key_rows, value_rows, segment_ids, normed, w_query):
    rows, width = key_rows.shape
    seg = segment_ids.reshape(-1, 128)
    full = jax.ShapeDtypeStruct((number * rows, width), key_rows.dtype)
    keys, values, segs, queries = pl.pallas_call(
        functools.partial(gather_kernel, number),
        out_shape=(
            full,
            full,
            jax.ShapeDtypeStruct((number,) + seg.shape, seg.dtype),
            jax.ShapeDtypeStruct((rows, width), key_rows.dtype),
        ),
        in_specs=[VMEM] * 5,
        out_specs=(ANY, ANY, ANY, VMEM),
        scratch_shapes=[
            pltpu.SemaphoreType.DMA((3 * number + 6,)),
            pltpu.SemaphoreType.DMA((3 * number + 6,)),
            pltpu.SemaphoreType.DMA((3,)),
        ],
        compiler_params=pltpu.CompilerParams(collective_id=0, has_side_effects=True),
    )(key_rows, value_rows, seg, normed, w_query)
    return keys, values, segs.reshape(-1), queries


def block_ranges(table, index):
    return [table[index, column] for column in range(4)]


def forward_kernel(
    heads, bq, bk, table, query_ref, key_ref, value_ref, start_ref, pos_ref, out_ref, log_ref
):
    factor = HEAD_DIM ** (-0.5) * LOG2E
    blocks = query_ref.shape[0] // bq

    def one_block(index, _):
        low, inner_low, inner_high, high = block_ranges(table, index)
        rows = pl.ds(pl.multiple_of(index * bq, bq), bq)
        start, pos = start_ref[index], pos_ref[index]

        def step(masked, piece, carry):
            keys_at = pl.ds(pl.multiple_of(piece * bk, bk), bk)
            if masked:
                key_pos = piece * bk + lax.broadcasted_iota(jnp.int32, (bk, bq), 0)
                allowed = (key_pos >= start) & (key_pos <= pos)
            result = []
            for head in range(heads):
                top, total, acc = carry[head]
                cols = pl.ds(head * HEAD_DIM, HEAD_DIM)
                scores = dot32(key_ref[keys_at, cols], query_ref[rows, cols], NT)
                if masked:
                    scores = jnp.where(allowed, scores, NEGATIVE)
                new_top = jnp.maximum(top, jnp.max(scores, axis=0, keepdims=True) * factor)
                weights = jnp.exp2(scores * factor - new_top)
                scale = jnp.exp2(top - new_top)
                total = total * scale + jnp.sum(weights, axis=0, keepdims=True)
                acc = acc * scale + dot32(
                    value_ref[keys_at, cols], weights.astype(jnp.bfloat16), TN
                )
                result.append((new_top, total, acc))
            return tuple(result)

        carry = tuple(
            (
                jnp.full((1, bq), NEGATIVE, jnp.float32),
                jnp.zeros((1, bq), jnp.float32),
                jnp.zeros((HEAD_DIM, bq), jnp.float32),
            )
            for _ in range(heads)
        )
        carry = lax.fori_loop(low, inner_low, functools.partial(step, True), carry)
        carry = lax.fori_loop(inner_low, inner_high, functools.partial(step, False), carry)
        carry = lax.fori_loop(inner_high, high, functools.partial(step, True), carry)
        for head in range(heads):
            top, total, acc = carry[head]
            out_ref[rows, pl.ds(head * HEAD_DIM, HEAD_DIM)] = (acc / total).T.astype(jnp.bfloat16)
            log_ref[index, pl.ds(head, 1), :] = top + jnp.log2(total)
        return 0

    lax.fori_loop(0, blocks, one_block, 0)


def backward_kernel(
    heads, bq, bk, table, query_ref, key_ref, value_ref, grad_ref, out_ref, log_ref, start_ref,
    pos_ref, query_out, pair_out, pair_acc,
):
    score_scale = HEAD_DIM ** (-0.5)
    factor = score_scale * LOG2E
    blocks = query_ref.shape[0] // bq
    width = heads * HEAD_DIM
    pair_rows = pair_acc.shape[0]

    def clear(piece, _):
        at = pl.ds(pl.multiple_of(piece * bk, bk), bk)
        pair_acc[at, :] = jnp.zeros((bk, 2 * width), jnp.float32)
        return 0

    lax.fori_loop(0, pair_rows // bk, clear, 0)

    def one_block(index, _):
        low, inner_low, inner_high, high = block_ranges(table, index)
        rows = pl.ds(pl.multiple_of(index * bq, bq), bq)
        start, pos = start_ref[index], pos_ref[index]
        deltas, logs = [], []
        for head in range(heads):
            cols = pl.ds(head * HEAD_DIM, HEAD_DIM)
            product = grad_ref[rows, cols].astype(jnp.float32) * out_ref[rows, cols].astype(
                jnp.float32
            )
            deltas.append(jnp.sum(product.T, axis=0, keepdims=True))
            logs.append(log_ref[index, pl.ds(head, 1), :])

        def step(masked, piece, carry):
            keys_at = pl.ds(pl.multiple_of(piece * bk, bk), bk)
            if masked:
                key_pos = piece * bk + lax.broadcasted_iota(jnp.int32, (bk, bq), 0)
                allowed = (key_pos >= start) & (key_pos <= pos)
            result = []
            for head in range(heads):
                cols = pl.ds(head * HEAD_DIM, HEAD_DIM)
                value_cols = pl.ds(width + head * HEAD_DIM, HEAD_DIM)
                key_block, query_block = key_ref[keys_at, cols], query_ref[rows, cols]
                grad_block = grad_ref[rows, cols]
                scores = dot32(key_block, query_block, NT)
                probabilities = jnp.exp2(scores * factor - logs[head])
                if masked:
                    probabilities = jnp.where(allowed, probabilities, 0.0)
                dprobs = dot32(value_ref[keys_at, cols], grad_block, NT)
                dscores = (probabilities * (dprobs - deltas[head])).astype(jnp.bfloat16)
                pair_acc[keys_at, value_cols] += jnp.dot(
                    probabilities.astype(jnp.bfloat16),
                    grad_block,
                    preferred_element_type=jnp.float32,
                )
                pair_acc[keys_at, cols] += jnp.dot(
                    dscores, query_block, preferred_element_type=jnp.float32
                )
                result.append(carry[head] + dot32(key_block, dscores, TN))
            return tuple(result)

        carry = tuple(jnp.zeros((HEAD_DIM, bq), jnp.float32) for _ in range(heads))
        carry = lax.fori_loop(low, inner_low, functools.partial(step, True), carry)
        carry = lax.fori_loop(inner_low, inner_high, functools.partial(step, False), carry)
        carry = lax.fori_loop(inner_high, high, functools.partial(step, True), carry)
        for head in range(heads):
            query_out[rows, pl.ds(head * HEAD_DIM, HEAD_DIM)] = (
                carry[head].T * score_scale
            ).astype(jnp.bfloat16)
        return 0

    lax.fori_loop(0, blocks, one_block, 0)

    def flush(piece, _):
        at = pl.ds(pl.multiple_of(piece * bk, bk), bk)
        pair_out[at, :width] = (pair_acc[at, :width] * score_scale).astype(jnp.bfloat16)
        pair_out[at, width:] = pair_acc[at, width:].astype(jnp.bfloat16)
        return 0

    lax.fori_loop(0, pair_rows // bk, flush, 0)


def make_table(start, pos, bq, bk):
    starts, places = start.reshape(-1, bq), pos.reshape(-1, bq)
    low = starts[:, 0] // bk
    inner_low = (starts[:, -1] + bk - 1) // bk
    inner_high = jnp.maximum(inner_low, (places[:, 0] + 1) // bk)
    high = places[:, -1] // bk + 1
    return jnp.stack([low, inner_low, inner_high, high], axis=1).astype(jnp.int32)


def middle_kernel(
    number, part_ref, w_any, state_ref, probe_ref, grad_out, readout_out, w_ref, joined, half,
    sending, landing, send_sem, recv_sem, back_send, back_recv, w_sem,
):
    me = lax.axis_index("head")
    width = part_ref.shape[1]
    own = state_ref.shape[0]
    model = state_ref.shape[1]
    w_copy = pltpu.make_async_copy(w_any, w_ref, w_sem)
    w_copy.start()
    greet("head", number, me)
    my_cols = pl.ds(pl.multiple_of(me * width, width), width)
    my_rows = pl.ds(pl.multiple_of(me * own, own), own)
    copies = []
    for step in range(1, number):
        peer = lax.rem(me + step, number)
        copy = pltpu.make_async_remote_copy(
            src_ref=part_ref.at[pl.ds(pl.multiple_of(peer * own, own), own)],
            dst_ref=joined.at[:, my_cols],
            send_sem=send_sem.at[step],
            recv_sem=recv_sem.at[step],
            device_id={"head": peer},
            device_id_type=MESH,
        )
        copy.start()
        copies.append(copy)
    joined[:, my_cols] = part_ref[my_rows, :]
    w_copy.wait()
    for copy in copies:
        copy.wait()

    tile = min(256, model)

    def project(piece, carry):
        squares, products = carry
        cols = pl.ds(pl.multiple_of(piece * tile, tile), tile)
        layer = state_ref[:, cols].astype(jnp.float32) + jnp.dot(
            joined[...], w_ref[:, cols], preferred_element_type=jnp.float32
        )
        readout_out[:, cols] = layer
        squares = squares + jnp.sum(layer * layer, axis=1, keepdims=True)
        products = products + jnp.sum(
            layer * probe_ref[:, cols].astype(jnp.float32), axis=1, keepdims=True
        )
        return squares, products

    zero = jnp.zeros((own, 1), jnp.float32)
    squares, products = lax.fori_loop(0, model // tile, project, (zero, zero))
    scale = lax.rsqrt(squares / model + EPSILON)
    bend = scale**3 * (products / model)

    def finish(piece, _):
        cols = pl.ds(pl.multiple_of(piece * tile, tile), tile)
        readout = scale * probe_ref[:, cols].astype(jnp.float32) - readout_out[:, cols] * bend
        readout_out[:, cols] = readout
        half[:, cols] = readout.astype(jnp.bfloat16)
        return 0

    lax.fori_loop(0, model // tile, finish, 0)
    copies = []
    for step in range(1, number):
        peer = lax.rem(me + step, number)
        sending[step] = dot32(
            half[...], w_ref[pl.ds(pl.multiple_of(peer * width, width), width), :], NT
        ).astype(jnp.bfloat16)
        copy = pltpu.make_async_remote_copy(
            src_ref=sending.at[step],
            dst_ref=landing.at[my_rows],
            send_sem=back_send.at[step],
            recv_sem=back_recv.at[step],
            device_id={"head": peer},
            device_id_type=MESH,
        )
        copy.start()
        copies.append(copy)
    landing[my_rows, :] = dot32(half[...], w_ref[my_cols, :], NT).astype(jnp.bfloat16)
    for copy in copies:
        copy.wait()
    grad_out[...] = landing[...]


def middle(number, part, w_full, state_own, probe_own):
    rows, width = part.shape
    own, model = state_own.shape
    return pl.pallas_call(
        functools.partial(middle_kernel, number),
        out_shape=(
            jax.ShapeDtypeStruct((rows, width), jnp.bfloat16),
            jax.ShapeDtypeStruct((own, model), jnp.float32),
        ),
        in_specs=[VMEM, ANY, VMEM, VMEM],
        out_specs=(VMEM, VMEM),
        scratch_shapes=[
            pltpu.VMEM(w_full.shape, jnp.bfloat16),
            pltpu.VMEM((own, number * width), jnp.bfloat16),
            pltpu.VMEM((own, model), jnp.bfloat16),
            pltpu.VMEM((number, own, width), jnp.bfloat16),
            pltpu.VMEM((rows, width), jnp.bfloat16),
            pltpu.SemaphoreType.DMA((number,)),
            pltpu.SemaphoreType.DMA((number,)),
            pltpu.SemaphoreType.DMA((number,)),
            pltpu.SemaphoreType.DMA((number,)),
            pltpu.SemaphoreType.DMA,
        ],
        compiler_params=pltpu.CompilerParams(
            collective_id=1, has_side_effects=True, vmem_limit_bytes=60 * 2**20
        ),
    )(part, w_full, state_own, probe_own)


def tail_kernel(
    ctx_count, number, pair_any, query_ref, w_ref, sum_out, own_pair, arriving, gathered, terms,
    from_partner, reduced, landing, ctx_send, ctx_recv, p_send, p_recv, z_send, z_recv, own_sem,
):
    ctx, me = lax.axis_index("ctx"), lax.axis_index("head")
    groups = number // 2
    group, core = me // 2, lax.rem(me, 2)
    partner = group * 2 + 1 - core
    rows, width = query_ref.shape
    own, model = sum_out.shape
    chunk = 2 * own
    own_copy = pltpu.make_async_copy(
        pair_any.at[pl.ds(pl.multiple_of(ctx * rows, rows), rows)], own_pair, own_sem
    )
    own_copy.start()
    barrier = pltpu.get_barrier_semaphore()
    peers = [{"ctx": lax.rem(ctx + step, ctx_count)} for step in range(1, ctx_count)]
    peers.append({"head": partner})
    for step in range(1, groups):
        peers.append({"head": lax.rem(group + step, groups) * 2 + core})
    for peer in peers:
        pl.semaphore_signal(barrier, inc=1, device_id=peer, device_id_type=MESH)
    pl.semaphore_wait(barrier, len(peers))

    def chunk_start(order):
        dest = lax.rem(group + order + 1, groups)
        return dest, pl.multiple_of(dest * chunk, chunk)

    def ctx_copy(order, step):
        target = lax.rem(ctx - step + ctx_count, ctx_count)
        _, first = chunk_start(order)
        return pltpu.make_async_remote_copy(
            src_ref=pair_any.at[pl.ds(pl.multiple_of(target * rows + first, chunk), chunk)],
            dst_ref=arriving.at[order, step - 1],
            send_sem=ctx_send.at[order, step],
            recv_sem=ctx_recv.at[order, step],
            device_id={"ctx": target},
            device_id_type=MESH,
        )

    for order in range(groups):
        for step in range(1, ctx_count):

            @pl.when(step <= ctx)
            def _():
                ctx_copy(order, step).start()

    own_copy.wait()
    tile = min(512, model)
    mine = pl.ds(pl.multiple_of(core * own, own), own)
    theirs = pl.ds(pl.multiple_of((1 - core) * own, own), own)
    waiting = []
    for order in range(groups):
        dest, first = chunk_start(order)
        at = pl.ds(first, chunk)
        gathered[...] = own_pair[at, :].astype(jnp.float32)
        for step in range(1, ctx_count):

            @pl.when(ctx + step < ctx_count)
            def _():
                ctx_copy(order, step).wait_recv()
                gathered[...] += arriving[order, step - 1].astype(jnp.float32)

        def multiply(piece, _):
            cols = pl.ds(pl.multiple_of(piece * tile, tile), tile)
            term = dot32(query_ref[at, :], w_ref[0, cols, :], NT)
            term += dot32(gathered[:, :width].astype(jnp.bfloat16), w_ref[1, cols, :], NT)
            term += dot32(gathered[:, width:].astype(jnp.bfloat16), w_ref[2, cols, :], NT)
            terms[order, :, cols] = term.astype(jnp.bfloat16)
            return 0

        lax.fori_loop(0, model // tile, multiply, 0)
        copy = pltpu.make_async_remote_copy(
            src_ref=terms.at[order, theirs],
            dst_ref=from_partner.at[order],
            send_sem=p_send.at[order],
            recv_sem=p_recv.at[order],
            device_id={"head": partner},
            device_id_type=MESH,
        )
        copy.start()
        copy.wait()
        both = terms[order, mine, :].astype(jnp.float32) + from_partner[order].astype(jnp.float32)
        if order < groups - 1:
            reduced[order] = both.astype(jnp.bfloat16)
            copy = pltpu.make_async_remote_copy(
                src_ref=reduced.at[order],
                dst_ref=landing.at[order],
                send_sem=z_send.at[order],
                recv_sem=z_recv.at[order],
                device_id={"head": dest * 2 + core},
                device_id_type=MESH,
            )
            copy.start()
            waiting.append(copy)
        else:
            sum_out[...] = both
    for order, copy in enumerate(waiting):
        copy.wait()
        sum_out[...] += landing[order].astype(jnp.float32)
    for order in range(groups):
        for step in range(1, ctx_count):

            @pl.when(step <= ctx)
            def _():
                ctx_copy(order, step).wait_send()


def tail(ctx_count, number, pair, query_grad, w_qkv):
    rows, width = query_grad.shape
    model = w_qkv.shape[1]
    own, groups = rows // number, number // 2
    half, full = jnp.bfloat16, jnp.float32
    dma = pltpu.SemaphoreType.DMA
    return pl.pallas_call(
        functools.partial(tail_kernel, ctx_count, number),
        out_shape=jax.ShapeDtypeStruct((own, model), full),
        in_specs=[ANY, VMEM, VMEM],
        out_specs=VMEM,
        scratch_shapes=[
            pltpu.VMEM((rows, 2 * width), half),
            pltpu.VMEM((groups, ctx_count - 1, 2 * own, 2 * width), half),
            pltpu.VMEM((2 * own, 2 * width), full),
            pltpu.VMEM((groups, 2 * own, model), half),
            pltpu.VMEM((groups, own, model), half),
            pltpu.VMEM((groups, own, model), half),
            pltpu.VMEM((groups, own, model), half),
            dma((groups, ctx_count)),
            dma((groups, ctx_count)),
            dma((groups,)),
            dma((groups,)),
            dma((groups,)),
            dma((groups,)),
            dma,
        ],
        compiler_params=pltpu.CompilerParams(
            collective_id=2, has_side_effects=True, vmem_limit_bytes=60 * 2**20
        ),
    )(pair, query_grad, w_qkv)


def body(state, norm_gain, w_qkv, w_out, probe, noise, segment_ids):
    local_rows, model_width = state.shape
    width = w_qkv.shape[2]
    local_heads = width // HEAD_DIM
    head_count = lax.axis_size("head")
    ctx_count = lax.axis_size("ctx")
    ctx_index = lax.axis_index("ctx")
    own_rows = local_rows // head_count
    row_start = lax.axis_index("head") * own_rows
    w_full = lax.all_gather(w_out, "head", axis=0, tiled=True)
    state_f = state.astype(jnp.float32)
    gain_full = norm_gain.astype(jnp.float32)
    inverse = row_scale(state_f)
    normed = (state_f * inverse * gain_full).astype(jnp.bfloat16)

    def project(index):
        return jnp.dot(normed, w_qkv[index], preferred_element_type=jnp.float32).astype(
            jnp.bfloat16
        )

    key_rows, value_rows = project(1), project(2)
    keys, values, segs, query_rows = gather_keys(
        ctx_count, key_rows, value_rows, segment_ids, normed, w_qkv[0]
    )
    total_rows = keys.shape[0]
    pos = ctx_index * local_rows + jnp.arange(local_rows, dtype=jnp.int32)
    start = jnp.sum((segs[None, :] < segment_ids[:, None]).astype(jnp.int32), axis=1)
    fq, fk = (min(local_rows, size) for size in FORWARD_BLOCKS)
    gq, gk = (min(local_rows, size) for size in BACKWARD_BLOCKS)
    smem = pl.BlockSpec(memory_space=pltpu.SMEM)
    params = pltpu.CompilerParams(vmem_limit_bytes=60 * 2**20)
    outputs, logs = pl.pallas_call(
        functools.partial(forward_kernel, local_heads, fq, fk),
        out_shape=(
            jax.ShapeDtypeStruct((local_rows, width), jnp.bfloat16),
            jax.ShapeDtypeStruct((local_rows // fq, local_heads, fq), jnp.float32),
        ),
        in_specs=[smem] + [VMEM] * 5,
        out_specs=(VMEM, VMEM),
        compiler_params=params,
        cost_estimate=pl.CostEstimate(
            flops=4 * local_rows * total_rows * width, bytes_accessed=0, transcendentals=0
        ),
    )(
        make_table(start, pos, fq, fk),
        query_rows,
        keys,
        values,
        start.reshape(-1, 1, fq),
        pos.reshape(-1, 1, fq),
    )
    state_half = lax.dynamic_slice_in_dim(state, row_start, own_rows, 0)
    probe_own = lax.dynamic_slice_in_dim(probe, row_start, own_rows, 0)
    state_own = state_half.astype(jnp.float32)
    inverse_own = row_scale(state_own)
    grads_out, readout_own = middle(head_count, outputs, w_full, state_half, probe_own)
    query_grad, pair = pl.pallas_call(
        functools.partial(backward_kernel, local_heads, gq, gk),
        out_shape=(
            jax.ShapeDtypeStruct((local_rows, width), jnp.bfloat16),
            jax.ShapeDtypeStruct((total_rows, 2 * width), jnp.bfloat16),
        ),
        in_specs=[smem] + [VMEM] * 8,
        out_specs=(VMEM, VMEM),
        scratch_shapes=[pltpu.VMEM((total_rows, 2 * width), jnp.float32)],
        compiler_params=params,
        cost_estimate=pl.CostEstimate(
            flops=10 * local_rows * total_rows * width, bytes_accessed=0, transcendentals=0
        ),
    )(
        make_table(start, pos, gq, gk),
        query_rows,
        keys,
        values,
        grads_out,
        outputs,
        logs.reshape(local_rows // fq, local_heads, fq),
        start.reshape(-1, 1, gq),
        pos.reshape(-1, 1, gq),
    )
    normed_grad = tail(ctx_count, head_count, pair, query_grad, w_qkv)
    gain_grad = normed_grad * gain_full
    gradient = (
        readout_own
        + inverse_own * gain_grad
        - state_own * inverse_own**3 * jnp.mean(gain_grad * state_own, axis=-1, keepdims=True)
    )
    return state_own - STEP_SIZE * gradient + jnp.sqrt(2.0 * STEP_SIZE) * noise.astype(jnp.float32)


def remote(source, target, send_sem, recv_sem, ctx, head):
    return pltpu.make_async_remote_copy(
        src_ref=source,
        dst_ref=target,
        send_sem=send_sem,
        recv_sem=recv_sem,
        device_id={"ctx": ctx, "head": head},
        device_id_type=MESH,
    )


def place():
    ctx, me = lax.axis_index("ctx"), lax.axis_index("head")
    return ctx, me, me // 2, lax.rem(me, 2)


def announce(peers):
    barrier = pltpu.get_barrier_semaphore()
    for ctx, head in peers:
        pl.semaphore_signal(
            barrier, inc=1, device_id={"ctx": ctx, "head": head}, device_id_type=MESH
        )


def await_all(peers):
    pl.semaphore_wait(pltpu.get_barrier_semaphore(), len(peers))


def far_first(groups, group, step):
    result = 0
    for index in range(groups):
        order = sorted(range(groups), key=lambda other: (-abs(other - index), -other))
        result = jnp.where(group == index, order[step], result)
    return result


def front_kernel(
    ctx_count, head_count, state_any, w_any, gain_ref, seg_ref, w_out_any, probe_any, query_any,
    kv_any, segs_out, part_any, log_out, grad_out, readout_any, w_pair, state_v, w_v, query_buf,
    kv_buf, w_ref, joined, half, sending, state_own, probe_own, query_out, kv_out, part_out,
    readout_out, load_sem, w_sem, q_send, q_recv, kv_send, kv_recv, pass_send, seg_send, seg_recv,
    line_send, line_recv, plane_send, plane_recv, beside_send, beside_recv, shard_send, shard_recv,
    shard_sem, out_send, out_recv, back_send, back_recv, own_sem, row_sem, pair_send, pair_recv,
    leave_sem,
):
    ctx, me, group, core = place()
    rows, model = state_any.shape
    own, groups = rows // head_count, head_count // 2
    slots = w_any.shape[2] // HEAD_DIM
    chunk = 2 * own
    partner = group * 2 + 1 - core

    def at(piece):
        return pl.ds(pl.multiple_of(piece * chunk, chunk), chunk)

    def own_at(piece):
        return pl.ds(pl.multiple_of(piece * own, own), own)

    def load_state(piece):
        return pltpu.make_async_copy(
            state_any.at[at(piece)], state_v.at[at(piece)], load_sem.at[piece]
        )

    load_state(0).start()
    w_loads = [pltpu.make_async_copy(w_any.at[t], w_v.at[t], w_sem.at[t]) for t in range(3)]
    for copy in w_loads:
        copy.start()
    for piece in range(1, groups):
        load_state(piece).start()
    my_rows = own_at(me)
    shard = w_out_any.shape[0]
    part, quarter = shard // 2, shard // ctx_count
    later_loads = [
        pltpu.make_async_copy(state_any.at[my_rows], state_own, row_sem.at[0]),
        pltpu.make_async_copy(probe_any.at[my_rows], probe_own, row_sem.at[1]),
        pltpu.make_async_copy(
            w_out_any, w_ref.at[pl.ds(pl.multiple_of(me * shard, shard), shard)], shard_sem
        ),
    ]
    for copy in later_loads:
        copy.start()
    peers = [(lax.rem(ctx + step, ctx_count), partner) for step in range(ctx_count)]
    for far in range(groups):
        for step in range(ctx_count):
            if far or step:
                peers.append(
                    (lax.rem(ctx + step, ctx_count), lax.rem(group + far, groups) * 2 + core)
                )
    announce(peers)

    low, high = lax.rem(ctx, 2), ctx // 2
    which = lax.rem(low + high, 2)
    across, along = high * 2 + 1 - low, (1 - high) * 2 + low

    def shard_rows(origin, first, size):
        return pl.ds(pl.multiple_of((origin * 2 + core) * shard + first, size), size)

    def line_copy(way, origin, axis, mine):
        first = which * part + axis * quarter
        here = shard_rows(origin, first, quarter)
        source = (
            w_out_any.at[pl.ds(pl.multiple_of(first, quarter), quarter)] if mine else w_ref.at[here]
        )
        other = group + 1 if way == 0 else group - 1
        return remote(
            source, w_ref.at[here], line_send.at[way, axis, origin], line_recv.at[axis, origin],
            ctx, other * 2 + core,
        )

    def plane_copy(axis, origin, kept):
        here = shard_rows(origin, kept * part + axis * quarter, quarter)
        return remote(
            w_ref.at[here], w_ref.at[here], plane_send.at[axis, origin],
            plane_recv.at[axis, origin], along if axis else across, me,
        )

    def beside_copy(kind, origin):
        kept = which if kind < 2 else 1 - which
        here = shard_rows(origin, kept * part + (kind % 2) * quarter, quarter)
        return remote(
            w_ref.at[here], w_ref.at[here], beside_send.at[kind, origin],
            beside_recv.at[kind, origin], ctx, partner,
        )

    def shard_copy():
        return remote(
            w_out_any, w_ref.at[pl.ds(pl.multiple_of(me * shard, shard), shard)], shard_send,
            shard_recv, ctx, partner,
        )

    has_up, has_down = group < groups - 1, group > 0

    def each_origin(distance, work):
        for way in range(2):
            origin = group - distance if way == 0 else group + distance

            @pl.when(origin >= 0 if way == 0 else origin < groups)
            def _():
                work(way, origin)

    def line_arrived(distance, axis):
        def work(way, origin):
            line_copy(way, origin, axis, False).wait_recv()

            @pl.when(has_up if way == 0 else has_down)
            def _():
                line_copy(way, origin, axis, False).start()

            plane_copy(axis, origin, which).start()
            beside_copy(axis, origin).start()

        each_origin(distance, work)

    def plane_arrived(distance, axis):
        def work(way, origin):
            plane_copy(axis, origin, 1 - which).wait_recv()
            beside_copy(2 + axis, origin).start()

        each_origin(distance, work)

    def weights_sent(distance):
        def work(way, origin):
            for axis in range(2):

                @pl.when(has_up if way == 0 else has_down)
                def _():
                    line_copy(way, origin, axis, False).wait_send()

                plane_copy(axis, origin, which).wait_send()
            for kind in range(4):
                beside_copy(kind, origin).wait_send()

        each_origin(distance, work)

    def own_lines(work):
        for axis in range(2):

            @pl.when(has_up)
            def _():
                work(line_copy(0, group, axis, True))

            @pl.when(has_down)
            def _():
                work(line_copy(1, group, axis, True))

    for copy in w_loads:
        copy.wait()
    gain = gain_ref[...].astype(jnp.float32).reshape(1, model)

    def away(slot, kind, piece, dest):
        head = group * 2 + kind
        return (
            remote(
                query_buf.at[slot, piece, kind], query_out.at[ctx, piece],
                q_send.at[slot, kind, piece], q_recv.at[ctx, piece], dest, head,
            ),
            remote(
                kv_buf.at[slot, kind, piece], kv_out.at[kind, ctx, piece],
                kv_send.at[slot, kind, piece], kv_recv.at[kind, ctx, piece], dest, head,
            ),
        )

    def beside(slot, piece):
        result = [
            remote(
                query_buf.at[slot, piece, 1 - core], query_out.at[ctx, piece],
                q_send.at[slot, 1 - core, piece], q_recv.at[ctx, piece], ctx, partner,
            )
        ]
        for kind in range(2):
            result.append(
                remote(
                    kv_buf.at[slot, kind, piece], kv_out.at[kind, ctx, piece],
                    kv_send.at[slot, kind, piece], kv_recv.at[kind, ctx, piece], ctx, partner,
                )
            )
        return result

    def project(piece):
        load_state(piece).wait()
        block = state_v[at(piece), :].astype(jnp.float32)
        normed = (block * row_scale(block) * gain).astype(jnp.bfloat16)
        for t in range(3):
            result = jnp.dot(normed, w_v[t], preferred_element_type=jnp.float32).astype(
                jnp.bfloat16
            )
            for slot in range(slots):
                cut = result[:, slot * HEAD_DIM : (slot + 1) * HEAD_DIM]
                if t == 0:
                    query_buf[slot, piece, 0] = cut[:own]
                    query_buf[slot, piece, 1] = cut[own:]
                else:
                    kv_buf[slot, t - 1, piece] = cut

    def send_heads(piece):
        for slot in range(slots):
            dest = core * slots + slot

            @pl.when(dest != ctx)
            def _():
                for kind in range(2):
                    for copy in away(slot, kind, piece, dest):
                        copy.start()

            @pl.when(dest == ctx)
            def _():
                query_out[ctx, piece] = query_buf[slot, piece, core]
                for kind in range(2):
                    kv_out[kind, ctx, piece] = kv_buf[slot, kind, piece]
                for copy in beside(slot, piece):
                    copy.start()

    project(0)
    await_all(peers)
    own_lines(lambda copy: copy.start())
    send_heads(0)
    shard_copy().start()
    segs = []
    for step in range(1, ctx_count):
        copy = remote(
            seg_ref, segs_out.at[ctx], seg_send.at[step], seg_recv.at[step],
            lax.rem(ctx + step, ctx_count), me,
        )
        copy.start()
        segs.append(copy)
    segs_out[ctx] = seg_ref[...]

    def project_and_send(piece, _):
        project(piece)
        send_heads(piece)
        return 0

    lax.fori_loop(1, groups, project_and_send, 0)

    def hand_over(piece, step):
        source = lax.rem(ctx + step, ctx_count)
        return remote(
            kv_out.at[core, source, piece], kv_out.at[core, source, piece],
            pass_send.at[step, piece], kv_recv.at[core, source, piece], ctx, partner,
        )

    for piece in range(groups):
        for step in range(1, ctx_count):
            copy = hand_over(piece, step)
            copy.wait_recv()
            copy.start()
        if piece == 0:
            line_arrived(1, 0)
        if piece == min(2, groups - 1):
            line_arrived(1, 1)
    line_arrived(2, 0)

    def got_query(source, piece):
        remote(
            query_out.at[source, piece], query_out.at[source, piece],
            q_send.at[0, 0, piece], q_recv.at[source, piece], ctx, partner,
        ).wait_recv()

    def got_kv(kind, source, piece):
        remote(
            kv_out.at[kind, source, piece], kv_out.at[kind, source, piece],
            kv_send.at[0, 0, piece], kv_recv.at[kind, source, piece], ctx, partner,
        ).wait_recv()

    def gather(piece, _):
        for step in range(1, ctx_count):
            source = lax.rem(ctx + step, ctx_count)
            got_query(source, piece)
            got_kv(1 - core, source, piece)
            hand_over(piece, step).wait_send()

        @pl.when(ctx // slots != core)
        def _():
            got_query(ctx, piece)
            for kind in range(2):
                got_kv(kind, ctx, piece)

        return 0

    lax.fori_loop(0, groups, gather, 0)
    for copy in segs:
        copy.wait()
    leaving = [
        pltpu.make_async_copy(query_out.at[source], query_any.at[:, source], leave_sem.at[0, source])
        for source in range(ctx_count)
    ]
    for kind in range(2):
        leaving += [
            pltpu.make_async_copy(
                kv_out.at[kind, source], kv_any.at[kind, :, source],
                leave_sem.at[1 + kind, source],
            )
            for source in range(ctx_count)
        ]
    for copy in leaving:
        copy.start()
    pair_copy = remote(w_any, w_pair, pair_send, pair_recv, ctx, partner)
    pair_copy.start()

    def cols_of(group_at, ctx_at):
        head = group_at * ctx_count + ctx_at
        return pl.ds(pl.multiple_of(head * HEAD_DIM, HEAD_DIM), HEAD_DIM)

    factor = HEAD_DIM ** (-0.5) * LOG2E
    sub = groups * own
    seg_all = segs_out[...]

    def below(value):
        count = jnp.where(seg_all < value, 1.0, 0.0)
        for axis in (0, 1, 2):
            count = jnp.sum(count, axis=axis, keepdims=True)
        return count[0]

    first_bound, second_bound = below(1), below(2)
    lane = lax.broadcasted_iota(jnp.int32, (1, sub), 1)
    inside = (lane // own) * (2 * own) + core * own + lane % own
    key_row = lax.broadcasted_iota(jnp.int32, (rows, sub), 0)

    def out_copy(tile, order, other):
        return remote(
            part_out.at[tile, other], joined.at[:, cols_of(group, ctx)],
            out_send.at[tile, order], out_recv.at[group, ctx], tile, other * 2 + core,
        )

    def one_tile(tile, _):
        query = query_out[tile].reshape(sub, HEAD_DIM)
        pos = (tile * rows + inside).astype(jnp.float32)
        start = jnp.where(
            pos >= second_bound, second_bound, jnp.where(pos >= first_bound, first_bound, 0.0)
        ).astype(jnp.int32)

        def step(diagonal, piece, carry):
            top, total, acc = carry
            scores = dot32(kv_out[0, piece].reshape(rows, HEAD_DIM), query, NT)
            allowed = key_row >= start - piece * rows
            if diagonal:
                allowed = allowed & (key_row <= inside)
            scores = jnp.where(allowed, scores, NEGATIVE)
            new_top = jnp.maximum(top, jnp.max(scores, axis=0, keepdims=True) * factor)
            weights = jnp.exp2(scores * factor - new_top)
            scale = jnp.exp2(top - new_top)
            total = total * scale + jnp.sum(weights, axis=0, keepdims=True)
            acc = acc * scale + dot32(
                kv_out[1, piece].reshape(rows, HEAD_DIM), weights.astype(jnp.bfloat16), TN
            )
            return new_top, total, acc

        carry = (
            jnp.full((1, sub), NEGATIVE, jnp.float32),
            jnp.zeros((1, sub), jnp.float32),
            jnp.zeros((HEAD_DIM, sub), jnp.float32),
        )
        carry = lax.fori_loop(0, tile, functools.partial(step, False), carry)
        top, total, acc = step(True, tile, carry)
        part_out[tile] = (acc / total).T.astype(jnp.bfloat16).reshape(groups, own, HEAD_DIM)
        log_row = top + jnp.log2(total)
        for index in range(groups):
            log_out[index, :, own_at(tile)] = log_row[:, index * own : (index + 1) * own]
        for order in range(groups):
            other = far_first(groups, group, order)
            if order == groups - 1:

                @pl.when(tile != ctx)
                def _():
                    out_copy(tile, order, other).start()

                @pl.when(tile == ctx)
                def _():
                    joined[:, cols_of(group, ctx)] = part_out[tile, group]

            else:
                out_copy(tile, order, other).start()

        @pl.when(tile == 1)
        def _():
            line_arrived(2, 1)

        return 0

    lax.fori_loop(0, ctx_count, one_tile, 0)
    for source in range(ctx_count):
        leaving.append(
            pltpu.make_async_copy(
                part_out.at[source], part_any.at[:, source], leave_sem.at[3, source]
            )
        )
        leaving[-1].start()
    for copy in later_loads:
        copy.wait()
    sources = []
    for far in range(groups):
        for step in range(ctx_count):
            if far or step:
                sources.append((lax.rem(group + far, groups), lax.rem(ctx + step, ctx_count)))
    tile = min(256, model)
    wide = ctx_count * HEAD_DIM
    zero = jnp.zeros((own, 1), jnp.float32)
    for axis in range(2):
        plane_arrived(1, axis)
    for distance in range(3, groups):
        line_arrived(distance, 0)
    for axis in range(2):
        plane_arrived(2, axis)
    for distance in range(3, groups):
        line_arrived(distance, 1)
    shard_copy().wait_recv()

    def heads_arrived(order):
        other = far_first(groups, group, order)
        if order < groups - 1:
            for kind in range(4):
                beside_copy(kind, other).wait_recv()
        for step in range(ctx_count):
            if order < groups - 1 or step:
                peer = lax.rem(ctx + step, ctx_count)
                remote(
                    part_out.at[0, 0], joined.at[:, cols_of(other, peer)],
                    out_send.at[0, 0], out_recv.at[other, peer], peer, other * 2 + core,
                ).wait_recv()

    for order in range(groups - 1, 0, -1):
        heads_arrived(order)
    farthest = far_first(groups, group, 0)
    near = pl.ds(pl.multiple_of(jnp.where(farthest == 0, wide, 0), wide), model - wide)
    far = pl.ds(pl.multiple_of(farthest * wide, wide), wide)

    def near_layer(piece, _):
        cols = pl.ds(pl.multiple_of(piece * tile, tile), tile)
        readout_out[:, cols] = state_own[:, cols].astype(jnp.float32) + jnp.dot(
            joined[:, near], w_ref[near, cols], preferred_element_type=jnp.float32
        )
        return 0

    lax.fori_loop(0, model // tile, near_layer, 0)
    for distance in range(3, groups):
        for axis in range(2):
            plane_arrived(distance, axis)
    heads_arrived(0)

    def layer(piece, carry):
        squares, products = carry
        cols = pl.ds(pl.multiple_of(piece * tile, tile), tile)
        result = readout_out[:, cols] + jnp.dot(
            joined[:, far], w_ref[far, cols], preferred_element_type=jnp.float32
        )
        readout_out[:, cols] = result
        squares = squares + jnp.sum(result * result, axis=1, keepdims=True)
        products = products + jnp.sum(
            result * probe_own[:, cols].astype(jnp.float32), axis=1, keepdims=True
        )
        return squares, products

    squares, products = lax.fori_loop(0, model // tile, layer, (zero, zero))
    scale = lax.rsqrt(squares / model + EPSILON)
    bend = scale**3 * (products / model)

    def finish(piece, _):
        cols = pl.ds(pl.multiple_of(piece * tile, tile), tile)
        readout = scale * probe_own[:, cols].astype(jnp.float32) - readout_out[:, cols] * bend
        readout_out[:, cols] = readout
        half[:, cols] = readout.astype(jnp.bfloat16)
        return 0

    lax.fori_loop(0, model // tile, finish, 0)
    leaving.append(pltpu.make_async_copy(readout_out, readout_any, leave_sem.at[4, 0]))
    leaving[-1].start()
    copies = []
    for order in range(groups):
        other = far_first(groups, group, order)
        result = dot32(
            half[...], w_ref[pl.ds(pl.multiple_of(other * wide, wide), wide), :], NT
        ).astype(jnp.bfloat16)
        for index in range(ctx_count):
            sending[order, index] = result[:, index * HEAD_DIM : (index + 1) * HEAD_DIM]
        for step in range(ctx_count):
            peer = lax.rem(ctx + step, ctx_count)
            if order == groups - 1 and step == 0:
                continue
            copy = remote(
                sending.at[order, peer], grad_out.at[group, ctx], back_send.at[order, step],
                back_recv.at[ctx, group], peer, other * 2 + core,
            )
            copy.start()
            copies.append(copy)
    last = pltpu.make_async_copy(sending.at[groups - 1, ctx], grad_out.at[group, ctx], own_sem)
    last.start()

    def sent(piece, _):
        for slot in range(slots):
            dest = core * slots + slot

            @pl.when(dest != ctx)
            def _():
                for kind in range(2):
                    for copy in away(slot, kind, piece, dest):
                        copy.wait_send()

            @pl.when(dest == ctx)
            def _():
                for copy in beside(slot, piece):
                    copy.wait_send()

        return 0

    lax.fori_loop(0, groups, sent, 0)

    own_lines(lambda copy: copy.wait_send())
    shard_copy().wait_send()
    for distance in range(1, groups):
        weights_sent(distance)

    def parts_sent(tile, _):
        for order in range(groups):
            other = far_first(groups, group, order)
            if order == groups - 1:

                @pl.when(tile != ctx)
                def _():
                    out_copy(tile, order, other).wait_send()

            else:
                out_copy(tile, order, other).wait_send()
        return 0

    lax.fori_loop(0, ctx_count, parts_sent, 0)
    for other, peer in sources:
        remote(
            sending.at[0, 0], grad_out.at[other, peer], back_send.at[0, 0],
            back_recv.at[peer, other], peer, other * 2 + core,
        ).wait_recv()
    for copy in copies:
        copy.wait_send()
    last.wait()
    for copy in leaving:
        copy.wait()
    pair_copy.wait()


def front(ctx_count, head_count, state, w_qkv, gain, segment_ids, w_out, probe):
    rows, model = state.shape
    width = w_qkv.shape[2]
    own, groups, slots = rows // head_count, head_count // 2, width // HEAD_DIM
    seg = segment_ids.reshape(-1, 128)
    half, full, dma = jnp.bfloat16, jnp.float32, pltpu.SemaphoreType.DMA
    shape = jax.ShapeDtypeStruct
    return pl.pallas_call(
        functools.partial(front_kernel, ctx_count, head_count),
        out_shape=(
            shape((groups, ctx_count, own, HEAD_DIM), half),
            shape((2, groups, ctx_count, 2 * own, HEAD_DIM), half),
            shape((ctx_count,) + seg.shape, seg.dtype),
            shape((groups, ctx_count, own, HEAD_DIM), half),
            shape((groups, 1, ctx_count * own), full),
            shape((groups, ctx_count, own, HEAD_DIM), half),
            shape((own, model), full),
            shape(w_qkv.shape, half),
        ),
        in_specs=[ANY, ANY, VMEM, VMEM, ANY, ANY],
        out_specs=(ANY, ANY, VMEM, ANY, VMEM, ANY, ANY, ANY),
        scratch_shapes=[
            pltpu.VMEM((rows, model), half),
            pltpu.VMEM(w_qkv.shape, half),
            pltpu.VMEM((slots, groups, 2, own, HEAD_DIM), half),
            pltpu.VMEM((slots, 2, groups, 2 * own, HEAD_DIM), half),
            pltpu.VMEM((model, model), half),
            pltpu.VMEM((own, model), half),
            pltpu.VMEM((own, model), half),
            pltpu.VMEM((groups, ctx_count, own, HEAD_DIM), half),
            pltpu.VMEM((own, model), half),
            pltpu.VMEM((own, model), half),
            pltpu.VMEM((ctx_count, groups, own, HEAD_DIM), half),
            pltpu.VMEM((2, ctx_count, groups, 2 * own, HEAD_DIM), half),
            pltpu.VMEM((ctx_count, groups, own, HEAD_DIM), half),
            pltpu.VMEM((own, model), full),
            dma((groups,)),
            dma((3,)),
            dma((slots, 2, groups)),
            dma((ctx_count, groups)),
            dma((slots, 2, groups)),
            dma((2, ctx_count, groups)),
            dma((ctx_count, groups)),
            dma((ctx_count,)),
            dma((ctx_count,)),
            dma((2, 2, groups)),
            dma((2, groups)),
            dma((2, groups)),
            dma((2, groups)),
            dma((4, groups)),
            dma((4, groups)),
            dma,
            dma,
            dma,
            dma((ctx_count, groups)),
            dma((groups, ctx_count)),
            dma((groups, ctx_count)),
            dma((ctx_count, groups)),
            dma,
            dma((2,)),
            dma,
            dma,
            dma((5, ctx_count)),
        ],
        compiler_params=pltpu.CompilerParams(
            collective_id=0, has_side_effects=True, vmem_limit_bytes=62 * 2**20
        ),
    )(state, w_qkv, gain, seg, w_out, probe)


def back_kernel(
    ctx_count, head_count, query_any, kv_any, grad_any, part_any, segs_ref, log_ref, w_any, w_pair,
    state_any, noise_any, readout_any, gain_ref, new_out, query_v, kv_v, grad_v, part_v, pair_acc,
    query_acc, deltas, query_fin, pair_buf, w_both, beside, away, terms_in, partial, sending, total,
    state_own, noise_own, readout_own, in_sem, b_send, b_recv, a_send, a_recv, z_send, z_recv,
    own_sem,
):
    ctx, me, group, core = place()
    groups = head_count // 2
    own, model = new_out.shape
    slots, halves = ctx_count // 2, 2
    rows = groups * 2 * own
    sub = ctx_count * own // halves
    partner = group * 2 + 1 - core
    my_rows = pl.ds(pl.multiple_of(me * own, own), own)
    inputs = [
        pltpu.make_async_copy(source, target, in_sem.at[index])
        for index, (source, target) in enumerate(
            ((grad_any, grad_v), (part_any, part_v), (query_any, query_v), (kv_any, kv_v))
        )
    ]
    loads = [
        pltpu.make_async_copy(w_any, w_both.at[core], own_sem.at[0]),
        pltpu.make_async_copy(w_pair, w_both.at[1 - core], own_sem.at[1]),
        pltpu.make_async_copy(state_any.at[my_rows], state_own, own_sem.at[2]),
        pltpu.make_async_copy(noise_any, noise_own, own_sem.at[3]),
        pltpu.make_async_copy(readout_any, readout_own, own_sem.at[4]),
    ]
    for copy in inputs:
        copy.start()
    peers = [(ctx, partner)]
    peers += [(lax.rem(ctx + step, ctx_count), me) for step in range(1, ctx_count)]
    peers += [(ctx, lax.rem(group + far, groups) * 2 + core) for far in range(1, groups)]
    announce(peers)
    dests = [far_first(groups, group, order) for order in range(groups)]

    def dest_of(order):
        result = dests[0]
        for index in range(1, groups):
            result = jnp.where(order == index, dests[index], result)
        return result

    score_scale = HEAD_DIM ** (-0.5)
    factor = score_scale * LOG2E
    seg_all = segs_ref[...]

    def below(value):
        count = jnp.where(seg_all < value, 1.0, 0.0)
        for axis in (0, 1, 2):
            count = jnp.sum(count, axis=axis, keepdims=True)
        return count[0]

    first_bound, second_bound = below(1), below(2)

    def clear(index, _):
        pair_acc[index] = jnp.zeros(pair_acc.shape[1:], jnp.float32)
        query_acc[index] = jnp.zeros(query_acc.shape[1:], jnp.float32)
        return 0

    lax.fori_loop(0, groups, clear, 0)
    for copy in inputs:
        copy.wait()
    for copy in loads:
        copy.start()

    def half_of(ref, index, half):
        count = ctx_count // halves
        return ref[index, half * count : (half + 1) * count].reshape(sub, HEAD_DIM)

    def find_deltas(index, _):
        for half in range(halves):
            product = half_of(grad_v, index, half).astype(jnp.float32) * half_of(
                part_v, index, half
            ).astype(jnp.float32)
            deltas[index, :, half * sub : (half + 1) * sub] = jnp.sum(
                product.T, axis=0, keepdims=True
            )
        return 0

    lax.fori_loop(0, groups, find_deltas, 0)
    await_all(peers)
    lane = lax.broadcasted_iota(jnp.int32, (1, sub), 1)

    def pair(query_at, key_at):
        for half in range(halves):
            blocks = (half + 1) * ctx_count // halves
            count = blocks * 2 * own
            lanes = slice(half * sub, (half + 1) * sub)
            key_block = kv_v[0, key_at, :blocks].reshape(count, HEAD_DIM)
            value_block = kv_v[1, key_at, :blocks].reshape(count, HEAD_DIM)
            query_block = half_of(query_v, query_at, half)
            grad_block = half_of(grad_v, query_at, half)
            spot = (half * (ctx_count // halves) + lane // own) * rows + lane % own
            pos = spot + (query_at * 2 + core) * own
            pos_f = pos.astype(jnp.float32)
            start = jnp.where(
                pos_f >= second_bound,
                second_bound,
                jnp.where(pos_f >= first_bound, first_bound, 0.0),
            ).astype(jnp.int32)
            line = lax.broadcasted_iota(jnp.int32, (count, sub), 0)
            key_pos = (line // (2 * own)) * rows + line % (2 * own)
            offset = key_at * 2 * own
            allowed = (key_pos >= start - offset) & (key_pos <= pos - offset)
            scores = dot32(key_block, query_block, NT)
            probabilities = jnp.where(
                allowed, jnp.exp2(scores * factor - log_ref[query_at, :, lanes]), 0.0
            )
            dprobs = dot32(value_block, grad_block, NT)
            dscores = (probabilities * (dprobs - deltas[query_at, :, lanes])).astype(jnp.bfloat16)
            pair_acc[key_at, :count, HEAD_DIM:] += jnp.dot(
                probabilities.astype(jnp.bfloat16), grad_block, preferred_element_type=jnp.float32
            )
            pair_acc[key_at, :count, :HEAD_DIM] += jnp.dot(
                dscores, query_block, preferred_element_type=jnp.float32
            )
            query_acc[query_at, :, lanes] += dot32(key_block, dscores, TN)

    def beside_copy(order):
        return remote(
            pair_buf.at[order], beside.at[order], b_send.at[order], b_recv.at[order], ctx, partner
        )

    def pair_rows(dest, source, kind):
        first = pl.multiple_of((source * 2 + kind) * own, own)
        keys = pair_acc[dest, pl.ds(first, own), :HEAD_DIM] * score_scale
        values = pair_acc[dest, pl.ds(first, own), HEAD_DIM:]
        return keys, values

    def settle(order):
        dest = dest_of(order)
        for source in range(ctx_count):
            keys, values = pair_rows(dest, source, 1 - core)
            pair_buf[order, source, :, :HEAD_DIM] = keys.astype(jnp.bfloat16)
            pair_buf[order, source, :, HEAD_DIM:] = values.astype(jnp.bfloat16)
        for half in range(halves):
            query_fin[order, half * sub : (half + 1) * sub, :] = (
                query_acc[dest, :, half * sub : (half + 1) * sub].T * score_scale
            ).astype(jnp.bfloat16)
        beside_copy(order).start()

    def stripe(source):
        slot = lax.rem(source, slots)
        return pl.ds(pl.multiple_of(slot * HEAD_DIM, HEAD_DIM), HEAD_DIM)

    def exchange(order, step):
        peer = lax.rem(ctx + step, ctx_count)
        return remote(
            away.at[order, step],
            terms_in.at[dest_of(order), ctx // slots, :, :, stripe(ctx)],
            a_send.at[order, step], a_recv.at[dest_of(order), ctx], peer, me,
        )

    def arrived(dest, step):
        source = lax.rem(ctx + step, ctx_count)
        remote(
            away.at[0, 0], terms_in.at[dest, source // slots, :, :, stripe(source)],
            a_send.at[0, 0], a_recv.at[dest, source], source, me,
        ).wait_recv()

    def spread(order):
        dest = dest_of(order)
        beside_copy(order).wait_recv()
        for step in range(1, ctx_count + 1):
            peer = lax.rem(ctx + step, ctx_count)
            keys, values = pair_rows(dest, peer, core)
            keys = (keys + beside[order, peer, :, :HEAD_DIM].astype(jnp.float32)).astype(
                jnp.bfloat16
            )
            values = (values + beside[order, peer, :, HEAD_DIM:].astype(jnp.float32)).astype(
                jnp.bfloat16
            )
            queries = query_fin[order, pl.ds(pl.multiple_of(peer * own, own), own), :]
            if step < ctx_count:
                away[order, step, 0] = queries
                away[order, step, 1] = keys
                away[order, step, 2] = values
                exchange(order, step).start()
            else:
                at = stripe(ctx)
                terms_in[dest, ctx // slots, 0, :, at] = queries
                terms_in[dest, ctx // slots, 1, :, at] = keys
                terms_in[dest, ctx // slots, 2, :, at] = values

    pieces = partial.shape[2]
    tile = model // pieces

    def chain(order, piece):
        dest = dest_of(order)
        up = dest > group
        line = jnp.where(up, 0, 1)
        peer = jnp.where(up, group + 1, group - 1)
        return remote(
            sending.at[order, piece], partial.at[line, dest, piece], z_send.at[order, piece],
            z_recv.at[line, dest, piece], ctx, peer * 2 + core,
        )

    def came(line, dest, piece):
        remote(
            sending.at[0, piece], partial.at[line, dest, piece], z_send.at[0, piece],
            z_recv.at[line, dest, piece], ctx, partner,
        ).wait_recv()

    def term(dest, piece):
        cols = pl.ds(pl.multiple_of(piece * tile, tile), tile)
        result = None
        for half in range(2):
            for kind in range(3):
                part = dot32(terms_in[dest, half, kind], w_both[half, kind, cols, :], NT)
                result = part if result is None else result + part
        return result

    inner = (group > 0) & (group < groups - 1)

    def pass_on(order, _):
        dest = dest_of(order)
        for step in range(1, ctx_count):
            arrived(dest, step)
        line = jnp.where(dest > group, 0, 1)

        def one_piece(piece, _):
            total[...] = term(dest, piece)

            @pl.when(inner)
            def _():
                came(line, dest, piece)
                total[...] += partial[line, dest, piece].astype(jnp.float32)

            sending[order, piece] = total[...].astype(jnp.bfloat16)
            chain(order, piece).start()
            return 0

        lax.fori_loop(0, pieces, one_piece, 0)
        return 0

    ends, number = [], 0
    for order in range(groups):
        number += 2 * (groups - order) - 1
        ends.append(number - 1)
    spreads = {order: end + 1 for order, end in enumerate(ends) if end + 1 < number}

    def one_pair(index, _):
        stage = 0
        for end in ends[:-1]:
            stage = stage + jnp.where(index > end, 1, 0)
        first = 0
        for order in range(1, groups):
            first = jnp.where(stage == order, ends[order - 1] + 1, first)
        inside = index - first
        other = stage + (inside + 1) // 2
        odd = lax.rem(inside, 2)
        pair(
            dest_of(jnp.where(odd == 1, stage, other)), dest_of(jnp.where(odd == 1, other, stage))
        )
        for order, end in enumerate(ends[:-1]):

            @pl.when(index == end)
            def _():
                settle(order)

        for order, at in spreads.items():

            @pl.when(index == at)
            def _():
                spread(order)

        return 0

    first = min(ends[min(1, groups - 1)] + 2, number)
    lax.fori_loop(0, first, one_pair, 0)
    for copy in loads:
        copy.wait()
    early = 1 if first < number else 0
    if early:

        @pl.when(jnp.logical_not(inner))
        def _():
            pass_on(0, 0)

        lax.fori_loop(first, number, one_pair, 0)
    settle(groups - 1)
    for order in range(groups):
        if order not in spreads:
            spread(order)
    lax.fori_loop(jnp.where(inner, 0, early), groups - 1, pass_on, 0)
    for step in range(1, ctx_count):
        arrived(group, step)

    state = state_own[...].astype(jnp.float32)
    inverse = row_scale(state)

    def last_piece(piece, slope):
        cols = pl.ds(pl.multiple_of(piece * tile, tile), tile)
        total[...] = term(group, piece)

        @pl.when(group > 0)
        def _():
            came(0, group, piece)
            total[...] += partial[0, group, piece].astype(jnp.float32)

        @pl.when(group < groups - 1)
        def _():
            came(1, group, piece)
            total[...] += partial[1, group, piece].astype(jnp.float32)

        gained = total[...] * gain_ref[cols].astype(jnp.float32).reshape(1, tile)
        new_out[:, cols] = gained
        return slope + jnp.sum(
            gained * state_own[:, cols].astype(jnp.float32), axis=1, keepdims=True
        )

    slope = lax.fori_loop(0, pieces, last_piece, jnp.zeros((own, 1), jnp.float32))
    bend = inverse**3 * (slope / model)

    def update(piece, _):
        cols = pl.ds(pl.multiple_of(piece * tile, tile), tile)
        here = state_own[:, cols].astype(jnp.float32)
        gradient = readout_own[:, cols] + inverse * new_out[:, cols] - here * bend
        new_out[:, cols] = (
            here - STEP_SIZE * gradient + NOISE_SCALE * noise_own[:, cols].astype(jnp.float32)
        )
        return 0

    lax.fori_loop(0, pieces, update, 0)

    def sent(order, _):
        beside_copy(order).wait_send()
        for step in range(1, ctx_count):
            exchange(order, step).wait_send()

        @pl.when(order < groups - 1)
        def _():
            for piece in range(pieces):
                chain(order, piece).wait_send()

        return 0

    lax.fori_loop(0, groups, sent, 0)


def back(
    ctx_count, head_count, queries, kv, grads, parts, segs, logs, w_qkv, w_pair, state, noise,
    readout, gain,
):
    own, model = readout.shape
    width = w_qkv.shape[2]
    groups, pieces = head_count // 2, 4
    half, full, dma = jnp.bfloat16, jnp.float32, pltpu.SemaphoreType.DMA
    tile, lanes = model // pieces, ctx_count * own
    return pl.pallas_call(
        functools.partial(back_kernel, ctx_count, head_count),
        out_shape=jax.ShapeDtypeStruct((own, model), full),
        in_specs=[ANY] * 4 + [VMEM] * 2 + [ANY] * 5 + [VMEM],
        out_specs=VMEM,
        scratch_shapes=[
            pltpu.VMEM(queries.shape, half),
            pltpu.VMEM(kv.shape, half),
            pltpu.VMEM(queries.shape, half),
            pltpu.VMEM(queries.shape, half),
            pltpu.VMEM((groups, 2 * lanes, 2 * HEAD_DIM), full),
            pltpu.VMEM((groups, HEAD_DIM, lanes), full),
            pltpu.VMEM((groups, 1, lanes), full),
            pltpu.VMEM((groups, lanes, HEAD_DIM), half),
            pltpu.VMEM((groups, ctx_count, own, 2 * HEAD_DIM), half),
            pltpu.VMEM((2,) + w_qkv.shape, half),
            pltpu.VMEM((groups, ctx_count, own, 2 * HEAD_DIM), half),
            pltpu.VMEM((groups, ctx_count, 3, own, HEAD_DIM), half),
            pltpu.VMEM((groups, 2, 3, own, width), half),
            pltpu.VMEM((2, groups, pieces, own, tile), half),
            pltpu.VMEM((groups, pieces, own, tile), half),
            pltpu.VMEM((own, tile), full),
            pltpu.VMEM((own, model), half),
            pltpu.VMEM((own, model), half),
            pltpu.VMEM((own, model), full),
            dma((4,)),
            dma((groups,)),
            dma((groups,)),
            dma((groups, ctx_count)),
            dma((groups, ctx_count)),
            dma((groups, pieces)),
            dma((2, groups, pieces)),
            dma((5,)),
        ],
        compiler_params=pltpu.CompilerParams(
            collective_id=2, has_side_effects=True, vmem_limit_bytes=62 * 2**20
        ),
    )(
        queries, kv, grads, parts, segs, logs, w_qkv, w_pair, state, noise, readout, gain,
    )


def heads_body(state, norm_gain, w_qkv, w_out, probe, noise, segment_ids):
    head_count, ctx_count = lax.axis_size("head"), lax.axis_size("ctx")
    queries, kv, segs, parts, logs, grads, readout, w_pair = front(
        ctx_count, head_count, state, w_qkv, norm_gain, segment_ids, w_out, probe
    )
    return back(
        ctx_count, head_count, queries, kv, grads, parts, segs, logs, w_qkv, w_pair, state, noise,
        readout, norm_gain,
    )


def solution(mesh):
    placed = (
        P("ctx", None),
        P(),
        P(None, None, "head"),
        P("head", None),
        P("ctx", None),
        P(("ctx", "head"), None),
        P("ctx"),
    )

    def step(*args):
        heads = args[2].shape[2] // HEAD_DIM
        return (heads_body if lax.axis_size("ctx") == 2 * heads == 4 else body)(*args)

    return jax.shard_map(
        step, mesh=mesh, in_specs=placed, out_specs=P(("ctx", "head"), None), check_vma=False
    )
```

```python
import functools

import jax
import jax.numpy as jnp
from jax import lax
from jax.experimental import pallas as pl
from jax.experimental.pallas import tpu as pltpu
from jax.sharding import PartitionSpec as P

HEAD_DIM = 128
EPSILON = 1e-05
STEP_SIZE = 0.25
NOISE_SCALE = (2.0 * STEP_SIZE) ** 0.5
NEGATIVE = -1e30
LOG2E = 1.4426950408889634
MESH = pl.DeviceIdType.MESH
VMEM = pl.BlockSpec(memory_space=pltpu.VMEM)
ANY = pl.BlockSpec(memory_space=pl.ANY)
NT = (((1,), (1,)), ((), ()))
TN = (((0,), (0,)), ((), ()))
FORWARD_BLOCKS = (512, 512)
BACKWARD_BLOCKS = (512, 512)


def row_scale(matrix):
    return lax.rsqrt(jnp.mean(matrix * matrix, axis=-1, keepdims=True) + EPSILON)


def dot32(left, right, dims):
    return lax.dot_general(left, right, dims, preferred_element_type=jnp.float32)


def greet(axis, number, me):
    barrier = pltpu.get_barrier_semaphore()
    for step in range(1, number):
        pl.semaphore_signal(
            barrier, inc=1, device_id={axis: lax.rem(me + step, number)}, device_id_type=MESH
        )
    pl.semaphore_wait(barrier, number - 1)


def gather_kernel(
    number, key_ref, value_ref, seg_ref, normed_ref, w_ref, keys, values, segs, query_out, send_sem,
    recv_sem, own_sem,
):
    me = lax.axis_index("ctx")
    rows = key_ref.shape[0]
    greet("ctx", number, me)

    def place(index):
        return pl.ds(pl.multiple_of(index * rows, rows), rows)

    def send(slot, source, target, peer):
        copy = pltpu.make_async_remote_copy(
            src_ref=source,
            dst_ref=target,
            send_sem=send_sem.at[slot],
            recv_sem=recv_sem.at[slot],
            device_id={"ctx": peer},
            device_id_type=MESH,
        )
        copy.start()
        return copy

    mine = place(me)
    copies = []
    for step in range(1, number):
        copies.append(send(step, seg_ref, segs.at[me], lax.rem(me + step, number)))
    relay = number == 4
    if relay:
        low, high = lax.rem(me, 2), me // 2
        across, along = high * 2 + 1 - low, (1 - high) * 2 + low
        key_first = send(number, key_ref, keys.at[mine], across)
        value_first = send(number + 1, value_ref, values.at[mine], along)
        copies.append(send(number + 2, value_ref, values.at[mine], across))
        copies.append(send(number + 3, key_ref, keys.at[mine], along))
    else:
        for step in range(1, number):
            peer = lax.rem(me + step, number)
            copies.append(send(number + 2 * step, key_ref, keys.at[mine], peer))
            copies.append(send(number + 2 * step + 1, value_ref, values.at[mine], peer))
    pairs = ((key_ref, keys.at[mine]), (value_ref, values.at[mine]), (seg_ref, segs.at[me]))
    for index, (source, target) in enumerate(pairs):
        copy = pltpu.make_async_copy(source, target, own_sem.at[index])
        copy.start()
        copies.append(copy)
    tile = min(256, rows)

    def project(piece, _):
        at = pl.ds(pl.multiple_of(piece * tile, tile), tile)
        query_out[at, :] = jnp.dot(
            normed_ref[at, :], w_ref[...], preferred_element_type=jnp.float32
        ).astype(jnp.bfloat16)
        return 0

    lax.fori_loop(0, rows // tile, project, 0)
    if relay:
        key_first.wait()
        copies.append(send(number + 4, keys.at[place(across)], keys.at[place(across)], along))
        value_first.wait()
        copies.append(send(number + 5, values.at[place(along)], values.at[place(along)], across))
    for copy in copies:
        copy.wait()


def gather_keys(number, key_rows, value_rows, segment_ids, normed, w_query):
    rows, width = key_rows.shape
    seg = segment_ids.reshape(-1, 128)
    full = jax.ShapeDtypeStruct((number * rows, width), key_rows.dtype)
    keys, values, segs, queries = pl.pallas_call(
        functools.partial(gather_kernel, number),
        out_shape=(
            full,
            full,
            jax.ShapeDtypeStruct((number,) + seg.shape, seg.dtype),
            jax.ShapeDtypeStruct((rows, width), key_rows.dtype),
        ),
        in_specs=[VMEM] * 5,
        out_specs=(ANY, ANY, ANY, VMEM),
        scratch_shapes=[
            pltpu.SemaphoreType.DMA((3 * number + 6,)),
            pltpu.SemaphoreType.DMA((3 * number + 6,)),
            pltpu.SemaphoreType.DMA((3,)),
        ],
        compiler_params=pltpu.CompilerParams(collective_id=0, has_side_effects=True),
    )(key_rows, value_rows, seg, normed, w_query)
    return keys, values, segs.reshape(-1), queries


def block_ranges(table, index):
    return [table[index, column] for column in range(4)]


def forward_kernel(
    heads, bq, bk, table, query_ref, key_ref, value_ref, start_ref, pos_ref, out_ref, log_ref
):
    factor = HEAD_DIM ** (-0.5) * LOG2E
    blocks = query_ref.shape[0] // bq

    def one_block(index, _):
        low, inner_low, inner_high, high = block_ranges(table, index)
        rows = pl.ds(pl.multiple_of(index * bq, bq), bq)
        start, pos = start_ref[index], pos_ref[index]

        def step(masked, piece, carry):
            keys_at = pl.ds(pl.multiple_of(piece * bk, bk), bk)
            if masked:
                key_pos = piece * bk + lax.broadcasted_iota(jnp.int32, (bk, bq), 0)
                allowed = (key_pos >= start) & (key_pos <= pos)
            result = []
            for head in range(heads):
                top, total, acc = carry[head]
                cols = pl.ds(head * HEAD_DIM, HEAD_DIM)
                scores = dot32(key_ref[keys_at, cols], query_ref[rows, cols], NT)
                if masked:
                    scores = jnp.where(allowed, scores, NEGATIVE)
                new_top = jnp.maximum(top, jnp.max(scores, axis=0, keepdims=True) * factor)
                weights = jnp.exp2(scores * factor - new_top)
                scale = jnp.exp2(top - new_top)
                total = total * scale + jnp.sum(weights, axis=0, keepdims=True)
                acc = acc * scale + dot32(
                    value_ref[keys_at, cols], weights.astype(jnp.bfloat16), TN
                )
                result.append((new_top, total, acc))
            return tuple(result)

        carry = tuple(
            (
                jnp.full((1, bq), NEGATIVE, jnp.float32),
                jnp.zeros((1, bq), jnp.float32),
                jnp.zeros((HEAD_DIM, bq), jnp.float32),
            )
            for _ in range(heads)
        )
        carry = lax.fori_loop(low, inner_low, functools.partial(step, True), carry)
        carry = lax.fori_loop(inner_low, inner_high, functools.partial(step, False), carry)
        carry = lax.fori_loop(inner_high, high, functools.partial(step, True), carry)
        for head in range(heads):
            top, total, acc = carry[head]
            out_ref[rows, pl.ds(head * HEAD_DIM, HEAD_DIM)] = (acc / total).T.astype(jnp.bfloat16)
            log_ref[index, pl.ds(head, 1), :] = top + jnp.log2(total)
        return 0

    lax.fori_loop(0, blocks, one_block, 0)


def backward_kernel(
    heads, bq, bk, table, query_ref, key_ref, value_ref, grad_ref, out_ref, log_ref, start_ref,
    pos_ref, query_out, pair_out, pair_acc,
):
    score_scale = HEAD_DIM ** (-0.5)
    factor = score_scale * LOG2E
    blocks = query_ref.shape[0] // bq
    width = heads * HEAD_DIM
    pair_rows = pair_acc.shape[0]

    def clear(piece, _):
        at = pl.ds(pl.multiple_of(piece * bk, bk), bk)
        pair_acc[at, :] = jnp.zeros((bk, 2 * width), jnp.float32)
        return 0

    lax.fori_loop(0, pair_rows // bk, clear, 0)

    def one_block(index, _):
        low, inner_low, inner_high, high = block_ranges(table, index)
        rows = pl.ds(pl.multiple_of(index * bq, bq), bq)
        start, pos = start_ref[index], pos_ref[index]
        deltas, logs = [], []
        for head in range(heads):
            cols = pl.ds(head * HEAD_DIM, HEAD_DIM)
            product = grad_ref[rows, cols].astype(jnp.float32) * out_ref[rows, cols].astype(
                jnp.float32
            )
            deltas.append(jnp.sum(product.T, axis=0, keepdims=True))
            logs.append(log_ref[index, pl.ds(head, 1), :])

        def step(masked, piece, carry):
            keys_at = pl.ds(pl.multiple_of(piece * bk, bk), bk)
            if masked:
                key_pos = piece * bk + lax.broadcasted_iota(jnp.int32, (bk, bq), 0)
                allowed = (key_pos >= start) & (key_pos <= pos)
            result = []
            for head in range(heads):
                cols = pl.ds(head * HEAD_DIM, HEAD_DIM)
                value_cols = pl.ds(width + head * HEAD_DIM, HEAD_DIM)
                key_block, query_block = key_ref[keys_at, cols], query_ref[rows, cols]
                grad_block = grad_ref[rows, cols]
                scores = dot32(key_block, query_block, NT)
                probabilities = jnp.exp2(scores * factor - logs[head])
                if masked:
                    probabilities = jnp.where(allowed, probabilities, 0.0)
                dprobs = dot32(value_ref[keys_at, cols], grad_block, NT)
                dscores = (probabilities * (dprobs - deltas[head])).astype(jnp.bfloat16)
                pair_acc[keys_at, value_cols] += jnp.dot(
                    probabilities.astype(jnp.bfloat16),
                    grad_block,
                    preferred_element_type=jnp.float32,
                )
                pair_acc[keys_at, cols] += jnp.dot(
                    dscores, query_block, preferred_element_type=jnp.float32
                )
                result.append(carry[head] + dot32(key_block, dscores, TN))
            return tuple(result)

        carry = tuple(jnp.zeros((HEAD_DIM, bq), jnp.float32) for _ in range(heads))
        carry = lax.fori_loop(low, inner_low, functools.partial(step, True), carry)
        carry = lax.fori_loop(inner_low, inner_high, functools.partial(step, False), carry)
        carry = lax.fori_loop(inner_high, high, functools.partial(step, True), carry)
        for head in range(heads):
            query_out[rows, pl.ds(head * HEAD_DIM, HEAD_DIM)] = (
                carry[head].T * score_scale
            ).astype(jnp.bfloat16)
        return 0

    lax.fori_loop(0, blocks, one_block, 0)

    def flush(piece, _):
        at = pl.ds(pl.multiple_of(piece * bk, bk), bk)
        pair_out[at, :width] = (pair_acc[at, :width] * score_scale).astype(jnp.bfloat16)
        pair_out[at, width:] = pair_acc[at, width:].astype(jnp.bfloat16)
        return 0

    lax.fori_loop(0, pair_rows // bk, flush, 0)


def make_table(start, pos, bq, bk):
    starts, places = start.reshape(-1, bq), pos.reshape(-1, bq)
    low = starts[:, 0] // bk
    inner_low = (starts[:, -1] + bk - 1) // bk
    inner_high = jnp.maximum(inner_low, (places[:, 0] + 1) // bk)
    high = places[:, -1] // bk + 1
    return jnp.stack([low, inner_low, inner_high, high], axis=1).astype(jnp.int32)


def middle_kernel(
    number, part_ref, w_any, state_ref, probe_ref, grad_out, readout_out, w_ref, joined, half,
    sending, landing, send_sem, recv_sem, back_send, back_recv, w_sem,
):
    me = lax.axis_index("head")
    width = part_ref.shape[1]
    own = state_ref.shape[0]
    model = state_ref.shape[1]
    w_copy = pltpu.make_async_copy(w_any, w_ref, w_sem)
    w_copy.start()
    greet("head", number, me)
    my_cols = pl.ds(pl.multiple_of(me * width, width), width)
    my_rows = pl.ds(pl.multiple_of(me * own, own), own)
    copies = []
    for step in range(1, number):
        peer = lax.rem(me + step, number)
        copy = pltpu.make_async_remote_copy(
            src_ref=part_ref.at[pl.ds(pl.multiple_of(peer * own, own), own)],
            dst_ref=joined.at[:, my_cols],
            send_sem=send_sem.at[step],
            recv_sem=recv_sem.at[step],
            device_id={"head": peer},
            device_id_type=MESH,
        )
        copy.start()
        copies.append(copy)
    joined[:, my_cols] = part_ref[my_rows, :]
    w_copy.wait()
    for copy in copies:
        copy.wait()

    tile = min(256, model)

    def project(piece, carry):
        squares, products = carry
        cols = pl.ds(pl.multiple_of(piece * tile, tile), tile)
        layer = state_ref[:, cols].astype(jnp.float32) + jnp.dot(
            joined[...], w_ref[:, cols], preferred_element_type=jnp.float32
        )
        readout_out[:, cols] = layer
        squares = squares + jnp.sum(layer * layer, axis=1, keepdims=True)
        products = products + jnp.sum(
            layer * probe_ref[:, cols].astype(jnp.float32), axis=1, keepdims=True
        )
        return squares, products

    zero = jnp.zeros((own, 1), jnp.float32)
    squares, products = lax.fori_loop(0, model // tile, project, (zero, zero))
    scale = lax.rsqrt(squares / model + EPSILON)
    bend = scale**3 * (products / model)

    def finish(piece, _):
        cols = pl.ds(pl.multiple_of(piece * tile, tile), tile)
        readout = scale * probe_ref[:, cols].astype(jnp.float32) - readout_out[:, cols] * bend
        readout_out[:, cols] = readout
        half[:, cols] = readout.astype(jnp.bfloat16)
        return 0

    lax.fori_loop(0, model // tile, finish, 0)
    copies = []
    for step in range(1, number):
        peer = lax.rem(me + step, number)
        sending[step] = dot32(
            half[...], w_ref[pl.ds(pl.multiple_of(peer * width, width), width), :], NT
        ).astype(jnp.bfloat16)
        copy = pltpu.make_async_remote_copy(
            src_ref=sending.at[step],
            dst_ref=landing.at[my_rows],
            send_sem=back_send.at[step],
            recv_sem=back_recv.at[step],
            device_id={"head": peer},
            device_id_type=MESH,
        )
        copy.start()
        copies.append(copy)
    landing[my_rows, :] = dot32(half[...], w_ref[my_cols, :], NT).astype(jnp.bfloat16)
    for copy in copies:
        copy.wait()
    grad_out[...] = landing[...]


def middle(number, part, w_full, state_own, probe_own):
    rows, width = part.shape
    own, model = state_own.shape
    return pl.pallas_call(
        functools.partial(middle_kernel, number),
        out_shape=(
            jax.ShapeDtypeStruct((rows, width), jnp.bfloat16),
            jax.ShapeDtypeStruct((own, model), jnp.float32),
        ),
        in_specs=[VMEM, ANY, VMEM, VMEM],
        out_specs=(VMEM, VMEM),
        scratch_shapes=[
            pltpu.VMEM(w_full.shape, jnp.bfloat16),
            pltpu.VMEM((own, number * width), jnp.bfloat16),
            pltpu.VMEM((own, model), jnp.bfloat16),
            pltpu.VMEM((number, own, width), jnp.bfloat16),
            pltpu.VMEM((rows, width), jnp.bfloat16),
            pltpu.SemaphoreType.DMA((number,)),
            pltpu.SemaphoreType.DMA((number,)),
            pltpu.SemaphoreType.DMA((number,)),
            pltpu.SemaphoreType.DMA((number,)),
            pltpu.SemaphoreType.DMA,
        ],
        compiler_params=pltpu.CompilerParams(
            collective_id=1, has_side_effects=True, vmem_limit_bytes=60 * 2**20
        ),
    )(part, w_full, state_own, probe_own)


def tail_kernel(
    ctx_count, number, pair_any, query_ref, w_ref, sum_out, own_pair, arriving, gathered, terms,
    from_partner, reduced, landing, ctx_send, ctx_recv, p_send, p_recv, z_send, z_recv, own_sem,
):
    ctx, me = lax.axis_index("ctx"), lax.axis_index("head")
    groups = number // 2
    group, core = me // 2, lax.rem(me, 2)
    partner = group * 2 + 1 - core
    rows, width = query_ref.shape
    own, model = sum_out.shape
    chunk = 2 * own
    own_copy = pltpu.make_async_copy(
        pair_any.at[pl.ds(pl.multiple_of(ctx * rows, rows), rows)], own_pair, own_sem
    )
    own_copy.start()
    barrier = pltpu.get_barrier_semaphore()
    peers = [{"ctx": lax.rem(ctx + step, ctx_count)} for step in range(1, ctx_count)]
    peers.append({"head": partner})
    for step in range(1, groups):
        peers.append({"head": lax.rem(group + step, groups) * 2 + core})
    for peer in peers:
        pl.semaphore_signal(barrier, inc=1, device_id=peer, device_id_type=MESH)
    pl.semaphore_wait(barrier, len(peers))

    def chunk_start(order):
        dest = lax.rem(group + order + 1, groups)
        return dest, pl.multiple_of(dest * chunk, chunk)

    def ctx_copy(order, step):
        target = lax.rem(ctx - step + ctx_count, ctx_count)
        _, first = chunk_start(order)
        return pltpu.make_async_remote_copy(
            src_ref=pair_any.at[pl.ds(pl.multiple_of(target * rows + first, chunk), chunk)],
            dst_ref=arriving.at[order, step - 1],
            send_sem=ctx_send.at[order, step],
            recv_sem=ctx_recv.at[order, step],
            device_id={"ctx": target},
            device_id_type=MESH,
        )

    for order in range(groups):
        for step in range(1, ctx_count):

            @pl.when(step <= ctx)
            def _():
                ctx_copy(order, step).start()

    own_copy.wait()
    tile = min(512, model)
    mine = pl.ds(pl.multiple_of(core * own, own), own)
    theirs = pl.ds(pl.multiple_of((1 - core) * own, own), own)
    waiting = []
    for order in range(groups):
        dest, first = chunk_start(order)
        at = pl.ds(first, chunk)
        gathered[...] = own_pair[at, :].astype(jnp.float32)
        for step in range(1, ctx_count):

            @pl.when(ctx + step < ctx_count)
            def _():
                ctx_copy(order, step).wait_recv()
                gathered[...] += arriving[order, step - 1].astype(jnp.float32)

        def multiply(piece, _):
            cols = pl.ds(pl.multiple_of(piece * tile, tile), tile)
            term = dot32(query_ref[at, :], w_ref[0, cols, :], NT)
            term += dot32(gathered[:, :width].astype(jnp.bfloat16), w_ref[1, cols, :], NT)
            term += dot32(gathered[:, width:].astype(jnp.bfloat16), w_ref[2, cols, :], NT)
            terms[order, :, cols] = term.astype(jnp.bfloat16)
            return 0

        lax.fori_loop(0, model // tile, multiply, 0)
        copy = pltpu.make_async_remote_copy(
            src_ref=terms.at[order, theirs],
            dst_ref=from_partner.at[order],
            send_sem=p_send.at[order],
            recv_sem=p_recv.at[order],
            device_id={"head": partner},
            device_id_type=MESH,
        )
        copy.start()
        copy.wait()
        both = terms[order, mine, :].astype(jnp.float32) + from_partner[order].astype(jnp.float32)
        if order < groups - 1:
            reduced[order] = both.astype(jnp.bfloat16)
            copy = pltpu.make_async_remote_copy(
                src_ref=reduced.at[order],
                dst_ref=landing.at[order],
                send_sem=z_send.at[order],
                recv_sem=z_recv.at[order],
                device_id={"head": dest * 2 + core},
                device_id_type=MESH,
            )
            copy.start()
            waiting.append(copy)
        else:
            sum_out[...] = both
    for order, copy in enumerate(waiting):
        copy.wait()
        sum_out[...] += landing[order].astype(jnp.float32)
    for order in range(groups):
        for step in range(1, ctx_count):

            @pl.when(step <= ctx)
            def _():
                ctx_copy(order, step).wait_send()


def tail(ctx_count, number, pair, query_grad, w_qkv):
    rows, width = query_grad.shape
    model = w_qkv.shape[1]
    own, groups = rows // number, number // 2
    half, full = jnp.bfloat16, jnp.float32
    dma = pltpu.SemaphoreType.DMA
    return pl.pallas_call(
        functools.partial(tail_kernel, ctx_count, number),
        out_shape=jax.ShapeDtypeStruct((own, model), full),
        in_specs=[ANY, VMEM, VMEM],
        out_specs=VMEM,
        scratch_shapes=[
            pltpu.VMEM((rows, 2 * width), half),
            pltpu.VMEM((groups, ctx_count - 1, 2 * own, 2 * width), half),
            pltpu.VMEM((2 * own, 2 * width), full),
            pltpu.VMEM((groups, 2 * own, model), half),
            pltpu.VMEM((groups, own, model), half),
            pltpu.VMEM((groups, own, model), half),
            pltpu.VMEM((groups, own, model), half),
            dma((groups, ctx_count)),
            dma((groups, ctx_count)),
            dma((groups,)),
            dma((groups,)),
            dma((groups,)),
            dma((groups,)),
            dma,
        ],
        compiler_params=pltpu.CompilerParams(
            collective_id=2, has_side_effects=True, vmem_limit_bytes=60 * 2**20
        ),
    )(pair, query_grad, w_qkv)


def body(state, norm_gain, w_qkv, w_out, probe, noise, segment_ids):
    local_rows, model_width = state.shape
    width = w_qkv.shape[2]
    local_heads = width // HEAD_DIM
    head_count = lax.axis_size("head")
    ctx_count = lax.axis_size("ctx")
    ctx_index = lax.axis_index("ctx")
    own_rows = local_rows // head_count
    row_start = lax.axis_index("head") * own_rows
    w_full = lax.all_gather(w_out, "head", axis=0, tiled=True)
    state_f = state.astype(jnp.float32)
    gain_full = norm_gain.astype(jnp.float32)
    inverse = row_scale(state_f)
    normed = (state_f * inverse * gain_full).astype(jnp.bfloat16)

    def project(index):
        return jnp.dot(normed, w_qkv[index], preferred_element_type=jnp.float32).astype(
            jnp.bfloat16
        )

    key_rows, value_rows = project(1), project(2)
    keys, values, segs, query_rows = gather_keys(
        ctx_count, key_rows, value_rows, segment_ids, normed, w_qkv[0]
    )
    total_rows = keys.shape[0]
    pos = ctx_index * local_rows + jnp.arange(local_rows, dtype=jnp.int32)
    start = jnp.sum((segs[None, :] < segment_ids[:, None]).astype(jnp.int32), axis=1)
    fq, fk = (min(local_rows, size) for size in FORWARD_BLOCKS)
    gq, gk = (min(local_rows, size) for size in BACKWARD_BLOCKS)
    smem = pl.BlockSpec(memory_space=pltpu.SMEM)
    params = pltpu.CompilerParams(vmem_limit_bytes=60 * 2**20)
    outputs, logs = pl.pallas_call(
        functools.partial(forward_kernel, local_heads, fq, fk),
        out_shape=(
            jax.ShapeDtypeStruct((local_rows, width), jnp.bfloat16),
            jax.ShapeDtypeStruct((local_rows // fq, local_heads, fq), jnp.float32),
        ),
        in_specs=[smem] + [VMEM] * 5,
        out_specs=(VMEM, VMEM),
        compiler_params=params,
        cost_estimate=pl.CostEstimate(
            flops=4 * local_rows * total_rows * width, bytes_accessed=0, transcendentals=0
        ),
    )(
        make_table(start, pos, fq, fk),
        query_rows,
        keys,
        values,
        start.reshape(-1, 1, fq),
        pos.reshape(-1, 1, fq),
    )
    state_half = lax.dynamic_slice_in_dim(state, row_start, own_rows, 0)
    probe_own = lax.dynamic_slice_in_dim(probe, row_start, own_rows, 0)
    state_own = state_half.astype(jnp.float32)
    inverse_own = row_scale(state_own)
    grads_out, readout_own = middle(head_count, outputs, w_full, state_half, probe_own)
    query_grad, pair = pl.pallas_call(
        functools.partial(backward_kernel, local_heads, gq, gk),
        out_shape=(
            jax.ShapeDtypeStruct((local_rows, width), jnp.bfloat16),
            jax.ShapeDtypeStruct((total_rows, 2 * width), jnp.bfloat16),
        ),
        in_specs=[smem] + [VMEM] * 8,
        out_specs=(VMEM, VMEM),
        scratch_shapes=[pltpu.VMEM((total_rows, 2 * width), jnp.float32)],
        compiler_params=params,
        cost_estimate=pl.CostEstimate(
            flops=10 * local_rows * total_rows * width, bytes_accessed=0, transcendentals=0
        ),
    )(
        make_table(start, pos, gq, gk),
        query_rows,
        keys,
        values,
        grads_out,
        outputs,
        logs.reshape(local_rows // fq, local_heads, fq),
        start.reshape(-1, 1, gq),
        pos.reshape(-1, 1, gq),
    )
    normed_grad = tail(ctx_count, head_count, pair, query_grad, w_qkv)
    gain_grad = normed_grad * gain_full
    gradient = (
        readout_own
        + inverse_own * gain_grad
        - state_own * inverse_own**3 * jnp.mean(gain_grad * state_own, axis=-1, keepdims=True)
    )
    return state_own - STEP_SIZE * gradient + jnp.sqrt(2.0 * STEP_SIZE) * noise.astype(jnp.float32)


def remote(source, target, send_sem, recv_sem, ctx, head):
    return pltpu.make_async_remote_copy(
        src_ref=source,
        dst_ref=target,
        send_sem=send_sem,
        recv_sem=recv_sem,
        device_id={"ctx": ctx, "head": head},
        device_id_type=MESH,
    )


def place():
    ctx, me = lax.axis_index("ctx"), lax.axis_index("head")
    return ctx, me, me // 2, lax.rem(me, 2)


def announce(peers):
    barrier = pltpu.get_barrier_semaphore()
    for ctx, head in peers:
        pl.semaphore_signal(
            barrier, inc=1, device_id={"ctx": ctx, "head": head}, device_id_type=MESH
        )


def await_all(peers):
    pl.semaphore_wait(pltpu.get_barrier_semaphore(), len(peers))


def far_first(groups, group, step):
    result = 0
    for index in range(groups):
        order = sorted(range(groups), key=lambda other: (-abs(other - index), -other))
        result = jnp.where(group == index, order[step], result)
    return result


def step_kernel(
    ctx_count, head_count, state_any, w_any, gain_ref, seg_ref, w_out_any, probe_any, noise_any,
    new_out, state_v, query_buf, kv_buf, w_ref, joined, half, sending, state_own, probe_own,
    noise_own, query_out, kv_out, part_out, readout_out, segs_out, log_v, grad_v, w_both, pair_acc,
    query_acc, deltas, query_fin, pair_buf, beside_in, away_buf, terms_in, partial, passing, sum_v,
    load_sem, w_sem, q_send, q_recv, kv_send, kv_recv, pass_send, seg_send, seg_recv, line_send,
    line_recv, plane_send, plane_recv, beside_send, beside_recv, shard_send, shard_recv, shard_sem,
    out_send, out_recv, back_send, back_recv, row_sem, pair_send, pair_recv, b_send, b_recv, a_send,
    a_recv, z_send, z_recv,
):
    ctx, me, group, core = place()
    rows, model = state_any.shape
    own, groups = rows // head_count, head_count // 2
    slots = w_any.shape[2] // HEAD_DIM
    chunk = 2 * own
    partner = group * 2 + 1 - core

    def at(piece):
        return pl.ds(pl.multiple_of(piece * chunk, chunk), chunk)

    def own_at(piece):
        return pl.ds(pl.multiple_of(piece * own, own), own)

    def load_state(piece):
        return pltpu.make_async_copy(
            state_any.at[at(piece)], state_v.at[at(piece)], load_sem.at[piece]
        )

    load_state(0).start()
    w_loads = [
        pltpu.make_async_copy(w_any.at[t], w_both.at[core, t], w_sem.at[t]) for t in range(3)
    ]
    for copy in w_loads:
        copy.start()
    for piece in range(1, groups):
        load_state(piece).start()
    my_rows = own_at(me)
    shard = w_out_any.shape[0]
    part, quarter = shard // 2, shard // ctx_count
    later_loads = [
        pltpu.make_async_copy(state_any.at[my_rows], state_own, row_sem.at[0]),
        pltpu.make_async_copy(probe_any.at[my_rows], probe_own, row_sem.at[1]),
        pltpu.make_async_copy(noise_any, noise_own, row_sem.at[2]),
        pltpu.make_async_copy(
            w_out_any, w_ref.at[pl.ds(pl.multiple_of(me * shard, shard), shard)], shard_sem
        ),
    ]
    for copy in later_loads:
        copy.start()
    peers = [(lax.rem(ctx + step, ctx_count), partner) for step in range(ctx_count)]
    for far in range(groups):
        for step in range(ctx_count):
            if far or step:
                peers.append(
                    (lax.rem(ctx + step, ctx_count), lax.rem(group + far, groups) * 2 + core)
                )
    announce(peers)

    low, high = lax.rem(ctx, 2), ctx // 2
    which = lax.rem(low + high, 2)
    across, along = high * 2 + 1 - low, (1 - high) * 2 + low

    def shard_rows(origin, first, size):
        return pl.ds(pl.multiple_of((origin * 2 + core) * shard + first, size), size)

    def line_copy(way, origin, axis, mine):
        first = which * part + axis * quarter
        here = shard_rows(origin, first, quarter)
        source = (
            w_out_any.at[pl.ds(pl.multiple_of(first, quarter), quarter)] if mine else w_ref.at[here]
        )
        other = group + 1 if way == 0 else group - 1
        return remote(
            source, w_ref.at[here], line_send.at[way, axis, origin], line_recv.at[axis, origin],
            ctx, other * 2 + core,
        )

    def plane_copy(axis, origin, kept):
        here = shard_rows(origin, kept * part + axis * quarter, quarter)
        return remote(
            w_ref.at[here], w_ref.at[here], plane_send.at[axis, origin],
            plane_recv.at[axis, origin], along if axis else across, me,
        )

    def beside_copy(kind, origin):
        kept = which if kind < 2 else 1 - which
        here = shard_rows(origin, kept * part + (kind % 2) * quarter, quarter)
        return remote(
            w_ref.at[here], w_ref.at[here], beside_send.at[kind, origin],
            beside_recv.at[kind, origin], ctx, partner,
        )

    def shard_copy():
        return remote(
            w_out_any, w_ref.at[pl.ds(pl.multiple_of(me * shard, shard), shard)], shard_send,
            shard_recv, ctx, partner,
        )

    has_up, has_down = group < groups - 1, group > 0

    def each_origin(distance, work):
        for way in range(2):
            origin = group - distance if way == 0 else group + distance

            @pl.when(origin >= 0 if way == 0 else origin < groups)
            def _():
                work(way, origin)

    def line_arrived(distance, axis):
        def work(way, origin):
            line_copy(way, origin, axis, False).wait_recv()

            @pl.when(has_up if way == 0 else has_down)
            def _():
                line_copy(way, origin, axis, False).start()

            plane_copy(axis, origin, which).start()
            beside_copy(axis, origin).start()

        each_origin(distance, work)

    def plane_arrived(distance, axis):
        def work(way, origin):
            plane_copy(axis, origin, 1 - which).wait_recv()
            beside_copy(2 + axis, origin).start()

        each_origin(distance, work)

    def weights_sent(distance):
        def work(way, origin):
            for axis in range(2):

                @pl.when(has_up if way == 0 else has_down)
                def _():
                    line_copy(way, origin, axis, False).wait_send()

                plane_copy(axis, origin, which).wait_send()
            for kind in range(4):
                beside_copy(kind, origin).wait_send()

        each_origin(distance, work)

    def own_lines(work):
        for axis in range(2):

            @pl.when(has_up)
            def _():
                work(line_copy(0, group, axis, True))

            @pl.when(has_down)
            def _():
                work(line_copy(1, group, axis, True))

    for copy in w_loads:
        copy.wait()
    gain = gain_ref[...].astype(jnp.float32).reshape(1, model)

    def away(slot, kind, piece, dest):
        head = group * 2 + kind
        return (
            remote(
                query_buf.at[slot, piece, kind], query_out.at[piece, ctx],
                q_send.at[slot, kind, piece], q_recv.at[ctx, piece], dest, head,
            ),
            remote(
                kv_buf.at[slot, kind, piece], kv_out.at[kind, piece, ctx],
                kv_send.at[slot, kind, piece], kv_recv.at[kind, ctx, piece], dest, head,
            ),
        )

    def beside(slot, piece):
        result = [
            remote(
                query_buf.at[slot, piece, 1 - core], query_out.at[piece, ctx],
                q_send.at[slot, 1 - core, piece], q_recv.at[ctx, piece], ctx, partner,
            )
        ]
        for kind in range(2):
            result.append(
                remote(
                    kv_buf.at[slot, kind, piece], kv_out.at[kind, piece, ctx],
                    kv_send.at[slot, kind, piece], kv_recv.at[kind, ctx, piece], ctx, partner,
                )
            )
        return result

    def project(piece):
        load_state(piece).wait()
        block = state_v[at(piece), :].astype(jnp.float32)
        normed = (block * row_scale(block) * gain).astype(jnp.bfloat16)
        for t in range(3):
            result = jnp.dot(normed, w_both[core, t], preferred_element_type=jnp.float32).astype(
                jnp.bfloat16
            )
            for slot in range(slots):
                cut = result[:, slot * HEAD_DIM : (slot + 1) * HEAD_DIM]
                if t == 0:
                    query_buf[slot, piece, 0] = cut[:own]
                    query_buf[slot, piece, 1] = cut[own:]
                else:
                    kv_buf[slot, t - 1, piece] = cut

    def send_heads(piece):
        for slot in range(slots):
            dest = core * slots + slot

            @pl.when(dest != ctx)
            def _():
                for kind in range(2):
                    for copy in away(slot, kind, piece, dest):
                        copy.start()

            @pl.when(dest == ctx)
            def _():
                query_out[piece, ctx] = query_buf[slot, piece, core]
                for kind in range(2):
                    kv_out[kind, piece, ctx] = kv_buf[slot, kind, piece]
                for copy in beside(slot, piece):
                    copy.start()

    project(0)
    await_all(peers)
    own_lines(lambda copy: copy.start())
    send_heads(0)
    shard_copy().start()
    segs = []
    for step in range(1, ctx_count):
        copy = remote(
            seg_ref, segs_out.at[ctx], seg_send.at[step], seg_recv.at[step],
            lax.rem(ctx + step, ctx_count), me,
        )
        copy.start()
        segs.append(copy)
    segs_out[ctx] = seg_ref[...]

    def project_and_send(piece, _):
        project(piece)
        send_heads(piece)
        return 0

    lax.fori_loop(1, groups, project_and_send, 0)

    def hand_over(piece, step):
        source = lax.rem(ctx + step, ctx_count)
        return remote(
            kv_out.at[core, piece, source], kv_out.at[core, piece, source],
            pass_send.at[step, piece], kv_recv.at[core, source, piece], ctx, partner,
        )

    for piece in range(groups):
        for step in range(1, ctx_count):
            copy = hand_over(piece, step)
            copy.wait_recv()
            copy.start()
        if piece == 0:
            line_arrived(1, 0)
        if piece == min(2, groups - 1):
            line_arrived(1, 1)
    line_arrived(2, 0)

    def got_query(source, piece):
        remote(
            query_out.at[piece, source], query_out.at[piece, source],
            q_send.at[0, 0, piece], q_recv.at[source, piece], ctx, partner,
        ).wait_recv()

    def got_kv(kind, source, piece):
        remote(
            kv_out.at[kind, piece, source], kv_out.at[kind, piece, source],
            kv_send.at[0, 0, piece], kv_recv.at[kind, source, piece], ctx, partner,
        ).wait_recv()

    def gather(piece, _):
        for step in range(1, ctx_count):
            source = lax.rem(ctx + step, ctx_count)
            got_query(source, piece)
            got_kv(1 - core, source, piece)
            hand_over(piece, step).wait_send()

        @pl.when(ctx // slots != core)
        def _():
            got_query(ctx, piece)
            for kind in range(2):
                got_kv(kind, ctx, piece)

        return 0

    lax.fori_loop(0, groups, gather, 0)
    for copy in segs:
        copy.wait()
    pair_copy = remote(w_any, w_both.at[core], pair_send, pair_recv, ctx, partner)
    pair_copy.start()

    def cols_of(group_at, ctx_at):
        head = group_at * ctx_count + ctx_at
        return pl.ds(pl.multiple_of(head * HEAD_DIM, HEAD_DIM), HEAD_DIM)

    factor = HEAD_DIM ** (-0.5) * LOG2E
    sub = groups * own
    seg_all = segs_out[...]

    def below(value):
        count = jnp.where(seg_all < value, 1.0, 0.0)
        for axis in (0, 1, 2):
            count = jnp.sum(count, axis=axis, keepdims=True)
        return count[0]

    first_bound, second_bound = below(1), below(2)
    lane = lax.broadcasted_iota(jnp.int32, (1, sub), 1)
    inside = (lane // own) * (2 * own) + core * own + lane % own
    key_row = lax.broadcasted_iota(jnp.int32, (rows, sub), 0)

    def out_copy(tile, order, other):
        return remote(
            part_out.at[other, tile], joined.at[:, cols_of(group, ctx)],
            out_send.at[tile, order], out_recv.at[group, ctx], tile, other * 2 + core,
        )

    def one_tile(tile, _):
        query = query_out[:, tile].reshape(sub, HEAD_DIM)
        pos = (tile * rows + inside).astype(jnp.float32)
        start = jnp.where(
            pos >= second_bound, second_bound, jnp.where(pos >= first_bound, first_bound, 0.0)
        ).astype(jnp.int32)

        def step(diagonal, piece, carry):
            top, total, acc = carry
            scores = dot32(kv_out[0, :, piece].reshape(rows, HEAD_DIM), query, NT)
            allowed = key_row >= start - piece * rows
            if diagonal:
                allowed = allowed & (key_row <= inside)
            scores = jnp.where(allowed, scores, NEGATIVE)
            new_top = jnp.maximum(top, jnp.max(scores, axis=0, keepdims=True) * factor)
            weights = jnp.exp2(scores * factor - new_top)
            scale = jnp.exp2(top - new_top)
            total = total * scale + jnp.sum(weights, axis=0, keepdims=True)
            acc = acc * scale + dot32(
                kv_out[1, :, piece].reshape(rows, HEAD_DIM), weights.astype(jnp.bfloat16), TN
            )
            return new_top, total, acc

        carry = (
            jnp.full((1, sub), NEGATIVE, jnp.float32),
            jnp.zeros((1, sub), jnp.float32),
            jnp.zeros((HEAD_DIM, sub), jnp.float32),
        )
        carry = lax.fori_loop(0, tile, functools.partial(step, False), carry)
        top, total, acc = step(True, tile, carry)
        result = (acc / total).T.astype(jnp.bfloat16)
        log_row = top + jnp.log2(total)
        for index in range(groups):
            part_out[index, tile] = result[index * own : (index + 1) * own]
            log_v[index, :, own_at(tile)] = log_row[:, index * own : (index + 1) * own]
        for order in range(groups):
            other = far_first(groups, group, order)
            if order == groups - 1:

                @pl.when(tile != ctx)
                def _():
                    out_copy(tile, order, other).start()

                @pl.when(tile == ctx)
                def _():
                    joined[:, cols_of(group, ctx)] = part_out[group, tile]

            else:
                out_copy(tile, order, other).start()

        @pl.when(tile == 1)
        def _():
            line_arrived(2, 1)

        return 0

    lax.fori_loop(0, ctx_count, one_tile, 0)
    for copy in later_loads:
        copy.wait()
    sources = []
    for far in range(groups):
        for step in range(ctx_count):
            if far or step:
                sources.append((lax.rem(group + far, groups), lax.rem(ctx + step, ctx_count)))
    tile = min(256, model)
    wide = ctx_count * HEAD_DIM
    zero = jnp.zeros((own, 1), jnp.float32)
    for axis in range(2):
        plane_arrived(1, axis)
    for distance in range(3, groups):
        line_arrived(distance, 0)
    for axis in range(2):
        plane_arrived(2, axis)
    for distance in range(3, groups):
        line_arrived(distance, 1)
    shard_copy().wait_recv()

    def heads_arrived(order):
        other = far_first(groups, group, order)
        if order < groups - 1:
            for kind in range(4):
                beside_copy(kind, other).wait_recv()
        for step in range(ctx_count):
            if order < groups - 1 or step:
                peer = lax.rem(ctx + step, ctx_count)
                remote(
                    part_out.at[0, 0], joined.at[:, cols_of(other, peer)],
                    out_send.at[0, 0], out_recv.at[other, peer], peer, other * 2 + core,
                ).wait_recv()

    for order in range(groups - 1, 0, -1):
        heads_arrived(order)
    farthest = far_first(groups, group, 0)
    near = pl.ds(pl.multiple_of(jnp.where(farthest == 0, wide, 0), wide), model - wide)
    far = pl.ds(pl.multiple_of(farthest * wide, wide), wide)

    def near_layer(piece, _):
        cols = pl.ds(pl.multiple_of(piece * tile, tile), tile)
        readout_out[:, cols] = state_own[:, cols].astype(jnp.float32) + jnp.dot(
            joined[:, near], w_ref[near, cols], preferred_element_type=jnp.float32
        )
        return 0

    lax.fori_loop(0, model // tile, near_layer, 0)
    for distance in range(3, groups):
        for axis in range(2):
            plane_arrived(distance, axis)
    heads_arrived(0)

    def layer(piece, carry):
        squares, products = carry
        cols = pl.ds(pl.multiple_of(piece * tile, tile), tile)
        result = readout_out[:, cols] + jnp.dot(
            joined[:, far], w_ref[far, cols], preferred_element_type=jnp.float32
        )
        readout_out[:, cols] = result
        squares = squares + jnp.sum(result * result, axis=1, keepdims=True)
        products = products + jnp.sum(
            result * probe_own[:, cols].astype(jnp.float32), axis=1, keepdims=True
        )
        return squares, products

    squares, products = lax.fori_loop(0, model // tile, layer, (zero, zero))
    scale = lax.rsqrt(squares / model + EPSILON)
    bend = scale**3 * (products / model)

    def finish(piece, _):
        cols = pl.ds(pl.multiple_of(piece * tile, tile), tile)
        readout = scale * probe_own[:, cols].astype(jnp.float32) - readout_out[:, cols] * bend
        readout_out[:, cols] = readout
        half[:, cols] = readout.astype(jnp.bfloat16)
        return 0

    lax.fori_loop(0, model // tile, finish, 0)
    copies = []
    for order in range(groups):
        other = far_first(groups, group, order)
        result = dot32(
            half[...], w_ref[pl.ds(pl.multiple_of(other * wide, wide), wide), :], NT
        ).astype(jnp.bfloat16)
        for index in range(ctx_count):
            sending[order, index] = result[:, index * HEAD_DIM : (index + 1) * HEAD_DIM]
        for step in range(ctx_count):
            peer = lax.rem(ctx + step, ctx_count)
            if order == groups - 1 and step == 0:
                continue
            copy = remote(
                sending.at[order, peer], grad_v.at[group, ctx], back_send.at[order, step],
                back_recv.at[ctx, group], peer, other * 2 + core,
            )
            copy.start()
            copies.append(copy)
    grad_v[group, ctx] = sending[groups - 1, ctx]

    def clear(index, _):
        pair_acc[index] = jnp.zeros(pair_acc.shape[1:], jnp.float32)
        query_acc[index] = jnp.zeros(query_acc.shape[1:], jnp.float32)
        return 0

    lax.fori_loop(0, groups, clear, 0)

    def sent(piece, _):
        for slot in range(slots):
            dest = core * slots + slot

            @pl.when(dest != ctx)
            def _():
                for kind in range(2):
                    for copy in away(slot, kind, piece, dest):
                        copy.wait_send()

            @pl.when(dest == ctx)
            def _():
                for copy in beside(slot, piece):
                    copy.wait_send()

        return 0

    lax.fori_loop(0, groups, sent, 0)

    own_lines(lambda copy: copy.wait_send())
    shard_copy().wait_send()
    for distance in range(1, groups):
        weights_sent(distance)

    def parts_sent(tile, _):
        for order in range(groups):
            other = far_first(groups, group, order)
            if order == groups - 1:

                @pl.when(tile != ctx)
                def _():
                    out_copy(tile, order, other).wait_send()

            else:
                out_copy(tile, order, other).wait_send()
        return 0

    lax.fori_loop(0, ctx_count, parts_sent, 0)
    for other, peer in sources:
        remote(
            sending.at[0, 0], grad_v.at[other, peer], back_send.at[0, 0],
            back_recv.at[peer, other], peer, other * 2 + core,
        ).wait_recv()
    for copy in copies:
        copy.wait_send()
    pair_copy.wait()

    halves = 2
    span = ctx_count * own // halves
    dests = [far_first(groups, group, order) for order in range(groups)]

    def dest_of(order):
        result = dests[0]
        for index in range(1, groups):
            result = jnp.where(order == index, dests[index], result)
        return result

    score_scale = HEAD_DIM ** (-0.5)
    def half_of(ref, index, half):
        count = ctx_count // halves
        return ref[index, half * count : (half + 1) * count].reshape(span, HEAD_DIM)

    def find_deltas(index, _):
        for half in range(halves):
            product = half_of(grad_v, index, half).astype(jnp.float32) * half_of(
                part_out, index, half
            ).astype(jnp.float32)
            deltas[index, :, half * span : (half + 1) * span] = jnp.sum(
                product.T, axis=0, keepdims=True
            )
        return 0

    lax.fori_loop(0, groups, find_deltas, 0)
    spot_lane = lax.broadcasted_iota(jnp.int32, (1, span), 1)

    def pair(query_at, key_at):
        for half in range(halves):
            blocks = (half + 1) * ctx_count // halves
            count = blocks * 2 * own
            lanes = slice(half * span, (half + 1) * span)
            key_block = kv_out[0, key_at, :blocks].reshape(count, HEAD_DIM)
            value_block = kv_out[1, key_at, :blocks].reshape(count, HEAD_DIM)
            query_block = half_of(query_out, query_at, half)
            grad_block = half_of(grad_v, query_at, half)
            spot = (half * (ctx_count // halves) + spot_lane // own) * rows + spot_lane % own
            pos = spot + (query_at * 2 + core) * own
            pos_f = pos.astype(jnp.float32)
            start = jnp.where(
                pos_f >= second_bound,
                second_bound,
                jnp.where(pos_f >= first_bound, first_bound, 0.0),
            ).astype(jnp.int32)
            line = lax.broadcasted_iota(jnp.int32, (count, span), 0)
            key_pos = (line // (2 * own)) * rows + line % (2 * own)
            offset = key_at * 2 * own
            allowed = (key_pos >= start - offset) & (key_pos <= pos - offset)
            scores = dot32(key_block, query_block, NT)
            probabilities = jnp.where(
                allowed, jnp.exp2(scores * factor - log_v[query_at, :, lanes]), 0.0
            )
            dprobs = dot32(value_block, grad_block, NT)
            dscores = (probabilities * (dprobs - deltas[query_at, :, lanes])).astype(jnp.bfloat16)
            pair_acc[key_at, :count, HEAD_DIM:] += jnp.dot(
                probabilities.astype(jnp.bfloat16), grad_block, preferred_element_type=jnp.float32
            )
            pair_acc[key_at, :count, :HEAD_DIM] += jnp.dot(
                dscores, query_block, preferred_element_type=jnp.float32
            )
            query_acc[query_at, :, lanes] += dot32(key_block, dscores, TN)

    def core_copy(order):
        return remote(
            pair_buf.at[order], beside_in.at[order], b_send.at[order], b_recv.at[order], ctx, partner
        )

    def pair_rows(dest, source, kind):
        first = pl.multiple_of((source * 2 + kind) * own, own)
        keys = pair_acc[dest, pl.ds(first, own), :HEAD_DIM] * score_scale
        values = pair_acc[dest, pl.ds(first, own), HEAD_DIM:]
        return keys, values

    def settle(order):
        dest = dest_of(order)
        for source in range(ctx_count):
            keys, values = pair_rows(dest, source, 1 - core)
            pair_buf[order, source, :, :HEAD_DIM] = keys.astype(jnp.bfloat16)
            pair_buf[order, source, :, HEAD_DIM:] = values.astype(jnp.bfloat16)
        for half in range(halves):
            query_fin[order, half * span : (half + 1) * span, :] = (
                query_acc[dest, :, half * span : (half + 1) * span].T * score_scale
            ).astype(jnp.bfloat16)
        core_copy(order).start()

    def stripe(source):
        slot = lax.rem(source, slots)
        return pl.ds(pl.multiple_of(slot * HEAD_DIM, HEAD_DIM), HEAD_DIM)

    def exchange(order, step):
        peer = lax.rem(ctx + step, ctx_count)
        return remote(
            away_buf.at[order, step],
            terms_in.at[dest_of(order), ctx // slots, :, :, stripe(ctx)],
            a_send.at[order, step], a_recv.at[dest_of(order), ctx], peer, me,
        )

    def arrived(dest, step):
        source = lax.rem(ctx + step, ctx_count)
        remote(
            away_buf.at[0, 0], terms_in.at[dest, source // slots, :, :, stripe(source)],
            a_send.at[0, 0], a_recv.at[dest, source], source, me,
        ).wait_recv()

    def spread(order):
        dest = dest_of(order)
        core_copy(order).wait_recv()
        for step in range(1, ctx_count + 1):
            peer = lax.rem(ctx + step, ctx_count)
            keys, values = pair_rows(dest, peer, core)
            keys = (keys + beside_in[order, peer, :, :HEAD_DIM].astype(jnp.float32)).astype(
                jnp.bfloat16
            )
            values = (values + beside_in[order, peer, :, HEAD_DIM:].astype(jnp.float32)).astype(
                jnp.bfloat16
            )
            queries = query_fin[order, pl.ds(pl.multiple_of(peer * own, own), own), :]
            if step < ctx_count:
                away_buf[order, step, 0] = queries
                away_buf[order, step, 1] = keys
                away_buf[order, step, 2] = values
                exchange(order, step).start()
            else:
                at = stripe(ctx)
                terms_in[dest, ctx // slots, 0, :, at] = queries
                terms_in[dest, ctx // slots, 1, :, at] = keys
                terms_in[dest, ctx // slots, 2, :, at] = values

    pieces = partial.shape[2]
    strip = model // pieces

    def chain(order, piece):
        dest = dest_of(order)
        up = dest > group
        line = jnp.where(up, 0, 1)
        peer = jnp.where(up, group + 1, group - 1)
        return remote(
            passing.at[order, piece], partial.at[line, dest, piece], z_send.at[order, piece],
            z_recv.at[line, dest, piece], ctx, peer * 2 + core,
        )

    def came(line, dest, piece):
        remote(
            passing.at[0, piece], partial.at[line, dest, piece], z_send.at[0, piece],
            z_recv.at[line, dest, piece], ctx, partner,
        ).wait_recv()

    def term(dest, piece):
        cols = pl.ds(pl.multiple_of(piece * strip, strip), strip)
        result = None
        for half in range(2):
            for kind in range(3):
                part = dot32(terms_in[dest, half, kind], w_both[half, kind, cols, :], NT)
                result = part if result is None else result + part
        return result

    inner = (group > 0) & (group < groups - 1)

    def pass_on(order, _):
        dest = dest_of(order)
        for step in range(1, ctx_count):
            arrived(dest, step)
        line = jnp.where(dest > group, 0, 1)

        def one_piece(piece, _):
            sum_v[...] = term(dest, piece)

            @pl.when(inner)
            def _():
                came(line, dest, piece)
                sum_v[...] += partial[line, dest, piece].astype(jnp.float32)

            passing[order, piece] = sum_v[...].astype(jnp.bfloat16)
            chain(order, piece).start()
            return 0

        lax.fori_loop(0, pieces, one_piece, 0)
        return 0

    ends, number = [], 0
    for order in range(groups):
        number += 2 * (groups - order) - 1
        ends.append(number - 1)
    spreads = {order: end + 1 for order, end in enumerate(ends) if end + 1 < number}

    def one_pair(index, _):
        stage = 0
        for end in ends[:-1]:
            stage = stage + jnp.where(index > end, 1, 0)
        first = 0
        for order in range(1, groups):
            first = jnp.where(stage == order, ends[order - 1] + 1, first)
        inside = index - first
        other = stage + (inside + 1) // 2
        odd = lax.rem(inside, 2)
        pair(
            dest_of(jnp.where(odd == 1, stage, other)), dest_of(jnp.where(odd == 1, other, stage))
        )
        for order, end in enumerate(ends[:-1]):

            @pl.when(index == end)
            def _():
                settle(order)

        for order, at in spreads.items():

            @pl.when(index == at)
            def _():
                spread(order)

        return 0

    first = min(ends[min(1, groups - 1)] + 2, number)
    lax.fori_loop(0, first, one_pair, 0)
    early = 1 if first < number else 0
    if early:

        @pl.when(jnp.logical_not(inner))
        def _():
            pass_on(0, 0)

        lax.fori_loop(first, number, one_pair, 0)
    settle(groups - 1)
    for order in range(groups):
        if order not in spreads:
            spread(order)
    lax.fori_loop(jnp.where(inner, 0, early), groups - 1, pass_on, 0)
    for step in range(1, ctx_count):
        arrived(group, step)

    state = state_own[...].astype(jnp.float32)
    inverse = row_scale(state)

    def last_piece(piece, slope):
        cols = pl.ds(pl.multiple_of(piece * strip, strip), strip)
        sum_v[...] = term(group, piece)

        @pl.when(group > 0)
        def _():
            came(0, group, piece)
            sum_v[...] += partial[0, group, piece].astype(jnp.float32)

        @pl.when(group < groups - 1)
        def _():
            came(1, group, piece)
            sum_v[...] += partial[1, group, piece].astype(jnp.float32)

        gained = sum_v[...] * gain_ref[cols].astype(jnp.float32).reshape(1, strip)
        new_out[:, cols] = gained
        return slope + jnp.sum(
            gained * state_own[:, cols].astype(jnp.float32), axis=1, keepdims=True
        )

    slope = lax.fori_loop(0, pieces, last_piece, jnp.zeros((own, 1), jnp.float32))
    bend = inverse**3 * (slope / model)

    def update(piece, _):
        cols = pl.ds(pl.multiple_of(piece * strip, strip), strip)
        here = state_own[:, cols].astype(jnp.float32)
        gradient = readout_out[:, cols] + inverse * new_out[:, cols] - here * bend
        new_out[:, cols] = (
            here - STEP_SIZE * gradient + NOISE_SCALE * noise_own[:, cols].astype(jnp.float32)
        )
        return 0

    lax.fori_loop(0, pieces, update, 0)

    def all_sent(order, _):
        core_copy(order).wait_send()
        for step in range(1, ctx_count):
            exchange(order, step).wait_send()

        @pl.when(order < groups - 1)
        def _():
            for piece in range(pieces):
                chain(order, piece).wait_send()

        return 0

    lax.fori_loop(0, groups, all_sent, 0)


def heads_body(state, norm_gain, w_qkv, w_out, probe, noise, segment_ids):
    ctx_count, head_count = lax.axis_size("ctx"), lax.axis_size("head")
    rows, model = state.shape
    width = w_qkv.shape[2]
    own, groups, slots = rows // head_count, head_count // 2, width // HEAD_DIM
    seg = segment_ids.reshape(-1, 128)
    half, full, dma = jnp.bfloat16, jnp.float32, pltpu.SemaphoreType.DMA
    pieces, lanes = 4, ctx_count * own
    tile, vmem = model // pieces, pltpu.VMEM
    heads = (groups, ctx_count, own, HEAD_DIM)
    return pl.pallas_call(
        functools.partial(step_kernel, ctx_count, head_count),
        out_shape=jax.ShapeDtypeStruct((own, model), full),
        in_specs=[ANY, ANY, VMEM, VMEM, ANY, ANY, ANY],
        out_specs=VMEM,
        scratch_shapes=[
            vmem((rows, model), half),
            vmem((slots, groups, 2, own, HEAD_DIM), half),
            vmem((slots, 2, groups, 2 * own, HEAD_DIM), half),
            vmem((model, model), half),
            vmem((own, model), half),
            vmem((own, model), half),
            vmem(heads, half),
            vmem((own, model), half),
            vmem((own, model), half),
            vmem((own, model), half),
            vmem(heads, half),
            vmem((2, groups, ctx_count, 2 * own, HEAD_DIM), half),
            vmem(heads, half),
            vmem((own, model), full),
            vmem((ctx_count,) + seg.shape, seg.dtype),
            vmem((groups, 1, lanes), full),
            vmem(heads, half),
            vmem((2,) + w_qkv.shape, half),
            vmem((groups, 2 * lanes, 2 * HEAD_DIM), full),
            vmem((groups, HEAD_DIM, lanes), full),
            vmem((groups, 1, lanes), full),
            vmem((groups, lanes, HEAD_DIM), half),
            vmem((groups, ctx_count, own, 2 * HEAD_DIM), half),
            vmem((groups, ctx_count, own, 2 * HEAD_DIM), half),
            vmem((groups, ctx_count, 3, own, HEAD_DIM), half),
            vmem((groups, 2, 3, own, width), half),
            vmem((2, groups, pieces, own, tile), half),
            vmem((groups, pieces, own, tile), half),
            vmem((own, tile), full),
            dma((groups,)),
            dma((3,)),
            dma((slots, 2, groups)),
            dma((ctx_count, groups)),
            dma((slots, 2, groups)),
            dma((2, ctx_count, groups)),
            dma((ctx_count, groups)),
            dma((ctx_count,)),
            dma((ctx_count,)),
            dma((2, 2, groups)),
            dma((2, groups)),
            dma((2, groups)),
            dma((2, groups)),
            dma((4, groups)),
            dma((4, groups)),
            dma,
            dma,
            dma,
            dma((ctx_count, groups)),
            dma((groups, ctx_count)),
            dma((groups, ctx_count)),
            dma((ctx_count, groups)),
            dma((3,)),
            dma,
            dma,
            dma((groups,)),
            dma((groups,)),
            dma((groups, ctx_count)),
            dma((groups, ctx_count)),
            dma((groups, pieces)),
            dma((2, groups, pieces)),
        ],
        compiler_params=pltpu.CompilerParams(
            collective_id=0, has_side_effects=True, vmem_limit_bytes=63 * 2**20
        ),
    )(state, w_qkv, norm_gain, seg, w_out, probe, noise)


def solution(mesh):
    placed = (
        P("ctx", None),
        P(),
        P(None, None, "head"),
        P("head", None),
        P("ctx", None),
        P(("ctx", "head"), None),
        P("ctx"),
    )

    def step(*args):
        heads = args[2].shape[2] // HEAD_DIM
        return (heads_body if lax.axis_size("ctx") == 2 * heads == 4 else body)(*args)

    return jax.shard_map(
        step, mesh=mesh, in_specs=placed, out_specs=P(("ctx", "head"), None), check_vma=False
    )
```

```python
import functools

import jax
import jax.numpy as jnp
from jax import lax
from jax.experimental import pallas as pl
from jax.experimental.pallas import tpu as pltpu
from jax.sharding import PartitionSpec as P

HEAD_DIM = 128
EPSILON = 1e-05
STEP_SIZE = 0.25
NOISE_SCALE = (2.0 * STEP_SIZE) ** 0.5
NEGATIVE = -1e30
LOG2E = 1.4426950408889634
MESH = pl.DeviceIdType.MESH
VMEM = pl.BlockSpec(memory_space=pltpu.VMEM)
ANY = pl.BlockSpec(memory_space=pl.ANY)
NT = (((1,), (1,)), ((), ()))
TN = (((0,), (0,)), ((), ()))
FORWARD_BLOCKS = (512, 512)
BACKWARD_BLOCKS = (512, 512)


def row_scale(matrix):
    return lax.rsqrt(jnp.mean(matrix * matrix, axis=-1, keepdims=True) + EPSILON)


def dot32(left, right, dims):
    return lax.dot_general(left, right, dims, preferred_element_type=jnp.float32)


def greet(axis, number, me):
    barrier = pltpu.get_barrier_semaphore()
    for step in range(1, number):
        pl.semaphore_signal(
            barrier, inc=1, device_id={axis: lax.rem(me + step, number)}, device_id_type=MESH
        )
    pl.semaphore_wait(barrier, number - 1)


def gather_kernel(
    number, key_ref, value_ref, seg_ref, normed_ref, w_ref, keys, values, segs, query_out, send_sem,
    recv_sem, own_sem,
):
    me = lax.axis_index("ctx")
    rows = key_ref.shape[0]
    greet("ctx", number, me)

    def place(index):
        return pl.ds(pl.multiple_of(index * rows, rows), rows)

    def send(slot, source, target, peer):
        copy = pltpu.make_async_remote_copy(
            src_ref=source,
            dst_ref=target,
            send_sem=send_sem.at[slot],
            recv_sem=recv_sem.at[slot],
            device_id={"ctx": peer},
            device_id_type=MESH,
        )
        copy.start()
        return copy

    mine = place(me)
    copies = []
    for step in range(1, number):
        copies.append(send(step, seg_ref, segs.at[me], lax.rem(me + step, number)))
    relay = number == 4
    if relay:
        low, high = lax.rem(me, 2), me // 2
        across, along = high * 2 + 1 - low, (1 - high) * 2 + low
        key_first = send(number, key_ref, keys.at[mine], across)
        value_first = send(number + 1, value_ref, values.at[mine], along)
        copies.append(send(number + 2, value_ref, values.at[mine], across))
        copies.append(send(number + 3, key_ref, keys.at[mine], along))
    else:
        for step in range(1, number):
            peer = lax.rem(me + step, number)
            copies.append(send(number + 2 * step, key_ref, keys.at[mine], peer))
            copies.append(send(number + 2 * step + 1, value_ref, values.at[mine], peer))
    pairs = ((key_ref, keys.at[mine]), (value_ref, values.at[mine]), (seg_ref, segs.at[me]))
    for index, (source, target) in enumerate(pairs):
        copy = pltpu.make_async_copy(source, target, own_sem.at[index])
        copy.start()
        copies.append(copy)
    tile = min(256, rows)

    def project(piece, _):
        at = pl.ds(pl.multiple_of(piece * tile, tile), tile)
        query_out[at, :] = jnp.dot(
            normed_ref[at, :], w_ref[...], preferred_element_type=jnp.float32
        ).astype(jnp.bfloat16)
        return 0

    lax.fori_loop(0, rows // tile, project, 0)
    if relay:
        key_first.wait()
        copies.append(send(number + 4, keys.at[place(across)], keys.at[place(across)], along))
        value_first.wait()
        copies.append(send(number + 5, values.at[place(along)], values.at[place(along)], across))
    for copy in copies:
        copy.wait()


def gather_keys(number, key_rows, value_rows, segment_ids, normed, w_query):
    rows, width = key_rows.shape
    seg = segment_ids.reshape(-1, 128)
    full = jax.ShapeDtypeStruct((number * rows, width), key_rows.dtype)
    keys, values, segs, queries = pl.pallas_call(
        functools.partial(gather_kernel, number),
        out_shape=(
            full,
            full,
            jax.ShapeDtypeStruct((number,) + seg.shape, seg.dtype),
            jax.ShapeDtypeStruct((rows, width), key_rows.dtype),
        ),
        in_specs=[VMEM] * 5,
        out_specs=(ANY, ANY, ANY, VMEM),
        scratch_shapes=[
            pltpu.SemaphoreType.DMA((3 * number + 6,)),
            pltpu.SemaphoreType.DMA((3 * number + 6,)),
            pltpu.SemaphoreType.DMA((3,)),
        ],
        compiler_params=pltpu.CompilerParams(collective_id=0, has_side_effects=True),
    )(key_rows, value_rows, seg, normed, w_query)
    return keys, values, segs.reshape(-1), queries


def block_ranges(table, index):
    return [table[index, column] for column in range(4)]


def forward_kernel(
    heads, bq, bk, table, query_ref, key_ref, value_ref, start_ref, pos_ref, out_ref, log_ref
):
    factor = HEAD_DIM ** (-0.5) * LOG2E
    blocks = query_ref.shape[0] // bq

    def one_block(index, _):
        low, inner_low, inner_high, high = block_ranges(table, index)
        rows = pl.ds(pl.multiple_of(index * bq, bq), bq)
        start, pos = start_ref[index], pos_ref[index]

        def step(masked, piece, carry):
            keys_at = pl.ds(pl.multiple_of(piece * bk, bk), bk)
            if masked:
                key_pos = piece * bk + lax.broadcasted_iota(jnp.int32, (bk, bq), 0)
                allowed = (key_pos >= start) & (key_pos <= pos)
            result = []
            for head in range(heads):
                top, total, acc = carry[head]
                cols = pl.ds(head * HEAD_DIM, HEAD_DIM)
                scores = dot32(key_ref[keys_at, cols], query_ref[rows, cols], NT)
                if masked:
                    scores = jnp.where(allowed, scores, NEGATIVE)
                new_top = jnp.maximum(top, jnp.max(scores, axis=0, keepdims=True) * factor)
                weights = jnp.exp2(scores * factor - new_top)
                scale = jnp.exp2(top - new_top)
                total = total * scale + jnp.sum(weights, axis=0, keepdims=True)
                acc = acc * scale + dot32(
                    value_ref[keys_at, cols], weights.astype(jnp.bfloat16), TN
                )
                result.append((new_top, total, acc))
            return tuple(result)

        carry = tuple(
            (
                jnp.full((1, bq), NEGATIVE, jnp.float32),
                jnp.zeros((1, bq), jnp.float32),
                jnp.zeros((HEAD_DIM, bq), jnp.float32),
            )
            for _ in range(heads)
        )
        carry = lax.fori_loop(low, inner_low, functools.partial(step, True), carry)
        carry = lax.fori_loop(inner_low, inner_high, functools.partial(step, False), carry)
        carry = lax.fori_loop(inner_high, high, functools.partial(step, True), carry)
        for head in range(heads):
            top, total, acc = carry[head]
            out_ref[rows, pl.ds(head * HEAD_DIM, HEAD_DIM)] = (acc / total).T.astype(jnp.bfloat16)
            log_ref[index, pl.ds(head, 1), :] = top + jnp.log2(total)
        return 0

    lax.fori_loop(0, blocks, one_block, 0)


def backward_kernel(
    heads, bq, bk, table, query_ref, key_ref, value_ref, grad_ref, out_ref, log_ref, start_ref,
    pos_ref, query_out, pair_out, pair_acc,
):
    score_scale = HEAD_DIM ** (-0.5)
    factor = score_scale * LOG2E
    blocks = query_ref.shape[0] // bq
    width = heads * HEAD_DIM
    pair_rows = pair_acc.shape[0]

    def clear(piece, _):
        at = pl.ds(pl.multiple_of(piece * bk, bk), bk)
        pair_acc[at, :] = jnp.zeros((bk, 2 * width), jnp.float32)
        return 0

    lax.fori_loop(0, pair_rows // bk, clear, 0)

    def one_block(index, _):
        low, inner_low, inner_high, high = block_ranges(table, index)
        rows = pl.ds(pl.multiple_of(index * bq, bq), bq)
        start, pos = start_ref[index], pos_ref[index]
        deltas, logs = [], []
        for head in range(heads):
            cols = pl.ds(head * HEAD_DIM, HEAD_DIM)
            product = grad_ref[rows, cols].astype(jnp.float32) * out_ref[rows, cols].astype(
                jnp.float32
            )
            deltas.append(jnp.sum(product.T, axis=0, keepdims=True))
            logs.append(log_ref[index, pl.ds(head, 1), :])

        def step(masked, piece, carry):
            keys_at = pl.ds(pl.multiple_of(piece * bk, bk), bk)
            if masked:
                key_pos = piece * bk + lax.broadcasted_iota(jnp.int32, (bk, bq), 0)
                allowed = (key_pos >= start) & (key_pos <= pos)
            result = []
            for head in range(heads):
                cols = pl.ds(head * HEAD_DIM, HEAD_DIM)
                value_cols = pl.ds(width + head * HEAD_DIM, HEAD_DIM)
                key_block, query_block = key_ref[keys_at, cols], query_ref[rows, cols]
                grad_block = grad_ref[rows, cols]
                scores = dot32(key_block, query_block, NT)
                probabilities = jnp.exp2(scores * factor - logs[head])
                if masked:
                    probabilities = jnp.where(allowed, probabilities, 0.0)
                dprobs = dot32(value_ref[keys_at, cols], grad_block, NT)
                dscores = (probabilities * (dprobs - deltas[head])).astype(jnp.bfloat16)
                pair_acc[keys_at, value_cols] += jnp.dot(
                    probabilities.astype(jnp.bfloat16),
                    grad_block,
                    preferred_element_type=jnp.float32,
                )
                pair_acc[keys_at, cols] += jnp.dot(
                    dscores, query_block, preferred_element_type=jnp.float32
                )
                result.append(carry[head] + dot32(key_block, dscores, TN))
            return tuple(result)

        carry = tuple(jnp.zeros((HEAD_DIM, bq), jnp.float32) for _ in range(heads))
        carry = lax.fori_loop(low, inner_low, functools.partial(step, True), carry)
        carry = lax.fori_loop(inner_low, inner_high, functools.partial(step, False), carry)
        carry = lax.fori_loop(inner_high, high, functools.partial(step, True), carry)
        for head in range(heads):
            query_out[rows, pl.ds(head * HEAD_DIM, HEAD_DIM)] = (
                carry[head].T * score_scale
            ).astype(jnp.bfloat16)
        return 0

    lax.fori_loop(0, blocks, one_block, 0)

    def flush(piece, _):
        at = pl.ds(pl.multiple_of(piece * bk, bk), bk)
        pair_out[at, :width] = (pair_acc[at, :width] * score_scale).astype(jnp.bfloat16)
        pair_out[at, width:] = pair_acc[at, width:].astype(jnp.bfloat16)
        return 0

    lax.fori_loop(0, pair_rows // bk, flush, 0)


def make_table(start, pos, bq, bk):
    starts, places = start.reshape(-1, bq), pos.reshape(-1, bq)
    low = starts[:, 0] // bk
    inner_low = (starts[:, -1] + bk - 1) // bk
    inner_high = jnp.maximum(inner_low, (places[:, 0] + 1) // bk)
    high = places[:, -1] // bk + 1
    return jnp.stack([low, inner_low, inner_high, high], axis=1).astype(jnp.int32)


def middle_kernel(
    number, part_ref, w_any, state_ref, probe_ref, grad_out, readout_out, w_ref, joined, half,
    sending, landing, send_sem, recv_sem, back_send, back_recv, w_sem,
):
    me = lax.axis_index("head")
    width = part_ref.shape[1]
    own = state_ref.shape[0]
    model = state_ref.shape[1]
    w_copy = pltpu.make_async_copy(w_any, w_ref, w_sem)
    w_copy.start()
    greet("head", number, me)
    my_cols = pl.ds(pl.multiple_of(me * width, width), width)
    my_rows = pl.ds(pl.multiple_of(me * own, own), own)
    copies = []
    for step in range(1, number):
        peer = lax.rem(me + step, number)
        copy = pltpu.make_async_remote_copy(
            src_ref=part_ref.at[pl.ds(pl.multiple_of(peer * own, own), own)],
            dst_ref=joined.at[:, my_cols],
            send_sem=send_sem.at[step],
            recv_sem=recv_sem.at[step],
            device_id={"head": peer},
            device_id_type=MESH,
        )
        copy.start()
        copies.append(copy)
    joined[:, my_cols] = part_ref[my_rows, :]
    w_copy.wait()
    for copy in copies:
        copy.wait()

    tile = min(256, model)

    def project(piece, carry):
        squares, products = carry
        cols = pl.ds(pl.multiple_of(piece * tile, tile), tile)
        layer = state_ref[:, cols].astype(jnp.float32) + jnp.dot(
            joined[...], w_ref[:, cols], preferred_element_type=jnp.float32
        )
        readout_out[:, cols] = layer
        squares = squares + jnp.sum(layer * layer, axis=1, keepdims=True)
        products = products + jnp.sum(
            layer * probe_ref[:, cols].astype(jnp.float32), axis=1, keepdims=True
        )
        return squares, products

    zero = jnp.zeros((own, 1), jnp.float32)
    squares, products = lax.fori_loop(0, model // tile, project, (zero, zero))
    scale = lax.rsqrt(squares / model + EPSILON)
    bend = scale**3 * (products / model)

    def finish(piece, _):
        cols = pl.ds(pl.multiple_of(piece * tile, tile), tile)
        readout = scale * probe_ref[:, cols].astype(jnp.float32) - readout_out[:, cols] * bend
        readout_out[:, cols] = readout
        half[:, cols] = readout.astype(jnp.bfloat16)
        return 0

    lax.fori_loop(0, model // tile, finish, 0)
    copies = []
    for step in range(1, number):
        peer = lax.rem(me + step, number)
        sending[step] = dot32(
            half[...], w_ref[pl.ds(pl.multiple_of(peer * width, width), width), :], NT
        ).astype(jnp.bfloat16)
        copy = pltpu.make_async_remote_copy(
            src_ref=sending.at[step],
            dst_ref=landing.at[my_rows],
            send_sem=back_send.at[step],
            recv_sem=back_recv.at[step],
            device_id={"head": peer},
            device_id_type=MESH,
        )
        copy.start()
        copies.append(copy)
    landing[my_rows, :] = dot32(half[...], w_ref[my_cols, :], NT).astype(jnp.bfloat16)
    for copy in copies:
        copy.wait()
    grad_out[...] = landing[...]


def middle(number, part, w_full, state_own, probe_own):
    rows, width = part.shape
    own, model = state_own.shape
    return pl.pallas_call(
        functools.partial(middle_kernel, number),
        out_shape=(
            jax.ShapeDtypeStruct((rows, width), jnp.bfloat16),
            jax.ShapeDtypeStruct((own, model), jnp.float32),
        ),
        in_specs=[VMEM, ANY, VMEM, VMEM],
        out_specs=(VMEM, VMEM),
        scratch_shapes=[
            pltpu.VMEM(w_full.shape, jnp.bfloat16),
            pltpu.VMEM((own, number * width), jnp.bfloat16),
            pltpu.VMEM((own, model), jnp.bfloat16),
            pltpu.VMEM((number, own, width), jnp.bfloat16),
            pltpu.VMEM((rows, width), jnp.bfloat16),
            pltpu.SemaphoreType.DMA((number,)),
            pltpu.SemaphoreType.DMA((number,)),
            pltpu.SemaphoreType.DMA((number,)),
            pltpu.SemaphoreType.DMA((number,)),
            pltpu.SemaphoreType.DMA,
        ],
        compiler_params=pltpu.CompilerParams(
            collective_id=1, has_side_effects=True, vmem_limit_bytes=60 * 2**20
        ),
    )(part, w_full, state_own, probe_own)


def tail_kernel(
    ctx_count, number, pair_any, query_ref, w_ref, sum_out, own_pair, arriving, gathered, terms,
    from_partner, reduced, landing, ctx_send, ctx_recv, p_send, p_recv, z_send, z_recv, own_sem,
):
    ctx, me = lax.axis_index("ctx"), lax.axis_index("head")
    groups = number // 2
    group, core = me // 2, lax.rem(me, 2)
    partner = group * 2 + 1 - core
    rows, width = query_ref.shape
    own, model = sum_out.shape
    chunk = 2 * own
    own_copy = pltpu.make_async_copy(
        pair_any.at[pl.ds(pl.multiple_of(ctx * rows, rows), rows)], own_pair, own_sem
    )
    own_copy.start()
    barrier = pltpu.get_barrier_semaphore()
    peers = [{"ctx": lax.rem(ctx + step, ctx_count)} for step in range(1, ctx_count)]
    peers.append({"head": partner})
    for step in range(1, groups):
        peers.append({"head": lax.rem(group + step, groups) * 2 + core})
    for peer in peers:
        pl.semaphore_signal(barrier, inc=1, device_id=peer, device_id_type=MESH)
    pl.semaphore_wait(barrier, len(peers))

    def chunk_start(order):
        dest = lax.rem(group + order + 1, groups)
        return dest, pl.multiple_of(dest * chunk, chunk)

    def ctx_copy(order, step):
        target = lax.rem(ctx - step + ctx_count, ctx_count)
        _, first = chunk_start(order)
        return pltpu.make_async_remote_copy(
            src_ref=pair_any.at[pl.ds(pl.multiple_of(target * rows + first, chunk), chunk)],
            dst_ref=arriving.at[order, step - 1],
            send_sem=ctx_send.at[order, step],
            recv_sem=ctx_recv.at[order, step],
            device_id={"ctx": target},
            device_id_type=MESH,
        )

    for order in range(groups):
        for step in range(1, ctx_count):

            @pl.when(step <= ctx)
            def _():
                ctx_copy(order, step).start()

    own_copy.wait()
    tile = min(512, model)
    mine = pl.ds(pl.multiple_of(core * own, own), own)
    theirs = pl.ds(pl.multiple_of((1 - core) * own, own), own)
    waiting = []
    for order in range(groups):
        dest, first = chunk_start(order)
        at = pl.ds(first, chunk)
        gathered[...] = own_pair[at, :].astype(jnp.float32)
        for step in range(1, ctx_count):

            @pl.when(ctx + step < ctx_count)
            def _():
                ctx_copy(order, step).wait_recv()
                gathered[...] += arriving[order, step - 1].astype(jnp.float32)

        def multiply(piece, _):
            cols = pl.ds(pl.multiple_of(piece * tile, tile), tile)
            term = dot32(query_ref[at, :], w_ref[0, cols, :], NT)
            term += dot32(gathered[:, :width].astype(jnp.bfloat16), w_ref[1, cols, :], NT)
            term += dot32(gathered[:, width:].astype(jnp.bfloat16), w_ref[2, cols, :], NT)
            terms[order, :, cols] = term.astype(jnp.bfloat16)
            return 0

        lax.fori_loop(0, model // tile, multiply, 0)
        copy = pltpu.make_async_remote_copy(
            src_ref=terms.at[order, theirs],
            dst_ref=from_partner.at[order],
            send_sem=p_send.at[order],
            recv_sem=p_recv.at[order],
            device_id={"head": partner},
            device_id_type=MESH,
        )
        copy.start()
        copy.wait()
        both = terms[order, mine, :].astype(jnp.float32) + from_partner[order].astype(jnp.float32)
        if order < groups - 1:
            reduced[order] = both.astype(jnp.bfloat16)
            copy = pltpu.make_async_remote_copy(
                src_ref=reduced.at[order],
                dst_ref=landing.at[order],
                send_sem=z_send.at[order],
                recv_sem=z_recv.at[order],
                device_id={"head": dest * 2 + core},
                device_id_type=MESH,
            )
            copy.start()
            waiting.append(copy)
        else:
            sum_out[...] = both
    for order, copy in enumerate(waiting):
        copy.wait()
        sum_out[...] += landing[order].astype(jnp.float32)
    for order in range(groups):
        for step in range(1, ctx_count):

            @pl.when(step <= ctx)
            def _():
                ctx_copy(order, step).wait_send()


def tail(ctx_count, number, pair, query_grad, w_qkv):
    rows, width = query_grad.shape
    model = w_qkv.shape[1]
    own, groups = rows // number, number // 2
    half, full = jnp.bfloat16, jnp.float32
    dma = pltpu.SemaphoreType.DMA
    return pl.pallas_call(
        functools.partial(tail_kernel, ctx_count, number),
        out_shape=jax.ShapeDtypeStruct((own, model), full),
        in_specs=[ANY, VMEM, VMEM],
        out_specs=VMEM,
        scratch_shapes=[
            pltpu.VMEM((rows, 2 * width), half),
            pltpu.VMEM((groups, ctx_count - 1, 2 * own, 2 * width), half),
            pltpu.VMEM((2 * own, 2 * width), full),
            pltpu.VMEM((groups, 2 * own, model), half),
            pltpu.VMEM((groups, own, model), half),
            pltpu.VMEM((groups, own, model), half),
            pltpu.VMEM((groups, own, model), half),
            dma((groups, ctx_count)),
            dma((groups, ctx_count)),
            dma((groups,)),
            dma((groups,)),
            dma((groups,)),
            dma((groups,)),
            dma,
        ],
        compiler_params=pltpu.CompilerParams(
            collective_id=2, has_side_effects=True, vmem_limit_bytes=60 * 2**20
        ),
    )(pair, query_grad, w_qkv)


def body(state, norm_gain, w_qkv, w_out, probe, noise, segment_ids):
    local_rows, model_width = state.shape
    width = w_qkv.shape[2]
    local_heads = width // HEAD_DIM
    head_count = lax.axis_size("head")
    ctx_count = lax.axis_size("ctx")
    ctx_index = lax.axis_index("ctx")
    own_rows = local_rows // head_count
    row_start = lax.axis_index("head") * own_rows
    w_full = lax.all_gather(w_out, "head", axis=0, tiled=True)
    state_f = state.astype(jnp.float32)
    gain_full = norm_gain.astype(jnp.float32)
    inverse = row_scale(state_f)
    normed = (state_f * inverse * gain_full).astype(jnp.bfloat16)

    def project(index):
        return jnp.dot(normed, w_qkv[index], preferred_element_type=jnp.float32).astype(
            jnp.bfloat16
        )

    key_rows, value_rows = project(1), project(2)
    keys, values, segs, query_rows = gather_keys(
        ctx_count, key_rows, value_rows, segment_ids, normed, w_qkv[0]
    )
    total_rows = keys.shape[0]
    pos = ctx_index * local_rows + jnp.arange(local_rows, dtype=jnp.int32)
    start = jnp.sum((segs[None, :] < segment_ids[:, None]).astype(jnp.int32), axis=1)
    fq, fk = (min(local_rows, size) for size in FORWARD_BLOCKS)
    gq, gk = (min(local_rows, size) for size in BACKWARD_BLOCKS)
    smem = pl.BlockSpec(memory_space=pltpu.SMEM)
    params = pltpu.CompilerParams(vmem_limit_bytes=60 * 2**20)
    outputs, logs = pl.pallas_call(
        functools.partial(forward_kernel, local_heads, fq, fk),
        out_shape=(
            jax.ShapeDtypeStruct((local_rows, width), jnp.bfloat16),
            jax.ShapeDtypeStruct((local_rows // fq, local_heads, fq), jnp.float32),
        ),
        in_specs=[smem] + [VMEM] * 5,
        out_specs=(VMEM, VMEM),
        compiler_params=params,
        cost_estimate=pl.CostEstimate(
            flops=4 * local_rows * total_rows * width, bytes_accessed=0, transcendentals=0
        ),
    )(
        make_table(start, pos, fq, fk),
        query_rows,
        keys,
        values,
        start.reshape(-1, 1, fq),
        pos.reshape(-1, 1, fq),
    )
    state_half = lax.dynamic_slice_in_dim(state, row_start, own_rows, 0)
    probe_own = lax.dynamic_slice_in_dim(probe, row_start, own_rows, 0)
    state_own = state_half.astype(jnp.float32)
    inverse_own = row_scale(state_own)
    grads_out, readout_own = middle(head_count, outputs, w_full, state_half, probe_own)
    query_grad, pair = pl.pallas_call(
        functools.partial(backward_kernel, local_heads, gq, gk),
        out_shape=(
            jax.ShapeDtypeStruct((local_rows, width), jnp.bfloat16),
            jax.ShapeDtypeStruct((total_rows, 2 * width), jnp.bfloat16),
        ),
        in_specs=[smem] + [VMEM] * 8,
        out_specs=(VMEM, VMEM),
        scratch_shapes=[pltpu.VMEM((total_rows, 2 * width), jnp.float32)],
        compiler_params=params,
        cost_estimate=pl.CostEstimate(
            flops=10 * local_rows * total_rows * width, bytes_accessed=0, transcendentals=0
        ),
    )(
        make_table(start, pos, gq, gk),
        query_rows,
        keys,
        values,
        grads_out,
        outputs,
        logs.reshape(local_rows // fq, local_heads, fq),
        start.reshape(-1, 1, gq),
        pos.reshape(-1, 1, gq),
    )
    normed_grad = tail(ctx_count, head_count, pair, query_grad, w_qkv)
    gain_grad = normed_grad * gain_full
    gradient = (
        readout_own
        + inverse_own * gain_grad
        - state_own * inverse_own**3 * jnp.mean(gain_grad * state_own, axis=-1, keepdims=True)
    )
    return state_own - STEP_SIZE * gradient + jnp.sqrt(2.0 * STEP_SIZE) * noise.astype(jnp.float32)


def remote(source, target, send_sem, recv_sem, ctx, head):
    return pltpu.make_async_remote_copy(
        src_ref=source,
        dst_ref=target,
        send_sem=send_sem,
        recv_sem=recv_sem,
        device_id={"ctx": ctx, "head": head},
        device_id_type=MESH,
    )


def place():
    ctx, me = lax.axis_index("ctx"), lax.axis_index("head")
    return ctx, me, me // 2, lax.rem(me, 2)


def announce(peers):
    barrier = pltpu.get_barrier_semaphore()
    for ctx, head in peers:
        pl.semaphore_signal(
            barrier, inc=1, device_id={"ctx": ctx, "head": head}, device_id_type=MESH
        )


def await_all(peers):
    pl.semaphore_wait(pltpu.get_barrier_semaphore(), len(peers))


def far_first(groups, group, step):
    result = 0
    for index in range(groups):
        order = sorted(range(groups), key=lambda other: (-abs(other - index), -other))
        result = jnp.where(group == index, order[step], result)
    return result


def by_arrival(groups, group, step):
    result = 0
    for index in range(groups):
        last = sorted(range(groups), key=lambda other: (-abs(other - index), -other))[0]
        order = sorted(
            (other for other in range(groups) if other != last),
            key=lambda other: (other in (0, groups - 1), abs(other - index)),
        )
        result = jnp.where(group == index, (order + [last])[step], result)
    return result


def step_kernel(
    ctx_count, head_count, state_any, w_any, gain_ref, seg_ref, w_out_any, probe_any, noise_any,
    new_out, state_v, query_buf, kv_buf, w_ref, joined, half, sending, state_own, probe_own,
    noise_own, query_out, kv_out, part_out, readout_out, segs_out, log_v, grad_v, w_both, pair_acc,
    query_acc, deltas, query_fin, pair_buf, beside_in, away_buf, terms_in, partial, passing, sum_v,
    load_sem, w_sem, q_send, q_recv, kv_send, kv_recv, pass_send, seg_send, seg_recv, line_send,
    line_recv, plane_send, plane_recv, beside_send, beside_recv, shard_send, shard_recv, shard_sem,
    out_send, out_recv, back_send, back_recv, row_sem, pair_send, pair_recv, b_send, b_recv, a_send,
    a_recv, z_send, z_recv,
):
    ctx, me, group, core = place()
    rows, model = state_any.shape
    own, groups = rows // head_count, head_count // 2
    slots = w_any.shape[2] // HEAD_DIM
    chunk = 2 * own
    partner = group * 2 + 1 - core

    def at(piece):
        return pl.ds(pl.multiple_of(piece * chunk, chunk), chunk)

    def own_at(piece):
        return pl.ds(pl.multiple_of(piece * own, own), own)

    def load_state(piece):
        return pltpu.make_async_copy(
            state_any.at[at(piece)], state_v.at[at(piece)], load_sem.at[piece]
        )

    load_state(0).start()
    w_loads = [
        pltpu.make_async_copy(w_any.at[t], w_both.at[core, t], w_sem.at[t]) for t in range(3)
    ]
    for copy in w_loads:
        copy.start()
    for piece in range(1, groups):
        load_state(piece).start()
    my_rows = own_at(me)
    shard = w_out_any.shape[0]
    part, quarter = shard // 2, shard // ctx_count
    later_loads = [
        pltpu.make_async_copy(state_any.at[my_rows], state_own, row_sem.at[0]),
        pltpu.make_async_copy(probe_any.at[my_rows], probe_own, row_sem.at[1]),
        pltpu.make_async_copy(noise_any, noise_own, row_sem.at[2]),
        pltpu.make_async_copy(
            w_out_any, w_ref.at[pl.ds(pl.multiple_of(me * shard, shard), shard)], shard_sem
        ),
    ]
    for copy in later_loads:
        copy.start()
    peers = [(lax.rem(ctx + step, ctx_count), partner) for step in range(ctx_count)]
    for far in range(groups):
        for step in range(ctx_count):
            if far or step:
                peers.append(
                    (lax.rem(ctx + step, ctx_count), lax.rem(group + far, groups) * 2 + core)
                )
    announce(peers)

    low, high = lax.rem(ctx, 2), ctx // 2
    which = lax.rem(low + high, 2)
    across, along = high * 2 + 1 - low, (1 - high) * 2 + low

    def shard_rows(origin, first, size):
        return pl.ds(pl.multiple_of((origin * 2 + core) * shard + first, size), size)

    def line_copy(way, origin, axis, mine):
        first = which * part + axis * quarter
        here = shard_rows(origin, first, quarter)
        source = (
            w_out_any.at[pl.ds(pl.multiple_of(first, quarter), quarter)] if mine else w_ref.at[here]
        )
        other = group + 1 if way == 0 else group - 1
        return remote(
            source, w_ref.at[here], line_send.at[way, axis, origin], line_recv.at[axis, origin],
            ctx, other * 2 + core,
        )

    def plane_copy(axis, origin, kept):
        here = shard_rows(origin, kept * part + axis * quarter, quarter)
        return remote(
            w_ref.at[here], w_ref.at[here], plane_send.at[axis, origin],
            plane_recv.at[axis, origin], along if axis else across, me,
        )

    def beside_copy(kind, origin):
        kept = which if kind < 2 else 1 - which
        here = shard_rows(origin, kept * part + (kind % 2) * quarter, quarter)
        return remote(
            w_ref.at[here], w_ref.at[here], beside_send.at[kind, origin],
            beside_recv.at[kind, origin], ctx, partner,
        )

    def shard_copy():
        return remote(
            w_out_any, w_ref.at[pl.ds(pl.multiple_of(me * shard, shard), shard)], shard_send,
            shard_recv, ctx, partner,
        )

    has_up, has_down = group < groups - 1, group > 0

    def each_origin(distance, work):
        for way in range(2):
            origin = group - distance if way == 0 else group + distance

            @pl.when(origin >= 0 if way == 0 else origin < groups)
            def _():
                work(way, origin)

    def line_arrived(distance, axis):
        def work(way, origin):
            line_copy(way, origin, axis, False).wait_recv()

            @pl.when(has_up if way == 0 else has_down)
            def _():
                line_copy(way, origin, axis, False).start()

            plane_copy(axis, origin, which).start()
            beside_copy(axis, origin).start()

        each_origin(distance, work)

    def plane_arrived(distance, axis):
        def work(way, origin):
            plane_copy(axis, origin, 1 - which).wait_recv()
            beside_copy(2 + axis, origin).start()

        each_origin(distance, work)

    def weights_sent(distance):
        def work(way, origin):
            for axis in range(2):

                @pl.when(has_up if way == 0 else has_down)
                def _():
                    line_copy(way, origin, axis, False).wait_send()

                plane_copy(axis, origin, which).wait_send()
            for kind in range(4):
                beside_copy(kind, origin).wait_send()

        each_origin(distance, work)

    def own_lines(work):
        for axis in range(2):

            @pl.when(has_up)
            def _():
                work(line_copy(0, group, axis, True))

            @pl.when(has_down)
            def _():
                work(line_copy(1, group, axis, True))

    for copy in w_loads:
        copy.wait()
    gain = gain_ref[...].astype(jnp.float32).reshape(1, model)

    def away(slot, kind, piece, dest):
        head = group * 2 + kind
        return (
            remote(
                query_buf.at[slot, piece, kind], query_out.at[piece, ctx],
                q_send.at[slot, kind, piece], q_recv.at[ctx, piece], dest, head,
            ),
            remote(
                kv_buf.at[slot, kind, piece], kv_out.at[kind, piece, ctx],
                kv_send.at[slot, kind, piece], kv_recv.at[kind, ctx, piece], dest, head,
            ),
        )

    def beside(slot, piece):
        result = [
            remote(
                query_buf.at[slot, piece, 1 - core], query_out.at[piece, ctx],
                q_send.at[slot, 1 - core, piece], q_recv.at[ctx, piece], ctx, partner,
            )
        ]
        for kind in range(2):
            result.append(
                remote(
                    kv_buf.at[slot, kind, piece], kv_out.at[kind, piece, ctx],
                    kv_send.at[slot, kind, piece], kv_recv.at[kind, ctx, piece], ctx, partner,
                )
            )
        return result

    def project(piece):
        load_state(piece).wait()
        block = state_v[at(piece), :].astype(jnp.float32)
        normed = (block * row_scale(block) * gain).astype(jnp.bfloat16)
        for t in range(3):
            result = jnp.dot(normed, w_both[core, t], preferred_element_type=jnp.float32).astype(
                jnp.bfloat16
            )
            for slot in range(slots):
                cut = result[:, slot * HEAD_DIM : (slot + 1) * HEAD_DIM]
                if t == 0:
                    query_buf[slot, piece, 0] = cut[:own]
                    query_buf[slot, piece, 1] = cut[own:]
                else:
                    kv_buf[slot, t - 1, piece] = cut

    def send_heads(piece):
        for slot in range(slots):
            dest = core * slots + slot

            @pl.when(dest != ctx)
            def _():
                for kind in range(2):
                    for copy in away(slot, kind, piece, dest):
                        copy.start()

            @pl.when(dest == ctx)
            def _():
                query_out[piece, ctx] = query_buf[slot, piece, core]
                for kind in range(2):
                    kv_out[kind, piece, ctx] = kv_buf[slot, kind, piece]
                for copy in beside(slot, piece):
                    copy.start()

    project(0)
    await_all(peers)
    own_lines(lambda copy: copy.start())
    send_heads(0)
    shard_copy().start()
    segs = []
    for step in range(1, ctx_count):
        copy = remote(
            seg_ref, segs_out.at[ctx], seg_send.at[step], seg_recv.at[step],
            lax.rem(ctx + step, ctx_count), me,
        )
        copy.start()
        segs.append(copy)
    segs_out[ctx] = seg_ref[...]

    def project_and_send(piece, _):
        project(piece)
        send_heads(piece)
        return 0

    lax.fori_loop(1, groups, project_and_send, 0)

    def hand_over(piece, step):
        source = lax.rem(ctx + step, ctx_count)
        return remote(
            kv_out.at[core, piece, source], kv_out.at[core, piece, source],
            pass_send.at[step, piece], kv_recv.at[core, source, piece], ctx, partner,
        )

    for piece in range(groups):
        for step in range(1, ctx_count):
            copy = hand_over(piece, step)
            copy.wait_recv()
            copy.start()
        if piece == 0:
            line_arrived(1, 0)
        if piece == min(2, groups - 1):
            line_arrived(1, 1)
    line_arrived(2, 0)

    def got_query(source, piece):
        remote(
            query_out.at[piece, source], query_out.at[piece, source],
            q_send.at[0, 0, piece], q_recv.at[source, piece], ctx, partner,
        ).wait_recv()

    def got_kv(kind, source, piece):
        remote(
            kv_out.at[kind, piece, source], kv_out.at[kind, piece, source],
            kv_send.at[0, 0, piece], kv_recv.at[kind, source, piece], ctx, partner,
        ).wait_recv()

    def gather(piece, _):
        for step in range(1, ctx_count):
            source = lax.rem(ctx + step, ctx_count)
            got_query(source, piece)
            got_kv(1 - core, source, piece)
            hand_over(piece, step).wait_send()

        @pl.when(ctx // slots != core)
        def _():
            got_query(ctx, piece)
            for kind in range(2):
                got_kv(kind, ctx, piece)

        return 0

    lax.fori_loop(0, groups, gather, 0)
    for copy in segs:
        copy.wait()
    pair_copy = remote(w_any, w_both.at[core], pair_send, pair_recv, ctx, partner)
    pair_copy.start()

    def cols_of(group_at, ctx_at):
        head = group_at * ctx_count + ctx_at
        return pl.ds(pl.multiple_of(head * HEAD_DIM, HEAD_DIM), HEAD_DIM)

    factor = HEAD_DIM ** (-0.5) * LOG2E
    sub = groups * own
    seg_all = segs_out[...]

    def below(value):
        count = jnp.where(seg_all < value, 1.0, 0.0)
        for axis in (0, 1, 2):
            count = jnp.sum(count, axis=axis, keepdims=True)
        return count[0]

    first_bound, second_bound = below(1), below(2)
    lane = lax.broadcasted_iota(jnp.int32, (1, sub), 1)
    inside = (lane // own) * (2 * own) + core * own + lane % own
    key_row = lax.broadcasted_iota(jnp.int32, (rows, sub), 0)

    def out_copy(tile, order, other):
        return remote(
            part_out.at[other, tile], joined.at[:, cols_of(group, ctx)],
            out_send.at[tile, order], out_recv.at[group, ctx], tile, other * 2 + core,
        )

    def one_tile(tile, _):
        query = query_out[:, tile].reshape(sub, HEAD_DIM)
        pos = (tile * rows + inside).astype(jnp.float32)
        start = jnp.where(
            pos >= second_bound, second_bound, jnp.where(pos >= first_bound, first_bound, 0.0)
        ).astype(jnp.int32)

        def step(diagonal, piece, carry):
            top, total, acc = carry
            scores = dot32(kv_out[0, :, piece].reshape(rows, HEAD_DIM), query, NT)
            allowed = key_row >= start - piece * rows
            if diagonal:
                allowed = allowed & (key_row <= inside)
            scores = jnp.where(allowed, scores, NEGATIVE)
            new_top = jnp.maximum(top, jnp.max(scores, axis=0, keepdims=True) * factor)
            weights = jnp.exp2(scores * factor - new_top)
            scale = jnp.exp2(top - new_top)
            total = total * scale + jnp.sum(weights, axis=0, keepdims=True)
            acc = acc * scale + dot32(
                kv_out[1, :, piece].reshape(rows, HEAD_DIM), weights.astype(jnp.bfloat16), TN
            )
            return new_top, total, acc

        carry = (
            jnp.full((1, sub), NEGATIVE, jnp.float32),
            jnp.zeros((1, sub), jnp.float32),
            jnp.zeros((HEAD_DIM, sub), jnp.float32),
        )
        carry = lax.fori_loop(0, tile, functools.partial(step, False), carry)
        top, total, acc = step(True, tile, carry)
        result = (acc / total).T.astype(jnp.bfloat16)
        log_row = top + jnp.log2(total)
        for index in range(groups):
            part_out[index, tile] = result[index * own : (index + 1) * own]
            log_v[index, :, own_at(tile)] = log_row[:, index * own : (index + 1) * own]
        for order in range(groups):
            other = far_first(groups, group, order)
            if order == groups - 1:

                @pl.when(tile != ctx)
                def _():
                    out_copy(tile, order, other).start()

                @pl.when(tile == ctx)
                def _():
                    joined[:, cols_of(group, ctx)] = part_out[group, tile]

            else:
                out_copy(tile, order, other).start()

        @pl.when(tile == 1)
        def _():
            line_arrived(2, 1)

        return 0

    lax.fori_loop(0, ctx_count, one_tile, 0)
    for copy in later_loads:
        copy.wait()
    sources = []
    for far in range(groups):
        for step in range(ctx_count):
            if far or step:
                sources.append((lax.rem(group + far, groups), lax.rem(ctx + step, ctx_count)))
    tile = min(256, model)
    wide = ctx_count * HEAD_DIM
    zero = jnp.zeros((own, 1), jnp.float32)
    for axis in range(2):
        plane_arrived(1, axis)
    for distance in range(3, groups):
        line_arrived(distance, 0)
    for axis in range(2):
        plane_arrived(2, axis)
    for distance in range(3, groups):
        line_arrived(distance, 1)
    shard_copy().wait_recv()

    def heads_arrived(order):
        other = far_first(groups, group, order)
        if order < groups - 1:
            for kind in range(4):
                beside_copy(kind, other).wait_recv()
        for step in range(ctx_count):
            if order < groups - 1 or step:
                peer = lax.rem(ctx + step, ctx_count)
                remote(
                    part_out.at[0, 0], joined.at[:, cols_of(other, peer)],
                    out_send.at[0, 0], out_recv.at[other, peer], peer, other * 2 + core,
                ).wait_recv()

    for order in range(groups - 1, 0, -1):
        heads_arrived(order)
    farthest = far_first(groups, group, 0)
    near = pl.ds(pl.multiple_of(jnp.where(farthest == 0, wide, 0), wide), model - wide)
    far = pl.ds(pl.multiple_of(farthest * wide, wide), wide)

    def near_layer(piece, _):
        cols = pl.ds(pl.multiple_of(piece * tile, tile), tile)
        readout_out[:, cols] = state_own[:, cols].astype(jnp.float32) + jnp.dot(
            joined[:, near], w_ref[near, cols], preferred_element_type=jnp.float32
        )
        return 0

    lax.fori_loop(0, model // tile, near_layer, 0)
    for distance in range(3, groups):
        for axis in range(2):
            plane_arrived(distance, axis)
    heads_arrived(0)

    def layer(piece, carry):
        squares, products = carry
        cols = pl.ds(pl.multiple_of(piece * tile, tile), tile)
        result = readout_out[:, cols] + jnp.dot(
            joined[:, far], w_ref[far, cols], preferred_element_type=jnp.float32
        )
        readout_out[:, cols] = result
        squares = squares + jnp.sum(result * result, axis=1, keepdims=True)
        products = products + jnp.sum(
            result * probe_own[:, cols].astype(jnp.float32), axis=1, keepdims=True
        )
        return squares, products

    squares, products = lax.fori_loop(0, model // tile, layer, (zero, zero))
    scale = lax.rsqrt(squares / model + EPSILON)
    bend = scale**3 * (products / model)

    def finish(piece, _):
        cols = pl.ds(pl.multiple_of(piece * tile, tile), tile)
        readout = scale * probe_own[:, cols].astype(jnp.float32) - readout_out[:, cols] * bend
        readout_out[:, cols] = readout
        half[:, cols] = readout.astype(jnp.bfloat16)
        return 0

    lax.fori_loop(0, model // tile, finish, 0)
    copies = []
    for order in range(groups):
        other = far_first(groups, group, order)
        result = dot32(
            half[...], w_ref[pl.ds(pl.multiple_of(other * wide, wide), wide), :], NT
        ).astype(jnp.bfloat16)
        for index in range(ctx_count):
            sending[order, index] = result[:, index * HEAD_DIM : (index + 1) * HEAD_DIM]
        for step in range(ctx_count):
            peer = lax.rem(ctx + step, ctx_count)
            if order == groups - 1 and step == 0:
                continue
            copy = remote(
                sending.at[order, peer], grad_v.at[group, ctx], back_send.at[order, step],
                back_recv.at[ctx, group], peer, other * 2 + core,
            )
            copy.start()
            copies.append(copy)
    grad_v[group, ctx] = sending[groups - 1, ctx]

    def clear(index, _):
        pair_acc[index] = jnp.zeros(pair_acc.shape[1:], jnp.float32)
        query_acc[index] = jnp.zeros(query_acc.shape[1:], jnp.float32)
        return 0

    lax.fori_loop(0, groups, clear, 0)

    def sent(piece, _):
        for slot in range(slots):
            dest = core * slots + slot

            @pl.when(dest != ctx)
            def _():
                for kind in range(2):
                    for copy in away(slot, kind, piece, dest):
                        copy.wait_send()

            @pl.when(dest == ctx)
            def _():
                for copy in beside(slot, piece):
                    copy.wait_send()

        return 0

    lax.fori_loop(0, groups, sent, 0)

    own_lines(lambda copy: copy.wait_send())
    shard_copy().wait_send()
    for distance in range(1, groups):
        weights_sent(distance)

    def parts_sent(tile, _):
        for order in range(groups):
            other = far_first(groups, group, order)
            if order == groups - 1:

                @pl.when(tile != ctx)
                def _():
                    out_copy(tile, order, other).wait_send()

            else:
                out_copy(tile, order, other).wait_send()
        return 0

    lax.fori_loop(0, ctx_count, parts_sent, 0)
    halves = 2
    span = ctx_count * own // halves
    dests = [far_first(groups, group, order) for order in range(groups)]

    def dest_of(order):
        result = dests[0]
        for index in range(1, groups):
            result = jnp.where(order == index, dests[index], result)
        return result

    score_scale = HEAD_DIM ** (-0.5)
    def half_of(ref, index, half):
        count = ctx_count // halves
        return ref[index, half * count : (half + 1) * count].reshape(span, HEAD_DIM)

    def find_deltas(index):
        for half in range(halves):
            product = half_of(grad_v, index, half).astype(jnp.float32) * half_of(
                part_out, index, half
            ).astype(jnp.float32)
            deltas[index, :, half * span : (half + 1) * span] = jnp.sum(
                product.T, axis=0, keepdims=True
            )

    def gradients_arrived(other):
        for peer in range(ctx_count):

            @pl.when(jnp.logical_or(other != group, ctx != peer))
            def _():
                remote(
                    sending.at[0, 0], grad_v.at[other, peer], back_send.at[0, 0],
                    back_recv.at[peer, other], ctx, partner,
                ).wait_recv()

        find_deltas(other)

    spot_lane = lax.broadcasted_iota(jnp.int32, (1, span), 1)
    key_line = lax.broadcasted_iota(jnp.int32, (2 * own, own), 0)

    def pair(query_at, key_at):
        for half in range(halves):
            blocks = (half + 1) * ctx_count // halves
            count = blocks * 2 * own
            lanes = slice(half * span, (half + 1) * span)
            key_block = kv_out[0, key_at, :blocks].reshape(count, HEAD_DIM)
            value_block = kv_out[1, key_at, :blocks].reshape(count, HEAD_DIM)
            query_block = half_of(query_out, query_at, half)
            grad_block = half_of(grad_v, query_at, half)
            first_ctx = half * (ctx_count // halves)
            pos = (first_ctx + spot_lane // own) * rows + spot_lane % own
            pos = pos + (query_at * 2 + core) * own
            pos_f = pos.astype(jnp.float32)
            start = jnp.where(
                pos_f >= second_bound,
                second_bound,
                jnp.where(pos_f >= first_bound, first_bound, 0.0),
            ).astype(jnp.int32)
            scores = dot32(key_block, query_block, NT)
            raw = jnp.exp2(scores * factor - log_v[query_at, :, lanes])
            strips = []
            for source in range(blocks):
                offset = source * rows + key_at * 2 * own
                row_cut = slice(source * 2 * own, (source + 1) * 2 * own)
                cells = []
                for index in range(ctx_count // halves):
                    lane_cut = slice(index * own, (index + 1) * own)
                    if source > first_ctx + index:
                        cells.append(jnp.zeros((2 * own, own), jnp.float32))
                        continue
                    allowed = key_line >= start[:, lane_cut] - offset
                    if source == first_ctx + index:
                        allowed = allowed & (key_line <= pos[:, lane_cut] - offset)
                    cells.append(jnp.where(allowed, raw[row_cut, lane_cut], 0.0))
                strips.append(jnp.concatenate(cells, axis=1))
            probabilities = jnp.concatenate(strips, axis=0)
            dprobs = dot32(value_block, grad_block, NT)
            dscores = (probabilities * (dprobs - deltas[query_at, :, lanes])).astype(jnp.bfloat16)
            pair_acc[key_at, :count, HEAD_DIM:] += jnp.dot(
                probabilities.astype(jnp.bfloat16), grad_block, preferred_element_type=jnp.float32
            )
            pair_acc[key_at, :count, :HEAD_DIM] += jnp.dot(
                dscores, query_block, preferred_element_type=jnp.float32
            )
            query_acc[query_at, :, lanes] += dot32(key_block, dscores, TN)

    def core_copy(order):
        return remote(
            pair_buf.at[order], beside_in.at[order], b_send.at[order], b_recv.at[order], ctx, partner
        )

    def pair_rows(dest, source, kind):
        first = pl.multiple_of((source * 2 + kind) * own, own)
        keys = pair_acc[dest, pl.ds(first, own), :HEAD_DIM] * score_scale
        values = pair_acc[dest, pl.ds(first, own), HEAD_DIM:]
        return keys, values

    def settle(order):
        dest = dest_of(order)
        for source in range(ctx_count):
            keys, values = pair_rows(dest, source, 1 - core)
            pair_buf[order, source, :, :HEAD_DIM] = keys.astype(jnp.bfloat16)
            pair_buf[order, source, :, HEAD_DIM:] = values.astype(jnp.bfloat16)
        for half in range(halves):
            query_fin[order, half * span : (half + 1) * span, :] = (
                query_acc[dest, :, half * span : (half + 1) * span].T * score_scale
            ).astype(jnp.bfloat16)
        core_copy(order).start()

    def stripe(source):
        slot = lax.rem(source, slots)
        return pl.ds(pl.multiple_of(slot * HEAD_DIM, HEAD_DIM), HEAD_DIM)

    def exchange(order, step):
        peer = lax.rem(ctx + step, ctx_count)
        return remote(
            away_buf.at[order, step],
            terms_in.at[dest_of(order), ctx // slots, :, :, stripe(ctx)],
            a_send.at[order, step], a_recv.at[dest_of(order), ctx], peer, me,
        )

    def arrived(dest, step):
        source = lax.rem(ctx + step, ctx_count)
        remote(
            away_buf.at[0, 0], terms_in.at[dest, source // slots, :, :, stripe(source)],
            a_send.at[0, 0], a_recv.at[dest, source], source, me,
        ).wait_recv()

    def spread(order):
        dest = dest_of(order)
        core_copy(order).wait_recv()
        for step in range(1, ctx_count + 1):
            peer = lax.rem(ctx + step, ctx_count)
            keys, values = pair_rows(dest, peer, core)
            keys = (keys + beside_in[order, peer, :, :HEAD_DIM].astype(jnp.float32)).astype(
                jnp.bfloat16
            )
            values = (values + beside_in[order, peer, :, HEAD_DIM:].astype(jnp.float32)).astype(
                jnp.bfloat16
            )
            queries = query_fin[order, pl.ds(pl.multiple_of(peer * own, own), own), :]
            if step < ctx_count:
                away_buf[order, step, 0] = queries
                away_buf[order, step, 1] = keys
                away_buf[order, step, 2] = values
                exchange(order, step).start()
            else:
                at = stripe(ctx)
                terms_in[dest, ctx // slots, 0, :, at] = queries
                terms_in[dest, ctx // slots, 1, :, at] = keys
                terms_in[dest, ctx // slots, 2, :, at] = values

    pieces = partial.shape[2]
    strip = model // pieces

    def chain(order, piece):
        dest = dest_of(order)
        up = dest > group
        line = jnp.where(up, 0, 1)
        peer = jnp.where(up, group + 1, group - 1)
        return remote(
            passing.at[order, piece], partial.at[line, dest, piece], z_send.at[order, piece],
            z_recv.at[line, dest, piece], ctx, peer * 2 + core,
        )

    def came(line, dest, piece):
        remote(
            passing.at[0, piece], partial.at[line, dest, piece], z_send.at[0, piece],
            z_recv.at[line, dest, piece], ctx, partner,
        ).wait_recv()

    def term(dest, piece):
        cols = pl.ds(pl.multiple_of(piece * strip, strip), strip)
        result = None
        for half in range(2):
            for kind in range(3):
                part = dot32(terms_in[dest, half, kind], w_both[half, kind, cols, :], NT)
                result = part if result is None else result + part
        return result

    inner = (group > 0) & (group < groups - 1)

    def pass_on(order, _):
        dest = dest_of(order)
        for step in range(1, ctx_count):
            arrived(dest, step)
        line = jnp.where(dest > group, 0, 1)

        def one_piece(piece, _):
            sum_v[...] = term(dest, piece)

            @pl.when(inner)
            def _():
                came(line, dest, piece)
                sum_v[...] += partial[line, dest, piece].astype(jnp.float32)

            passing[order, piece] = sum_v[...].astype(jnp.bfloat16)
            chain(order, piece).start()
            return 0

        lax.fori_loop(0, pieces, one_piece, 0)
        return 0

    ends, number = [], 0
    for order in range(groups):
        number += 2 * (groups - order) - 1
        ends.append(number - 1)
    spreads = {order: end + 1 for order, end in enumerate(ends) if end + 1 < number}

    def one_pair(index, _):
        stage = 0
        for end in ends[:-1]:
            stage = stage + jnp.where(index > end, 1, 0)
        first = 0
        for order in range(1, groups):
            first = jnp.where(stage == order, ends[order - 1] + 1, first)
        inside = index - first
        other = stage + (inside + 1) // 2
        odd = lax.rem(inside, 2)
        pair(
            dest_of(jnp.where(odd == 1, stage, other)), dest_of(jnp.where(odd == 1, other, stage))
        )
        for order, end in list(enumerate(ends))[1:-1]:

            @pl.when(index == end)
            def _():
                settle(order)

        for order, at in spreads.items():

            @pl.when(index == at)
            def _():
                spread(order)

        return 0

    def farthest_pair(index, _):
        arriving = index < groups
        other = 0
        for step in range(groups):
            visit = by_arrival(groups, group, step)
            other = jnp.where(index == step, visit, other)
            other = jnp.where(index == groups + step, visit, other)

        @pl.when(arriving)
        def _():
            gradients_arrived(other)

        pair(jnp.where(arriving, other, dests[0]), jnp.where(arriving, dests[0], other))
        return 0

    first = min(ends[min(1, groups - 1)] + 2, number)
    lax.fori_loop(0, ends[0] + 1, farthest_pair, 0)
    settle(0)
    lax.fori_loop(ends[0] + 1, first, one_pair, 0)
    pair_copy.wait()
    early = 1 if first < number else 0
    if early:

        @pl.when(jnp.logical_not(inner))
        def _():
            pass_on(0, 0)

        lax.fori_loop(first, number, one_pair, 0)
    settle(groups - 1)
    for order in range(groups):
        if order not in spreads:
            spread(order)
    lax.fori_loop(jnp.where(inner, 0, early), groups - 1, pass_on, 0)
    for step in range(1, ctx_count):
        arrived(group, step)

    state = state_own[...].astype(jnp.float32)
    inverse = row_scale(state)

    def last_piece(piece, slope):
        cols = pl.ds(pl.multiple_of(piece * strip, strip), strip)
        sum_v[...] = term(group, piece)

        @pl.when(group > 0)
        def _():
            came(0, group, piece)
            sum_v[...] += partial[0, group, piece].astype(jnp.float32)

        @pl.when(group < groups - 1)
        def _():
            came(1, group, piece)
            sum_v[...] += partial[1, group, piece].astype(jnp.float32)

        gained = sum_v[...] * gain_ref[cols].astype(jnp.float32).reshape(1, strip)
        new_out[:, cols] = gained
        return slope + jnp.sum(
            gained * state_own[:, cols].astype(jnp.float32), axis=1, keepdims=True
        )

    slope = lax.fori_loop(0, pieces, last_piece, jnp.zeros((own, 1), jnp.float32))
    bend = inverse**3 * (slope / model)

    def update(piece, _):
        cols = pl.ds(pl.multiple_of(piece * strip, strip), strip)
        here = state_own[:, cols].astype(jnp.float32)
        gradient = readout_out[:, cols] + inverse * new_out[:, cols] - here * bend
        new_out[:, cols] = (
            here - STEP_SIZE * gradient + NOISE_SCALE * noise_own[:, cols].astype(jnp.float32)
        )
        return 0

    lax.fori_loop(0, pieces, update, 0)

    def all_sent(order, _):
        core_copy(order).wait_send()
        for step in range(1, ctx_count):
            exchange(order, step).wait_send()

        @pl.when(order < groups - 1)
        def _():
            for piece in range(pieces):
                chain(order, piece).wait_send()

        return 0

    for copy in copies:
        copy.wait_send()
    lax.fori_loop(0, groups, all_sent, 0)


def heads_body(state, norm_gain, w_qkv, w_out, probe, noise, segment_ids):
    ctx_count, head_count = lax.axis_size("ctx"), lax.axis_size("head")
    rows, model = state.shape
    width = w_qkv.shape[2]
    own, groups, slots = rows // head_count, head_count // 2, width // HEAD_DIM
    seg = segment_ids.reshape(-1, 128)
    half, full, dma = jnp.bfloat16, jnp.float32, pltpu.SemaphoreType.DMA
    pieces, lanes = 4, ctx_count * own
    tile, vmem = model // pieces, pltpu.VMEM
    heads = (groups, ctx_count, own, HEAD_DIM)
    return pl.pallas_call(
        functools.partial(step_kernel, ctx_count, head_count),
        out_shape=jax.ShapeDtypeStruct((own, model), full),
        in_specs=[ANY, ANY, VMEM, VMEM, ANY, ANY, ANY],
        out_specs=VMEM,
        scratch_shapes=[
            vmem((rows, model), half),
            vmem((slots, groups, 2, own, HEAD_DIM), half),
            vmem((slots, 2, groups, 2 * own, HEAD_DIM), half),
            vmem((model, model), half),
            vmem((own, model), half),
            vmem((own, model), half),
            vmem(heads, half),
            vmem((own, model), half),
            vmem((own, model), half),
            vmem((own, model), half),
            vmem(heads, half),
            vmem((2, groups, ctx_count, 2 * own, HEAD_DIM), half),
            vmem(heads, half),
            vmem((own, model), full),
            vmem((ctx_count,) + seg.shape, seg.dtype),
            vmem((groups, 1, lanes), full),
            vmem(heads, half),
            vmem((2,) + w_qkv.shape, half),
            vmem((groups, 2 * lanes, 2 * HEAD_DIM), full),
            vmem((groups, HEAD_DIM, lanes), full),
            vmem((groups, 1, lanes), full),
            vmem((groups, lanes, HEAD_DIM), half),
            vmem((groups, ctx_count, own, 2 * HEAD_DIM), half),
            vmem((groups, ctx_count, own, 2 * HEAD_DIM), half),
            vmem((groups, ctx_count, 3, own, HEAD_DIM), half),
            vmem((groups, 2, 3, own, width), half),
            vmem((2, groups, pieces, own, tile), half),
            vmem((groups, pieces, own, tile), half),
            vmem((own, tile), full),
            dma((groups,)),
            dma((3,)),
            dma((slots, 2, groups)),
            dma((ctx_count, groups)),
            dma((slots, 2, groups)),
            dma((2, ctx_count, groups)),
            dma((ctx_count, groups)),
            dma((ctx_count,)),
            dma((ctx_count,)),
            dma((2, 2, groups)),
            dma((2, groups)),
            dma((2, groups)),
            dma((2, groups)),
            dma((4, groups)),
            dma((4, groups)),
            dma,
            dma,
            dma,
            dma((ctx_count, groups)),
            dma((groups, ctx_count)),
            dma((groups, ctx_count)),
            dma((ctx_count, groups)),
            dma((3,)),
            dma,
            dma,
            dma((groups,)),
            dma((groups,)),
            dma((groups, ctx_count)),
            dma((groups, ctx_count)),
            dma((groups, pieces)),
            dma((2, groups, pieces)),
        ],
        compiler_params=pltpu.CompilerParams(
            collective_id=0, has_side_effects=True, vmem_limit_bytes=63 * 2**20
        ),
    )(state, w_qkv, norm_gain, seg, w_out, probe, noise)


def solution(mesh):
    placed = (
        P("ctx", None),
        P(),
        P(None, None, "head"),
        P("head", None),
        P("ctx", None),
        P(("ctx", "head"), None),
        P("ctx"),
    )

    def step(*args):
        heads = args[2].shape[2] // HEAD_DIM
        return (heads_body if lax.axis_size("ctx") == 2 * heads == 4 else body)(*args)

    return jax.shard_map(
        step, mesh=mesh, in_specs=placed, out_specs=P(("ctx", "head"), None), check_vma=False
    )
```

```python
import functools

import jax
import jax.numpy as jnp
from jax import lax
from jax.experimental import pallas as pl
from jax.experimental.pallas import tpu as pltpu
from jax.sharding import PartitionSpec as P

HEAD_DIM = 128
EPSILON = 1e-05
STEP_SIZE = 0.25
NOISE_SCALE = (2.0 * STEP_SIZE) ** 0.5
NEGATIVE = -1e30
LOG2E = 1.4426950408889634
MESH = pl.DeviceIdType.MESH
VMEM = pl.BlockSpec(memory_space=pltpu.VMEM)
ANY = pl.BlockSpec(memory_space=pl.ANY)
NT = (((1,), (1,)), ((), ()))
TN = (((0,), (0,)), ((), ()))
FORWARD_BLOCKS = (512, 512)
BACKWARD_BLOCKS = (512, 512)


def row_scale(matrix):
    return lax.rsqrt(jnp.mean(matrix * matrix, axis=-1, keepdims=True) + EPSILON)


def dot32(left, right, dims):
    return lax.dot_general(left, right, dims, preferred_element_type=jnp.float32)


def greet(axis, number, me):
    barrier = pltpu.get_barrier_semaphore()
    for step in range(1, number):
        pl.semaphore_signal(
            barrier, inc=1, device_id={axis: lax.rem(me + step, number)}, device_id_type=MESH
        )
    pl.semaphore_wait(barrier, number - 1)


def gather_kernel(
    number, key_ref, value_ref, seg_ref, normed_ref, w_ref, keys, values, segs, query_out, send_sem,
    recv_sem, own_sem,
):
    me = lax.axis_index("ctx")
    rows = key_ref.shape[0]
    greet("ctx", number, me)

    def place(index):
        return pl.ds(pl.multiple_of(index * rows, rows), rows)

    def send(slot, source, target, peer):
        copy = pltpu.make_async_remote_copy(
            src_ref=source,
            dst_ref=target,
            send_sem=send_sem.at[slot],
            recv_sem=recv_sem.at[slot],
            device_id={"ctx": peer},
            device_id_type=MESH,
        )
        copy.start()
        return copy

    mine = place(me)
    copies = []
    for step in range(1, number):
        copies.append(send(step, seg_ref, segs.at[me], lax.rem(me + step, number)))
    relay = number == 4
    if relay:
        low, high = lax.rem(me, 2), me // 2
        across, along = high * 2 + 1 - low, (1 - high) * 2 + low
        key_first = send(number, key_ref, keys.at[mine], across)
        value_first = send(number + 1, value_ref, values.at[mine], along)
        copies.append(send(number + 2, value_ref, values.at[mine], across))
        copies.append(send(number + 3, key_ref, keys.at[mine], along))
    else:
        for step in range(1, number):
            peer = lax.rem(me + step, number)
            copies.append(send(number + 2 * step, key_ref, keys.at[mine], peer))
            copies.append(send(number + 2 * step + 1, value_ref, values.at[mine], peer))
    pairs = ((key_ref, keys.at[mine]), (value_ref, values.at[mine]), (seg_ref, segs.at[me]))
    for index, (source, target) in enumerate(pairs):
        copy = pltpu.make_async_copy(source, target, own_sem.at[index])
        copy.start()
        copies.append(copy)
    tile = min(256, rows)

    def project(piece, _):
        at = pl.ds(pl.multiple_of(piece * tile, tile), tile)
        query_out[at, :] = jnp.dot(
            normed_ref[at, :], w_ref[...], preferred_element_type=jnp.float32
        ).astype(jnp.bfloat16)
        return 0

    lax.fori_loop(0, rows // tile, project, 0)
    if relay:
        key_first.wait()
        copies.append(send(number + 4, keys.at[place(across)], keys.at[place(across)], along))
        value_first.wait()
        copies.append(send(number + 5, values.at[place(along)], values.at[place(along)], across))
    for copy in copies:
        copy.wait()


def gather_keys(number, key_rows, value_rows, segment_ids, normed, w_query):
    rows, width = key_rows.shape
    seg = segment_ids.reshape(-1, 128)
    full = jax.ShapeDtypeStruct((number * rows, width), key_rows.dtype)
    keys, values, segs, queries = pl.pallas_call(
        functools.partial(gather_kernel, number),
        out_shape=(
            full,
            full,
            jax.ShapeDtypeStruct((number,) + seg.shape, seg.dtype),
            jax.ShapeDtypeStruct((rows, width), key_rows.dtype),
        ),
        in_specs=[VMEM] * 5,
        out_specs=(ANY, ANY, ANY, VMEM),
        scratch_shapes=[
            pltpu.SemaphoreType.DMA((3 * number + 6,)),
            pltpu.SemaphoreType.DMA((3 * number + 6,)),
            pltpu.SemaphoreType.DMA((3,)),
        ],
        compiler_params=pltpu.CompilerParams(collective_id=0, has_side_effects=True),
    )(key_rows, value_rows, seg, normed, w_query)
    return keys, values, segs.reshape(-1), queries


def block_ranges(table, index):
    return [table[index, column] for column in range(4)]


def forward_kernel(
    heads, bq, bk, table, query_ref, key_ref, value_ref, start_ref, pos_ref, out_ref, log_ref
):
    factor = HEAD_DIM ** (-0.5) * LOG2E
    blocks = query_ref.shape[0] // bq

    def one_block(index, _):
        low, inner_low, inner_high, high = block_ranges(table, index)
        rows = pl.ds(pl.multiple_of(index * bq, bq), bq)
        start, pos = start_ref[index], pos_ref[index]

        def step(masked, piece, carry):
            keys_at = pl.ds(pl.multiple_of(piece * bk, bk), bk)
            if masked:
                key_pos = piece * bk + lax.broadcasted_iota(jnp.int32, (bk, bq), 0)
                allowed = (key_pos >= start) & (key_pos <= pos)
            result = []
            for head in range(heads):
                top, total, acc = carry[head]
                cols = pl.ds(head * HEAD_DIM, HEAD_DIM)
                scores = dot32(key_ref[keys_at, cols], query_ref[rows, cols], NT)
                if masked:
                    scores = jnp.where(allowed, scores, NEGATIVE)
                new_top = jnp.maximum(top, jnp.max(scores, axis=0, keepdims=True) * factor)
                weights = jnp.exp2(scores * factor - new_top)
                scale = jnp.exp2(top - new_top)
                total = total * scale + jnp.sum(weights, axis=0, keepdims=True)
                acc = acc * scale + dot32(
                    value_ref[keys_at, cols], weights.astype(jnp.bfloat16), TN
                )
                result.append((new_top, total, acc))
            return tuple(result)

        carry = tuple(
            (
                jnp.full((1, bq), NEGATIVE, jnp.float32),
                jnp.zeros((1, bq), jnp.float32),
                jnp.zeros((HEAD_DIM, bq), jnp.float32),
            )
            for _ in range(heads)
        )
        carry = lax.fori_loop(low, inner_low, functools.partial(step, True), carry)
        carry = lax.fori_loop(inner_low, inner_high, functools.partial(step, False), carry)
        carry = lax.fori_loop(inner_high, high, functools.partial(step, True), carry)
        for head in range(heads):
            top, total, acc = carry[head]
            out_ref[rows, pl.ds(head * HEAD_DIM, HEAD_DIM)] = (acc / total).T.astype(jnp.bfloat16)
            log_ref[index, pl.ds(head, 1), :] = top + jnp.log2(total)
        return 0

    lax.fori_loop(0, blocks, one_block, 0)


def backward_kernel(
    heads, bq, bk, table, query_ref, key_ref, value_ref, grad_ref, out_ref, log_ref, start_ref,
    pos_ref, query_out, pair_out, pair_acc,
):
    score_scale = HEAD_DIM ** (-0.5)
    factor = score_scale * LOG2E
    blocks = query_ref.shape[0] // bq
    width = heads * HEAD_DIM
    pair_rows = pair_acc.shape[0]

    def clear(piece, _):
        at = pl.ds(pl.multiple_of(piece * bk, bk), bk)
        pair_acc[at, :] = jnp.zeros((bk, 2 * width), jnp.float32)
        return 0

    lax.fori_loop(0, pair_rows // bk, clear, 0)

    def one_block(index, _):
        low, inner_low, inner_high, high = block_ranges(table, index)
        rows = pl.ds(pl.multiple_of(index * bq, bq), bq)
        start, pos = start_ref[index], pos_ref[index]
        deltas, logs = [], []
        for head in range(heads):
            cols = pl.ds(head * HEAD_DIM, HEAD_DIM)
            product = grad_ref[rows, cols].astype(jnp.float32) * out_ref[rows, cols].astype(
                jnp.float32
            )
            deltas.append(jnp.sum(product.T, axis=0, keepdims=True))
            logs.append(log_ref[index, pl.ds(head, 1), :])

        def step(masked, piece, carry):
            keys_at = pl.ds(pl.multiple_of(piece * bk, bk), bk)
            if masked:
                key_pos = piece * bk + lax.broadcasted_iota(jnp.int32, (bk, bq), 0)
                allowed = (key_pos >= start) & (key_pos <= pos)
            result = []
            for head in range(heads):
                cols = pl.ds(head * HEAD_DIM, HEAD_DIM)
                value_cols = pl.ds(width + head * HEAD_DIM, HEAD_DIM)
                key_block, query_block = key_ref[keys_at, cols], query_ref[rows, cols]
                grad_block = grad_ref[rows, cols]
                scores = dot32(key_block, query_block, NT)
                probabilities = jnp.exp2(scores * factor - logs[head])
                if masked:
                    probabilities = jnp.where(allowed, probabilities, 0.0)
                dprobs = dot32(value_ref[keys_at, cols], grad_block, NT)
                dscores = (probabilities * (dprobs - deltas[head])).astype(jnp.bfloat16)
                pair_acc[keys_at, value_cols] += jnp.dot(
                    probabilities.astype(jnp.bfloat16),
                    grad_block,
                    preferred_element_type=jnp.float32,
                )
                pair_acc[keys_at, cols] += jnp.dot(
                    dscores, query_block, preferred_element_type=jnp.float32
                )
                result.append(carry[head] + dot32(key_block, dscores, TN))
            return tuple(result)

        carry = tuple(jnp.zeros((HEAD_DIM, bq), jnp.float32) for _ in range(heads))
        carry = lax.fori_loop(low, inner_low, functools.partial(step, True), carry)
        carry = lax.fori_loop(inner_low, inner_high, functools.partial(step, False), carry)
        carry = lax.fori_loop(inner_high, high, functools.partial(step, True), carry)
        for head in range(heads):
            query_out[rows, pl.ds(head * HEAD_DIM, HEAD_DIM)] = (
                carry[head].T * score_scale
            ).astype(jnp.bfloat16)
        return 0

    lax.fori_loop(0, blocks, one_block, 0)

    def flush(piece, _):
        at = pl.ds(pl.multiple_of(piece * bk, bk), bk)
        pair_out[at, :width] = (pair_acc[at, :width] * score_scale).astype(jnp.bfloat16)
        pair_out[at, width:] = pair_acc[at, width:].astype(jnp.bfloat16)
        return 0

    lax.fori_loop(0, pair_rows // bk, flush, 0)


def make_table(start, pos, bq, bk):
    starts, places = start.reshape(-1, bq), pos.reshape(-1, bq)
    low = starts[:, 0] // bk
    inner_low = (starts[:, -1] + bk - 1) // bk
    inner_high = jnp.maximum(inner_low, (places[:, 0] + 1) // bk)
    high = places[:, -1] // bk + 1
    return jnp.stack([low, inner_low, inner_high, high], axis=1).astype(jnp.int32)


def middle_kernel(
    number, part_ref, w_any, state_ref, probe_ref, grad_out, readout_out, w_ref, joined, half,
    sending, landing, send_sem, recv_sem, back_send, back_recv, w_sem,
):
    me = lax.axis_index("head")
    width = part_ref.shape[1]
    own = state_ref.shape[0]
    model = state_ref.shape[1]
    w_copy = pltpu.make_async_copy(w_any, w_ref, w_sem)
    w_copy.start()
    greet("head", number, me)
    my_cols = pl.ds(pl.multiple_of(me * width, width), width)
    my_rows = pl.ds(pl.multiple_of(me * own, own), own)
    copies = []
    for step in range(1, number):
        peer = lax.rem(me + step, number)
        copy = pltpu.make_async_remote_copy(
            src_ref=part_ref.at[pl.ds(pl.multiple_of(peer * own, own), own)],
            dst_ref=joined.at[:, my_cols],
            send_sem=send_sem.at[step],
            recv_sem=recv_sem.at[step],
            device_id={"head": peer},
            device_id_type=MESH,
        )
        copy.start()
        copies.append(copy)
    joined[:, my_cols] = part_ref[my_rows, :]
    w_copy.wait()
    for copy in copies:
        copy.wait()

    tile = min(256, model)

    def project(piece, carry):
        squares, products = carry
        cols = pl.ds(pl.multiple_of(piece * tile, tile), tile)
        layer = state_ref[:, cols].astype(jnp.float32) + jnp.dot(
            joined[...], w_ref[:, cols], preferred_element_type=jnp.float32
        )
        readout_out[:, cols] = layer
        squares = squares + jnp.sum(layer * layer, axis=1, keepdims=True)
        products = products + jnp.sum(
            layer * probe_ref[:, cols].astype(jnp.float32), axis=1, keepdims=True
        )
        return squares, products

    zero = jnp.zeros((own, 1), jnp.float32)
    squares, products = lax.fori_loop(0, model // tile, project, (zero, zero))
    scale = lax.rsqrt(squares / model + EPSILON)
    bend = scale**3 * (products / model)

    def finish(piece, _):
        cols = pl.ds(pl.multiple_of(piece * tile, tile), tile)
        readout = scale * probe_ref[:, cols].astype(jnp.float32) - readout_out[:, cols] * bend
        readout_out[:, cols] = readout
        half[:, cols] = readout.astype(jnp.bfloat16)
        return 0

    lax.fori_loop(0, model // tile, finish, 0)
    copies = []
    for step in range(1, number):
        peer = lax.rem(me + step, number)
        sending[step] = dot32(
            half[...], w_ref[pl.ds(pl.multiple_of(peer * width, width), width), :], NT
        ).astype(jnp.bfloat16)
        copy = pltpu.make_async_remote_copy(
            src_ref=sending.at[step],
            dst_ref=landing.at[my_rows],
            send_sem=back_send.at[step],
            recv_sem=back_recv.at[step],
            device_id={"head": peer},
            device_id_type=MESH,
        )
        copy.start()
        copies.append(copy)
    landing[my_rows, :] = dot32(half[...], w_ref[my_cols, :], NT).astype(jnp.bfloat16)
    for copy in copies:
        copy.wait()
    grad_out[...] = landing[...]


def middle(number, part, w_full, state_own, probe_own):
    rows, width = part.shape
    own, model = state_own.shape
    return pl.pallas_call(
        functools.partial(middle_kernel, number),
        out_shape=(
            jax.ShapeDtypeStruct((rows, width), jnp.bfloat16),
            jax.ShapeDtypeStruct((own, model), jnp.float32),
        ),
        in_specs=[VMEM, ANY, VMEM, VMEM],
        out_specs=(VMEM, VMEM),
        scratch_shapes=[
            pltpu.VMEM(w_full.shape, jnp.bfloat16),
            pltpu.VMEM((own, number * width), jnp.bfloat16),
            pltpu.VMEM((own, model), jnp.bfloat16),
            pltpu.VMEM((number, own, width), jnp.bfloat16),
            pltpu.VMEM((rows, width), jnp.bfloat16),
            pltpu.SemaphoreType.DMA((number,)),
            pltpu.SemaphoreType.DMA((number,)),
            pltpu.SemaphoreType.DMA((number,)),
            pltpu.SemaphoreType.DMA((number,)),
            pltpu.SemaphoreType.DMA,
        ],
        compiler_params=pltpu.CompilerParams(
            collective_id=1, has_side_effects=True, vmem_limit_bytes=60 * 2**20
        ),
    )(part, w_full, state_own, probe_own)


def tail_kernel(
    ctx_count, number, pair_any, query_ref, w_ref, sum_out, own_pair, arriving, gathered, terms,
    from_partner, reduced, landing, ctx_send, ctx_recv, p_send, p_recv, z_send, z_recv, own_sem,
):
    ctx, me = lax.axis_index("ctx"), lax.axis_index("head")
    groups = number // 2
    group, core = me // 2, lax.rem(me, 2)
    partner = group * 2 + 1 - core
    rows, width = query_ref.shape
    own, model = sum_out.shape
    chunk = 2 * own
    own_copy = pltpu.make_async_copy(
        pair_any.at[pl.ds(pl.multiple_of(ctx * rows, rows), rows)], own_pair, own_sem
    )
    own_copy.start()
    barrier = pltpu.get_barrier_semaphore()
    peers = [{"ctx": lax.rem(ctx + step, ctx_count)} for step in range(1, ctx_count)]
    peers.append({"head": partner})
    for step in range(1, groups):
        peers.append({"head": lax.rem(group + step, groups) * 2 + core})
    for peer in peers:
        pl.semaphore_signal(barrier, inc=1, device_id=peer, device_id_type=MESH)
    pl.semaphore_wait(barrier, len(peers))

    def chunk_start(order):
        dest = lax.rem(group + order + 1, groups)
        return dest, pl.multiple_of(dest * chunk, chunk)

    def ctx_copy(order, step):
        target = lax.rem(ctx - step + ctx_count, ctx_count)
        _, first = chunk_start(order)
        return pltpu.make_async_remote_copy(
            src_ref=pair_any.at[pl.ds(pl.multiple_of(target * rows + first, chunk), chunk)],
            dst_ref=arriving.at[order, step - 1],
            send_sem=ctx_send.at[order, step],
            recv_sem=ctx_recv.at[order, step],
            device_id={"ctx": target},
            device_id_type=MESH,
        )

    for order in range(groups):
        for step in range(1, ctx_count):

            @pl.when(step <= ctx)
            def _():
                ctx_copy(order, step).start()

    own_copy.wait()
    tile = min(512, model)
    mine = pl.ds(pl.multiple_of(core * own, own), own)
    theirs = pl.ds(pl.multiple_of((1 - core) * own, own), own)
    waiting = []
    for order in range(groups):
        dest, first = chunk_start(order)
        at = pl.ds(first, chunk)
        gathered[...] = own_pair[at, :].astype(jnp.float32)
        for step in range(1, ctx_count):

            @pl.when(ctx + step < ctx_count)
            def _():
                ctx_copy(order, step).wait_recv()
                gathered[...] += arriving[order, step - 1].astype(jnp.float32)

        def multiply(piece, _):
            cols = pl.ds(pl.multiple_of(piece * tile, tile), tile)
            term = dot32(query_ref[at, :], w_ref[0, cols, :], NT)
            term += dot32(gathered[:, :width].astype(jnp.bfloat16), w_ref[1, cols, :], NT)
            term += dot32(gathered[:, width:].astype(jnp.bfloat16), w_ref[2, cols, :], NT)
            terms[order, :, cols] = term.astype(jnp.bfloat16)
            return 0

        lax.fori_loop(0, model // tile, multiply, 0)
        copy = pltpu.make_async_remote_copy(
            src_ref=terms.at[order, theirs],
            dst_ref=from_partner.at[order],
            send_sem=p_send.at[order],
            recv_sem=p_recv.at[order],
            device_id={"head": partner},
            device_id_type=MESH,
        )
        copy.start()
        copy.wait()
        both = terms[order, mine, :].astype(jnp.float32) + from_partner[order].astype(jnp.float32)
        if order < groups - 1:
            reduced[order] = both.astype(jnp.bfloat16)
            copy = pltpu.make_async_remote_copy(
                src_ref=reduced.at[order],
                dst_ref=landing.at[order],
                send_sem=z_send.at[order],
                recv_sem=z_recv.at[order],
                device_id={"head": dest * 2 + core},
                device_id_type=MESH,
            )
            copy.start()
            waiting.append(copy)
        else:
            sum_out[...] = both
    for order, copy in enumerate(waiting):
        copy.wait()
        sum_out[...] += landing[order].astype(jnp.float32)
    for order in range(groups):
        for step in range(1, ctx_count):

            @pl.when(step <= ctx)
            def _():
                ctx_copy(order, step).wait_send()


def tail(ctx_count, number, pair, query_grad, w_qkv):
    rows, width = query_grad.shape
    model = w_qkv.shape[1]
    own, groups = rows // number, number // 2
    half, full = jnp.bfloat16, jnp.float32
    dma = pltpu.SemaphoreType.DMA
    return pl.pallas_call(
        functools.partial(tail_kernel, ctx_count, number),
        out_shape=jax.ShapeDtypeStruct((own, model), full),
        in_specs=[ANY, VMEM, VMEM],
        out_specs=VMEM,
        scratch_shapes=[
            pltpu.VMEM((rows, 2 * width), half),
            pltpu.VMEM((groups, ctx_count - 1, 2 * own, 2 * width), half),
            pltpu.VMEM((2 * own, 2 * width), full),
            pltpu.VMEM((groups, 2 * own, model), half),
            pltpu.VMEM((groups, own, model), half),
            pltpu.VMEM((groups, own, model), half),
            pltpu.VMEM((groups, own, model), half),
            dma((groups, ctx_count)),
            dma((groups, ctx_count)),
            dma((groups,)),
            dma((groups,)),
            dma((groups,)),
            dma((groups,)),
            dma,
        ],
        compiler_params=pltpu.CompilerParams(
            collective_id=2, has_side_effects=True, vmem_limit_bytes=60 * 2**20
        ),
    )(pair, query_grad, w_qkv)


def body(state, norm_gain, w_qkv, w_out, probe, noise, segment_ids):
    local_rows, model_width = state.shape
    width = w_qkv.shape[2]
    local_heads = width // HEAD_DIM
    head_count = lax.axis_size("head")
    ctx_count = lax.axis_size("ctx")
    ctx_index = lax.axis_index("ctx")
    own_rows = local_rows // head_count
    row_start = lax.axis_index("head") * own_rows
    w_full = lax.all_gather(w_out, "head", axis=0, tiled=True)
    state_f = state.astype(jnp.float32)
    gain_full = norm_gain.astype(jnp.float32)
    inverse = row_scale(state_f)
    normed = (state_f * inverse * gain_full).astype(jnp.bfloat16)

    def project(index):
        return jnp.dot(normed, w_qkv[index], preferred_element_type=jnp.float32).astype(
            jnp.bfloat16
        )

    key_rows, value_rows = project(1), project(2)
    keys, values, segs, query_rows = gather_keys(
        ctx_count, key_rows, value_rows, segment_ids, normed, w_qkv[0]
    )
    total_rows = keys.shape[0]
    pos = ctx_index * local_rows + jnp.arange(local_rows, dtype=jnp.int32)
    start = jnp.sum((segs[None, :] < segment_ids[:, None]).astype(jnp.int32), axis=1)
    fq, fk = (min(local_rows, size) for size in FORWARD_BLOCKS)
    gq, gk = (min(local_rows, size) for size in BACKWARD_BLOCKS)
    smem = pl.BlockSpec(memory_space=pltpu.SMEM)
    params = pltpu.CompilerParams(vmem_limit_bytes=60 * 2**20)
    outputs, logs = pl.pallas_call(
        functools.partial(forward_kernel, local_heads, fq, fk),
        out_shape=(
            jax.ShapeDtypeStruct((local_rows, width), jnp.bfloat16),
            jax.ShapeDtypeStruct((local_rows // fq, local_heads, fq), jnp.float32),
        ),
        in_specs=[smem] + [VMEM] * 5,
        out_specs=(VMEM, VMEM),
        compiler_params=params,
        cost_estimate=pl.CostEstimate(
            flops=4 * local_rows * total_rows * width, bytes_accessed=0, transcendentals=0
        ),
    )(
        make_table(start, pos, fq, fk),
        query_rows,
        keys,
        values,
        start.reshape(-1, 1, fq),
        pos.reshape(-1, 1, fq),
    )
    state_half = lax.dynamic_slice_in_dim(state, row_start, own_rows, 0)
    probe_own = lax.dynamic_slice_in_dim(probe, row_start, own_rows, 0)
    state_own = state_half.astype(jnp.float32)
    inverse_own = row_scale(state_own)
    grads_out, readout_own = middle(head_count, outputs, w_full, state_half, probe_own)
    query_grad, pair = pl.pallas_call(
        functools.partial(backward_kernel, local_heads, gq, gk),
        out_shape=(
            jax.ShapeDtypeStruct((local_rows, width), jnp.bfloat16),
            jax.ShapeDtypeStruct((total_rows, 2 * width), jnp.bfloat16),
        ),
        in_specs=[smem] + [VMEM] * 8,
        out_specs=(VMEM, VMEM),
        scratch_shapes=[pltpu.VMEM((total_rows, 2 * width), jnp.float32)],
        compiler_params=params,
        cost_estimate=pl.CostEstimate(
            flops=10 * local_rows * total_rows * width, bytes_accessed=0, transcendentals=0
        ),
    )(
        make_table(start, pos, gq, gk),
        query_rows,
        keys,
        values,
        grads_out,
        outputs,
        logs.reshape(local_rows // fq, local_heads, fq),
        start.reshape(-1, 1, gq),
        pos.reshape(-1, 1, gq),
    )
    normed_grad = tail(ctx_count, head_count, pair, query_grad, w_qkv)
    gain_grad = normed_grad * gain_full
    gradient = (
        readout_own
        + inverse_own * gain_grad
        - state_own * inverse_own**3 * jnp.mean(gain_grad * state_own, axis=-1, keepdims=True)
    )
    return state_own - STEP_SIZE * gradient + jnp.sqrt(2.0 * STEP_SIZE) * noise.astype(jnp.float32)


def remote(source, target, send_sem, recv_sem, ctx, head):
    return pltpu.make_async_remote_copy(
        src_ref=source,
        dst_ref=target,
        send_sem=send_sem,
        recv_sem=recv_sem,
        device_id={"ctx": ctx, "head": head},
        device_id_type=MESH,
    )


def place():
    ctx, me = lax.axis_index("ctx"), lax.axis_index("head")
    return ctx, me, me // 2, lax.rem(me, 2)


def announce(peers):
    barrier = pltpu.get_barrier_semaphore()
    for ctx, head in peers:
        pl.semaphore_signal(
            barrier, inc=1, device_id={"ctx": ctx, "head": head}, device_id_type=MESH
        )


def await_all(peers):
    pl.semaphore_wait(pltpu.get_barrier_semaphore(), len(peers))


def far_first(groups, group, step):
    result = 0
    for index in range(groups):
        order = sorted(range(groups), key=lambda other: (-abs(other - index), -other))
        result = jnp.where(group == index, order[step], result)
    return result


def by_arrival(groups, group, step):
    result = 0
    for index in range(groups):
        last = sorted(range(groups), key=lambda other: (-abs(other - index), -other))[0]
        order = sorted(
            (other for other in range(groups) if other != last),
            key=lambda other: (other in (0, groups - 1), abs(other - index)),
        )
        result = jnp.where(group == index, (order + [last])[step], result)
    return result


def step_kernel(
    ctx_count, head_count, state_any, w_any, gain_ref, seg_ref, w_out_any, probe_any, noise_any,
    new_out, state_v, query_buf, kv_buf, w_ref, joined, half, sending, state_own, probe_own,
    noise_own, query_out, kv_out, part_out, readout_out, segs_out, log_v, grad_v, w_both, pair_acc,
    query_acc, deltas, query_fin, pair_buf, beside_in, away_buf, terms_in, partial, passing, sum_v,
    load_sem, w_sem, q_send, q_recv, kv_send, kv_recv, pass_send, seg_send, seg_recv, line_send,
    line_recv, plane_send, plane_recv, beside_send, beside_recv, shard_send, shard_recv, shard_sem,
    out_send, out_recv, back_send, back_recv, row_sem, pair_send, pair_recv, b_send, b_recv, a_send,
    a_recv, z_send, z_recv,
):
    ctx, me, group, core = place()
    rows, model = state_any.shape
    own, groups = rows // head_count, head_count // 2
    slots = w_any.shape[2] // HEAD_DIM
    chunk = 2 * own
    partner = group * 2 + 1 - core

    def at(piece):
        return pl.ds(pl.multiple_of(piece * chunk, chunk), chunk)

    def own_at(piece):
        return pl.ds(pl.multiple_of(piece * own, own), own)

    def load_state(piece):
        return pltpu.make_async_copy(
            state_any.at[at(piece)], state_v.at[at(piece)], load_sem.at[piece]
        )

    load_state(0).start()
    w_loads = [
        pltpu.make_async_copy(w_any.at[t], w_both.at[core, t], w_sem.at[t]) for t in range(3)
    ]
    for copy in w_loads:
        copy.start()
    for piece in range(1, groups):
        load_state(piece).start()
    my_rows = own_at(me)
    shard = w_out_any.shape[0]
    part, quarter = shard // 2, shard // ctx_count
    later_loads = [
        pltpu.make_async_copy(state_any.at[my_rows], state_own, row_sem.at[0]),
        pltpu.make_async_copy(probe_any.at[my_rows], probe_own, row_sem.at[1]),
        pltpu.make_async_copy(noise_any, noise_own, row_sem.at[2]),
        pltpu.make_async_copy(
            w_out_any, w_ref.at[pl.ds(pl.multiple_of(me * shard, shard), shard)], shard_sem
        ),
    ]
    for copy in later_loads:
        copy.start()
    peers = [(lax.rem(ctx + step, ctx_count), partner) for step in range(ctx_count)]
    for far in range(groups):
        for step in range(ctx_count):
            if far or step:
                peers.append(
                    (lax.rem(ctx + step, ctx_count), lax.rem(group + far, groups) * 2 + core)
                )
    announce(peers)

    low, high = lax.rem(ctx, 2), ctx // 2
    which = lax.rem(low + high, 2)
    across, along = high * 2 + 1 - low, (1 - high) * 2 + low

    def shard_rows(origin, first, size):
        return pl.ds(pl.multiple_of((origin * 2 + core) * shard + first, size), size)

    def line_copy(way, origin, axis, mine):
        first = which * part + axis * quarter
        here = shard_rows(origin, first, quarter)
        source = (
            w_out_any.at[pl.ds(pl.multiple_of(first, quarter), quarter)] if mine else w_ref.at[here]
        )
        other = group + 1 if way == 0 else group - 1
        return remote(
            source, w_ref.at[here], line_send.at[way, axis, origin], line_recv.at[axis, origin],
            ctx, other * 2 + core,
        )

    def plane_copy(axis, origin, kept):
        here = shard_rows(origin, kept * part + axis * quarter, quarter)
        return remote(
            w_ref.at[here], w_ref.at[here], plane_send.at[axis, origin],
            plane_recv.at[axis, origin], along if axis else across, me,
        )

    def beside_copy(kind, origin):
        kept = which if kind < 2 else 1 - which
        here = shard_rows(origin, kept * part + (kind % 2) * quarter, quarter)
        return remote(
            w_ref.at[here], w_ref.at[here], beside_send.at[kind, origin],
            beside_recv.at[kind, origin], ctx, partner,
        )

    def shard_copy():
        return remote(
            w_out_any, w_ref.at[pl.ds(pl.multiple_of(me * shard, shard), shard)], shard_send,
            shard_recv, ctx, partner,
        )

    has_up, has_down = group < groups - 1, group > 0

    def each_origin(distance, work):
        for way in range(2):
            origin = group - distance if way == 0 else group + distance

            @pl.when(origin >= 0 if way == 0 else origin < groups)
            def _():
                work(way, origin)

    def line_arrived(distance, axis):
        def work(way, origin):
            line_copy(way, origin, axis, False).wait_recv()

            @pl.when(has_up if way == 0 else has_down)
            def _():
                line_copy(way, origin, axis, False).start()

            plane_copy(axis, origin, which).start()
            beside_copy(axis, origin).start()

        each_origin(distance, work)

    def plane_arrived(distance, axis):
        def work(way, origin):
            plane_copy(axis, origin, 1 - which).wait_recv()
            beside_copy(2 + axis, origin).start()

        each_origin(distance, work)

    def weights_sent(distance):
        def work(way, origin):
            for axis in range(2):

                @pl.when(has_up if way == 0 else has_down)
                def _():
                    line_copy(way, origin, axis, False).wait_send()

                plane_copy(axis, origin, which).wait_send()
            for kind in range(4):
                beside_copy(kind, origin).wait_send()

        each_origin(distance, work)

    def own_lines(work):
        for axis in range(2):

            @pl.when(has_up)
            def _():
                work(line_copy(0, group, axis, True))

            @pl.when(has_down)
            def _():
                work(line_copy(1, group, axis, True))

    for copy in w_loads:
        copy.wait()
    gain = gain_ref[...].astype(jnp.float32).reshape(1, model)

    def away(slot, kind, piece, dest):
        head = group * 2 + kind
        return (
            remote(
                query_buf.at[slot, piece, kind], query_out.at[piece, ctx],
                q_send.at[slot, kind, piece], q_recv.at[ctx, piece], dest, head,
            ),
            remote(
                kv_buf.at[slot, kind, piece], kv_out.at[kind, piece, ctx],
                kv_send.at[slot, kind, piece], kv_recv.at[kind, ctx, piece], dest, head,
            ),
        )

    def beside(slot, piece):
        result = [
            remote(
                query_buf.at[slot, piece, 1 - core], query_out.at[piece, ctx],
                q_send.at[slot, 1 - core, piece], q_recv.at[ctx, piece], ctx, partner,
            )
        ]
        for kind in range(2):
            result.append(
                remote(
                    kv_buf.at[slot, kind, piece], kv_out.at[kind, piece, ctx],
                    kv_send.at[slot, kind, piece], kv_recv.at[kind, ctx, piece], ctx, partner,
                )
            )
        return result

    def project(piece):
        load_state(piece).wait()
        block = state_v[at(piece), :].astype(jnp.float32)
        normed = (block * row_scale(block) * gain).astype(jnp.bfloat16)
        for t in range(3):
            result = jnp.dot(normed, w_both[core, t], preferred_element_type=jnp.float32).astype(
                jnp.bfloat16
            )
            for slot in range(slots):
                cut = result[:, slot * HEAD_DIM : (slot + 1) * HEAD_DIM]
                if t == 0:
                    query_buf[slot, piece, 0] = cut[:own]
                    query_buf[slot, piece, 1] = cut[own:]
                else:
                    kv_buf[slot, t - 1, piece] = cut

    def send_heads(piece):
        for slot in range(slots):
            dest = core * slots + slot

            @pl.when(dest != ctx)
            def _():
                for kind in range(2):
                    for copy in away(slot, kind, piece, dest):
                        copy.start()

            @pl.when(dest == ctx)
            def _():
                query_out[piece, ctx] = query_buf[slot, piece, core]
                for kind in range(2):
                    kv_out[kind, piece, ctx] = kv_buf[slot, kind, piece]
                for copy in beside(slot, piece):
                    copy.start()

    project(0)
    await_all(peers)
    own_lines(lambda copy: copy.start())
    send_heads(0)
    shard_copy().start()
    segs = []
    for step in range(1, ctx_count):
        copy = remote(
            seg_ref, segs_out.at[ctx], seg_send.at[step], seg_recv.at[step],
            lax.rem(ctx + step, ctx_count), me,
        )
        copy.start()
        segs.append(copy)
    segs_out[ctx] = seg_ref[...]

    def project_and_send(piece, _):
        project(piece)
        send_heads(piece)
        return 0

    lax.fori_loop(1, groups, project_and_send, 0)

    def hand_over(piece, step):
        source = lax.rem(ctx + step, ctx_count)
        return remote(
            kv_out.at[core, piece, source], kv_out.at[core, piece, source],
            pass_send.at[step, piece], kv_recv.at[core, source, piece], ctx, partner,
        )

    for piece in range(groups):
        for step in range(1, ctx_count):
            copy = hand_over(piece, step)
            copy.wait_recv()
            copy.start()
        if piece == 0:
            line_arrived(1, 0)
        if piece == min(2, groups - 1):
            line_arrived(1, 1)
    line_arrived(2, 0)

    def got_query(source, piece):
        remote(
            query_out.at[piece, source], query_out.at[piece, source],
            q_send.at[0, 0, piece], q_recv.at[source, piece], ctx, partner,
        ).wait_recv()

    def got_kv(kind, source, piece):
        remote(
            kv_out.at[kind, piece, source], kv_out.at[kind, piece, source],
            kv_send.at[0, 0, piece], kv_recv.at[kind, source, piece], ctx, partner,
        ).wait_recv()

    def gather(piece, _):
        for step in range(1, ctx_count):
            source = lax.rem(ctx + step, ctx_count)
            got_query(source, piece)
            got_kv(1 - core, source, piece)
            hand_over(piece, step).wait_send()

        @pl.when(ctx // slots != core)
        def _():
            got_query(ctx, piece)
            for kind in range(2):
                got_kv(kind, ctx, piece)

        return 0

    lax.fori_loop(0, groups, gather, 0)
    for copy in segs:
        copy.wait()
    pair_copy = remote(w_any, w_both.at[core], pair_send, pair_recv, ctx, partner)
    pair_copy.start()

    def cols_of(group_at, ctx_at):
        head = group_at * ctx_count + ctx_at
        return pl.ds(pl.multiple_of(head * HEAD_DIM, HEAD_DIM), HEAD_DIM)

    factor = HEAD_DIM ** (-0.5) * LOG2E
    sub = groups * own
    seg_all = segs_out[...]

    def below(value):
        count = jnp.where(seg_all < value, 1.0, 0.0)
        for axis in (0, 1, 2):
            count = jnp.sum(count, axis=axis, keepdims=True)
        return count[0]

    first_bound, second_bound = below(1), below(2)
    lane = lax.broadcasted_iota(jnp.int32, (1, sub), 1)
    inside = (lane // own) * (2 * own) + core * own + lane % own
    key_row = lax.broadcasted_iota(jnp.int32, (rows, sub), 0)

    def out_copy(tile, order, other):
        return remote(
            part_out.at[other, tile], joined.at[:, cols_of(group, ctx)],
            out_send.at[tile, order], out_recv.at[group, ctx], tile, other * 2 + core,
        )

    def one_tile(tile, _):
        query = query_out[:, tile].reshape(sub, HEAD_DIM)
        pos = (tile * rows + inside).astype(jnp.float32)
        start = jnp.where(
            pos >= second_bound, second_bound, jnp.where(pos >= first_bound, first_bound, 0.0)
        ).astype(jnp.int32)

        def step(diagonal, piece, carry):
            top, total, acc = carry
            scores = dot32(kv_out[0, :, piece].reshape(rows, HEAD_DIM), query, NT)
            allowed = key_row >= start - piece * rows
            if diagonal:
                allowed = allowed & (key_row <= inside)
            scores = jnp.where(allowed, scores, NEGATIVE)
            new_top = jnp.maximum(top, jnp.max(scores, axis=0, keepdims=True) * factor)
            weights = jnp.exp2(scores * factor - new_top)
            scale = jnp.exp2(top - new_top)
            total = total * scale + jnp.sum(weights, axis=0, keepdims=True)
            acc = acc * scale + dot32(
                kv_out[1, :, piece].reshape(rows, HEAD_DIM), weights.astype(jnp.bfloat16), TN
            )
            return new_top, total, acc

        carry = (
            jnp.full((1, sub), NEGATIVE, jnp.float32),
            jnp.zeros((1, sub), jnp.float32),
            jnp.zeros((HEAD_DIM, sub), jnp.float32),
        )
        carry = lax.fori_loop(0, tile, functools.partial(step, False), carry)
        top, total, acc = step(True, tile, carry)
        result = (acc / total).T.astype(jnp.bfloat16)
        log_row = top + jnp.log2(total)
        for index in range(groups):
            part_out[index, tile] = result[index * own : (index + 1) * own]
            log_v[index, :, own_at(tile)] = log_row[:, index * own : (index + 1) * own]
        for order in range(groups):
            other = far_first(groups, group, order)
            if order == groups - 1:

                @pl.when(tile != ctx)
                def _():
                    out_copy(tile, order, other).start()

                @pl.when(tile == ctx)
                def _():
                    joined[:, cols_of(group, ctx)] = part_out[group, tile]

            else:
                out_copy(tile, order, other).start()

        @pl.when(tile == 1)
        def _():
            line_arrived(2, 1)

        return 0

    lax.fori_loop(0, ctx_count, one_tile, 0)
    for copy in later_loads:
        copy.wait()
    sources = []
    for far in range(groups):
        for step in range(ctx_count):
            if far or step:
                sources.append((lax.rem(group + far, groups), lax.rem(ctx + step, ctx_count)))
    tile = min(512, model)
    wide = ctx_count * HEAD_DIM
    zero = jnp.zeros((own, 1), jnp.float32)
    for axis in range(2):
        plane_arrived(1, axis)
    for distance in range(3, groups):
        line_arrived(distance, 0)
    for axis in range(2):
        plane_arrived(2, axis)
    for distance in range(3, groups):
        line_arrived(distance, 1)
    shard_copy().wait_recv()

    def heads_arrived(order):
        other = far_first(groups, group, order)
        if order < groups - 1:
            for kind in range(4):
                beside_copy(kind, other).wait_recv()
        for step in range(ctx_count):
            if order < groups - 1 or step:
                peer = lax.rem(ctx + step, ctx_count)
                remote(
                    part_out.at[0, 0], joined.at[:, cols_of(other, peer)],
                    out_send.at[0, 0], out_recv.at[other, peer], peer, other * 2 + core,
                ).wait_recv()

    for order in range(groups - 1, 0, -1):
        heads_arrived(order)
    farthest = far_first(groups, group, 0)
    near = pl.ds(pl.multiple_of(jnp.where(farthest == 0, wide, 0), wide), model - wide)
    far = pl.ds(pl.multiple_of(farthest * wide, wide), wide)

    def near_layer(piece, _):
        cols = pl.ds(pl.multiple_of(piece * tile, tile), tile)
        readout_out[:, cols] = state_own[:, cols].astype(jnp.float32) + jnp.dot(
            joined[:, near], w_ref[near, cols], preferred_element_type=jnp.float32
        )
        return 0

    lax.fori_loop(0, model // tile, near_layer, 0)
    for distance in range(3, groups):
        for axis in range(2):
            plane_arrived(distance, axis)
    heads_arrived(0)

    def layer(piece, carry):
        squares, products = carry
        cols = pl.ds(pl.multiple_of(piece * tile, tile), tile)
        result = readout_out[:, cols] + jnp.dot(
            joined[:, far], w_ref[far, cols], preferred_element_type=jnp.float32
        )
        readout_out[:, cols] = result
        squares = squares + jnp.sum(result * result, axis=1, keepdims=True)
        products = products + jnp.sum(
            result * probe_own[:, cols].astype(jnp.float32), axis=1, keepdims=True
        )
        return squares, products

    squares, products = lax.fori_loop(0, model // tile, layer, (zero, zero))
    scale = lax.rsqrt(squares / model + EPSILON)
    bend = scale**3 * (products / model)

    def finish(piece, _):
        cols = pl.ds(pl.multiple_of(piece * tile, tile), tile)
        readout = scale * probe_own[:, cols].astype(jnp.float32) - readout_out[:, cols] * bend
        readout_out[:, cols] = readout
        half[:, cols] = readout.astype(jnp.bfloat16)
        return 0

    lax.fori_loop(0, model // tile, finish, 0)
    copies = []
    for order in range(groups):
        other = far_first(groups, group, order)
        result = dot32(
            half[...], w_ref[pl.ds(pl.multiple_of(other * wide, wide), wide), :], NT
        ).astype(jnp.bfloat16)
        for index in range(ctx_count):
            sending[order, index] = result[:, index * HEAD_DIM : (index + 1) * HEAD_DIM]
        for step in range(ctx_count):
            peer = lax.rem(ctx + step, ctx_count)
            if order == groups - 1 and step == 0:
                continue
            copy = remote(
                sending.at[order, peer], grad_v.at[group, ctx], back_send.at[order, step],
                back_recv.at[ctx, group], peer, other * 2 + core,
            )
            copy.start()
            copies.append(copy)
    grad_v[group, ctx] = sending[groups - 1, ctx]

    def clear(index, _):
        pair_acc[index] = jnp.zeros(pair_acc.shape[1:], jnp.float32)
        query_acc[index] = jnp.zeros(query_acc.shape[1:], jnp.float32)
        return 0

    lax.fori_loop(0, groups, clear, 0)

    def sent(piece, _):
        for slot in range(slots):
            dest = core * slots + slot

            @pl.when(dest != ctx)
            def _():
                for kind in range(2):
                    for copy in away(slot, kind, piece, dest):
                        copy.wait_send()

            @pl.when(dest == ctx)
            def _():
                for copy in beside(slot, piece):
                    copy.wait_send()

        return 0

    lax.fori_loop(0, groups, sent, 0)

    own_lines(lambda copy: copy.wait_send())
    shard_copy().wait_send()
    for distance in range(1, groups):
        weights_sent(distance)

    def parts_sent(tile, _):
        for order in range(groups):
            other = far_first(groups, group, order)
            if order == groups - 1:

                @pl.when(tile != ctx)
                def _():
                    out_copy(tile, order, other).wait_send()

            else:
                out_copy(tile, order, other).wait_send()
        return 0

    lax.fori_loop(0, ctx_count, parts_sent, 0)
    halves = 2
    span = ctx_count * own // halves
    dests = [far_first(groups, group, order) for order in range(groups)]

    def dest_of(order):
        result = dests[0]
        for index in range(1, groups):
            result = jnp.where(order == index, dests[index], result)
        return result

    score_scale = HEAD_DIM ** (-0.5)
    def half_of(ref, index, half):
        count = ctx_count // halves
        return ref[index, half * count : (half + 1) * count].reshape(span, HEAD_DIM)

    def find_deltas(index):
        for half in range(halves):
            product = half_of(grad_v, index, half).astype(jnp.float32) * half_of(
                part_out, index, half
            ).astype(jnp.float32)
            deltas[index, :, half * span : (half + 1) * span] = jnp.sum(
                product.T, axis=0, keepdims=True
            )

    def gradients_arrived(other):
        for peer in range(ctx_count):

            @pl.when(jnp.logical_or(other != group, ctx != peer))
            def _():
                remote(
                    sending.at[0, 0], grad_v.at[other, peer], back_send.at[0, 0],
                    back_recv.at[peer, other], ctx, partner,
                ).wait_recv()

        find_deltas(other)

    spot_lane = lax.broadcasted_iota(jnp.int32, (1, span), 1)
    key_line = lax.broadcasted_iota(jnp.int32, (2 * own, own), 0)

    def pair(query_at, key_at):
        for half in range(halves):
            blocks = (half + 1) * ctx_count // halves
            count = blocks * 2 * own
            lanes = slice(half * span, (half + 1) * span)
            key_block = kv_out[0, key_at, :blocks].reshape(count, HEAD_DIM)
            value_block = kv_out[1, key_at, :blocks].reshape(count, HEAD_DIM)
            query_block = half_of(query_out, query_at, half)
            grad_block = half_of(grad_v, query_at, half)
            first_ctx = half * (ctx_count // halves)
            pos = (first_ctx + spot_lane // own) * rows + spot_lane % own
            pos = pos + (query_at * 2 + core) * own
            pos_f = pos.astype(jnp.float32)
            start = jnp.where(
                pos_f >= second_bound,
                second_bound,
                jnp.where(pos_f >= first_bound, first_bound, 0.0),
            ).astype(jnp.int32)
            scores = dot32(key_block, query_block, NT)
            raw = jnp.exp2(scores * factor - log_v[query_at, :, lanes])
            strips = []
            for source in range(blocks):
                offset = source * rows + key_at * 2 * own
                row_cut = slice(source * 2 * own, (source + 1) * 2 * own)
                cells = []
                for index in range(ctx_count // halves):
                    lane_cut = slice(index * own, (index + 1) * own)
                    if source > first_ctx + index:
                        cells.append(jnp.zeros((2 * own, own), jnp.float32))
                        continue
                    allowed = key_line >= start[:, lane_cut] - offset
                    if source == first_ctx + index:
                        allowed = allowed & (key_line <= pos[:, lane_cut] - offset)
                    cells.append(jnp.where(allowed, raw[row_cut, lane_cut], 0.0))
                strips.append(jnp.concatenate(cells, axis=1))
            probabilities = jnp.concatenate(strips, axis=0)
            dprobs = dot32(value_block, grad_block, NT)
            dscores = (probabilities * (dprobs - deltas[query_at, :, lanes])).astype(jnp.bfloat16)
            pair_acc[key_at, :count, HEAD_DIM:] += jnp.dot(
                probabilities.astype(jnp.bfloat16), grad_block, preferred_element_type=jnp.float32
            )
            pair_acc[key_at, :count, :HEAD_DIM] += jnp.dot(
                dscores, query_block, preferred_element_type=jnp.float32
            )
            query_acc[query_at, :, lanes] += dot32(key_block, dscores, TN)

    def core_copy(order):
        return remote(
            pair_buf.at[order], beside_in.at[order], b_send.at[order], b_recv.at[order], ctx, partner
        )

    def pair_rows(dest, source, kind):
        first = pl.multiple_of((source * 2 + kind) * own, own)
        keys = pair_acc[dest, pl.ds(first, own), :HEAD_DIM] * score_scale
        values = pair_acc[dest, pl.ds(first, own), HEAD_DIM:]
        return keys, values

    def settle(order):
        dest = dest_of(order)
        for source in range(ctx_count):
            keys, values = pair_rows(dest, source, 1 - core)
            pair_buf[order, source, :, :HEAD_DIM] = keys.astype(jnp.bfloat16)
            pair_buf[order, source, :, HEAD_DIM:] = values.astype(jnp.bfloat16)
        for half in range(halves):
            query_fin[order, half * span : (half + 1) * span, :] = (
                query_acc[dest, :, half * span : (half + 1) * span].T * score_scale
            ).astype(jnp.bfloat16)
        core_copy(order).start()

    def stripe(source):
        slot = lax.rem(source, slots)
        return pl.ds(pl.multiple_of(slot * HEAD_DIM, HEAD_DIM), HEAD_DIM)

    def exchange(order, step):
        peer = lax.rem(ctx + step, ctx_count)
        return remote(
            away_buf.at[order, step],
            terms_in.at[dest_of(order), ctx // slots, :, :, stripe(ctx)],
            a_send.at[order, step], a_recv.at[dest_of(order), ctx], peer, me,
        )

    def arrived(dest, step):
        source = lax.rem(ctx + step, ctx_count)
        remote(
            away_buf.at[0, 0], terms_in.at[dest, source // slots, :, :, stripe(source)],
            a_send.at[0, 0], a_recv.at[dest, source], source, me,
        ).wait_recv()

    def spread(order):
        dest = dest_of(order)
        core_copy(order).wait_recv()
        for step in range(1, ctx_count + 1):
            peer = lax.rem(ctx + step, ctx_count)
            keys, values = pair_rows(dest, peer, core)
            keys = (keys + beside_in[order, peer, :, :HEAD_DIM].astype(jnp.float32)).astype(
                jnp.bfloat16
            )
            values = (values + beside_in[order, peer, :, HEAD_DIM:].astype(jnp.float32)).astype(
                jnp.bfloat16
            )
            queries = query_fin[order, pl.ds(pl.multiple_of(peer * own, own), own), :]
            if step < ctx_count:
                away_buf[order, step, 0] = queries
                away_buf[order, step, 1] = keys
                away_buf[order, step, 2] = values
                exchange(order, step).start()
            else:
                at = stripe(ctx)
                terms_in[dest, ctx // slots, 0, :, at] = queries
                terms_in[dest, ctx // slots, 1, :, at] = keys
                terms_in[dest, ctx // slots, 2, :, at] = values

    pieces = partial.shape[2]
    strip = model // pieces

    def chain(order, piece):
        dest = dest_of(order)
        up = dest > group
        line = jnp.where(up, 0, 1)
        peer = jnp.where(up, group + 1, group - 1)
        return remote(
            passing.at[order, piece], partial.at[line, dest, piece], z_send.at[order, piece],
            z_recv.at[line, dest, piece], ctx, peer * 2 + core,
        )

    def came(line, dest, piece):
        remote(
            passing.at[0, piece], partial.at[line, dest, piece], z_send.at[0, piece],
            z_recv.at[line, dest, piece], ctx, partner,
        ).wait_recv()

    def term(dest, piece):
        cols = pl.ds(pl.multiple_of(piece * strip, strip), strip)
        result = None
        for half in range(2):
            for kind in range(3):
                part = dot32(terms_in[dest, half, kind], w_both[half, kind, cols, :], NT)
                result = part if result is None else result + part
        return result

    inner = (group > 0) & (group < groups - 1)

    def pass_on(order, _):
        dest = dest_of(order)
        for step in range(1, ctx_count):
            arrived(dest, step)
        line = jnp.where(dest > group, 0, 1)

        def one_piece(piece, _):
            sum_v[...] = term(dest, piece)

            @pl.when(inner)
            def _():
                came(line, dest, piece)
                sum_v[...] += partial[line, dest, piece].astype(jnp.float32)

            passing[order, piece] = sum_v[...].astype(jnp.bfloat16)
            chain(order, piece).start()
            return 0

        lax.fori_loop(0, pieces, one_piece, 0)
        return 0

    ends, number = [], 0
    for order in range(groups):
        number += 2 * (groups - order) - 1
        ends.append(number - 1)
    spreads = {order: end + 1 for order, end in enumerate(ends) if end + 1 < number}

    def one_pair(index, _):
        stage = 0
        for end in ends[:-1]:
            stage = stage + jnp.where(index > end, 1, 0)
        first = 0
        for order in range(1, groups):
            first = jnp.where(stage == order, ends[order - 1] + 1, first)
        inside = index - first
        other = stage + (inside + 1) // 2
        odd = lax.rem(inside, 2)
        pair(
            dest_of(jnp.where(odd == 1, stage, other)), dest_of(jnp.where(odd == 1, other, stage))
        )
        for order, end in list(enumerate(ends))[1:-1]:

            @pl.when(index == end)
            def _():
                settle(order)

        for order, at in spreads.items():

            @pl.when(index == at)
            def _():
                spread(order)

        return 0

    def farthest_pair(index, _):
        arriving = index < groups
        other = 0
        for step in range(groups):
            visit = by_arrival(groups, group, step)
            other = jnp.where(index == step, visit, other)
            other = jnp.where(index == groups + step, visit, other)

        @pl.when(arriving)
        def _():
            gradients_arrived(other)

        pair(jnp.where(arriving, other, dests[0]), jnp.where(arriving, dests[0], other))
        return 0

    first = min(ends[min(1, groups - 1)] + 1, number)
    lax.fori_loop(0, ends[0] + 1, farthest_pair, 0)
    settle(0)
    lax.fori_loop(ends[0] + 1, first, one_pair, 0)
    pair_copy.wait()
    early = 1 if first < number else 0
    if early:

        @pl.when(jnp.logical_not(inner))
        def _():
            pass_on(0, 0)

        lax.fori_loop(first, number, one_pair, 0)
    settle(groups - 1)
    for order in range(groups):
        if order not in spreads:
            spread(order)
    lax.fori_loop(jnp.where(inner, 0, early), groups - 1, pass_on, 0)
    for step in range(1, ctx_count):
        arrived(group, step)

    state = state_own[...].astype(jnp.float32)
    inverse = row_scale(state)

    def last_piece(piece, slope):
        cols = pl.ds(pl.multiple_of(piece * strip, strip), strip)
        sum_v[...] = term(group, piece)

        @pl.when(group > 0)
        def _():
            came(0, group, piece)
            sum_v[...] += partial[0, group, piece].astype(jnp.float32)

        @pl.when(group < groups - 1)
        def _():
            came(1, group, piece)
            sum_v[...] += partial[1, group, piece].astype(jnp.float32)

        gained = sum_v[...] * gain_ref[cols].astype(jnp.float32).reshape(1, strip)
        new_out[:, cols] = gained
        return slope + jnp.sum(
            gained * state_own[:, cols].astype(jnp.float32), axis=1, keepdims=True
        )

    slope = lax.fori_loop(0, pieces, last_piece, jnp.zeros((own, 1), jnp.float32))
    bend = inverse**3 * (slope / model)

    def update(piece, _):
        cols = pl.ds(pl.multiple_of(piece * strip, strip), strip)
        here = state_own[:, cols].astype(jnp.float32)
        gradient = readout_out[:, cols] + inverse * new_out[:, cols] - here * bend
        new_out[:, cols] = (
            here - STEP_SIZE * gradient + NOISE_SCALE * noise_own[:, cols].astype(jnp.float32)
        )
        return 0

    lax.fori_loop(0, pieces, update, 0)

    def all_sent(order, _):
        core_copy(order).wait_send()
        for step in range(1, ctx_count):
            exchange(order, step).wait_send()

        @pl.when(order < groups - 1)
        def _():
            for piece in range(pieces):
                chain(order, piece).wait_send()

        return 0

    for copy in copies:
        copy.wait_send()
    lax.fori_loop(0, groups, all_sent, 0)


def heads_body(state, norm_gain, w_qkv, w_out, probe, noise, segment_ids):
    ctx_count, head_count = lax.axis_size("ctx"), lax.axis_size("head")
    rows, model = state.shape
    width = w_qkv.shape[2]
    own, groups, slots = rows // head_count, head_count // 2, width // HEAD_DIM
    seg = segment_ids.reshape(-1, 128)
    half, full, dma = jnp.bfloat16, jnp.float32, pltpu.SemaphoreType.DMA
    pieces, lanes = 4, ctx_count * own
    tile, vmem = model // pieces, pltpu.VMEM
    heads = (groups, ctx_count, own, HEAD_DIM)
    return pl.pallas_call(
        functools.partial(step_kernel, ctx_count, head_count),
        out_shape=jax.ShapeDtypeStruct((own, model), full),
        in_specs=[ANY, ANY, VMEM, VMEM, ANY, ANY, ANY],
        out_specs=VMEM,
        scratch_shapes=[
            vmem((rows, model), half),
            vmem((slots, groups, 2, own, HEAD_DIM), half),
            vmem((slots, 2, groups, 2 * own, HEAD_DIM), half),
            vmem((model, model), half),
            vmem((own, model), half),
            vmem((own, model), half),
            vmem(heads, half),
            vmem((own, model), half),
            vmem((own, model), half),
            vmem((own, model), half),
            vmem(heads, half),
            vmem((2, groups, ctx_count, 2 * own, HEAD_DIM), half),
            vmem(heads, half),
            vmem((own, model), full),
            vmem((ctx_count,) + seg.shape, seg.dtype),
            vmem((groups, 1, lanes), full),
            vmem(heads, half),
            vmem((2,) + w_qkv.shape, half),
            vmem((groups, 2 * lanes, 2 * HEAD_DIM), full),
            vmem((groups, HEAD_DIM, lanes), full),
            vmem((groups, 1, lanes), full),
            vmem((groups, lanes, HEAD_DIM), half),
            vmem((groups, ctx_count, own, 2 * HEAD_DIM), half),
            vmem((groups, ctx_count, own, 2 * HEAD_DIM), half),
            vmem((groups, ctx_count, 3, own, HEAD_DIM), half),
            vmem((groups, 2, 3, own, width), half),
            vmem((2, groups, pieces, own, tile), half),
            vmem((groups, pieces, own, tile), half),
            vmem((own, tile), full),
            dma((groups,)),
            dma((3,)),
            dma((slots, 2, groups)),
            dma((ctx_count, groups)),
            dma((slots, 2, groups)),
            dma((2, ctx_count, groups)),
            dma((ctx_count, groups)),
            dma((ctx_count,)),
            dma((ctx_count,)),
            dma((2, 2, groups)),
            dma((2, groups)),
            dma((2, groups)),
            dma((2, groups)),
            dma((4, groups)),
            dma((4, groups)),
            dma,
            dma,
            dma,
            dma((ctx_count, groups)),
            dma((groups, ctx_count)),
            dma((groups, ctx_count)),
            dma((ctx_count, groups)),
            dma((3,)),
            dma,
            dma,
            dma((groups,)),
            dma((groups,)),
            dma((groups, ctx_count)),
            dma((groups, ctx_count)),
            dma((groups, pieces)),
            dma((2, groups, pieces)),
        ],
        compiler_params=pltpu.CompilerParams(
            collective_id=0, has_side_effects=True, vmem_limit_bytes=52 * 2**20
        ),
    )(state, w_qkv, norm_gain, seg, w_out, probe, noise)


def solution(mesh):
    placed = (
        P("ctx", None),
        P(),
        P(None, None, "head"),
        P("head", None),
        P("ctx", None),
        P(("ctx", "head"), None),
        P("ctx"),
    )

    def step(*args):
        heads = args[2].shape[2] // HEAD_DIM
        return (heads_body if lax.axis_size("ctx") == 2 * heads == 4 else body)(*args)

    return jax.shard_map(
        step, mesh=mesh, in_specs=placed, out_specs=P(("ctx", "head"), None), check_vma=False
    )
```

```python
import functools

import jax
import jax.numpy as jnp
from jax import lax
from jax.experimental import pallas as pl
from jax.experimental.pallas import tpu as pltpu
from jax.sharding import PartitionSpec as P

HEAD_DIM = 128
EPSILON = 1e-05
STEP_SIZE = 0.25
NOISE_SCALE = (2.0 * STEP_SIZE) ** 0.5
NEGATIVE = -1e30
LOG2E = 1.4426950408889634
MESH = pl.DeviceIdType.MESH
VMEM = pl.BlockSpec(memory_space=pltpu.VMEM)
ANY = pl.BlockSpec(memory_space=pl.ANY)
NT = (((1,), (1,)), ((), ()))
TN = (((0,), (0,)), ((), ()))
FORWARD_BLOCKS = (512, 512)
BACKWARD_BLOCKS = (512, 512)


def row_scale(matrix):
    return lax.rsqrt(jnp.mean(matrix * matrix, axis=-1, keepdims=True) + EPSILON)


def dot32(left, right, dims):
    return lax.dot_general(left, right, dims, preferred_element_type=jnp.float32)


def greet(axis, number, me):
    barrier = pltpu.get_barrier_semaphore()
    for step in range(1, number):
        pl.semaphore_signal(
            barrier, inc=1, device_id={axis: lax.rem(me + step, number)}, device_id_type=MESH
        )
    pl.semaphore_wait(barrier, number - 1)


def gather_kernel(
    number, key_ref, value_ref, seg_ref, normed_ref, w_ref, keys, values, segs, query_out, send_sem,
    recv_sem, own_sem,
):
    me = lax.axis_index("ctx")
    rows = key_ref.shape[0]
    greet("ctx", number, me)

    def place(index):
        return pl.ds(pl.multiple_of(index * rows, rows), rows)

    def send(slot, source, target, peer):
        copy = pltpu.make_async_remote_copy(
            src_ref=source,
            dst_ref=target,
            send_sem=send_sem.at[slot],
            recv_sem=recv_sem.at[slot],
            device_id={"ctx": peer},
            device_id_type=MESH,
        )
        copy.start()
        return copy

    mine = place(me)
    copies = []
    for step in range(1, number):
        copies.append(send(step, seg_ref, segs.at[me], lax.rem(me + step, number)))
    relay = number == 4
    if relay:
        low, high = lax.rem(me, 2), me // 2
        across, along = high * 2 + 1 - low, (1 - high) * 2 + low
        key_first = send(number, key_ref, keys.at[mine], across)
        value_first = send(number + 1, value_ref, values.at[mine], along)
        copies.append(send(number + 2, value_ref, values.at[mine], across))
        copies.append(send(number + 3, key_ref, keys.at[mine], along))
    else:
        for step in range(1, number):
            peer = lax.rem(me + step, number)
            copies.append(send(number + 2 * step, key_ref, keys.at[mine], peer))
            copies.append(send(number + 2 * step + 1, value_ref, values.at[mine], peer))
    pairs = ((key_ref, keys.at[mine]), (value_ref, values.at[mine]), (seg_ref, segs.at[me]))
    for index, (source, target) in enumerate(pairs):
        copy = pltpu.make_async_copy(source, target, own_sem.at[index])
        copy.start()
        copies.append(copy)
    tile = min(256, rows)

    def project(piece, _):
        at = pl.ds(pl.multiple_of(piece * tile, tile), tile)
        query_out[at, :] = jnp.dot(
            normed_ref[at, :], w_ref[...], preferred_element_type=jnp.float32
        ).astype(jnp.bfloat16)
        return 0

    lax.fori_loop(0, rows // tile, project, 0)
    if relay:
        key_first.wait()
        copies.append(send(number + 4, keys.at[place(across)], keys.at[place(across)], along))
        value_first.wait()
        copies.append(send(number + 5, values.at[place(along)], values.at[place(along)], across))
    for copy in copies:
        copy.wait()


def gather_keys(number, key_rows, value_rows, segment_ids, normed, w_query):
    rows, width = key_rows.shape
    seg = segment_ids.reshape(-1, 128)
    full = jax.ShapeDtypeStruct((number * rows, width), key_rows.dtype)
    keys, values, segs, queries = pl.pallas_call(
        functools.partial(gather_kernel, number),
        out_shape=(
            full,
            full,
            jax.ShapeDtypeStruct((number,) + seg.shape, seg.dtype),
            jax.ShapeDtypeStruct((rows, width), key_rows.dtype),
        ),
        in_specs=[VMEM] * 5,
        out_specs=(ANY, ANY, ANY, VMEM),
        scratch_shapes=[
            pltpu.SemaphoreType.DMA((3 * number + 6,)),
            pltpu.SemaphoreType.DMA((3 * number + 6,)),
            pltpu.SemaphoreType.DMA((3,)),
        ],
        compiler_params=pltpu.CompilerParams(collective_id=0, has_side_effects=True),
    )(key_rows, value_rows, seg, normed, w_query)
    return keys, values, segs.reshape(-1), queries


def block_ranges(table, index):
    return [table[index, column] for column in range(4)]


def forward_kernel(
    heads, bq, bk, table, query_ref, key_ref, value_ref, start_ref, pos_ref, out_ref, log_ref
):
    factor = HEAD_DIM ** (-0.5) * LOG2E
    blocks = query_ref.shape[0] // bq

    def one_block(index, _):
        low, inner_low, inner_high, high = block_ranges(table, index)
        rows = pl.ds(pl.multiple_of(index * bq, bq), bq)
        start, pos = start_ref[index], pos_ref[index]

        def step(masked, piece, carry):
            keys_at = pl.ds(pl.multiple_of(piece * bk, bk), bk)
            if masked:
                key_pos = piece * bk + lax.broadcasted_iota(jnp.int32, (bk, bq), 0)
                allowed = (key_pos >= start) & (key_pos <= pos)
            result = []
            for head in range(heads):
                top, total, acc = carry[head]
                cols = pl.ds(head * HEAD_DIM, HEAD_DIM)
                scores = dot32(key_ref[keys_at, cols], query_ref[rows, cols], NT)
                if masked:
                    scores = jnp.where(allowed, scores, NEGATIVE)
                new_top = jnp.maximum(top, jnp.max(scores, axis=0, keepdims=True) * factor)
                weights = jnp.exp2(scores * factor - new_top)
                scale = jnp.exp2(top - new_top)
                total = total * scale + jnp.sum(weights, axis=0, keepdims=True)
                acc = acc * scale + dot32(
                    value_ref[keys_at, cols], weights.astype(jnp.bfloat16), TN
                )
                result.append((new_top, total, acc))
            return tuple(result)

        carry = tuple(
            (
                jnp.full((1, bq), NEGATIVE, jnp.float32),
                jnp.zeros((1, bq), jnp.float32),
                jnp.zeros((HEAD_DIM, bq), jnp.float32),
            )
            for _ in range(heads)
        )
        carry = lax.fori_loop(low, inner_low, functools.partial(step, True), carry)
        carry = lax.fori_loop(inner_low, inner_high, functools.partial(step, False), carry)
        carry = lax.fori_loop(inner_high, high, functools.partial(step, True), carry)
        for head in range(heads):
            top, total, acc = carry[head]
            out_ref[rows, pl.ds(head * HEAD_DIM, HEAD_DIM)] = (acc / total).T.astype(jnp.bfloat16)
            log_ref[index, pl.ds(head, 1), :] = top + jnp.log2(total)
        return 0

    lax.fori_loop(0, blocks, one_block, 0)


def backward_kernel(
    heads, bq, bk, table, query_ref, key_ref, value_ref, grad_ref, out_ref, log_ref, start_ref,
    pos_ref, query_out, pair_out, pair_acc,
):
    score_scale = HEAD_DIM ** (-0.5)
    factor = score_scale * LOG2E
    blocks = query_ref.shape[0] // bq
    width = heads * HEAD_DIM
    pair_rows = pair_acc.shape[0]

    def clear(piece, _):
        at = pl.ds(pl.multiple_of(piece * bk, bk), bk)
        pair_acc[at, :] = jnp.zeros((bk, 2 * width), jnp.float32)
        return 0

    lax.fori_loop(0, pair_rows // bk, clear, 0)

    def one_block(index, _):
        low, inner_low, inner_high, high = block_ranges(table, index)
        rows = pl.ds(pl.multiple_of(index * bq, bq), bq)
        start, pos = start_ref[index], pos_ref[index]
        deltas, logs = [], []
        for head in range(heads):
            cols = pl.ds(head * HEAD_DIM, HEAD_DIM)
            product = grad_ref[rows, cols].astype(jnp.float32) * out_ref[rows, cols].astype(
                jnp.float32
            )
            deltas.append(jnp.sum(product.T, axis=0, keepdims=True))
            logs.append(log_ref[index, pl.ds(head, 1), :])

        def step(masked, piece, carry):
            keys_at = pl.ds(pl.multiple_of(piece * bk, bk), bk)
            if masked:
                key_pos = piece * bk + lax.broadcasted_iota(jnp.int32, (bk, bq), 0)
                allowed = (key_pos >= start) & (key_pos <= pos)
            result = []
            for head in range(heads):
                cols = pl.ds(head * HEAD_DIM, HEAD_DIM)
                value_cols = pl.ds(width + head * HEAD_DIM, HEAD_DIM)
                key_block, query_block = key_ref[keys_at, cols], query_ref[rows, cols]
                grad_block = grad_ref[rows, cols]
                scores = dot32(key_block, query_block, NT)
                probabilities = jnp.exp2(scores * factor - logs[head])
                if masked:
                    probabilities = jnp.where(allowed, probabilities, 0.0)
                dprobs = dot32(value_ref[keys_at, cols], grad_block, NT)
                dscores = (probabilities * (dprobs - deltas[head])).astype(jnp.bfloat16)
                pair_acc[keys_at, value_cols] += jnp.dot(
                    probabilities.astype(jnp.bfloat16),
                    grad_block,
                    preferred_element_type=jnp.float32,
                )
                pair_acc[keys_at, cols] += jnp.dot(
                    dscores, query_block, preferred_element_type=jnp.float32
                )
                result.append(carry[head] + dot32(key_block, dscores, TN))
            return tuple(result)

        carry = tuple(jnp.zeros((HEAD_DIM, bq), jnp.float32) for _ in range(heads))
        carry = lax.fori_loop(low, inner_low, functools.partial(step, True), carry)
        carry = lax.fori_loop(inner_low, inner_high, functools.partial(step, False), carry)
        carry = lax.fori_loop(inner_high, high, functools.partial(step, True), carry)
        for head in range(heads):
            query_out[rows, pl.ds(head * HEAD_DIM, HEAD_DIM)] = (
                carry[head].T * score_scale
            ).astype(jnp.bfloat16)
        return 0

    lax.fori_loop(0, blocks, one_block, 0)

    def flush(piece, _):
        at = pl.ds(pl.multiple_of(piece * bk, bk), bk)
        pair_out[at, :width] = (pair_acc[at, :width] * score_scale).astype(jnp.bfloat16)
        pair_out[at, width:] = pair_acc[at, width:].astype(jnp.bfloat16)
        return 0

    lax.fori_loop(0, pair_rows // bk, flush, 0)


def make_table(start, pos, bq, bk):
    starts, places = start.reshape(-1, bq), pos.reshape(-1, bq)
    low = starts[:, 0] // bk
    inner_low = (starts[:, -1] + bk - 1) // bk
    inner_high = jnp.maximum(inner_low, (places[:, 0] + 1) // bk)
    high = places[:, -1] // bk + 1
    return jnp.stack([low, inner_low, inner_high, high], axis=1).astype(jnp.int32)


def middle_kernel(
    number, part_ref, w_any, state_ref, probe_ref, grad_out, readout_out, w_ref, joined, half,
    sending, landing, send_sem, recv_sem, back_send, back_recv, w_sem,
):
    me = lax.axis_index("head")
    width = part_ref.shape[1]
    own = state_ref.shape[0]
    model = state_ref.shape[1]
    w_copy = pltpu.make_async_copy(w_any, w_ref, w_sem)
    w_copy.start()
    greet("head", number, me)
    my_cols = pl.ds(pl.multiple_of(me * width, width), width)
    my_rows = pl.ds(pl.multiple_of(me * own, own), own)
    copies = []
    for step in range(1, number):
        peer = lax.rem(me + step, number)
        copy = pltpu.make_async_remote_copy(
            src_ref=part_ref.at[pl.ds(pl.multiple_of(peer * own, own), own)],
            dst_ref=joined.at[:, my_cols],
            send_sem=send_sem.at[step],
            recv_sem=recv_sem.at[step],
            device_id={"head": peer},
            device_id_type=MESH,
        )
        copy.start()
        copies.append(copy)
    joined[:, my_cols] = part_ref[my_rows, :]
    w_copy.wait()
    for copy in copies:
        copy.wait()

    tile = min(256, model)

    def project(piece, carry):
        squares, products = carry
        cols = pl.ds(pl.multiple_of(piece * tile, tile), tile)
        layer = state_ref[:, cols].astype(jnp.float32) + jnp.dot(
            joined[...], w_ref[:, cols], preferred_element_type=jnp.float32
        )
        readout_out[:, cols] = layer
        squares = squares + jnp.sum(layer * layer, axis=1, keepdims=True)
        products = products + jnp.sum(
            layer * probe_ref[:, cols].astype(jnp.float32), axis=1, keepdims=True
        )
        return squares, products

    zero = jnp.zeros((own, 1), jnp.float32)
    squares, products = lax.fori_loop(0, model // tile, project, (zero, zero))
    scale = lax.rsqrt(squares / model + EPSILON)
    bend = scale**3 * (products / model)

    def finish(piece, _):
        cols = pl.ds(pl.multiple_of(piece * tile, tile), tile)
        readout = scale * probe_ref[:, cols].astype(jnp.float32) - readout_out[:, cols] * bend
        readout_out[:, cols] = readout
        half[:, cols] = readout.astype(jnp.bfloat16)
        return 0

    lax.fori_loop(0, model // tile, finish, 0)
    copies = []
    for step in range(1, number):
        peer = lax.rem(me + step, number)
        sending[step] = dot32(
            half[...], w_ref[pl.ds(pl.multiple_of(peer * width, width), width), :], NT
        ).astype(jnp.bfloat16)
        copy = pltpu.make_async_remote_copy(
            src_ref=sending.at[step],
            dst_ref=landing.at[my_rows],
            send_sem=back_send.at[step],
            recv_sem=back_recv.at[step],
            device_id={"head": peer},
            device_id_type=MESH,
        )
        copy.start()
        copies.append(copy)
    landing[my_rows, :] = dot32(half[...], w_ref[my_cols, :], NT).astype(jnp.bfloat16)
    for copy in copies:
        copy.wait()
    grad_out[...] = landing[...]


def middle(number, part, w_full, state_own, probe_own):
    rows, width = part.shape
    own, model = state_own.shape
    return pl.pallas_call(
        functools.partial(middle_kernel, number),
        out_shape=(
            jax.ShapeDtypeStruct((rows, width), jnp.bfloat16),
            jax.ShapeDtypeStruct((own, model), jnp.float32),
        ),
        in_specs=[VMEM, ANY, VMEM, VMEM],
        out_specs=(VMEM, VMEM),
        scratch_shapes=[
            pltpu.VMEM(w_full.shape, jnp.bfloat16),
            pltpu.VMEM((own, number * width), jnp.bfloat16),
            pltpu.VMEM((own, model), jnp.bfloat16),
            pltpu.VMEM((number, own, width), jnp.bfloat16),
            pltpu.VMEM((rows, width), jnp.bfloat16),
            pltpu.SemaphoreType.DMA((number,)),
            pltpu.SemaphoreType.DMA((number,)),
            pltpu.SemaphoreType.DMA((number,)),
            pltpu.SemaphoreType.DMA((number,)),
            pltpu.SemaphoreType.DMA,
        ],
        compiler_params=pltpu.CompilerParams(
            collective_id=1, has_side_effects=True, vmem_limit_bytes=60 * 2**20
        ),
    )(part, w_full, state_own, probe_own)


def tail_kernel(
    ctx_count, number, pair_any, query_ref, w_ref, sum_out, own_pair, arriving, gathered, terms,
    from_partner, reduced, landing, ctx_send, ctx_recv, p_send, p_recv, z_send, z_recv, own_sem,
):
    ctx, me = lax.axis_index("ctx"), lax.axis_index("head")
    groups = number // 2
    group, core = me // 2, lax.rem(me, 2)
    partner = group * 2 + 1 - core
    rows, width = query_ref.shape
    own, model = sum_out.shape
    chunk = 2 * own
    own_copy = pltpu.make_async_copy(
        pair_any.at[pl.ds(pl.multiple_of(ctx * rows, rows), rows)], own_pair, own_sem
    )
    own_copy.start()
    barrier = pltpu.get_barrier_semaphore()
    peers = [{"ctx": lax.rem(ctx + step, ctx_count)} for step in range(1, ctx_count)]
    peers.append({"head": partner})
    for step in range(1, groups):
        peers.append({"head": lax.rem(group + step, groups) * 2 + core})
    for peer in peers:
        pl.semaphore_signal(barrier, inc=1, device_id=peer, device_id_type=MESH)
    pl.semaphore_wait(barrier, len(peers))

    def chunk_start(order):
        dest = lax.rem(group + order + 1, groups)
        return dest, pl.multiple_of(dest * chunk, chunk)

    def ctx_copy(order, step):
        target = lax.rem(ctx - step + ctx_count, ctx_count)
        _, first = chunk_start(order)
        return pltpu.make_async_remote_copy(
            src_ref=pair_any.at[pl.ds(pl.multiple_of(target * rows + first, chunk), chunk)],
            dst_ref=arriving.at[order, step - 1],
            send_sem=ctx_send.at[order, step],
            recv_sem=ctx_recv.at[order, step],
            device_id={"ctx": target},
            device_id_type=MESH,
        )

    for order in range(groups):
        for step in range(1, ctx_count):

            @pl.when(step <= ctx)
            def _():
                ctx_copy(order, step).start()

    own_copy.wait()
    tile = min(512, model)
    mine = pl.ds(pl.multiple_of(core * own, own), own)
    theirs = pl.ds(pl.multiple_of((1 - core) * own, own), own)
    waiting = []
    for order in range(groups):
        dest, first = chunk_start(order)
        at = pl.ds(first, chunk)
        gathered[...] = own_pair[at, :].astype(jnp.float32)
        for step in range(1, ctx_count):

            @pl.when(ctx + step < ctx_count)
            def _():
                ctx_copy(order, step).wait_recv()
                gathered[...] += arriving[order, step - 1].astype(jnp.float32)

        def multiply(piece, _):
            cols = pl.ds(pl.multiple_of(piece * tile, tile), tile)
            term = dot32(query_ref[at, :], w_ref[0, cols, :], NT)
            term += dot32(gathered[:, :width].astype(jnp.bfloat16), w_ref[1, cols, :], NT)
            term += dot32(gathered[:, width:].astype(jnp.bfloat16), w_ref[2, cols, :], NT)
            terms[order, :, cols] = term.astype(jnp.bfloat16)
            return 0

        lax.fori_loop(0, model // tile, multiply, 0)
        copy = pltpu.make_async_remote_copy(
            src_ref=terms.at[order, theirs],
            dst_ref=from_partner.at[order],
            send_sem=p_send.at[order],
            recv_sem=p_recv.at[order],
            device_id={"head": partner},
            device_id_type=MESH,
        )
        copy.start()
        copy.wait()
        both = terms[order, mine, :].astype(jnp.float32) + from_partner[order].astype(jnp.float32)
        if order < groups - 1:
            reduced[order] = both.astype(jnp.bfloat16)
            copy = pltpu.make_async_remote_copy(
                src_ref=reduced.at[order],
                dst_ref=landing.at[order],
                send_sem=z_send.at[order],
                recv_sem=z_recv.at[order],
                device_id={"head": dest * 2 + core},
                device_id_type=MESH,
            )
            copy.start()
            waiting.append(copy)
        else:
            sum_out[...] = both
    for order, copy in enumerate(waiting):
        copy.wait()
        sum_out[...] += landing[order].astype(jnp.float32)
    for order in range(groups):
        for step in range(1, ctx_count):

            @pl.when(step <= ctx)
            def _():
                ctx_copy(order, step).wait_send()


def tail(ctx_count, number, pair, query_grad, w_qkv):
    rows, width = query_grad.shape
    model = w_qkv.shape[1]
    own, groups = rows // number, number // 2
    half, full = jnp.bfloat16, jnp.float32
    dma = pltpu.SemaphoreType.DMA
    return pl.pallas_call(
        functools.partial(tail_kernel, ctx_count, number),
        out_shape=jax.ShapeDtypeStruct((own, model), full),
        in_specs=[ANY, VMEM, VMEM],
        out_specs=VMEM,
        scratch_shapes=[
            pltpu.VMEM((rows, 2 * width), half),
            pltpu.VMEM((groups, ctx_count - 1, 2 * own, 2 * width), half),
            pltpu.VMEM((2 * own, 2 * width), full),
            pltpu.VMEM((groups, 2 * own, model), half),
            pltpu.VMEM((groups, own, model), half),
            pltpu.VMEM((groups, own, model), half),
            pltpu.VMEM((groups, own, model), half),
            dma((groups, ctx_count)),
            dma((groups, ctx_count)),
            dma((groups,)),
            dma((groups,)),
            dma((groups,)),
            dma((groups,)),
            dma,
        ],
        compiler_params=pltpu.CompilerParams(
            collective_id=2, has_side_effects=True, vmem_limit_bytes=60 * 2**20
        ),
    )(pair, query_grad, w_qkv)


def body(state, norm_gain, w_qkv, w_out, probe, noise, segment_ids):
    local_rows, model_width = state.shape
    width = w_qkv.shape[2]
    local_heads = width // HEAD_DIM
    head_count = lax.axis_size("head")
    ctx_count = lax.axis_size("ctx")
    ctx_index = lax.axis_index("ctx")
    own_rows = local_rows // head_count
    row_start = lax.axis_index("head") * own_rows
    w_full = lax.all_gather(w_out, "head", axis=0, tiled=True)
    state_f = state.astype(jnp.float32)
    gain_full = norm_gain.astype(jnp.float32)
    inverse = row_scale(state_f)
    normed = (state_f * inverse * gain_full).astype(jnp.bfloat16)

    def project(index):
        return jnp.dot(normed, w_qkv[index], preferred_element_type=jnp.float32).astype(
            jnp.bfloat16
        )

    key_rows, value_rows = project(1), project(2)
    keys, values, segs, query_rows = gather_keys(
        ctx_count, key_rows, value_rows, segment_ids, normed, w_qkv[0]
    )
    total_rows = keys.shape[0]
    pos = ctx_index * local_rows + jnp.arange(local_rows, dtype=jnp.int32)
    start = jnp.sum((segs[None, :] < segment_ids[:, None]).astype(jnp.int32), axis=1)
    fq, fk = (min(local_rows, size) for size in FORWARD_BLOCKS)
    gq, gk = (min(local_rows, size) for size in BACKWARD_BLOCKS)
    smem = pl.BlockSpec(memory_space=pltpu.SMEM)
    params = pltpu.CompilerParams(vmem_limit_bytes=60 * 2**20)
    outputs, logs = pl.pallas_call(
        functools.partial(forward_kernel, local_heads, fq, fk),
        out_shape=(
            jax.ShapeDtypeStruct((local_rows, width), jnp.bfloat16),
            jax.ShapeDtypeStruct((local_rows // fq, local_heads, fq), jnp.float32),
        ),
        in_specs=[smem] + [VMEM] * 5,
        out_specs=(VMEM, VMEM),
        compiler_params=params,
        cost_estimate=pl.CostEstimate(
            flops=4 * local_rows * total_rows * width, bytes_accessed=0, transcendentals=0
        ),
    )(
        make_table(start, pos, fq, fk),
        query_rows,
        keys,
        values,
        start.reshape(-1, 1, fq),
        pos.reshape(-1, 1, fq),
    )
    state_half = lax.dynamic_slice_in_dim(state, row_start, own_rows, 0)
    probe_own = lax.dynamic_slice_in_dim(probe, row_start, own_rows, 0)
    state_own = state_half.astype(jnp.float32)
    inverse_own = row_scale(state_own)
    grads_out, readout_own = middle(head_count, outputs, w_full, state_half, probe_own)
    query_grad, pair = pl.pallas_call(
        functools.partial(backward_kernel, local_heads, gq, gk),
        out_shape=(
            jax.ShapeDtypeStruct((local_rows, width), jnp.bfloat16),
            jax.ShapeDtypeStruct((total_rows, 2 * width), jnp.bfloat16),
        ),
        in_specs=[smem] + [VMEM] * 8,
        out_specs=(VMEM, VMEM),
        scratch_shapes=[pltpu.VMEM((total_rows, 2 * width), jnp.float32)],
        compiler_params=params,
        cost_estimate=pl.CostEstimate(
            flops=10 * local_rows * total_rows * width, bytes_accessed=0, transcendentals=0
        ),
    )(
        make_table(start, pos, gq, gk),
        query_rows,
        keys,
        values,
        grads_out,
        outputs,
        logs.reshape(local_rows // fq, local_heads, fq),
        start.reshape(-1, 1, gq),
        pos.reshape(-1, 1, gq),
    )
    normed_grad = tail(ctx_count, head_count, pair, query_grad, w_qkv)
    gain_grad = normed_grad * gain_full
    gradient = (
        readout_own
        + inverse_own * gain_grad
        - state_own * inverse_own**3 * jnp.mean(gain_grad * state_own, axis=-1, keepdims=True)
    )
    return state_own - STEP_SIZE * gradient + jnp.sqrt(2.0 * STEP_SIZE) * noise.astype(jnp.float32)


def remote(source, target, send_sem, recv_sem, ctx, head):
    return pltpu.make_async_remote_copy(
        src_ref=source,
        dst_ref=target,
        send_sem=send_sem,
        recv_sem=recv_sem,
        device_id={"ctx": ctx, "head": head},
        device_id_type=MESH,
    )


def place():
    ctx, me = lax.axis_index("ctx"), lax.axis_index("head")
    return ctx, me, me // 2, lax.rem(me, 2)


def announce(peers):
    barrier = pltpu.get_barrier_semaphore()
    for ctx, head in peers:
        pl.semaphore_signal(
            barrier, inc=1, device_id={"ctx": ctx, "head": head}, device_id_type=MESH
        )


def await_all(peers):
    pl.semaphore_wait(pltpu.get_barrier_semaphore(), len(peers))


def far_first(groups, group, step):
    result = 0
    for index in range(groups):
        order = sorted(range(groups), key=lambda other: (-abs(other - index), -other))
        result = jnp.where(group == index, order[step], result)
    return result


def by_arrival(groups, group, step):
    result = 0
    for index in range(groups):
        last = sorted(range(groups), key=lambda other: (-abs(other - index), -other))[0]
        order = sorted(
            (other for other in range(groups) if other != last),
            key=lambda other: (other in (0, groups - 1), abs(other - index)),
        )
        result = jnp.where(group == index, (order + [last])[step], result)
    return result


def step_kernel(
    ctx_count, head_count, state_any, w_any, gain_ref, seg_ref, w_out_any, probe_any, noise_any,
    new_out, state_v, query_buf, kv_buf, w_ref, joined, half, sending, state_own, probe_own,
    noise_own, query_out, kv_out, part_out, readout_out, segs_out, log_v, grad_v, w_both, pair_acc,
    query_acc, deltas, query_fin, pair_buf, beside_in, away_buf, terms_in, partial, passing, sum_v,
    load_sem, w_sem, q_send, q_recv, kv_send, kv_recv, pass_send, seg_send, seg_recv, line_send,
    line_recv, plane_send, plane_recv, beside_send, beside_recv, shard_send, shard_recv, shard_sem,
    out_send, out_recv, back_send, back_recv, row_sem, pair_send, pair_recv, b_send, b_recv, a_send,
    a_recv, z_send, z_recv,
):
    ctx, me, group, core = place()
    rows, model = state_any.shape
    own, groups = rows // head_count, head_count // 2
    slots = w_any.shape[2] // HEAD_DIM
    chunk = 2 * own
    partner = group * 2 + 1 - core

    def at(piece):
        return pl.ds(pl.multiple_of(piece * chunk, chunk), chunk)

    def own_at(piece):
        return pl.ds(pl.multiple_of(piece * own, own), own)

    def load_state(piece):
        return pltpu.make_async_copy(
            state_any.at[at(piece)], state_v.at[at(piece)], load_sem.at[piece]
        )

    load_state(0).start()
    w_loads = [
        pltpu.make_async_copy(w_any.at[t], w_both.at[core, t], w_sem.at[t]) for t in range(3)
    ]
    for copy in w_loads:
        copy.start()
    for piece in range(1, groups):
        load_state(piece).start()
    my_rows = own_at(me)
    shard = w_out_any.shape[0]
    part, quarter = shard // 2, shard // ctx_count
    later_loads = [
        pltpu.make_async_copy(state_any.at[my_rows], state_own, row_sem.at[0]),
        pltpu.make_async_copy(probe_any.at[my_rows], probe_own, row_sem.at[1]),
        pltpu.make_async_copy(noise_any, noise_own, row_sem.at[2]),
        pltpu.make_async_copy(
            w_out_any, w_ref.at[pl.ds(pl.multiple_of(me * shard, shard), shard)], shard_sem
        ),
    ]
    for copy in later_loads:
        copy.start()
    peers = [(lax.rem(ctx + step, ctx_count), partner) for step in range(ctx_count)]
    for far in range(groups):
        for step in range(ctx_count):
            if far or step:
                peers.append(
                    (lax.rem(ctx + step, ctx_count), lax.rem(group + far, groups) * 2 + core)
                )
    announce(peers)

    low, high = lax.rem(ctx, 2), ctx // 2
    which = lax.rem(low + high, 2)
    across, along = high * 2 + 1 - low, (1 - high) * 2 + low

    def shard_rows(origin, first, size):
        return pl.ds(pl.multiple_of((origin * 2 + core) * shard + first, size), size)

    def line_copy(way, origin, axis, mine):
        first = which * part + axis * quarter
        here = shard_rows(origin, first, quarter)
        source = (
            w_out_any.at[pl.ds(pl.multiple_of(first, quarter), quarter)] if mine else w_ref.at[here]
        )
        other = group + 1 if way == 0 else group - 1
        return remote(
            source, w_ref.at[here], line_send.at[way, axis, origin], line_recv.at[axis, origin],
            ctx, other * 2 + core,
        )

    def plane_copy(axis, origin, kept):
        here = shard_rows(origin, kept * part + axis * quarter, quarter)
        return remote(
            w_ref.at[here], w_ref.at[here], plane_send.at[axis, origin],
            plane_recv.at[axis, origin], along if axis else across, me,
        )

    def beside_copy(kind, origin):
        kept = which if kind < 2 else 1 - which
        here = shard_rows(origin, kept * part + (kind % 2) * quarter, quarter)
        return remote(
            w_ref.at[here], w_ref.at[here], beside_send.at[kind, origin],
            beside_recv.at[kind, origin], ctx, partner,
        )

    def shard_copy():
        return remote(
            w_out_any, w_ref.at[pl.ds(pl.multiple_of(me * shard, shard), shard)], shard_send,
            shard_recv, ctx, partner,
        )

    has_up, has_down = group < groups - 1, group > 0

    def each_origin(distance, work):
        for way in range(2):
            origin = group - distance if way == 0 else group + distance

            @pl.when(origin >= 0 if way == 0 else origin < groups)
            def _():
                work(way, origin)

    def line_arrived(distance, axis):
        def work(way, origin):
            line_copy(way, origin, axis, False).wait_recv()

            @pl.when(has_up if way == 0 else has_down)
            def _():
                line_copy(way, origin, axis, False).start()

            plane_copy(axis, origin, which).start()
            beside_copy(axis, origin).start()

        each_origin(distance, work)

    def plane_arrived(distance, axis):
        def work(way, origin):
            plane_copy(axis, origin, 1 - which).wait_recv()
            beside_copy(2 + axis, origin).start()

        each_origin(distance, work)

    def weights_sent(distance):
        def work(way, origin):
            for axis in range(2):

                @pl.when(has_up if way == 0 else has_down)
                def _():
                    line_copy(way, origin, axis, False).wait_send()

                plane_copy(axis, origin, which).wait_send()
            for kind in range(4):
                beside_copy(kind, origin).wait_send()

        each_origin(distance, work)

    def own_lines(work):
        for axis in range(2):

            @pl.when(has_up)
            def _():
                work(line_copy(0, group, axis, True))

            @pl.when(has_down)
            def _():
                work(line_copy(1, group, axis, True))

    for copy in w_loads:
        copy.wait()
    gain = gain_ref[...].astype(jnp.float32).reshape(1, model)

    def away(slot, kind, piece, dest):
        head = group * 2 + kind
        return (
            remote(
                query_buf.at[slot, piece, kind], query_out.at[piece, ctx],
                q_send.at[slot, kind, piece], q_recv.at[ctx, piece], dest, head,
            ),
            remote(
                kv_buf.at[slot, kind, piece], kv_out.at[kind, piece, ctx],
                kv_send.at[slot, kind, piece], kv_recv.at[kind, ctx, piece], dest, head,
            ),
        )

    def beside(slot, piece):
        result = [
            remote(
                query_buf.at[slot, piece, 1 - core], query_out.at[piece, ctx],
                q_send.at[slot, 1 - core, piece], q_recv.at[ctx, piece], ctx, partner,
            )
        ]
        for kind in range(2):
            result.append(
                remote(
                    kv_buf.at[slot, kind, piece], kv_out.at[kind, piece, ctx],
                    kv_send.at[slot, kind, piece], kv_recv.at[kind, ctx, piece], ctx, partner,
                )
            )
        return result

    def project(piece):
        load_state(piece).wait()
        block = state_v[at(piece), :].astype(jnp.float32)
        normed = (block * row_scale(block) * gain).astype(jnp.bfloat16)
        for t in range(3):
            result = jnp.dot(normed, w_both[core, t], preferred_element_type=jnp.float32).astype(
                jnp.bfloat16
            )
            for slot in range(slots):
                cut = result[:, slot * HEAD_DIM : (slot + 1) * HEAD_DIM]
                if t == 0:
                    query_buf[slot, piece, 0] = cut[:own]
                    query_buf[slot, piece, 1] = cut[own:]
                else:
                    kv_buf[slot, t - 1, piece] = cut

    def send_heads(piece):
        for slot in range(slots):
            dest = core * slots + slot

            @pl.when(dest != ctx)
            def _():
                for kind in range(2):
                    for copy in away(slot, kind, piece, dest):
                        copy.start()

            @pl.when(dest == ctx)
            def _():
                query_out[piece, ctx] = query_buf[slot, piece, core]
                for kind in range(2):
                    kv_out[kind, piece, ctx] = kv_buf[slot, kind, piece]
                for copy in beside(slot, piece):
                    copy.start()

    project(0)
    await_all(peers)
    own_lines(lambda copy: copy.start())
    send_heads(0)
    shard_copy().start()
    segs = []
    for step in range(1, ctx_count):
        copy = remote(
            seg_ref, segs_out.at[ctx], seg_send.at[step], seg_recv.at[step],
            lax.rem(ctx + step, ctx_count), me,
        )
        copy.start()
        segs.append(copy)
    segs_out[ctx] = seg_ref[...]

    def project_and_send(piece, _):
        project(piece)
        send_heads(piece)
        return 0

    lax.fori_loop(1, groups, project_and_send, 0)

    def hand_over(piece, step):
        source = lax.rem(ctx + step, ctx_count)
        return remote(
            kv_out.at[core, piece, source], kv_out.at[core, piece, source],
            pass_send.at[step, piece], kv_recv.at[core, source, piece], ctx, partner,
        )

    for piece in range(groups):
        for step in range(1, ctx_count):
            copy = hand_over(piece, step)
            copy.wait_recv()
            copy.start()
        if piece == 0:
            line_arrived(1, 0)
        if piece == min(2, groups - 1):
            line_arrived(1, 1)
    line_arrived(2, 0)

    def got_query(source, piece):
        remote(
            query_out.at[piece, source], query_out.at[piece, source],
            q_send.at[0, 0, piece], q_recv.at[source, piece], ctx, partner,
        ).wait_recv()

    def got_kv(kind, source, piece):
        remote(
            kv_out.at[kind, piece, source], kv_out.at[kind, piece, source],
            kv_send.at[0, 0, piece], kv_recv.at[kind, source, piece], ctx, partner,
        ).wait_recv()

    def gather(piece, _):
        for step in range(1, ctx_count):
            source = lax.rem(ctx + step, ctx_count)
            got_query(source, piece)
            got_kv(1 - core, source, piece)
            hand_over(piece, step).wait_send()

        @pl.when(ctx // slots != core)
        def _():
            got_query(ctx, piece)
            for kind in range(2):
                got_kv(kind, ctx, piece)

        return 0

    lax.fori_loop(0, groups, gather, 0)
    for copy in segs:
        copy.wait()
    pair_copy = remote(w_any, w_both.at[core], pair_send, pair_recv, ctx, partner)
    pair_copy.start()

    def cols_of(group_at, ctx_at):
        head = group_at * ctx_count + ctx_at
        return pl.ds(pl.multiple_of(head * HEAD_DIM, HEAD_DIM), HEAD_DIM)

    factor = HEAD_DIM ** (-0.5) * LOG2E
    sub = groups * own
    seg_all = segs_out[...]

    def below(value):
        count = jnp.where(seg_all < value, 1.0, 0.0)
        for axis in (0, 1, 2):
            count = jnp.sum(count, axis=axis, keepdims=True)
        return count[0]

    first_bound, second_bound = below(1), below(2)
    lane = lax.broadcasted_iota(jnp.int32, (1, sub), 1)
    inside = (lane // own) * (2 * own) + core * own + lane % own
    key_row = lax.broadcasted_iota(jnp.int32, (rows, sub), 0)

    def out_copy(tile, order, other):
        return remote(
            part_out.at[other, tile], joined.at[:, cols_of(group, ctx)],
            out_send.at[tile, order], out_recv.at[group, ctx], tile, other * 2 + core,
        )

    def one_tile(tile, _):
        query = query_out[:, tile].reshape(sub, HEAD_DIM)
        pos = (tile * rows + inside).astype(jnp.float32)
        start = jnp.where(
            pos >= second_bound, second_bound, jnp.where(pos >= first_bound, first_bound, 0.0)
        ).astype(jnp.int32)

        def step(diagonal, piece, carry):
            top, total, acc = carry
            scores = dot32(kv_out[0, :, piece].reshape(rows, HEAD_DIM), query, NT)
            allowed = key_row >= start - piece * rows
            if diagonal:
                allowed = allowed & (key_row <= inside)
            scores = jnp.where(allowed, scores, NEGATIVE)
            new_top = jnp.maximum(top, jnp.max(scores, axis=0, keepdims=True) * factor)
            weights = jnp.exp2(scores * factor - new_top)
            scale = jnp.exp2(top - new_top)
            total = total * scale + jnp.sum(weights, axis=0, keepdims=True)
            acc = acc * scale + dot32(
                kv_out[1, :, piece].reshape(rows, HEAD_DIM), weights.astype(jnp.bfloat16), TN
            )
            return new_top, total, acc

        carry = (
            jnp.full((1, sub), NEGATIVE, jnp.float32),
            jnp.zeros((1, sub), jnp.float32),
            jnp.zeros((HEAD_DIM, sub), jnp.float32),
        )
        carry = lax.fori_loop(0, tile, functools.partial(step, False), carry)
        top, total, acc = step(True, tile, carry)
        result = (acc / total).T.astype(jnp.bfloat16)
        log_row = top + jnp.log2(total)
        for index in range(groups):
            part_out[index, tile] = result[index * own : (index + 1) * own]
            log_v[index, :, own_at(tile)] = log_row[:, index * own : (index + 1) * own]
        for order in range(groups):
            other = far_first(groups, group, order)
            if order == groups - 1:

                @pl.when(tile != ctx)
                def _():
                    out_copy(tile, order, other).start()

                @pl.when(tile == ctx)
                def _():
                    joined[:, cols_of(group, ctx)] = part_out[group, tile]

            else:
                out_copy(tile, order, other).start()

        return 0

    line_arrived(2, 1)
    lax.fori_loop(0, ctx_count, one_tile, 0)
    for copy in later_loads:
        copy.wait()
    sources = []
    for far in range(groups):
        for step in range(ctx_count):
            if far or step:
                sources.append((lax.rem(group + far, groups), lax.rem(ctx + step, ctx_count)))
    tile = min(512, model)
    wide = ctx_count * HEAD_DIM
    zero = jnp.zeros((own, 1), jnp.float32)
    for axis in range(2):
        plane_arrived(1, axis)
    for distance in range(3, groups):
        line_arrived(distance, 0)
    for axis in range(2):
        plane_arrived(2, axis)
    for distance in range(3, groups):
        line_arrived(distance, 1)
    shard_copy().wait_recv()

    def heads_arrived(order):
        other = far_first(groups, group, order)
        if order < groups - 1:
            for kind in range(4):
                beside_copy(kind, other).wait_recv()
        for step in range(ctx_count):
            if order < groups - 1 or step:
                peer = lax.rem(ctx + step, ctx_count)
                remote(
                    part_out.at[0, 0], joined.at[:, cols_of(other, peer)],
                    out_send.at[0, 0], out_recv.at[other, peer], peer, other * 2 + core,
                ).wait_recv()

    for order in range(groups - 1, 0, -1):
        heads_arrived(order)
    farthest = far_first(groups, group, 0)
    near = pl.ds(pl.multiple_of(jnp.where(farthest == 0, wide, 0), wide), model - wide)
    far = pl.ds(pl.multiple_of(farthest * wide, wide), wide)

    def near_layer(piece, _):
        cols = pl.ds(pl.multiple_of(piece * tile, tile), tile)
        readout_out[:, cols] = state_own[:, cols].astype(jnp.float32) + jnp.dot(
            joined[:, near], w_ref[near, cols], preferred_element_type=jnp.float32
        )
        return 0

    lax.fori_loop(0, model // tile, near_layer, 0)
    for distance in range(3, groups):
        for axis in range(2):
            plane_arrived(distance, axis)
    heads_arrived(0)

    def layer(piece, carry):
        squares, products = carry
        cols = pl.ds(pl.multiple_of(piece * tile, tile), tile)
        result = readout_out[:, cols] + jnp.dot(
            joined[:, far], w_ref[far, cols], preferred_element_type=jnp.float32
        )
        readout_out[:, cols] = result
        squares = squares + jnp.sum(result * result, axis=1, keepdims=True)
        products = products + jnp.sum(
            result * probe_own[:, cols].astype(jnp.float32), axis=1, keepdims=True
        )
        return squares, products

    squares, products = lax.fori_loop(0, model // tile, layer, (zero, zero))
    scale = lax.rsqrt(squares / model + EPSILON)
    bend = scale**3 * (products / model)

    def finish(piece, _):
        cols = pl.ds(pl.multiple_of(piece * tile, tile), tile)
        readout = scale * probe_own[:, cols].astype(jnp.float32) - readout_out[:, cols] * bend
        readout_out[:, cols] = readout
        half[:, cols] = readout.astype(jnp.bfloat16)
        return 0

    lax.fori_loop(0, model // tile, finish, 0)
    copies = []
    for order in range(groups):
        other = far_first(groups, group, order)
        result = dot32(
            half[...], w_ref[pl.ds(pl.multiple_of(other * wide, wide), wide), :], NT
        ).astype(jnp.bfloat16)
        for index in range(ctx_count):
            sending[order, index] = result[:, index * HEAD_DIM : (index + 1) * HEAD_DIM]
        for step in range(ctx_count):
            peer = lax.rem(ctx + step, ctx_count)
            if order == groups - 1 and step == 0:
                continue
            copy = remote(
                sending.at[order, peer], grad_v.at[group, ctx], back_send.at[order, step],
                back_recv.at[ctx, group], peer, other * 2 + core,
            )
            copy.start()
            copies.append(copy)
    grad_v[group, ctx] = sending[groups - 1, ctx]

    def clear(index, _):
        pair_acc[index] = jnp.zeros(pair_acc.shape[1:], jnp.float32)
        query_acc[index] = jnp.zeros(query_acc.shape[1:], jnp.float32)
        return 0

    lax.fori_loop(0, groups, clear, 0)

    def sent(piece, _):
        for slot in range(slots):
            dest = core * slots + slot

            @pl.when(dest != ctx)
            def _():
                for kind in range(2):
                    for copy in away(slot, kind, piece, dest):
                        copy.wait_send()

            @pl.when(dest == ctx)
            def _():
                for copy in beside(slot, piece):
                    copy.wait_send()

        return 0

    lax.fori_loop(0, groups, sent, 0)

    own_lines(lambda copy: copy.wait_send())
    shard_copy().wait_send()
    for distance in range(1, groups):
        weights_sent(distance)

    def parts_sent(tile, _):
        for order in range(groups):
            other = far_first(groups, group, order)
            if order == groups - 1:

                @pl.when(tile != ctx)
                def _():
                    out_copy(tile, order, other).wait_send()

            else:
                out_copy(tile, order, other).wait_send()
        return 0

    lax.fori_loop(0, ctx_count, parts_sent, 0)
    halves = 2
    span = ctx_count * own // halves
    dests = [far_first(groups, group, order) for order in range(groups)]

    def dest_of(order):
        result = dests[0]
        for index in range(1, groups):
            result = jnp.where(order == index, dests[index], result)
        return result

    score_scale = HEAD_DIM ** (-0.5)
    def half_of(ref, index, half):
        count = ctx_count // halves
        return ref[index, half * count : (half + 1) * count].reshape(span, HEAD_DIM)

    def find_deltas(index):
        for half in range(halves):
            product = half_of(grad_v, index, half).astype(jnp.float32) * half_of(
                part_out, index, half
            ).astype(jnp.float32)
            deltas[index, :, half * span : (half + 1) * span] = jnp.sum(
                product.T, axis=0, keepdims=True
            )

    def gradients_arrived(other):
        for peer in range(ctx_count):

            @pl.when(jnp.logical_or(other != group, ctx != peer))
            def _():
                remote(
                    sending.at[0, 0], grad_v.at[other, peer], back_send.at[0, 0],
                    back_recv.at[peer, other], ctx, partner,
                ).wait_recv()

        find_deltas(other)

    spot_lane = lax.broadcasted_iota(jnp.int32, (1, span), 1)
    key_line = lax.broadcasted_iota(jnp.int32, (2 * own, own), 0)

    def pair(query_at, key_at):
        for half in range(halves):
            blocks = (half + 1) * ctx_count // halves
            count = blocks * 2 * own
            lanes = slice(half * span, (half + 1) * span)
            key_block = kv_out[0, key_at, :blocks].reshape(count, HEAD_DIM)
            value_block = kv_out[1, key_at, :blocks].reshape(count, HEAD_DIM)
            query_block = half_of(query_out, query_at, half)
            grad_block = half_of(grad_v, query_at, half)
            first_ctx = half * (ctx_count // halves)
            pos = (first_ctx + spot_lane // own) * rows + spot_lane % own
            pos = pos + (query_at * 2 + core) * own
            pos_f = pos.astype(jnp.float32)
            start = jnp.where(
                pos_f >= second_bound,
                second_bound,
                jnp.where(pos_f >= first_bound, first_bound, 0.0),
            ).astype(jnp.int32)
            scores = dot32(key_block, query_block, NT)
            raw = jnp.exp2(scores * factor - log_v[query_at, :, lanes])
            strips = []
            for source in range(blocks):
                offset = source * rows + key_at * 2 * own
                row_cut = slice(source * 2 * own, (source + 1) * 2 * own)
                cells = []
                for index in range(ctx_count // halves):
                    lane_cut = slice(index * own, (index + 1) * own)
                    if source > first_ctx + index:
                        cells.append(jnp.zeros((2 * own, own), jnp.float32))
                        continue
                    allowed = key_line >= start[:, lane_cut] - offset
                    if source == first_ctx + index:
                        allowed = allowed & (key_line <= pos[:, lane_cut] - offset)
                    cells.append(jnp.where(allowed, raw[row_cut, lane_cut], 0.0))
                strips.append(jnp.concatenate(cells, axis=1))
            probabilities = jnp.concatenate(strips, axis=0)
            dprobs = dot32(value_block, grad_block, NT)
            dscores = (probabilities * (dprobs - deltas[query_at, :, lanes])).astype(jnp.bfloat16)
            pair_acc[key_at, :count, HEAD_DIM:] += jnp.dot(
                probabilities.astype(jnp.bfloat16), grad_block, preferred_element_type=jnp.float32
            )
            pair_acc[key_at, :count, :HEAD_DIM] += jnp.dot(
                dscores, query_block, preferred_element_type=jnp.float32
            )
            query_acc[query_at, :, lanes] += dot32(key_block, dscores, TN)

    def core_copy(order):
        return remote(
            pair_buf.at[order], beside_in.at[order], b_send.at[order], b_recv.at[order], ctx, partner
        )

    def pair_rows(dest, source, kind):
        first = pl.multiple_of((source * 2 + kind) * own, own)
        keys = pair_acc[dest, pl.ds(first, own), :HEAD_DIM] * score_scale
        values = pair_acc[dest, pl.ds(first, own), HEAD_DIM:]
        return keys, values

    def settle(order):
        dest = dest_of(order)
        for source in range(ctx_count):
            keys, values = pair_rows(dest, source, 1 - core)
            pair_buf[order, source, :, :HEAD_DIM] = keys.astype(jnp.bfloat16)
            pair_buf[order, source, :, HEAD_DIM:] = values.astype(jnp.bfloat16)
        for half in range(halves):
            query_fin[order, half * span : (half + 1) * span, :] = (
                query_acc[dest, :, half * span : (half + 1) * span].T * score_scale
            ).astype(jnp.bfloat16)
        core_copy(order).start()

    def stripe(source):
        slot = lax.rem(source, slots)
        return pl.ds(pl.multiple_of(slot * HEAD_DIM, HEAD_DIM), HEAD_DIM)

    def exchange(order, step):
        peer = lax.rem(ctx + step, ctx_count)
        return remote(
            away_buf.at[order, step],
            terms_in.at[dest_of(order), ctx // slots, :, :, stripe(ctx)],
            a_send.at[order, step], a_recv.at[dest_of(order), ctx], peer, me,
        )

    def arrived(dest, step):
        source = lax.rem(ctx + step, ctx_count)
        remote(
            away_buf.at[0, 0], terms_in.at[dest, source // slots, :, :, stripe(source)],
            a_send.at[0, 0], a_recv.at[dest, source], source, me,
        ).wait_recv()

    def spread(order):
        dest = dest_of(order)
        core_copy(order).wait_recv()
        for step in range(1, ctx_count + 1):
            peer = lax.rem(ctx + step, ctx_count)
            keys, values = pair_rows(dest, peer, core)
            keys = (keys + beside_in[order, peer, :, :HEAD_DIM].astype(jnp.float32)).astype(
                jnp.bfloat16
            )
            values = (values + beside_in[order, peer, :, HEAD_DIM:].astype(jnp.float32)).astype(
                jnp.bfloat16
            )
            queries = query_fin[order, pl.ds(pl.multiple_of(peer * own, own), own), :]
            if step < ctx_count:
                away_buf[order, step, 0] = queries
                away_buf[order, step, 1] = keys
                away_buf[order, step, 2] = values
                exchange(order, step).start()
            else:
                at = stripe(ctx)
                terms_in[dest, ctx // slots, 0, :, at] = queries
                terms_in[dest, ctx // slots, 1, :, at] = keys
                terms_in[dest, ctx // slots, 2, :, at] = values

    pieces = partial.shape[2]
    strip = model // pieces

    def chain(order, piece):
        dest = dest_of(order)
        up = dest > group
        line = jnp.where(up, 0, 1)
        peer = jnp.where(up, group + 1, group - 1)
        return remote(
            passing.at[order, piece], partial.at[line, dest, piece], z_send.at[order, piece],
            z_recv.at[line, dest, piece], ctx, peer * 2 + core,
        )

    def came(line, dest, piece):
        remote(
            passing.at[0, piece], partial.at[line, dest, piece], z_send.at[0, piece],
            z_recv.at[line, dest, piece], ctx, partner,
        ).wait_recv()

    def term(dest, piece):
        cols = pl.ds(pl.multiple_of(piece * strip, strip), strip)
        result = None
        for half in range(2):
            for kind in range(3):
                part = dot32(terms_in[dest, half, kind], w_both[half, kind, cols, :], NT)
                result = part if result is None else result + part
        return result

    inner = (group > 0) & (group < groups - 1)

    def pass_on(order, _):
        dest = dest_of(order)
        for step in range(1, ctx_count):
            arrived(dest, step)
        line = jnp.where(dest > group, 0, 1)

        def one_piece(piece, _):
            sum_v[...] = term(dest, piece)

            @pl.when(inner)
            def _():
                came(line, dest, piece)
                sum_v[...] += partial[line, dest, piece].astype(jnp.float32)

            passing[order, piece] = sum_v[...].astype(jnp.bfloat16)
            chain(order, piece).start()
            return 0

        lax.fori_loop(0, pieces, one_piece, 0)
        return 0

    ends, number = [], 0
    for order in range(groups):
        number += 2 * (groups - order) - 1
        ends.append(number - 1)
    spreads = {order: end + 1 for order, end in enumerate(ends) if end + 1 < number}

    def one_pair(index, _):
        stage = 0
        for end in ends[:-1]:
            stage = stage + jnp.where(index > end, 1, 0)
        first = 0
        for order in range(1, groups):
            first = jnp.where(stage == order, ends[order - 1] + 1, first)
        inside = index - first
        other = stage + (inside + 1) // 2
        odd = lax.rem(inside, 2)
        pair(
            dest_of(jnp.where(odd == 1, stage, other)), dest_of(jnp.where(odd == 1, other, stage))
        )
        for order, end in list(enumerate(ends))[1:-1]:

            @pl.when(index == end)
            def _():
                settle(order)

        for order, at in spreads.items():

            @pl.when(index == at)
            def _():
                spread(order)

        return 0

    def farthest_pair(index, _):
        arriving = index < groups
        other = 0
        for step in range(groups):
            visit = by_arrival(groups, group, step)
            other = jnp.where(index == step, visit, other)
            other = jnp.where(index == groups + step, visit, other)

        @pl.when(arriving)
        def _():
            gradients_arrived(other)

        pair(jnp.where(arriving, other, dests[0]), jnp.where(arriving, dests[0], other))
        return 0

    first = min(ends[min(1, groups - 1)] + 1, number)
    lax.fori_loop(0, ends[0] + 1, farthest_pair, 0)
    settle(0)
    lax.fori_loop(ends[0] + 1, first, one_pair, 0)
    pair_copy.wait()
    early = 1 if first < number else 0
    if early:

        @pl.when(jnp.logical_not(inner))
        def _():
            pass_on(0, 0)

        lax.fori_loop(first, number, one_pair, 0)
    settle(groups - 1)
    for order in range(groups):
        if order not in spreads:
            spread(order)
    lax.fori_loop(jnp.where(inner, 0, early), groups - 1, pass_on, 0)
    for step in range(1, ctx_count):
        arrived(group, step)

    state = state_own[...].astype(jnp.float32)
    inverse = row_scale(state)

    def last_piece(piece, slope):
        cols = pl.ds(pl.multiple_of(piece * strip, strip), strip)
        sum_v[...] = term(group, piece)

        @pl.when(group > 0)
        def _():
            came(0, group, piece)
            sum_v[...] += partial[0, group, piece].astype(jnp.float32)

        @pl.when(group < groups - 1)
        def _():
            came(1, group, piece)
            sum_v[...] += partial[1, group, piece].astype(jnp.float32)

        gained = sum_v[...] * gain_ref[cols].astype(jnp.float32).reshape(1, strip)
        new_out[:, cols] = gained
        return slope + jnp.sum(
            gained * state_own[:, cols].astype(jnp.float32), axis=1, keepdims=True
        )

    slope = lax.fori_loop(0, pieces, last_piece, jnp.zeros((own, 1), jnp.float32))
    bend = inverse**3 * (slope / model)

    def update(piece, _):
        cols = pl.ds(pl.multiple_of(piece * strip, strip), strip)
        here = state_own[:, cols].astype(jnp.float32)
        gradient = readout_out[:, cols] + inverse * new_out[:, cols] - here * bend
        new_out[:, cols] = (
            here - STEP_SIZE * gradient + NOISE_SCALE * noise_own[:, cols].astype(jnp.float32)
        )
        return 0

    lax.fori_loop(0, pieces, update, 0)

    def all_sent(order, _):
        core_copy(order).wait_send()
        for step in range(1, ctx_count):
            exchange(order, step).wait_send()

        @pl.when(order < groups - 1)
        def _():
            for piece in range(pieces):
                chain(order, piece).wait_send()

        return 0

    for copy in copies:
        copy.wait_send()
    lax.fori_loop(0, groups, all_sent, 0)


def heads_body(state, norm_gain, w_qkv, w_out, probe, noise, segment_ids):
    ctx_count, head_count = lax.axis_size("ctx"), lax.axis_size("head")
    rows, model = state.shape
    width = w_qkv.shape[2]
    own, groups, slots = rows // head_count, head_count // 2, width // HEAD_DIM
    seg = segment_ids.reshape(-1, 128)
    half, full, dma = jnp.bfloat16, jnp.float32, pltpu.SemaphoreType.DMA
    pieces, lanes = 4, ctx_count * own
    tile, vmem = model // pieces, pltpu.VMEM
    heads = (groups, ctx_count, own, HEAD_DIM)
    return pl.pallas_call(
        functools.partial(step_kernel, ctx_count, head_count),
        out_shape=jax.ShapeDtypeStruct((own, model), full),
        in_specs=[ANY, ANY, VMEM, VMEM, ANY, ANY, ANY],
        out_specs=VMEM,
        scratch_shapes=[
            vmem((rows, model), half),
            vmem((slots, groups, 2, own, HEAD_DIM), half),
            vmem((slots, 2, groups, 2 * own, HEAD_DIM), half),
            vmem((model, model), half),
            vmem((own, model), half),
            vmem((own, model), half),
            vmem(heads, half),
            vmem((own, model), half),
            vmem((own, model), half),
            vmem((own, model), half),
            vmem(heads, half),
            vmem((2, groups, ctx_count, 2 * own, HEAD_DIM), half),
            vmem(heads, half),
            vmem((own, model), full),
            vmem((ctx_count,) + seg.shape, seg.dtype),
            vmem((groups, 1, lanes), full),
            vmem(heads, half),
            vmem((2,) + w_qkv.shape, half),
            vmem((groups, 2 * lanes, 2 * HEAD_DIM), full),
            vmem((groups, HEAD_DIM, lanes), full),
            vmem((groups, 1, lanes), full),
            vmem((groups, lanes, HEAD_DIM), half),
            vmem((groups, ctx_count, own, 2 * HEAD_DIM), half),
            vmem((groups, ctx_count, own, 2 * HEAD_DIM), half),
            vmem((groups, ctx_count, 3, own, HEAD_DIM), half),
            vmem((groups, 2, 3, own, width), half),
            vmem((2, groups, pieces, own, tile), half),
            vmem((groups, pieces, own, tile), half),
            vmem((own, tile), full),
            dma((groups,)),
            dma((3,)),
            dma((slots, 2, groups)),
            dma((ctx_count, groups)),
            dma((slots, 2, groups)),
            dma((2, ctx_count, groups)),
            dma((ctx_count, groups)),
            dma((ctx_count,)),
            dma((ctx_count,)),
            dma((2, 2, groups)),
            dma((2, groups)),
            dma((2, groups)),
            dma((2, groups)),
            dma((4, groups)),
            dma((4, groups)),
            dma,
            dma,
            dma,
            dma((ctx_count, groups)),
            dma((groups, ctx_count)),
            dma((groups, ctx_count)),
            dma((ctx_count, groups)),
            dma((3,)),
            dma,
            dma,
            dma((groups,)),
            dma((groups,)),
            dma((groups, ctx_count)),
            dma((groups, ctx_count)),
            dma((groups, pieces)),
            dma((2, groups, pieces)),
        ],
        compiler_params=pltpu.CompilerParams(
            collective_id=0, has_side_effects=True, vmem_limit_bytes=52 * 2**20
        ),
    )(state, w_qkv, norm_gain, seg, w_out, probe, noise)


def solution(mesh):
    placed = (
        P("ctx", None),
        P(),
        P(None, None, "head"),
        P("head", None),
        P("ctx", None),
        P(("ctx", "head"), None),
        P("ctx"),
    )

    def step(*args):
        heads = args[2].shape[2] // HEAD_DIM
        return (heads_body if lax.axis_size("ctx") == 2 * heads == 4 else body)(*args)

    return jax.shard_map(
        step, mesh=mesh, in_specs=placed, out_specs=P(("ctx", "head"), None), check_vma=False
    )
```
